32 devices in a mesh: dp: 8 (over y, x, core), tensor: 4 (over z).
Axes of the slice: x: 2, y: 2, z: 4, core: 2. Of those that a mesh axis runs over, the one named last changes fastest.
Arguments:
- tokens: bfloat16 [9216, 2048], P(('dp', 'tensor')), may hold values from -6 to 6
- segment_ids: int32 [8, 1152], P('dp'), may hold values from 0 to 2, as said below
- attn_gain: bfloat16 [1, 2048], P(None, 'dp'), may hold values from 0.5 to 1.5
- q_weight: bfloat16 [1, 2048, 2048], P(None, 'dp', 'tensor'), may hold values from -0.125 to 0.125
- key_matrix: bfloat16 [1, 2048, 1024], P(None, 'dp', 'tensor'), may hold values from -0.125 to 0.125
- value_matrix: bfloat16 [1, 2048, 1024], P(None, 'dp', 'tensor'), may hold values from -0.125 to 0.125
- o_weight: bfloat16 [1, 2048, 2048], P(None, 'dp', 'tensor'), may hold values from -0.75 to 0.75
- q_gain: bfloat16 [1, 128], P(None, 'dp'), may hold values from 0.25 to 1.75
- k_gain: bfloat16 [1, 128], P(None, 'dp'), may hold values from 0.25 to 1.75
- mlp_gain: bfloat16 [1, 2048], P(None, 'dp'), may hold values from 0.5 to 1.5
- gate_weight: bfloat16 [1, 2048, 6144], P(None, 'dp', 'tensor'), may hold values from -0.125 to 0.125
- up_weight: bfloat16 [1, 2048, 6144], P(None, 'dp', 'tensor'), may hold values from -0.125 to 0.125
- down_weight: bfloat16 [1, 2048, 6144], P(None, 'dp', 'tensor'), may hold values from -0.078125 to 0.078125
- cotangent: bfloat16 [9216, 2048], P(('dp', 'tensor')), may hold values from -6 to 6
Outputs:
- activations: bfloat16 [9216, 2048], P(('dp', 'tensor'))
- input_grad: float32 [9216, 2048], P(('dp', 'tensor'))
- attn_gain_grad: float32 [1, 2048], P(None, 'dp')
- q_weight_grad: float32 [1, 2048, 2048], P(None, 'dp', 'tensor')
- k_weight_grad: float32 [1, 2048, 1024], P(None, 'dp', 'tensor')
- v_weight_grad: float32 [1, 2048, 1024], P(None, 'dp', 'tensor')
- o_weight_grad: float32 [1, 2048, 2048], P(None, 'dp', 'tensor')
- q_gain_grad: float32 [1, 128], P(None, 'dp')
- k_gain_grad: float32 [1, 128], P(None, 'dp')
- mlp_gain_grad: float32 [1, 2048], P(None, 'dp')
- gate_weight_grad: float32 [1, 2048, 6144], P(None, 'dp', 'tensor')
- up_weight_grad: float32 [1, 2048, 6144], P(None, 'dp', 'tensor')
- down_weight_grad: float32 [1, 2048, 6144], P(None, 'dp', 'tensor')
The draws below stay inside these ranges and needn't reach their ends.
Inputs may be any that keep to these rules, and one draw needn't show every extreme that they name: `segment_ids`: in each group the numbers never fall, each of the 3 sequences has one token or more, and one sequence of each group has exactly 1024 tokens.
All inputs are finite; a program needn't handle non-finite values.
Results may differ from the reference program's by a relative error of at most 0.02.
Values may be sent and summed in bfloat16 or wider, within the bound.
A program may use at most 192 MiB of HBM per device.

```python
import jax
import jax.numpy as jnp
from jax import lax

MODEL_WIDTH = 2048
QUERY_HEADS = 16
KEY_VALUE_HEADS = 8
HEAD_WIDTH = 128
FF = 6144
DECODER_LAYERS = 1
NSEQ = 3
QBLOCK = 576
GROUP = 1152
MAXLEN = 1024
GROUPS = 8
TOKENS = 9216


def draw_segment_ids(key, part):
    remainder = GROUP - MAXLEN

    def one_row(row_key):
        cut_key, place_key = jax.random.split(row_key)
        cuts = jnp.sort(jax.random.permutation(cut_key, remainder - 1)[:NSEQ - 2] + 1).astype(jnp.int32)
        bounds = jnp.concatenate([jnp.zeros((1,), jnp.int32), cuts, jnp.full((1,), remainder, jnp.int32)])
        shorter = bounds[1:] - bounds[:-1]
        place = jax.random.randint(place_key, (), 0, NSEQ)
        slots = jnp.arange(NSEQ, dtype=jnp.int32)
        before = jnp.concatenate([shorter, jnp.zeros((1,), jnp.int32)])
        after = jnp.concatenate([jnp.zeros((1,), jnp.int32), shorter])
        lengths = jnp.where(slots < place, before, jnp.where(slots == place, MAXLEN, after))
        ends = jnp.cumsum(lengths)
        row_index = jnp.arange(GROUP, dtype=jnp.int32)
        return jnp.sum((row_index[:, None] >= ends[None, :-1]).astype(jnp.int32), axis=1)
    return jax.vmap(one_row)(jax.random.split(key, GROUPS)).astype(jnp.int32)


def levels(stream_key, extent, cuts, smallest, largest):
    level = 1.0
    for dim, parts in cuts:
        steps = jax.random.uniform(jax.random.fold_in(jax.random.fold_in(stream_key, 6), dim), (parts,), jnp.float32, smallest / len(cuts), largest / len(cuts))
        level = level * jnp.repeat(jnp.exp(steps), extent[dim] // parts).reshape((-1,) + (1,) * (len(extent) - 1 - dim))
    return level


def gaussian(own_key, shape, scale, bound, cuts=(), held_as=jnp.bfloat16):
    factor_of = levels(own_key, shape, cuts, -0.22, 0.18) if cuts else 1.0
    values = jax.random.normal(own_key, shape, jnp.float32) * scale * factor_of
    return jnp.minimum(jnp.maximum(values, -bound), bound).astype(held_as)


def setup_inputs(seed: int = 0) -> dict:
    key_of = jax.random.split(jax.random.key(seed), 15)
    return {
        "tokens": gaussian(key_of[0], (TOKENS, MODEL_WIDTH), 1.0, 6.0, ((0, 32),)),
        "segment_ids": draw_segment_ids(jax.random.fold_in(key_of[14], 71), 0),
        "attn_gain": jnp.clip(1.0 + 0.1 * jax.random.normal(key_of[2], (DECODER_LAYERS, MODEL_WIDTH), jnp.float32), 0.5, 1.5).astype(jnp.bfloat16),
        "q_weight": gaussian(key_of[3], (DECODER_LAYERS, MODEL_WIDTH, QUERY_HEADS * HEAD_WIDTH), MODEL_WIDTH ** -0.5, 0.125, ((1, 8), (2, 4))),
        "key_matrix": gaussian(key_of[4], (DECODER_LAYERS, MODEL_WIDTH, KEY_VALUE_HEADS * HEAD_WIDTH), MODEL_WIDTH ** -0.5, 0.125, ((1, 8), (2, 4))),
        "value_matrix": gaussian(key_of[5], (DECODER_LAYERS, MODEL_WIDTH, KEY_VALUE_HEADS * HEAD_WIDTH), MODEL_WIDTH ** -0.5, 0.125, ((1, 8), (2, 4))),
        "o_weight": gaussian(key_of[6], (DECODER_LAYERS, MODEL_WIDTH, QUERY_HEADS * HEAD_WIDTH), (QUERY_HEADS * HEAD_WIDTH // 32) ** -0.5, 0.75, ((1, 8), (2, 4))),
        "q_gain": jnp.clip(1.0 + 0.15 * jax.random.normal(key_of[7], (DECODER_LAYERS, HEAD_WIDTH), jnp.float32), 0.25, 1.75).astype(jnp.bfloat16),
        "k_gain": jnp.clip(1.0 + 0.15 * jax.random.normal(key_of[8], (DECODER_LAYERS, HEAD_WIDTH), jnp.float32), 0.25, 1.75).astype(jnp.bfloat16),
        "mlp_gain": jnp.clip(1.0 + 0.1 * jax.random.normal(key_of[9], (DECODER_LAYERS, MODEL_WIDTH), jnp.float32), 0.5, 1.5).astype(jnp.bfloat16),
        "gate_weight": gaussian(key_of[10], (DECODER_LAYERS, MODEL_WIDTH, FF), MODEL_WIDTH ** -0.5, 0.125, ((1, 8), (2, 4))),
        "up_weight": gaussian(key_of[11], (DECODER_LAYERS, MODEL_WIDTH, FF), MODEL_WIDTH ** -0.5, 0.125, ((1, 8), (2, 4))),
        "down_weight": gaussian(key_of[12], (DECODER_LAYERS, MODEL_WIDTH, FF), FF ** -0.5, 0.078125, ((1, 8), (2, 4))),
        "cotangent": gaussian(key_of[13], (TOKENS, MODEL_WIDTH), 1.0, 6.0, ((0, 32),)),
    }


@jax.custom_vjp
def reduced_precision(v):
    return lax.optimization_barrier(v.astype(jnp.bfloat16)).astype(jnp.float32)

@jax.custom_vjp
def reduced_backward(v):
    return v

def low_keep(v):
    return (reduced_precision(v), None)

def low_pass(kept, grad):
    return (grad,)

def back_keep(v):
    return (v, None)

def back_low(kept, grad):
    return (reduced_precision(grad),)
reduced_precision.defvjp(low_keep, low_pass)
reduced_backward.defvjp(back_keep, back_low)
EPS = 1e-06
THETA = 1000000.0
HIGHEST = lax.Precision.HIGHEST

def matrix_product(left, right):
    return jnp.dot(left, right, precision=HIGHEST, preferred_element_type=jnp.float32)

def rms_scale(values, gain):
    return values * lax.rsqrt(lax.optimization_barrier(jnp.mean(values * values, axis=-1, keepdims=True)) + EPS) * gain

def rotate(values, cosine, sine_table):
    half_size = values.shape[-1] // 2
    turned = jnp.concatenate([-values[..., half_size:], values[..., :half_size]], axis=-1)
    return values * cosine + turned * sine_table

def rotary_tables(sequence_labels):
    grouped_rows = sequence_labels.shape[0]
    row_index = jnp.arange(grouped_rows, dtype=jnp.int32)
    labels = jnp.arange(NSEQ, dtype=jnp.int32)
    starts = lax.optimization_barrier(jnp.sum((sequence_labels[None, :] < labels[:, None]).astype(jnp.int32), axis=1))
    first_row = lax.optimization_barrier(jnp.sum(jnp.where(sequence_labels[:, None] == labels[None, :], starts[None, :], 0), axis=1))
    position = (row_index - first_row).astype(jnp.float32)
    frequency = THETA ** (-(jnp.arange(HEAD_WIDTH // 2, dtype=jnp.float32) * (2.0 / HEAD_WIDTH)))
    angles = position[:, None] * frequency[None, :]
    cosine = jnp.concatenate([jnp.cos(angles), jnp.cos(angles)], axis=1)[:, None, :]
    sine_table = jnp.concatenate([jnp.sin(angles), jnp.sin(angles)], axis=1)[:, None, :]
    return (cosine, sine_table)

def attention_kernel_body(queries, key_reduced, value_reduced, sequence_labels):
    grouped_rows, kv_heads, repeat, head_size = queries.shape
    blocks = grouped_rows // QBLOCK
    columns = jnp.arange(grouped_rows, dtype=jnp.int32)
    score_scale = HEAD_WIDTH ** (-0.5)

    def one_block(block_item):
        q_block, id_block, row_block = block_item
        allowed = (id_block[:, None] == sequence_labels[None, :]) & (columns[None, :] <= row_block[:, None])
        scores = reduced_backward(jnp.einsum('qgrd,kgd->grqk', q_block, key_reduced, precision=HIGHEST) * score_scale)
        weights = jnp.where(allowed[None, None], jnp.exp(scores), 0.0)
        shares = reduced_precision(weights / lax.optimization_barrier(jnp.sum(weights, axis=-1, keepdims=True)))
        return jnp.einsum('grqk,kgd->qgrd', shares, value_reduced, precision=HIGHEST)
    items = (queries.reshape(blocks, QBLOCK, kv_heads, repeat, head_size), sequence_labels.reshape(blocks, QBLOCK), columns.reshape(blocks, QBLOCK))
    attention_result = lax.map(jax.checkpoint(one_block), items)
    return attention_result.reshape(grouped_rows, kv_heads * repeat * head_size)

def one_layer(stream, params, sequence_labels, cosine, sine_table):
    attn_gain, q_weight, key_matrix, value_matrix, o_weight, q_gain, k_gain, mlp_gain, gate_weight, up_weight, down_weight = params
    grouped_rows = stream.shape[0]
    norm_result = reduced_precision(rms_scale(stream, attn_gain))
    queries = reduced_backward(matrix_product(norm_result, q_weight)).reshape(grouped_rows, QUERY_HEADS, HEAD_WIDTH)
    key_unrotated = reduced_backward(matrix_product(norm_result, key_matrix)).reshape(grouped_rows, KEY_VALUE_HEADS, HEAD_WIDTH)
    value_reduced = reduced_precision(reduced_backward(matrix_product(norm_result, value_matrix))).reshape(grouped_rows, KEY_VALUE_HEADS, HEAD_WIDTH)
    query_reduced = reduced_precision(rotate(rms_scale(queries, q_gain), cosine, sine_table))
    key_reduced = reduced_precision(rotate(rms_scale(key_unrotated, k_gain), cosine, sine_table))
    attention_result = attention_kernel_body(query_reduced.reshape(grouped_rows, KEY_VALUE_HEADS, QUERY_HEADS // KEY_VALUE_HEADS, HEAD_WIDTH), key_reduced, value_reduced, sequence_labels)
    attention_result = reduced_precision(reduced_backward(attention_result))
    middle = stream + reduced_backward(matrix_product(attention_result, o_weight.T))
    normed_mlp = reduced_precision(rms_scale(middle, mlp_gain))
    gate_raw = reduced_backward(matrix_product(normed_mlp, gate_weight))
    up_raw = reduced_backward(matrix_product(normed_mlp, up_weight))
    hidden = reduced_precision(jax.nn.silu(gate_raw) * up_raw)
    return middle + reduced_backward(matrix_product(hidden, down_weight.T))

def group_forward(stream, sequence_labels, params):
    cosine, sine_table = rotary_tables(sequence_labels)
    for layer_index in range(DECODER_LAYERS):
        stream = one_layer(stream, [array_item[layer_index] for array_item in params], sequence_labels, cosine, sine_table)
    return stream

def reference(tokens, segment_ids, attn_gain, q_weight, key_matrix, value_matrix, o_weight, q_gain, k_gain, mlp_gain, gate_weight, up_weight, down_weight, cotangent):
    params = tuple((array_item.astype(jnp.float32) for array_item in (attn_gain, q_weight, key_matrix, value_matrix, o_weight, q_gain, k_gain, mlp_gain, gate_weight, up_weight, down_weight)))
    streams = tokens.astype(jnp.float32).reshape(GROUPS, GROUP, MODEL_WIDTH)
    cot_groups = cotangent.astype(jnp.float32).reshape(GROUPS, GROUP, MODEL_WIDTH)

    def one_group(running, group_item):
        stream, sequence_labels, cot_rows = group_item

        def forward(stream_in, *weights_in):
            return group_forward(stream_in, sequence_labels, weights_in)
        result, pull_back = jax.vjp(forward, stream, *params)
        gradients = pull_back(cot_rows)
        running = tuple((running_sum + piece_grad for running_sum, piece_grad in zip(running, gradients[1:])))
        return (running, (result, gradients[0]))
    initial = tuple((jnp.zeros(array_item.shape, jnp.float32) for array_item in params))
    totals, (results, input_grads) = lax.scan(one_group, initial, (streams, segment_ids, cot_groups))
    return (results.reshape(TOKENS, MODEL_WIDTH).astype(jnp.bfloat16), input_grads.reshape(TOKENS, MODEL_WIDTH), totals[0], totals[1], totals[2], totals[3], totals[4], totals[5], totals[6], totals[7], totals[8], totals[9], totals[10])
```

```python
import jax
import jax.numpy as jnp
from jax import lax
from jax.sharding import Mesh
from jax.sharding import PartitionSpec as P

HEAD_WIDTH = 128
DECODER_LAYERS = 1
NSEQ = 3
QBLOCK = 576


EPS = 1e-06
THETA = 1000000.0


def rms_scale(values, gain):
    return values * lax.rsqrt(jnp.mean(values * values, axis=-1, keepdims=True) + EPS) * gain


def rotate(values, cosine, sine_table):
    half_size = values.shape[-1] // 2
    turned = jnp.concatenate([-values[..., half_size:], values[..., :half_size]], axis=-1)
    return values * cosine + turned * sine_table


def swiglu(gate_raw, up_raw):
    return jax.nn.silu(gate_raw) * up_raw


def rotary_tables(sequence_labels, row_index):
    labels = jnp.arange(NSEQ, dtype=jnp.int32)
    starts = jnp.sum((sequence_labels[None, :] < labels[:, None]).astype(jnp.int32), axis=1)
    first_row = jnp.sum(
        jnp.where(sequence_labels[:, None] == labels[None, :], starts[None, :], 0), axis=1
    )
    position = (row_index - first_row).astype(jnp.float32)
    frequency = THETA ** (-(jnp.arange(HEAD_WIDTH // 2, dtype=jnp.float32) * (2.0 / HEAD_WIDTH)))
    angles = position[:, None] * frequency[None, :]
    cosine = jnp.concatenate([jnp.cos(angles), jnp.cos(angles)], axis=1)[:, None, :]
    sine_table = jnp.concatenate([jnp.sin(angles), jnp.sin(angles)], axis=1)[:, None, :]
    return (cosine, sine_table)


def contract_rows(left, right):
    return lax.dot_general(
        left, right, (((0,), (0,)), ((), ())), preferred_element_type=jnp.float32
    )


def contract_cols(left, right):
    return lax.dot_general(
        left, right, (((1,), (1,)), ((), ())), preferred_element_type=jnp.float32
    )


def block_items(queries, sequence_labels, columns):
    grouped_rows, kv_heads, repeat, head_size = queries.shape
    blocks = grouped_rows // QBLOCK
    return (
        (
            queries.reshape(blocks, QBLOCK, kv_heads, repeat, head_size),
            sequence_labels.reshape(blocks, QBLOCK),
            columns.reshape(blocks, QBLOCK),
        ),
        columns,
    )


def attend_forward(queries, key_reduced, value_reduced, sequence_labels, row_index):
    grouped_rows, kv_heads, repeat, head_size = queries.shape
    score_scale = HEAD_WIDTH ** (-0.5)
    items, columns = block_items(queries, sequence_labels, row_index)

    def one_block(block_item):
        q_block, id_block, row_block = block_item
        allowed = (id_block[:, None] == sequence_labels[None, :]) & (
            columns[None, :] <= row_block[:, None]
        )
        scores = (
            jnp.einsum("qgrd,kgd->grqk", q_block, key_reduced, preferred_element_type=jnp.float32)
            * score_scale
        )
        weights = jnp.where(allowed[None, None], jnp.exp(scores), 0.0)
        totals = jnp.sum(weights, axis=-1, keepdims=True)
        shares = (weights / totals).astype(jnp.bfloat16)
        attention_result = jnp.einsum(
            "grqk,kgd->qgrd", shares, value_reduced, preferred_element_type=jnp.float32
        )
        return (attention_result.astype(jnp.bfloat16), totals)

    attention_result, totals = lax.map(one_block, items)
    return (attention_result.reshape(grouped_rows, kv_heads * repeat * head_size), totals)


def attend_backward(
    queries, key_reduced, value_reduced, sequence_labels, row_index, totals, out_grad
):
    grouped_rows, kv_heads, repeat, head_size = queries.shape
    score_scale = HEAD_WIDTH ** (-0.5)
    items, columns = block_items(queries, sequence_labels, row_index)
    grad_blocks = out_grad.reshape(grouped_rows // QBLOCK, QBLOCK, kv_heads, repeat, head_size)

    def one_block(running, block_item):
        key_grad, value_grad = running
        q_block, id_block, row_block, total_block, grad_block = block_item
        allowed = (id_block[:, None] == sequence_labels[None, :]) & (
            columns[None, :] <= row_block[:, None]
        )
        scores = (
            jnp.einsum("qgrd,kgd->grqk", q_block, key_reduced, preferred_element_type=jnp.float32)
            * score_scale
        )
        shares = jnp.where(allowed[None, None], jnp.exp(scores), 0.0) / total_block
        low_shares = shares.astype(jnp.bfloat16)
        share_grad = jnp.einsum(
            "qgrd,kgd->grqk", grad_block, value_reduced, preferred_element_type=jnp.float32
        )
        row_inner = jnp.sum(shares * share_grad, axis=-1, keepdims=True)
        score_grad = (shares * (share_grad - row_inner)).astype(jnp.bfloat16)
        query_grad = (
            jnp.einsum(
                "grqk,kgd->qgrd", score_grad, key_reduced, preferred_element_type=jnp.float32
            )
            * score_scale
        )
        key_grad = (
            key_grad
            + jnp.einsum("grqk,qgrd->kgd", score_grad, q_block, preferred_element_type=jnp.float32)
            * score_scale
        )
        value_grad = value_grad + jnp.einsum(
            "grqk,qgrd->kgd", low_shares, grad_block, preferred_element_type=jnp.float32
        )
        return ((key_grad, value_grad), query_grad)

    zero_keys = jnp.zeros(key_reduced.shape, jnp.float32)
    (key_grad, value_grad), query_grad = lax.scan(
        one_block, (zero_keys, zero_keys), items + (totals, grad_blocks)
    )
    return (query_grad.reshape(grouped_rows, kv_heads * repeat, head_size), key_grad, value_grad)


def shift_perm(size, step):
    return [((place + step) % size, place) for place in range(size)]


def trade(values):
    return lax.ppermute(values, ("c", "h"), [(0, 0), (1, 2), (2, 1), (3, 3)])


def gather_tokens(own):
    places = lax.axis_size("l")
    parts = [own] + [lax.ppermute(own, "l", shift_perm(places, step)) for step in range(1, places)]
    half = jnp.concatenate(parts, axis=0)
    return jnp.concatenate([half, lax.ppermute(half, "c", shift_perm(2, 1))], axis=0)


def scatter_tokens(partial):
    places = lax.axis_size("l")
    half = partial.shape[0] // 2
    rows = half // places
    other = lax.ppermute(partial[half:].astype(jnp.bfloat16), "c", shift_perm(2, 1))
    total = partial[:half] + other.astype(jnp.float32)
    own = total[:rows]
    for step in range(1, places):
        sent = total[step * rows : (step + 1) * rows].astype(jnp.bfloat16)
        own = own + lax.ppermute(sent, "l", shift_perm(places, -step)).astype(jnp.float32)
    return own


def gather_weights(shard):
    core, upper = lax.axis_index("c"), lax.axis_index("h")
    far = lax.ppermute(shard, "h", shift_perm(2, 1))
    same = core == upper
    mine = jnp.where(same, shard, far)
    other = lax.ppermute(jnp.where(same, far, shard), "c", shift_perm(2, 1))
    rows = jnp.concatenate(
        [jnp.where(core == 0, mine, other), jnp.where(core == 0, other, mine)], axis=0
    )
    return lax.all_gather(rows, "d", axis=0, tiled=True)


def scatter_weights(partial):
    core, upper = lax.axis_index("c"), lax.axis_index("h")
    rows = lax.psum_scatter(partial.astype(jnp.bfloat16), "d", scatter_dimension=0, tiled=True)
    half = rows.shape[0] // 2
    first, second = rows[:half], rows[half:]
    mine = jnp.where(core == 0, first, second)
    other = lax.ppermute(jnp.where(core == 0, second, first), "c", shift_perm(2, 1))
    same = core == upper
    far = lax.ppermute(jnp.where(same, other, mine), "h", shift_perm(2, 1))
    return jnp.where(same, mine, other).astype(jnp.float32) + far.astype(jnp.float32)


def per_device(
    tokens,
    segment_ids,
    attn_gain,
    q_weight,
    key_matrix,
    value_matrix,
    o_weight,
    q_gain,
    k_gain,
    mlp_gain,
    gate_weight,
    up_weight,
    down_weight,
    cotangent,
):
    width = attn_gain.shape[1] * lax.axis_size("d") * 2
    own_rows = tokens.shape[0]
    places = lax.axis_size("l")
    core, place = lax.axis_index("c"), lax.axis_index("l")
    q_cols, kv_cols, ff_cols = q_weight.shape[2], key_matrix.shape[2], gate_weight.shape[2]

    tokens = trade(tokens)
    labels = trade(segment_ids)[0]
    attn_weights = gather_weights(
        jnp.concatenate([q_weight[0], key_matrix[0], value_matrix[0], o_weight[0]], axis=1)
    )
    mid_weights = gather_weights(jnp.concatenate([gate_weight[0], up_weight[0]], axis=1))
    down_full = gather_weights(down_weight[0])
    cotangent = trade(cotangent)

    gains = lax.all_gather(
        jnp.concatenate([attn_gain[0], mlp_gain[0], q_gain[0], k_gain[0]]), ("d", "c"), axis=0
    ).astype(jnp.float32)
    cut = attn_gain.shape[1]
    head_cut = q_gain.shape[1]
    attn_scale = gains[:, :cut].reshape(-1)
    mlp_scale = gains[:, cut : 2 * cut].reshape(-1)
    q_scale = gains[:, 2 * cut : 2 * cut + head_cut].reshape(-1)
    k_scale = gains[:, 2 * cut + head_cut :].reshape(-1)

    order = jnp.stack(
        [
            ((core + core_step) % 2) * places + (place + step) % places
            for core_step in range(2)
            for step in range(places)
        ]
    )
    row_index = (order[:, None] * own_rows + jnp.arange(own_rows, dtype=jnp.int32)[None, :]).reshape(-1)
    labels = labels.reshape(2 * places, own_rows)[order].reshape(-1)
    cosine, sine_table = rotary_tables(labels, row_index)

    stream = tokens.astype(jnp.float32)
    normed = gather_tokens(rms_scale(stream, attn_scale).astype(jnp.bfloat16))
    rows = normed.shape[0]
    head_count, kv_heads = q_cols // HEAD_WIDTH, kv_cols // HEAD_WIDTH
    q_full = attn_weights[:, :q_cols]
    k_full = attn_weights[:, q_cols : q_cols + kv_cols]
    v_full = attn_weights[:, q_cols + kv_cols : q_cols + 2 * kv_cols]
    o_full = attn_weights[:, q_cols + 2 * kv_cols :]
    queries = jnp.dot(normed, q_full, preferred_element_type=jnp.float32).reshape(
        rows, head_count, HEAD_WIDTH
    )
    keys = jnp.dot(normed, k_full, preferred_element_type=jnp.float32).reshape(
        rows, kv_heads, HEAD_WIDTH
    )
    value_reduced = (
        jnp.dot(normed, v_full, preferred_element_type=jnp.float32)
        .reshape(rows, kv_heads, HEAD_WIDTH)
        .astype(jnp.bfloat16)
    )
    query_reduced = rotate(rms_scale(queries, q_scale), cosine, sine_table).astype(jnp.bfloat16)
    key_reduced = rotate(rms_scale(keys, k_scale), cosine, sine_table).astype(jnp.bfloat16)
    query_reduced = query_reduced.reshape(rows, kv_heads, head_count // kv_heads, HEAD_WIDTH)
    attended, totals = attend_forward(
        query_reduced, key_reduced, value_reduced, labels, row_index
    )
    middle = stream + scatter_tokens(contract_cols(attended, o_full))

    normed_mid = gather_tokens(rms_scale(middle, mlp_scale).astype(jnp.bfloat16))
    gate_full, up_full = mid_weights[:, :ff_cols], mid_weights[:, ff_cols:]
    gate_raw = jnp.dot(normed_mid, gate_full, preferred_element_type=jnp.float32)
    up_raw = jnp.dot(normed_mid, up_full, preferred_element_type=jnp.float32)
    hidden = swiglu(gate_raw, up_raw).astype(jnp.bfloat16)
    branch = scatter_tokens(contract_cols(hidden, down_full))
    activations = trade((middle + branch).astype(jnp.bfloat16))

    grad_rows = gather_tokens(cotangent)
    gradient = cotangent.astype(jnp.float32)
    down_grad = scatter_weights(contract_rows(grad_rows, hidden))
    hidden_grad = jnp.dot(grad_rows, down_full, preferred_element_type=jnp.float32)
    _, pull_back = jax.vjp(swiglu, gate_raw, up_raw)
    gate_grad, up_grad = pull_back(hidden_grad)
    gate_low = gate_grad.astype(jnp.bfloat16)
    up_low = up_grad.astype(jnp.bfloat16)
    mid_grad = scatter_weights(
        jnp.concatenate(
            [
                contract_rows(normed_mid, gate_low).astype(jnp.bfloat16),
                contract_rows(normed_mid, up_low).astype(jnp.bfloat16),
            ],
            axis=1,
        )
    )
    normed_grad = scatter_tokens(
        contract_cols(gate_low, gate_full) + contract_cols(up_low, up_full)
    )
    _, pull_norm = jax.vjp(rms_scale, middle, mlp_scale)
    middle_grad, mlp_gain_grad = pull_norm(normed_grad)
    gradient = gradient + middle_grad

    grad_rows = gather_tokens(gradient.astype(jnp.bfloat16))
    out_grad = jnp.dot(grad_rows, o_full, preferred_element_type=jnp.float32).astype(jnp.bfloat16)
    o_wgrad = contract_rows(grad_rows, attended)
    query_grad, key_grad, value_grad = attend_backward(
        query_reduced,
        key_reduced,
        value_reduced,
        labels,
        row_index,
        totals,
        out_grad.reshape(query_reduced.shape),
    )

    def query_path(raw_values, scales):
        return rotate(rms_scale(raw_values, scales), cosine, sine_table)

    _, pull_query = jax.vjp(query_path, queries, q_scale)
    query_raw_grad, q_gain_grad = pull_query(query_grad)
    _, pull_key = jax.vjp(query_path, keys, k_scale)
    key_raw_grad, k_gain_grad = pull_key(key_grad)
    query_back = query_raw_grad.reshape(rows, -1).astype(jnp.bfloat16)
    key_back = key_raw_grad.reshape(rows, -1).astype(jnp.bfloat16)
    value_back = value_grad.reshape(rows, -1).astype(jnp.bfloat16)
    attn_grad = scatter_weights(
        jnp.concatenate(
            [
                contract_rows(normed, query_back).astype(jnp.bfloat16),
                contract_rows(normed, key_back).astype(jnp.bfloat16),
                contract_rows(normed, value_back).astype(jnp.bfloat16),
                o_wgrad.astype(jnp.bfloat16),
            ],
            axis=1,
        )
    )
    normed_grad = scatter_tokens(
        contract_cols(query_back, q_full)
        + contract_cols(key_back, k_full)
        + contract_cols(value_back, v_full)
    )
    _, pull_norm = jax.vjp(rms_scale, stream, attn_scale)
    stream_grad, attn_gain_grad = pull_norm(normed_grad)
    gradient = gradient + stream_grad
    moved = trade(gradient.astype(jnp.bfloat16))
    gradient = jnp.where(core == lax.axis_index("h"), gradient, moved.astype(jnp.float32))

    sums = lax.psum(
        jnp.concatenate([attn_gain_grad, mlp_gain_grad, q_gain_grad, k_gain_grad]),
        ("d", "c", "h", "l"),
    )
    row = lax.axis_index("d") * 2 + core

    def owned(start, whole, part):
        return lax.dynamic_slice(sums[start : start + whole], (row * part,), (part,))[None]

    return (
        activations,
        gradient,
        owned(0, width, cut),
        attn_grad[None, :, :q_cols],
        attn_grad[None, :, q_cols : q_cols + kv_cols],
        attn_grad[None, :, q_cols + kv_cols : q_cols + 2 * kv_cols],
        attn_grad[None, :, q_cols + 2 * kv_cols :],
        owned(2 * width, HEAD_WIDTH, head_cut),
        owned(2 * width + HEAD_WIDTH, HEAD_WIDTH, head_cut),
        owned(width, width, cut),
        mid_grad[None, :, :ff_cols],
        mid_grad[None, :, ff_cols:],
        down_grad[None],
    )


def solution(mesh):
    dp, tensor = mesh.shape["dp"], mesh.shape["tensor"]
    cut = Mesh(mesh.devices.reshape(dp // 2, 2, 2, tensor // 2), ("d", "c", "h", "l"))
    rows, cols = ("d", "c"), ("h", "l")
    tokens, labels = P(rows + cols, None), P(rows, None)
    gain, weight = P(None, rows), P(None, rows, cols)
    return jax.shard_map(
        per_device,
        mesh=cut,
        in_specs=(
            tokens,
            labels,
            gain,
            weight,
            weight,
            weight,
            weight,
            gain,
            gain,
            gain,
            weight,
            weight,
            weight,
            tokens,
        ),
        out_specs=(
            tokens,
            tokens,
            gain,
            weight,
            weight,
            weight,
            weight,
            gain,
            gain,
            gain,
            weight,
            weight,
            weight,
        ),
        check_vma=False,
    )
```

```python
import functools

import jax
import jax.numpy as jnp
from jax import lax
from jax.experimental import pallas as pl
from jax.experimental.pallas import tpu as pltpu
from jax.sharding import Mesh
from jax.sharding import PartitionSpec as P

HEAD_WIDTH = 128
DECODER_LAYERS = 1
NSEQ = 3
QBLOCK = 576


EPS = 1e-06
THETA = 1000000.0


def rms_scale(values, gain):
    return values * lax.rsqrt(jnp.mean(values * values, axis=-1, keepdims=True) + EPS) * gain


def rotate(values, cosine, sine_table):
    half_size = values.shape[-1] // 2
    turned = jnp.concatenate([-values[..., half_size:], values[..., :half_size]], axis=-1)
    return values * cosine + turned * sine_table


def swiglu(gate_raw, up_raw):
    return jax.nn.silu(gate_raw) * up_raw


def rotary_tables(sequence_labels, row_index):
    labels = jnp.arange(NSEQ, dtype=jnp.int32)
    starts = jnp.sum((sequence_labels[None, :] < labels[:, None]).astype(jnp.int32), axis=1)
    first_row = jnp.sum(
        jnp.where(sequence_labels[:, None] == labels[None, :], starts[None, :], 0), axis=1
    )
    position = (row_index - first_row).astype(jnp.float32)
    frequency = THETA ** (-(jnp.arange(HEAD_WIDTH // 2, dtype=jnp.float32) * (2.0 / HEAD_WIDTH)))
    angles = position[:, None] * frequency[None, :]
    cosine = jnp.concatenate([jnp.cos(angles), jnp.cos(angles)], axis=1)[:, None, :]
    sine_table = jnp.concatenate([jnp.sin(angles), jnp.sin(angles)], axis=1)[:, None, :]
    return (cosine, sine_table)


def contract_rows(left, right):
    return lax.dot_general(
        left, right, (((0,), (0,)), ((), ())), preferred_element_type=jnp.float32
    )


def contract_cols(left, right):
    return lax.dot_general(
        left, right, (((1,), (1,)), ((), ())), preferred_element_type=jnp.float32
    )


def block_items(queries, sequence_labels, columns):
    grouped_rows, kv_heads, repeat, head_size = queries.shape
    blocks = grouped_rows // QBLOCK
    return (
        (
            queries.reshape(blocks, QBLOCK, kv_heads, repeat, head_size),
            sequence_labels.reshape(blocks, QBLOCK),
            columns.reshape(blocks, QBLOCK),
        ),
        columns,
    )


def attend_forward(queries, key_reduced, value_reduced, sequence_labels, row_index):
    grouped_rows, kv_heads, repeat, head_size = queries.shape
    score_scale = HEAD_WIDTH ** (-0.5)
    items, columns = block_items(queries, sequence_labels, row_index)

    def one_block(block_item):
        q_block, id_block, row_block = block_item
        allowed = (id_block[:, None] == sequence_labels[None, :]) & (
            columns[None, :] <= row_block[:, None]
        )
        scores = (
            jnp.einsum("qgrd,kgd->grqk", q_block, key_reduced, preferred_element_type=jnp.float32)
            * score_scale
        )
        weights = jnp.where(allowed[None, None], jnp.exp(scores), 0.0)
        totals = jnp.sum(weights, axis=-1, keepdims=True)
        shares = (weights / totals).astype(jnp.bfloat16)
        attention_result = jnp.einsum(
            "grqk,kgd->qgrd", shares, value_reduced, preferred_element_type=jnp.float32
        )
        return (attention_result.astype(jnp.bfloat16), totals)

    attention_result, totals = lax.map(one_block, items)
    return (attention_result.reshape(grouped_rows, kv_heads * repeat * head_size), totals)


def attend_backward(
    queries, key_reduced, value_reduced, sequence_labels, row_index, totals, out_grad
):
    grouped_rows, kv_heads, repeat, head_size = queries.shape
    score_scale = HEAD_WIDTH ** (-0.5)
    items, columns = block_items(queries, sequence_labels, row_index)
    grad_blocks = out_grad.reshape(grouped_rows // QBLOCK, QBLOCK, kv_heads, repeat, head_size)

    def one_block(running, block_item):
        key_grad, value_grad = running
        q_block, id_block, row_block, total_block, grad_block = block_item
        allowed = (id_block[:, None] == sequence_labels[None, :]) & (
            columns[None, :] <= row_block[:, None]
        )
        scores = (
            jnp.einsum("qgrd,kgd->grqk", q_block, key_reduced, preferred_element_type=jnp.float32)
            * score_scale
        )
        shares = jnp.where(allowed[None, None], jnp.exp(scores), 0.0) / total_block
        low_shares = shares.astype(jnp.bfloat16)
        share_grad = jnp.einsum(
            "qgrd,kgd->grqk", grad_block, value_reduced, preferred_element_type=jnp.float32
        )
        row_inner = jnp.sum(shares * share_grad, axis=-1, keepdims=True)
        score_grad = (shares * (share_grad - row_inner)).astype(jnp.bfloat16)
        query_grad = (
            jnp.einsum(
                "grqk,kgd->qgrd", score_grad, key_reduced, preferred_element_type=jnp.float32
            )
            * score_scale
        )
        key_grad = (
            key_grad
            + jnp.einsum("grqk,qgrd->kgd", score_grad, q_block, preferred_element_type=jnp.float32)
            * score_scale
        )
        value_grad = value_grad + jnp.einsum(
            "grqk,qgrd->kgd", low_shares, grad_block, preferred_element_type=jnp.float32
        )
        return ((key_grad, value_grad), query_grad)

    zero_keys = jnp.zeros(key_reduced.shape, jnp.float32)
    (key_grad, value_grad), query_grad = lax.scan(
        one_block, (zero_keys, zero_keys), items + (totals, grad_blocks)
    )
    return (query_grad.reshape(grouped_rows, kv_heads * repeat, head_size), key_grad, value_grad)


MESH = pl.DeviceIdType.MESH
CHUNKS = 3


def remote(source, target, send_sem, recv_sem, **place):
    return pltpu.make_async_remote_copy(
        src_ref=source,
        dst_ref=target,
        send_sem=send_sem,
        recv_sem=recv_sem,
        device_id=place,
        device_id_type=MESH,
    )


def rows_at(index, size):
    return pl.ds(pl.multiple_of(index * size, size), size)


def entry_kernel(nd, tl, *refs):
    (q_ref, k_ref, v_ref, o_ref, tok_ref, gain_ref) = refs[:6]
    (qkv_full, o_full, tok_full, gain_full) = refs[6:10]
    (stage, tok_stage) = refs[10:12]
    (zs, zr, cs, li, lo, xs, xr, ts, tr, tli, tlo, ls, lr, fs, fr, gs, gr, gl) = refs[12:]
    d, c, h, l = (lax.axis_index(name) for name in ("d", "c", "h", "l"))
    same = c == h
    apart = c != h
    rows = q_ref.shape[0]
    own = tok_ref.shape[0]
    chunk = own // CHUNKS
    q_cols, kv_cols = q_ref.shape[1], k_ref.shape[1]
    weights = (
        (q_ref, qkv_full, 0, 0),
        (k_ref, qkv_full, q_cols, q_cols),
        (v_ref, qkv_full, q_cols + kv_cols, q_cols + kv_cols),
        (o_ref, o_full, 0, q_cols + 2 * kv_cols),
    )

    def block(j, row):
        source, full, start, _ = weights[j]
        return full.at[rows_at(row, rows), pl.ds(start, source.shape[1])]

    def held(j):
        source, _, _, start = weights[j]
        return stage.at[:, pl.ds(start, source.shape[1])]

    def from_far(j, part):
        return remote(block(j, d * 2 + part), block(j, d * 2 + part), zs.at[j], zr.at[j, part], h=1 - h)

    def to_far(j):
        return remote(weights[j][0], block(j, d * 2 + c), zs.at[j], zr.at[j, c], c=h, h=1 - h)

    def to_core(j):
        return remote(weights[j][0], block(j, d * 2 + c), cs.at[j], zr.at[j, c], c=h)

    def local_in(j):
        return pltpu.make_async_copy(weights[j][0], held(j), li.at[j])

    def local_out(j):
        return pltpu.make_async_copy(held(j), block(j, d * 2 + c), lo.at[j])

    def tokens_at(index, k):
        return tok_full.at[pl.ds(index * own + k * chunk, chunk)]

    def trade_tokens(k):
        return remote(tok_ref.at[pl.ds(k * chunk, chunk)], tokens_at(0, k), ts.at[k], tr.at[k], c=h, h=c)

    def along(step, k):
        return remote(
            tokens_at(0, k),
            tokens_at(tl - step, k),
            ls.at[(step - 1) * CHUNKS + k],
            lr.at[(tl - step - 1) * CHUNKS + k],
            l=lax.rem(l + step, tl),
        )

    def from_along(index, k):
        return remote(
            tokens_at(index, k),
            tokens_at(index, k),
            ls.at[(index - 1) * CHUNKS + k],
            lr.at[(index - 1) * CHUNKS + k],
            l=l,
        )

    def across(index, k):
        at = index * CHUNKS + k
        return remote(tokens_at(index, k), tokens_at(tl + index, k), fs.at[at], fr.at[at], c=1 - c)

    def gain_peer(step):
        place = lax.rem(d * 2 + c + step, 2 * nd)
        return place // 2, lax.rem(place, 2)

    def gains_to(step):
        to_d, to_c = gain_peer(step)
        return remote(
            gain_ref, gain_full.at[d * 2 + c], gs.at[step - 1], gr.at[2 * nd - step - 1], d=to_d, c=to_c
        )

    def gains_from(step):
        from_d, from_c = gain_peer(step)
        return remote(
            gain_ref, gain_full.at[from_d * 2 + from_c], gs.at[step - 1], gr.at[step - 1], d=from_d, c=from_c
        )

    def local_gains():
        return pltpu.make_async_copy(gain_ref, gain_full.at[d * 2 + c], gl)

    local_gains().start()
    for j in range(3):
        to_far(j).start()

        @pl.when(apart)
        def _():
            to_core(j).start()

    @pl.when(apart)
    def _():
        for k in range(CHUNKS):
            trade_tokens(k).start()

    to_far(3).start()

    @pl.when(apart)
    def _():
        to_core(3).start()

    @pl.when(same)
    def _():
        pltpu.make_async_copy(tok_ref, tok_stage, tli).start()
        for j in range(4):
            local_in(j).start()
        pltpu.make_async_copy(tok_ref, tok_stage, tli).wait()
        for k in range(CHUNKS):
            part = pl.ds(k * chunk, chunk)
            pltpu.make_async_copy(tok_stage.at[part], tokens_at(0, k), tlo.at[k]).start()
        for j in range(4):
            local_in(j).wait()
            local_out(j).start()

    for step in range(1, 2 * nd):
        gains_to(step).start()

    if nd == 4:
        side_x = d + 1 - 2 * lax.rem(d, 2)
        side_y = d + 2 - 4 * (d // 2)
        hops = (
            (0, d, side_x),
            (1, d, side_x),
            (0, d, side_y),
            (1, d, side_y),
            (0, side_x, side_y),
            (1, side_y, side_x),
        )
        sources = (
            (0, side_x),
            (1, side_x),
            (0, side_y),
            (1, side_y),
            (0, side_x + side_y - d),
            (1, side_x + side_y - d),
        )
        first, relayed = 4, ((0, 4), (3, 5))
    else:
        hops = tuple((part, d, lax.rem(d + step, nd)) for step in range(1, nd) for part in range(2))
        sources = tuple(
            (part, lax.rem(d + nd - step, nd)) for step in range(1, nd) for part in range(2)
        )
        first, relayed = len(hops), ()

    def hop(j, kind):
        part, of, to = hops[kind]
        at = block(j, of * 2 + part)
        return remote(at, at, xs.at[j, kind], xr.at[j, kind], d=to)

    def arrived(j, kind):
        part, of = sources[kind]
        at = block(j, of * 2 + part)
        return remote(at, at, xs.at[j, kind], xr.at[j, kind], d=hops[kind][2])

    def spread(j):
        for part in range(2):
            here = jnp.logical_and(same, c == part)

            @pl.when(here)
            def _():
                local_out(j).wait()

            @pl.when(jnp.logical_not(here))
            def _():
                from_far(j, part).wait_recv()

            for kind in range(first):
                if hops[kind][0] == part:
                    hop(j, kind).start()

    def relay(j):
        for after, kind in relayed:
            arrived(j, after).wait_recv()
            hop(j, kind).start()

    spread(0)
    spread(1)
    relay(0)
    spread(2)
    relay(1)
    for k in range(CHUNKS):

        @pl.when(same)
        def _():
            part = pl.ds(k * chunk, chunk)
            pltpu.make_async_copy(tok_stage.at[part], tokens_at(0, k), tlo.at[k]).wait()

        @pl.when(apart)
        def _():
            remote(tokens_at(0, k), tokens_at(0, k), ts.at[k], tr.at[k], c=1 - c, h=1 - h).wait_recv()

        for step in range(1, tl):
            along(step, k).start()
        across(0, k).start()
    relay(2)
    spread(3)
    for k in range(CHUNKS):
        for index in range(1, tl):
            from_along(index, k).wait_recv()
            across(index, k).start()
    relay(3)

    handled = {after for after, _ in relayed}
    for j in range(4):
        for kind in range(len(hops)):
            if kind not in handled:
                arrived(j, kind).wait_recv()
            hop(j, kind).wait_send()
        to_far(j).wait_send()
    for k in range(CHUNKS):
        for index in range(tl):
            across(index, k).wait()
        for step in range(1, tl):
            along(step, k).wait_send()
    for step in range(1, 2 * nd):
        gains_from(step).wait_recv()
        gains_to(step).wait_send()
    local_gains().wait()

    @pl.when(apart)
    def _():
        for j in range(4):
            to_core(j).wait_send()
        for k in range(CHUNKS):
            trade_tokens(k).wait_send()


def enter(q_weight, key_matrix, value_matrix, o_weight, tokens, gains):
    nd, tl = lax.axis_size("d"), lax.axis_size("l")
    rows, q_cols = q_weight.shape
    kv_cols = key_matrix.shape[1]
    own, width = tokens.shape
    hops = 6 if nd == 4 else 2 * (nd - 1)
    dma = pltpu.SemaphoreType.DMA
    return pl.pallas_call(
        functools.partial(entry_kernel, nd, tl),
        name="entry",
        out_shape=(
            jax.ShapeDtypeStruct((width, q_cols + 2 * kv_cols), jnp.bfloat16),
            jax.ShapeDtypeStruct((width, o_weight.shape[1]), jnp.bfloat16),
            jax.ShapeDtypeStruct((2 * tl * own, width), jnp.bfloat16),
            jax.ShapeDtypeStruct((2 * nd,) + gains.shape, jnp.float32),
        ),
        in_specs=[pl.BlockSpec(memory_space=pl.ANY)] * 6,
        out_specs=[pl.BlockSpec(memory_space=pl.ANY)] * 4,
        scratch_shapes=[
            pltpu.VMEM((rows, q_cols + 2 * kv_cols + o_weight.shape[1]), jnp.bfloat16),
            pltpu.VMEM((own, width), jnp.bfloat16),
            dma((4,)),
            dma((4, 2)),
            dma((4,)),
            dma((4,)),
            dma((4,)),
            dma((4, hops)),
            dma((4, hops)),
            dma((CHUNKS,)),
            dma((CHUNKS,)),
            dma,
            dma((CHUNKS,)),
            dma(((tl - 1) * CHUNKS,)),
            dma(((tl - 1) * CHUNKS,)),
            dma((tl * CHUNKS,)),
            dma((tl * CHUNKS,)),
            dma((2 * nd - 1,)),
            dma((2 * nd - 1,)),
            dma,
        ],
        compiler_params=pltpu.CompilerParams(has_side_effects=True),
        cost_estimate=pl.CostEstimate(flops=0, bytes_accessed=250_000_000, transcendentals=0),
    )(q_weight, key_matrix, value_matrix, o_weight, tokens, gains)


def exchange_kernel(tl, epilogue, aux_count, out_count, gather, *refs):
    partial = refs[0]
    aux = refs[1 : 1 + aux_count]
    outs = refs[1 + aux_count : 1 + aux_count + out_count]
    rest = refs[1 + aux_count + out_count :]
    if gather:
        full, rest = rest[0], rest[1:]
        finished, ls, lr, fs, fr, keep, rest = rest[0], *rest[1:6], rest[6:]
    mine, other, sums, arrivals, cs, cr, loc, ss, sr = rest
    c, l = lax.axis_index("c"), lax.axis_index("l")
    own = arrivals.shape[0] // (tl - 1)
    chunk = own // CHUNKS

    barrier = pltpu.get_barrier_semaphore()
    pl.semaphore_signal(barrier, inc=1, device_id={"c": 1 - c}, device_id_type=MESH)
    for step in range(1, tl):
        pl.semaphore_signal(
            barrier, inc=1, device_id={"l": lax.rem(l + step, tl)}, device_id_type=MESH
        )
    pl.semaphore_wait(barrier, tl)

    def part(base, k):
        return rows_at(base * CHUNKS + k, chunk)

    def to_core(index, k):
        at = index * CHUNKS + k
        return remote(
            partial.at[part(tl + index, k)], other.at[part(index, k)], cs.at[at], cr.at[at], c=1 - c
        )

    def local(index, k):
        return pltpu.make_async_copy(
            partial.at[part(index, k)], mine.at[part(index, k)], loc.at[index * CHUNKS + k]
        )

    def along(step, k):
        at = (step - 1) * CHUNKS + k
        return remote(
            sums.at[part(step - 1, k)],
            arrivals.at[part(step - 1, k)],
            ss.at[at],
            sr.at[at],
            l=lax.rem(l + step, tl),
        )

    order = list(range(1, tl)) + [0]
    for index in order:
        for k in range(CHUNKS):
            to_core(index, k).start()
            local(index, k).start()

    def both(index, k):
        local(index, k).wait()
        to_core(index, k).wait_recv()
        at = part(index, k)
        return mine[at, :].astype(jnp.float32) + other[at, :].astype(jnp.float32)

    for step in range(1, tl):

        def pass_on(k, carry):
            sums[part(step - 1, k), :] = both(step, k).astype(jnp.bfloat16)
            along(step, k).start()
            return carry

        lax.fori_loop(0, CHUNKS, pass_on, 0)

    def gathered(index, k):
        return full.at[part(index, k)]

    def keep_own(k):
        return pltpu.make_async_copy(finished.at[part(0, k)], gathered(0, k), keep.at[k])

    def own_along(step, k):
        return remote(
            finished.at[part(0, k)],
            gathered(tl - step, k),
            ls.at[(step - 1) * CHUNKS + k],
            lr.at[(tl - step - 1) * CHUNKS + k],
            l=lax.rem(l + step, tl),
        )

    def from_along(index, k):
        at = (index - 1) * CHUNKS + k
        return remote(gathered(index, k), gathered(index, k), ls.at[at], lr.at[at], l=l)

    def across(index, k):
        source = finished.at[part(0, k)] if index == 0 else gathered(index, k)
        at = index * CHUNKS + k
        return remote(source, gathered(tl + index, k), fs.at[at], fr.at[at], c=1 - c)

    def finish(k, carry):
        total = both(0, k)
        for step in range(1, tl):
            along(step, k).wait_recv()
            total = total + arrivals[part(step - 1, k), :].astype(jnp.float32)
        row = epilogue(total, part(0, k), k, aux, outs)
        if gather:
            finished[part(0, k), :] = row
            keep_own(k).start()
            for step in range(1, tl):
                own_along(step, k).start()
            across(0, k).start()
        return carry

    lax.fori_loop(0, CHUNKS, finish, 0)
    if gather:
        for k in range(CHUNKS):
            for index in range(1, tl):
                from_along(index, k).wait_recv()
                across(index, k).start()
        for k in range(CHUNKS):
            keep_own(k).wait()
            for index in range(tl):
                across(index, k).wait()
            for step in range(1, tl):
                own_along(step, k).wait_send()
    for k in range(CHUNKS):
        for index in range(tl):
            to_core(index, k).wait_send()
        for step in range(1, tl):
            along(step, k).wait_send()


def exchange(name, collective_id, partial, aux, outs, epilogue, gather):
    tl = lax.axis_size("l")
    total, width = partial.shape
    own = total // (2 * tl)
    dma = pltpu.SemaphoreType.DMA
    vmem = pl.BlockSpec(memory_space=pltpu.VMEM)
    anywhere = pl.BlockSpec(memory_space=pl.ANY)
    out_shape = list(outs)
    out_specs = [vmem] * len(outs)
    scratch = []
    if gather:
        out_shape.append(jax.ShapeDtypeStruct((total, width), jnp.bfloat16))
        out_specs.append(anywhere)
        scratch += [
            pltpu.VMEM((own, width), jnp.bfloat16),
            dma(((tl - 1) * CHUNKS,)),
            dma(((tl - 1) * CHUNKS,)),
            dma((tl * CHUNKS,)),
            dma((tl * CHUNKS,)),
            dma((CHUNKS,)),
        ]
    scratch += [
        pltpu.VMEM((tl * own, width), jnp.bfloat16),
        pltpu.VMEM((tl * own, width), jnp.bfloat16),
        pltpu.VMEM(((tl - 1) * own, width), jnp.bfloat16),
        pltpu.VMEM(((tl - 1) * own, width), jnp.bfloat16),
        dma((tl * CHUNKS,)),
        dma((tl * CHUNKS,)),
        dma((tl * CHUNKS,)),
        dma(((tl - 1) * CHUNKS,)),
        dma(((tl - 1) * CHUNKS,)),
    ]
    return pl.pallas_call(
        functools.partial(exchange_kernel, tl, epilogue, len(aux), len(outs), gather),
        name=name,
        out_shape=tuple(out_shape),
        in_specs=[anywhere] + [vmem] * len(aux),
        out_specs=out_specs,
        scratch_shapes=scratch,
        compiler_params=pltpu.CompilerParams(
            has_side_effects=True, collective_id=collective_id, vmem_limit_bytes=40 << 20
        ),
        cost_estimate=pl.CostEstimate(
            flops=0, bytes_accessed=200_000_000 if gather else 110_000_000, transcendentals=0
        ),
    )(partial, *aux)


def middle_rows(total, rows, k, aux, outs):
    stream, gain = aux
    value = stream[rows, :].astype(jnp.float32) + total
    outs[0][rows, :] = value
    return rms_scale(value, gain[...]).astype(jnp.bfloat16)


def norm_pull(value, gain, grad):
    scale = lax.rsqrt(jnp.mean(value * value, axis=-1, keepdims=True) + EPS)
    scaled = grad * gain
    inner = jnp.mean(value * scaled, axis=-1, keepdims=True)
    return scale * scaled - value * (scale * scale * scale * inner), jnp.sum(
        grad * value * scale, axis=0, keepdims=True
    )


def add_rows(out, value, k):
    @pl.when(k == 0)
    def _():
        out[...] = value

    @pl.when(k > 0)
    def _():
        out[...] += value


def middle_pull_rows(total, rows, k, aux, outs):
    middle, cotangent, gain = aux
    pulled, gain_part = norm_pull(middle[rows, :], gain[...], total)
    value = cotangent[rows, :].astype(jnp.float32) + pulled
    outs[0][rows, :] = value
    add_rows(outs[1], gain_part, k)
    return value.astype(jnp.bfloat16)


def stream_pull_rows(total, rows, k, aux, outs):
    stream, gradient, gain = aux
    pulled, gain_part = norm_pull(stream[rows, :].astype(jnp.float32), gain[...], total)
    value = gradient[rows, :] + pulled
    outs[0][rows, :] = value
    outs[1][rows, :] = value.astype(jnp.bfloat16)
    add_rows(outs[2], gain_part, k)
    return None


def shift_perm(size, step):
    return [((place + step) % size, place) for place in range(size)]


def trade(values):
    return lax.ppermute(values, ("c", "h"), [(0, 0), (1, 2), (2, 1), (3, 3)])


def gather_tokens(own, *first):
    places = lax.axis_size("l")
    parts = [own] + [
        after(lax.ppermute(own, "l", shift_perm(places, step)), *first) for step in range(1, places)
    ]
    half = jnp.concatenate(parts, axis=0)
    return jnp.concatenate([half, lax.ppermute(half, "c", shift_perm(2, 1))], axis=0)


def scatter_tokens(partial):
    places = lax.axis_size("l")
    half = partial.shape[0] // 2
    rows = half // places
    other = lax.ppermute(partial[half:].astype(jnp.bfloat16), "c", shift_perm(2, 1))
    total = partial[:half] + other.astype(jnp.float32)
    own = total[:rows]
    for step in range(1, places):
        sent = total[step * rows : (step + 1) * rows].astype(jnp.bfloat16)
        own = own + lax.ppermute(sent, "l", shift_perm(places, -step)).astype(jnp.float32)
    return own


def after(value, *others):
    return lax.optimization_barrier((value,) + others)[0]


def core_halves(shard):
    core = lax.axis_index("c")
    half = shard.shape[-1] // 2
    first, second = shard[..., :half], shard[..., half:]
    mine = jnp.where(core == 0, first, second)
    other = lax.ppermute(jnp.where(core == 0, second, first), "c", shift_perm(2, 1))
    both = jnp.where(core == 0, jnp.stack([mine, other]), jnp.stack([other, mine]))
    return jnp.moveaxis(both, 0, -3).reshape(shard.shape[:-2] + (2 * shard.shape[-2], half))


def return_halves(near, far):
    core = lax.axis_index("c")
    sums = near.astype(jnp.float32) + lax.ppermute(far, "h", shift_perm(2, 1)).astype(jnp.float32)
    rows = sums.shape[0] // 2
    first, second = sums[:rows], sums[rows:]
    mine = jnp.where(core == 0, first, second)
    sent = jnp.where(core == 0, second, first).astype(jnp.bfloat16)
    other = lax.ppermute(sent, "c", shift_perm(2, 1)).astype(jnp.float32)
    return mine, other


def columns_of(mine, other):
    core = lax.axis_index("c")
    return jnp.concatenate(
        [jnp.where(core == 0, mine, other), jnp.where(core == 0, other, mine)], axis=1
    )


def sum_over_d(partial):
    return lax.psum_scatter(partial.astype(jnp.bfloat16), "d", scatter_dimension=0, tiled=True)


def as_row(values):
    return values.reshape(1, -1)


def split(values):
    half = values.shape[1] // 2
    return values[:, :half], values[:, half:]


def scatter_weights(partial):
    core, upper = lax.axis_index("c"), lax.axis_index("h")
    rows = lax.psum_scatter(partial.astype(jnp.bfloat16), "d", scatter_dimension=0, tiled=True)
    half = rows.shape[0] // 2
    first, second = rows[:half], rows[half:]
    mine = jnp.where(core == 0, first, second)
    other = lax.ppermute(jnp.where(core == 0, second, first), "c", shift_perm(2, 1))
    same = core == upper
    far = lax.ppermute(jnp.where(same, other, mine), "h", shift_perm(2, 1))
    return jnp.where(same, mine, other).astype(jnp.float32) + far.astype(jnp.float32)


def per_device(
    tokens,
    segment_ids,
    attn_gain,
    q_weight,
    key_matrix,
    value_matrix,
    o_weight,
    q_gain,
    k_gain,
    mlp_gain,
    gate_weight,
    up_weight,
    down_weight,
    cotangent,
):
    width = attn_gain.shape[1] * lax.axis_size("d") * 2
    own_rows = tokens.shape[0]
    places = lax.axis_size("l")
    core, place = lax.axis_index("c"), lax.axis_index("l")
    q_cols, kv_cols, ff_cols = q_weight.shape[2], key_matrix.shape[2], gate_weight.shape[2]
    half_cols = ff_cols // 2

    gate_half = core_halves(gate_weight[0])
    up_half = core_halves(up_weight[0])
    mid_rows = jnp.concatenate([gate_half, up_half], axis=1)
    down_rows = core_halves(down_weight[0])
    mid_near = lax.all_gather(mid_rows, "d", axis=0, tiled=True)
    down_near = lax.all_gather(down_rows, "d", axis=0, tiled=True)

    cut = attn_gain.shape[1]
    head_cut = q_gain.shape[1]
    gains = jnp.concatenate([attn_gain[0], mlp_gain[0], q_gain[0], k_gain[0]]).astype(jnp.float32)
    gains = jnp.pad(gains, (0, 1024 - gains.shape[0])).reshape(8, 128)
    labels = trade(segment_ids)[0]
    qkv_full, o_full, group, gains = enter(
        q_weight[0], key_matrix[0], value_matrix[0], o_weight[0], after(tokens, mid_rows), gains
    )
    mid_far = lax.ppermute(after(mid_rows, group), "h", shift_perm(2, 1))
    gains = gains.reshape(gains.shape[0], -1)
    attn_scale = gains[:, :cut].reshape(-1)
    mlp_scale = gains[:, cut : 2 * cut].reshape(-1)
    q_scale = gains[:, 2 * cut : 2 * cut + head_cut].reshape(-1)
    k_scale = gains[:, 2 * cut + head_cut : 2 * cut + 2 * head_cut].reshape(-1)

    order = jnp.stack(
        [
            ((core + core_step) % 2) * places + (place + step) % places
            for core_step in range(2)
            for step in range(places)
        ]
    )
    row_index = (order[:, None] * own_rows + jnp.arange(own_rows, dtype=jnp.int32)[None, :]).reshape(-1)
    labels = labels.reshape(2 * places, own_rows)[order].reshape(-1)
    cosine, sine_table = rotary_tables(labels, row_index)

    stream = group[:own_rows]
    normed = rms_scale(group.astype(jnp.float32), attn_scale).astype(jnp.bfloat16)
    rows = normed.shape[0]
    head_count, kv_heads = q_cols // HEAD_WIDTH, kv_cols // HEAD_WIDTH
    qkv = jnp.dot(normed, qkv_full, preferred_element_type=jnp.float32)
    queries = qkv[:, :q_cols].reshape(rows, head_count, HEAD_WIDTH)
    keys = qkv[:, q_cols : q_cols + kv_cols].reshape(rows, kv_heads, HEAD_WIDTH)
    value_reduced = (
        qkv[:, q_cols + kv_cols :].reshape(rows, kv_heads, HEAD_WIDTH).astype(jnp.bfloat16)
    )
    query_reduced = rotate(rms_scale(queries, q_scale), cosine, sine_table).astype(jnp.bfloat16)
    key_reduced = rotate(rms_scale(keys, k_scale), cosine, sine_table).astype(jnp.bfloat16)
    query_reduced = query_reduced.reshape(rows, kv_heads, head_count // kv_heads, HEAD_WIDTH)
    attended, totals = attend_forward(
        query_reduced, key_reduced, value_reduced, labels, row_index
    )
    mid_far = lax.all_gather(after(mid_far, attended, down_near), "d", axis=0, tiled=True)
    down_far = lax.ppermute(after(down_rows, attended), "h", shift_perm(2, 1))
    cotangent = trade(after(cotangent, attended))

    def whole(values):
        return jax.ShapeDtypeStruct((own_rows, width), values)

    gain_sum = jax.ShapeDtypeStruct((1, width), jnp.float32)
    middle, normed_mid = exchange(
        "attention_sum",
        1,
        contract_cols(attended, o_full).astype(jnp.bfloat16),
        (stream, as_row(mlp_scale)),
        (whole(jnp.float32),),
        middle_rows,
        True,
    )
    down_far = lax.all_gather(after(down_far, normed_mid), "d", axis=0, tiled=True)
    cotangent = after(cotangent, normed_mid)

    gate_near, up_near = split(jnp.dot(normed_mid, mid_near, preferred_element_type=jnp.float32))
    hidden_near = swiglu(gate_near, up_near).astype(jnp.bfloat16)
    gate_far, up_far = split(jnp.dot(normed_mid, mid_far, preferred_element_type=jnp.float32))
    hidden_far = swiglu(gate_far, up_far).astype(jnp.bfloat16)
    grad_rows = gather_tokens(cotangent, hidden_near)
    down_grads = sum_over_d(
        jnp.concatenate(
            [
                contract_rows(grad_rows, hidden_near).astype(jnp.bfloat16),
                contract_rows(grad_rows, hidden_far).astype(jnp.bfloat16),
            ],
            axis=1,
        )
    )

    def hidden_pull(gate, up, down):
        hidden_grad = jnp.dot(grad_rows, down, preferred_element_type=jnp.float32)
        _, pull_back = jax.vjp(swiglu, gate, up)
        gate_grad, up_grad = pull_back(hidden_grad)
        return jnp.concatenate(
            [gate_grad.astype(jnp.bfloat16), up_grad.astype(jnp.bfloat16)], axis=1
        )

    mid_back_near = hidden_pull(gate_near, up_near, down_near)
    mid_back_far = hidden_pull(gate_far, up_far, down_far)
    mid_grad_far = contract_rows(normed_mid, mid_back_far).astype(jnp.bfloat16)
    mid_sum_far = sum_over_d(mid_grad_far)
    normed_grad = (contract_cols(mid_back_near, mid_near) + contract_cols(mid_back_far, mid_far)).astype(
        jnp.bfloat16
    )
    gradient, mlp_gain_grad, grad_rows = exchange(
        "middle_pull",
        2,
        after(normed_grad, mid_grad_far),
        (middle, cotangent, as_row(mlp_scale)),
        (whole(jnp.float32), gain_sum),
        middle_pull_rows,
        True,
    )
    mid_grad_near = contract_rows(normed_mid, after(mid_back_near, grad_rows)).astype(jnp.bfloat16)
    mid_sum_near = sum_over_d(mid_grad_near)

    grad_rows = after(grad_rows, mid_grad_near)
    out_grad = jnp.dot(grad_rows, o_full, preferred_element_type=jnp.float32).astype(jnp.bfloat16)
    o_wgrad = contract_rows(grad_rows, attended)
    query_grad, key_grad, value_grad = attend_backward(
        query_reduced,
        key_reduced,
        value_reduced,
        labels,
        row_index,
        totals,
        out_grad.reshape(query_reduced.shape),
    )

    def query_path(raw_values, scales):
        return rotate(rms_scale(raw_values, scales), cosine, sine_table)

    _, pull_query = jax.vjp(query_path, queries, q_scale)
    query_raw_grad, q_gain_grad = pull_query(query_grad)
    _, pull_key = jax.vjp(query_path, keys, k_scale)
    key_raw_grad, k_gain_grad = pull_key(key_grad)
    qkv_back = jnp.concatenate(
        [
            query_raw_grad.reshape(rows, -1).astype(jnp.bfloat16),
            key_raw_grad.reshape(rows, -1).astype(jnp.bfloat16),
            value_grad.reshape(rows, -1).astype(jnp.bfloat16),
        ],
        axis=1,
    )
    qkv_grad = contract_rows(normed, qkv_back).astype(jnp.bfloat16)
    attn_grad = scatter_weights(
        after(jnp.concatenate([qkv_grad, o_wgrad.astype(jnp.bfloat16)], axis=1), mid_sum_far)
    )
    gradient, moved, attn_gain_grad = exchange(
        "stream_pull",
        3,
        contract_cols(after(qkv_back, qkv_grad), qkv_full).astype(jnp.bfloat16),
        (stream, gradient, as_row(attn_scale)),
        (whole(jnp.float32), whole(jnp.bfloat16), gain_sum),
        stream_pull_rows,
        False,
    )
    moved = trade(moved)
    gradient = jnp.where(core == lax.axis_index("h"), gradient, moved.astype(jnp.float32))

    hidden_near = after(hidden_near, attn_gain_grad)
    branch = scatter_tokens(
        contract_cols(hidden_near, down_near) + contract_cols(hidden_far, down_far)
    )
    activations = trade((middle + branch).astype(jnp.bfloat16))

    split_at = down_rows.shape[1]
    down_grad = columns_of(*return_halves(down_grads[:, :split_at], down_grads[:, split_at:]))
    mine, other = return_halves(mid_sum_near, mid_sum_far)
    gate_grad = columns_of(mine[:, :half_cols], other[:, :half_cols])
    up_grad = columns_of(mine[:, half_cols:], other[:, half_cols:])

    sums = lax.psum(
        jnp.concatenate([attn_gain_grad[0], mlp_gain_grad[0], q_gain_grad, k_gain_grad]),
        ("d", "c", "h", "l"),
    )
    row = lax.axis_index("d") * 2 + core

    def owned(start, whole, part):
        return lax.dynamic_slice(sums[start : start + whole], (row * part,), (part,))[None]

    return (
        activations,
        gradient,
        owned(0, width, cut),
        attn_grad[None, :, :q_cols],
        attn_grad[None, :, q_cols : q_cols + kv_cols],
        attn_grad[None, :, q_cols + kv_cols : q_cols + 2 * kv_cols],
        attn_grad[None, :, q_cols + 2 * kv_cols :],
        owned(2 * width, HEAD_WIDTH, head_cut),
        owned(2 * width + HEAD_WIDTH, HEAD_WIDTH, head_cut),
        owned(width, width, cut),
        gate_grad[None],
        up_grad[None],
        down_grad[None],
    )


def solution(mesh):
    dp, tensor = mesh.shape["dp"], mesh.shape["tensor"]
    cut = Mesh(mesh.devices.reshape(dp // 2, 2, 2, tensor // 2), ("d", "c", "h", "l"))
    rows, cols = ("d", "c"), ("h", "l")
    tokens, labels = P(rows + cols, None), P(rows, None)
    gain, weight = P(None, rows), P(None, rows, cols)
    return jax.shard_map(
        per_device,
        mesh=cut,
        in_specs=(
            tokens,
            labels,
            gain,
            weight,
            weight,
            weight,
            weight,
            gain,
            gain,
            gain,
            weight,
            weight,
            weight,
            tokens,
        ),
        out_specs=(
            tokens,
            tokens,
            gain,
            weight,
            weight,
            weight,
            weight,
            gain,
            gain,
            gain,
            weight,
            weight,
            weight,
        ),
        check_vma=False,
    )
```

```python
import functools

import jax
import jax.numpy as jnp
from jax import lax
from jax.experimental import pallas as pl
from jax.experimental.pallas import tpu as pltpu
from jax.sharding import Mesh
from jax.sharding import PartitionSpec as P


HEAD_WIDTH = 128
NSEQ = 3


EPS = 1e-06
THETA = 1000000.0


def rms_scale(values, gain):
    return values * lax.rsqrt(jnp.mean(values * values, axis=-1, keepdims=True) + EPS) * gain


def swiglu(gate_raw, up_raw):
    return jax.nn.silu(gate_raw) * up_raw


def rotary_tables(sequence_labels, row_index):
    labels = jnp.arange(NSEQ, dtype=jnp.int32)
    starts = jnp.sum((sequence_labels[None, :] < labels[:, None]).astype(jnp.int32), axis=1)
    first_row = jnp.sum(
        jnp.where(sequence_labels[:, None] == labels[None, :], starts[None, :], 0), axis=1
    )
    position = (row_index - first_row).astype(jnp.float32)
    frequency = THETA ** (-(jnp.arange(HEAD_WIDTH // 2, dtype=jnp.float32) * (2.0 / HEAD_WIDTH)))
    angles = position[:, None] * frequency[None, :]
    sine = jnp.sin(angles)
    cosine = jnp.cos(angles)
    return (
        jnp.concatenate([cosine, cosine], axis=1),
        jnp.concatenate([-sine, sine], axis=1),
        first_row[:, None],
    )


def contract_rows(left, right):
    return lax.dot_general(
        left, right, (((0,), (0,)), ((), ())), preferred_element_type=jnp.float32
    )


def contract_cols(left, right):
    return lax.dot_general(
        left, right, (((1,), (1,)), ((), ())), preferred_element_type=jnp.float32
    )


MESH = pl.DeviceIdType.MESH
CHUNKS = 3


def remote(source, target, send_sem, recv_sem, **place):
    return pltpu.make_async_remote_copy(
        src_ref=source,
        dst_ref=target,
        send_sem=send_sem,
        recv_sem=recv_sem,
        device_id=place,
        device_id_type=MESH,
    )


def rows_at(index, size):
    return pl.ds(pl.multiple_of(index * size, size), size)


def entry_kernel(nd, tl, *refs):
    (q_ref, k_ref, v_ref, o_ref, tok_ref, gain_ref) = refs[:6]
    (qkv_full, o_full, tok_full, gain_full) = refs[6:10]
    (stage, tok_stage) = refs[10:12]
    (zs, zr, cs, li, lo, xs, xr, ts, tr, tli, tlo, ls, lr, fs, fr, gs, gr, gl) = refs[12:]
    d, c, h, l = (lax.axis_index(name) for name in ("d", "c", "h", "l"))
    same = c == h
    apart = c != h
    rows = q_ref.shape[0]
    own = tok_ref.shape[0]
    chunk = own // CHUNKS
    q_cols, kv_cols = q_ref.shape[1], k_ref.shape[1]
    weights = (
        (q_ref, qkv_full, 0, 0),
        (k_ref, qkv_full, q_cols, q_cols),
        (v_ref, qkv_full, q_cols + kv_cols, q_cols + kv_cols),
        (o_ref, o_full, 0, q_cols + 2 * kv_cols),
    )

    def block(j, row):
        source, full, start, _ = weights[j]
        return full.at[rows_at(row, rows), pl.ds(start, source.shape[1])]

    def held(j):
        source, _, _, start = weights[j]
        return stage.at[:, pl.ds(start, source.shape[1])]

    def from_far(j, part):
        return remote(block(j, d * 2 + part), block(j, d * 2 + part), zs.at[j], zr.at[j, part], h=1 - h)

    def to_far(j):
        return remote(weights[j][0], block(j, d * 2 + c), zs.at[j], zr.at[j, c], c=h, h=1 - h)

    def to_core(j):
        return remote(weights[j][0], block(j, d * 2 + c), cs.at[j], zr.at[j, c], c=h)

    def local_in(j):
        return pltpu.make_async_copy(weights[j][0], held(j), li.at[j])

    def local_out(j):
        return pltpu.make_async_copy(held(j), block(j, d * 2 + c), lo.at[j])

    def tokens_at(index, k):
        return tok_full.at[pl.ds(index * own + k * chunk, chunk)]

    def trade_tokens(k):
        return remote(tok_ref.at[pl.ds(k * chunk, chunk)], tokens_at(0, k), ts.at[k], tr.at[k], c=h, h=c)

    def along(step, k):
        return remote(
            tokens_at(0, k),
            tokens_at(tl - step, k),
            ls.at[(step - 1) * CHUNKS + k],
            lr.at[(tl - step - 1) * CHUNKS + k],
            l=lax.rem(l + step, tl),
        )

    def from_along(index, k):
        return remote(
            tokens_at(index, k),
            tokens_at(index, k),
            ls.at[(index - 1) * CHUNKS + k],
            lr.at[(index - 1) * CHUNKS + k],
            l=l,
        )

    def across(index, k):
        at = index * CHUNKS + k
        return remote(tokens_at(index, k), tokens_at(tl + index, k), fs.at[at], fr.at[at], c=1 - c)

    def gain_peer(step):
        place = lax.rem(d * 2 + c + step, 2 * nd)
        return place // 2, lax.rem(place, 2)

    def gains_to(step):
        to_d, to_c = gain_peer(step)
        return remote(
            gain_ref, gain_full.at[d * 2 + c], gs.at[step - 1], gr.at[2 * nd - step - 1], d=to_d, c=to_c
        )

    def gains_from(step):
        from_d, from_c = gain_peer(step)
        return remote(
            gain_ref, gain_full.at[from_d * 2 + from_c], gs.at[step - 1], gr.at[step - 1], d=from_d, c=from_c
        )

    def local_gains():
        return pltpu.make_async_copy(gain_ref, gain_full.at[d * 2 + c], gl)

    local_gains().start()
    for j in range(3):
        to_far(j).start()

        @pl.when(apart)
        def _():
            to_core(j).start()

    @pl.when(apart)
    def _():
        for k in range(CHUNKS):
            trade_tokens(k).start()

    to_far(3).start()

    @pl.when(apart)
    def _():
        to_core(3).start()

    @pl.when(same)
    def _():
        pltpu.make_async_copy(tok_ref, tok_stage, tli).start()
        for j in range(4):
            local_in(j).start()
        pltpu.make_async_copy(tok_ref, tok_stage, tli).wait()
        for k in range(CHUNKS):
            part = pl.ds(k * chunk, chunk)
            pltpu.make_async_copy(tok_stage.at[part], tokens_at(0, k), tlo.at[k]).start()
        for j in range(4):
            local_in(j).wait()
            local_out(j).start()

    for step in range(1, 2 * nd):
        gains_to(step).start()

    if nd == 4:
        side_x = d + 1 - 2 * lax.rem(d, 2)
        side_y = d + 2 - 4 * (d // 2)
        hops = (
            (0, d, side_x),
            (1, d, side_x),
            (0, d, side_y),
            (1, d, side_y),
            (0, side_x, side_y),
            (1, side_y, side_x),
        )
        sources = (
            (0, side_x),
            (1, side_x),
            (0, side_y),
            (1, side_y),
            (0, side_x + side_y - d),
            (1, side_x + side_y - d),
        )
        first, relayed = 4, ((0, 4), (3, 5))
    else:
        hops = tuple((part, d, lax.rem(d + step, nd)) for step in range(1, nd) for part in range(2))
        sources = tuple(
            (part, lax.rem(d + nd - step, nd)) for step in range(1, nd) for part in range(2)
        )
        first, relayed = len(hops), ()

    def hop(j, kind):
        part, of, to = hops[kind]
        at = block(j, of * 2 + part)
        return remote(at, at, xs.at[j, kind], xr.at[j, kind], d=to)

    def arrived(j, kind):
        part, of = sources[kind]
        at = block(j, of * 2 + part)
        return remote(at, at, xs.at[j, kind], xr.at[j, kind], d=hops[kind][2])

    def spread(j):
        for part in range(2):
            here = jnp.logical_and(same, c == part)

            @pl.when(here)
            def _():
                local_out(j).wait()

            @pl.when(jnp.logical_not(here))
            def _():
                from_far(j, part).wait_recv()

            for kind in range(first):
                if hops[kind][0] == part:
                    hop(j, kind).start()

    def relay(j):
        for after, kind in relayed:
            arrived(j, after).wait_recv()
            hop(j, kind).start()

    spread(0)
    spread(1)
    relay(0)
    spread(2)
    relay(1)
    for k in range(CHUNKS):

        @pl.when(same)
        def _():
            part = pl.ds(k * chunk, chunk)
            pltpu.make_async_copy(tok_stage.at[part], tokens_at(0, k), tlo.at[k]).wait()

        @pl.when(apart)
        def _():
            remote(tokens_at(0, k), tokens_at(0, k), ts.at[k], tr.at[k], c=1 - c, h=1 - h).wait_recv()

        for step in range(1, tl):
            along(step, k).start()
        across(0, k).start()
    relay(2)
    spread(3)
    for k in range(CHUNKS):
        for index in range(1, tl):
            from_along(index, k).wait_recv()
            across(index, k).start()
    relay(3)

    handled = {after for after, _ in relayed}
    for j in range(4):
        for kind in range(len(hops)):
            if kind not in handled:
                arrived(j, kind).wait_recv()
            hop(j, kind).wait_send()
        to_far(j).wait_send()
    for k in range(CHUNKS):
        for index in range(tl):
            across(index, k).wait()
        for step in range(1, tl):
            along(step, k).wait_send()
    for step in range(1, 2 * nd):
        gains_from(step).wait_recv()
        gains_to(step).wait_send()
    local_gains().wait()

    @pl.when(apart)
    def _():
        for j in range(4):
            to_core(j).wait_send()
        for k in range(CHUNKS):
            trade_tokens(k).wait_send()


def enter(q_weight, key_matrix, value_matrix, o_weight, tokens, gains):
    nd, tl = lax.axis_size("d"), lax.axis_size("l")
    rows, q_cols = q_weight.shape
    kv_cols = key_matrix.shape[1]
    own, width = tokens.shape
    hops = 6 if nd == 4 else 2 * (nd - 1)
    dma = pltpu.SemaphoreType.DMA
    return pl.pallas_call(
        functools.partial(entry_kernel, nd, tl),
        name="entry",
        out_shape=(
            jax.ShapeDtypeStruct((width, q_cols + 2 * kv_cols), jnp.bfloat16),
            jax.ShapeDtypeStruct((width, o_weight.shape[1]), jnp.bfloat16),
            jax.ShapeDtypeStruct((2 * tl * own, width), jnp.bfloat16),
            jax.ShapeDtypeStruct((2 * nd,) + gains.shape, jnp.float32),
        ),
        in_specs=[pl.BlockSpec(memory_space=pl.ANY)] * 6,
        out_specs=[pl.BlockSpec(memory_space=pl.ANY)] * 4,
        scratch_shapes=[
            pltpu.VMEM((rows, q_cols + 2 * kv_cols + o_weight.shape[1]), jnp.bfloat16),
            pltpu.VMEM((own, width), jnp.bfloat16),
            dma((4,)),
            dma((4, 2)),
            dma((4,)),
            dma((4,)),
            dma((4,)),
            dma((4, hops)),
            dma((4, hops)),
            dma((CHUNKS,)),
            dma((CHUNKS,)),
            dma,
            dma((CHUNKS,)),
            dma(((tl - 1) * CHUNKS,)),
            dma(((tl - 1) * CHUNKS,)),
            dma((tl * CHUNKS,)),
            dma((tl * CHUNKS,)),
            dma((2 * nd - 1,)),
            dma((2 * nd - 1,)),
            dma,
        ],
        compiler_params=pltpu.CompilerParams(has_side_effects=True),
        cost_estimate=pl.CostEstimate(flops=0, bytes_accessed=250_000_000, transcendentals=0),
    )(q_weight, key_matrix, value_matrix, o_weight, tokens, gains)


def exchange_kernel(tl, epilogue, aux_count, out_count, gather, *refs):
    partial = refs[0]
    aux = refs[1 : 1 + aux_count]
    outs = refs[1 + aux_count : 1 + aux_count + out_count]
    rest = refs[1 + aux_count + out_count :]
    if gather:
        full, rest = rest[0], rest[1:]
        finished, ls, lr, fs, fr, keep, rest = rest[0], *rest[1:6], rest[6:]
    mine, other, sums, arrivals, cs, cr, loc, ss, sr = rest
    c, l = lax.axis_index("c"), lax.axis_index("l")
    own = arrivals.shape[0] // (tl - 1)
    chunk = own // CHUNKS

    barrier = pltpu.get_barrier_semaphore()
    pl.semaphore_signal(barrier, inc=1, device_id={"c": 1 - c}, device_id_type=MESH)
    for step in range(1, tl):
        pl.semaphore_signal(
            barrier, inc=1, device_id={"l": lax.rem(l + step, tl)}, device_id_type=MESH
        )
    pl.semaphore_wait(barrier, tl)

    def part(base, k):
        return rows_at(base * CHUNKS + k, chunk)

    def to_core(index, k):
        at = index * CHUNKS + k
        return remote(
            partial.at[part(tl + index, k)], other.at[part(index, k)], cs.at[at], cr.at[at], c=1 - c
        )

    def local(index, k):
        return pltpu.make_async_copy(
            partial.at[part(index, k)], mine.at[part(index, k)], loc.at[index * CHUNKS + k]
        )

    def along(step, k):
        at = (step - 1) * CHUNKS + k
        return remote(
            sums.at[part(step - 1, k)],
            arrivals.at[part(step - 1, k)],
            ss.at[at],
            sr.at[at],
            l=lax.rem(l + step, tl),
        )

    order = list(range(1, tl)) + [0]
    for index in order:
        for k in range(CHUNKS):
            to_core(index, k).start()
            local(index, k).start()

    def both(index, k):
        local(index, k).wait()
        to_core(index, k).wait_recv()
        at = part(index, k)
        return mine[at, :].astype(jnp.float32) + other[at, :].astype(jnp.float32)

    for step in range(1, tl):

        def pass_on(k, carry):
            sums[part(step - 1, k), :] = both(step, k).astype(jnp.bfloat16)
            along(step, k).start()
            return carry

        lax.fori_loop(0, CHUNKS, pass_on, 0)

    def gathered(index, k):
        return full.at[part(index, k)]

    def keep_own(k):
        return pltpu.make_async_copy(finished.at[part(0, k)], gathered(0, k), keep.at[k])

    def own_along(step, k):
        return remote(
            finished.at[part(0, k)],
            gathered(tl - step, k),
            ls.at[(step - 1) * CHUNKS + k],
            lr.at[(tl - step - 1) * CHUNKS + k],
            l=lax.rem(l + step, tl),
        )

    def from_along(index, k):
        at = (index - 1) * CHUNKS + k
        return remote(gathered(index, k), gathered(index, k), ls.at[at], lr.at[at], l=l)

    def across(index, k):
        source = finished.at[part(0, k)] if index == 0 else gathered(index, k)
        at = index * CHUNKS + k
        return remote(source, gathered(tl + index, k), fs.at[at], fr.at[at], c=1 - c)

    def finish(k, carry):
        total = both(0, k)
        for step in range(1, tl):
            along(step, k).wait_recv()
            total = total + arrivals[part(step - 1, k), :].astype(jnp.float32)
        row = epilogue(total, part(0, k), k, aux, outs)
        if gather:
            finished[part(0, k), :] = row
            keep_own(k).start()
            for step in range(1, tl):
                own_along(step, k).start()
            across(0, k).start()
        return carry

    lax.fori_loop(0, CHUNKS, finish, 0)
    if gather:
        for k in range(CHUNKS):
            for index in range(1, tl):
                from_along(index, k).wait_recv()
                across(index, k).start()
        for k in range(CHUNKS):
            keep_own(k).wait()
            for index in range(tl):
                across(index, k).wait()
            for step in range(1, tl):
                own_along(step, k).wait_send()
    for k in range(CHUNKS):
        for index in range(tl):
            to_core(index, k).wait_send()
        for step in range(1, tl):
            along(step, k).wait_send()


def exchange(collective_id, partial, aux, outs, epilogue, gather):
    tl = lax.axis_size("l")
    total, width = partial.shape
    own = total // (2 * tl)
    dma = pltpu.SemaphoreType.DMA
    vmem = pl.BlockSpec(memory_space=pltpu.VMEM)
    anywhere = pl.BlockSpec(memory_space=pl.ANY)
    out_shape = list(outs)
    out_specs = [vmem] * len(outs)
    scratch = []
    if gather:
        out_shape.append(jax.ShapeDtypeStruct((total, width), jnp.bfloat16))
        out_specs.append(anywhere)
        scratch += [
            pltpu.VMEM((own, width), jnp.bfloat16),
            dma(((tl - 1) * CHUNKS,)),
            dma(((tl - 1) * CHUNKS,)),
            dma((tl * CHUNKS,)),
            dma((tl * CHUNKS,)),
            dma((CHUNKS,)),
        ]
    scratch += [
        pltpu.VMEM((tl * own, width), jnp.bfloat16),
        pltpu.VMEM((tl * own, width), jnp.bfloat16),
        pltpu.VMEM(((tl - 1) * own, width), jnp.bfloat16),
        pltpu.VMEM(((tl - 1) * own, width), jnp.bfloat16),
        dma((tl * CHUNKS,)),
        dma((tl * CHUNKS,)),
        dma((tl * CHUNKS,)),
        dma(((tl - 1) * CHUNKS,)),
        dma(((tl - 1) * CHUNKS,)),
    ]
    return pl.pallas_call(
        functools.partial(exchange_kernel, tl, epilogue, len(aux), len(outs), gather),
        out_shape=tuple(out_shape),
        in_specs=[anywhere] + [vmem] * len(aux),
        out_specs=out_specs,
        scratch_shapes=scratch,
        compiler_params=pltpu.CompilerParams(
            has_side_effects=True, collective_id=collective_id, vmem_limit_bytes=40 << 20
        ),
        cost_estimate=pl.CostEstimate(
            flops=0, bytes_accessed=200_000_000 if gather else 110_000_000, transcendentals=0
        ),
    )(partial, *aux)


def middle_rows(total, rows, k, aux, outs):
    stream, gain = aux
    value = stream[rows, :].astype(jnp.float32) + total
    outs[0][rows, :] = value
    return rms_scale(value, gain[...]).astype(jnp.bfloat16)


def norm_pull(value, gain, grad):
    scale = lax.rsqrt(jnp.mean(value * value, axis=-1, keepdims=True) + EPS)
    scaled = grad * gain
    inner = jnp.mean(value * scaled, axis=-1, keepdims=True)
    return scale * scaled - value * (scale * scale * scale * inner), jnp.sum(
        grad * value * scale, axis=0, keepdims=True
    )


def add_rows(out, value, k):
    @pl.when(k == 0)
    def _():
        out[...] = value

    @pl.when(k > 0)
    def _():
        out[...] += value


def middle_pull_rows(total, rows, k, aux, outs):
    middle, cotangent, gain = aux
    pulled, gain_part = norm_pull(middle[rows, :], gain[...], total)
    value = cotangent[rows, :].astype(jnp.float32) + pulled
    outs[0][rows, :] = value
    add_rows(outs[1], gain_part, k)
    return value.astype(jnp.bfloat16)


def stream_pull_rows(total, rows, k, aux, outs):
    stream, gradient, gain = aux
    pulled, gain_part = norm_pull(stream[rows, :].astype(jnp.float32), gain[...], total)
    value = gradient[rows, :] + pulled
    outs[0][rows, :] = value
    outs[1][rows, :] = value.astype(jnp.bfloat16)
    add_rows(outs[2], gain_part, k)
    return None


def key_tile(rows):
    return next(size for size in (384, 256, 128) if rows % size == 0)


def turn(values):
    return pltpu.roll(values, HEAD_WIDTH // 2, 1)


def head_norm(values):
    return lax.rsqrt(jnp.mean(values * values, axis=-1, keepdims=True) + EPS)


def tile_mask(first, start, tile, row0, rows):
    keys = start + lax.broadcasted_iota(jnp.int32, (rows, tile), 1)
    last = row0 + lax.broadcasted_iota(jnp.int32, (rows, tile), 0)
    return jnp.logical_and(keys >= first, keys <= last)


def dot_last(left, right):
    return lax.dot_general(
        left, right, (((1,), (1,)), ((), ())), preferred_element_type=jnp.float32
    )


def attention_kernel(blocks, repeat, order_ref, *refs):
    q, k, v, cosine, sine, q_gain, k_gain, first = refs[:8]
    qr, kr, vb, out, total = refs[8:13]
    acc, den = refs[13:]
    rows = q.shape[0] // blocks
    tile = key_tile(q.shape[0])
    scale = HEAD_WIDTH**-0.5

    def rotated(values, gain, at):
        scaled = values * head_norm(values) * gain
        return (scaled * cosine[at, :] + turn(scaled) * sine[at, :]).astype(jnp.bfloat16)

    def prepare(i, carry):
        at, to = rows_at(i, rows), rows_at(order_ref[i], rows)
        for r in range(repeat):
            head = slice(r * HEAD_WIDTH, (r + 1) * HEAD_WIDTH)
            qr[at, head] = rotated(q[at, head], q_gain[...], at)
        kr[to, :] = rotated(k[at, :], k_gain[...], at)
        vb[to, :] = v[at, :].astype(jnp.bfloat16)
        return carry

    lax.fori_loop(0, blocks, prepare, 0)

    def attend(i, carry):
        at = rows_at(i, rows)
        row0 = order_ref[i] * rows
        acc[...] = jnp.zeros_like(acc)
        den[...] = jnp.zeros_like(den)

        def over_keys(t, inner):
            keys = rows_at(t, tile)
            mask = tile_mask(first[at, :], t * tile, tile, row0, rows)
            for r in range(repeat):
                head = slice(r * HEAD_WIDTH, (r + 1) * HEAD_WIDTH)
                scores = dot_last(qr[at, head], kr[keys, :]) * scale
                weights = jnp.where(mask, jnp.exp(scores), 0.0)
                den[r] += jnp.sum(weights, axis=-1, keepdims=True)
                acc[r] += jnp.dot(
                    weights.astype(jnp.bfloat16), vb[keys, :], preferred_element_type=jnp.float32
                )
            return inner

        lax.fori_loop(0, (row0 + rows + tile - 1) // tile, over_keys, 0)
        for r in range(repeat):
            head = slice(r * HEAD_WIDTH, (r + 1) * HEAD_WIDTH)
            out[at, head] = (acc[r] / den[r]).astype(jnp.bfloat16)
            total[at, r : r + 1] = den[r]
        return carry

    lax.fori_loop(0, blocks, attend, 0)


def attention_specs(rows, q_heads, kv_heads):
    repeat = q_heads // kv_heads

    def columns(width, start=0):
        return pl.BlockSpec((rows, width * HEAD_WIDTH), lambda g, order: (0, start // width + g))

    def fixed(*shape):
        return pl.BlockSpec(shape, lambda g, order: (0, 0))

    raw = [columns(repeat), columns(1, q_heads), columns(1, q_heads + kv_heads)]
    tables = [
        fixed(rows, HEAD_WIDTH),
        fixed(rows, HEAD_WIDTH),
        fixed(1, HEAD_WIDTH),
        fixed(1, HEAD_WIDTH),
        fixed(rows, 1),
    ]
    return repeat, columns, fixed, raw, tables


def attention(qkv, tables, order, q_heads, kv_heads):
    rows = qkv.shape[0]
    blocks = order.shape[0]
    repeat, columns, _, raw, table_specs = attention_specs(rows, q_heads, kv_heads)
    wide, narrow = q_heads * HEAD_WIDTH, kv_heads * HEAD_WIDTH
    return pl.pallas_call(
        functools.partial(attention_kernel, blocks, repeat),
        name="attention",
        out_shape=(
            jax.ShapeDtypeStruct((rows, wide), jnp.bfloat16),
            jax.ShapeDtypeStruct((rows, narrow), jnp.bfloat16),
            jax.ShapeDtypeStruct((rows, narrow), jnp.bfloat16),
            jax.ShapeDtypeStruct((rows, wide), jnp.bfloat16),
            jax.ShapeDtypeStruct((rows, narrow), jnp.float32),
        ),
        grid_spec=pltpu.PrefetchScalarGridSpec(
            num_scalar_prefetch=1,
            grid=(kv_heads,),
            in_specs=raw + table_specs,
            out_specs=[columns(repeat), columns(1), columns(1), columns(repeat), columns(1)],
            scratch_shapes=[
                pltpu.VMEM((repeat, rows // blocks, HEAD_WIDTH), jnp.float32),
                pltpu.VMEM((repeat, rows // blocks, 1), jnp.float32),
            ],
        ),
        compiler_params=pltpu.CompilerParams(vmem_limit_bytes=50 << 20),
        cost_estimate=pl.CostEstimate(
            flops=4 * rows * rows * wide, bytes_accessed=60_000_000, transcendentals=0
        ),
    )(order, qkv, qkv, qkv, *tables)


def attention_pull_kernel(blocks, repeat, order_ref, *refs):
    q, k, cosine, sine, q_gain, k_gain, first, qr, kr, vb, total, grad = refs[:12]
    dq, dk, dv, dq_gain, dk_gain = refs[12:17]
    shares, share_grads, dq_acc, dk_acc, dv_acc, inner_sum = refs[17:]
    rows = q.shape[0] // blocks
    tile = key_tile(q.shape[0])
    scale = HEAD_WIDTH**-0.5
    dk_acc[...] = jnp.zeros_like(dk_acc)
    dv_acc[...] = jnp.zeros_like(dv_acc)

    @pl.when(pl.program_id(0) == 0)
    def _():
        dq_gain[...] = jnp.zeros_like(dq_gain)
        dk_gain[...] = jnp.zeros_like(dk_gain)

    def pull(raw, gain, turned_grad, at, gain_out):
        scaled_grad = turned_grad * cosine[at, :] + turn(turned_grad * sine[at, :])
        r = head_norm(raw)
        gain_out[0:1, :] += jnp.sum(scaled_grad * raw * r, axis=0, keepdims=True)
        scaled = scaled_grad * gain
        inner = jnp.mean(raw * scaled, axis=-1, keepdims=True)
        return (r * scaled - raw * (r * r * r * inner)).astype(jnp.bfloat16)

    def over_rows(i, carry):
        at = rows_at(i, rows)
        row0 = order_ref[i] * rows
        tiles = (row0 + rows + tile - 1) // tile
        dq_acc[...] = jnp.zeros_like(dq_acc)
        inner_sum[...] = jnp.zeros_like(inner_sum)

        def first_pass(t, inner):
            keys = rows_at(t, tile)
            mask = tile_mask(first[at, :], t * tile, tile, row0, rows)
            for r in range(repeat):
                head = slice(r * HEAD_WIDTH, (r + 1) * HEAD_WIDTH)
                scores = dot_last(qr[at, head], kr[keys, :]) * scale
                share = jnp.where(mask, jnp.exp(scores), 0.0) * (1.0 / total[at, r : r + 1])
                share_grad = dot_last(grad[at, head], vb[keys, :])
                inner_sum[r] += jnp.sum(share * share_grad, axis=-1, keepdims=True)
                shares[t, r] = share
                share_grads[t, r] = share_grad
            return inner

        lax.fori_loop(0, tiles, first_pass, 0)

        def second_pass(t, inner):
            keys = rows_at(t, tile)
            for r in range(repeat):
                head = slice(r * HEAD_WIDTH, (r + 1) * HEAD_WIDTH)
                share = shares[t, r]
                score_grad = (share * (share_grads[t, r] - inner_sum[r])).astype(jnp.bfloat16)
                dq_acc[r] += jnp.dot(score_grad, kr[keys, :], preferred_element_type=jnp.float32)
                dk_acc[keys, :] += contract_rows(score_grad, qr[at, head])
                dv_acc[keys, :] += contract_rows(share.astype(jnp.bfloat16), grad[at, head])
            return inner

        lax.fori_loop(0, tiles, second_pass, 0)
        for r in range(repeat):
            head = slice(r * HEAD_WIDTH, (r + 1) * HEAD_WIDTH)
            dq[at, head] = pull(q[at, head], q_gain[...], dq_acc[r] * scale, at, dq_gain)
        return carry

    lax.fori_loop(0, blocks, over_rows, 0)

    def finish(i, carry):
        at, to = rows_at(i, rows), rows_at(order_ref[i], rows)
        dk[at, :] = pull(k[at, :], k_gain[...], dk_acc[to, :] * scale, at, dk_gain)
        dv[at, :] = dv_acc[to, :].astype(jnp.bfloat16)
        return carry

    lax.fori_loop(0, blocks, finish, 0)


def attention_pull(qkv, tables, order, kept, grad, q_heads, kv_heads):
    rows = qkv.shape[0]
    blocks = order.shape[0]
    repeat, columns, fixed, raw, table_specs = attention_specs(rows, q_heads, kv_heads)
    wide, narrow = q_heads * HEAD_WIDTH, kv_heads * HEAD_WIDTH
    own, tile = rows // blocks, key_tile(rows)
    return pl.pallas_call(
        functools.partial(attention_pull_kernel, blocks, repeat),
        name="attention_pull",
        out_shape=(
            jax.ShapeDtypeStruct((rows, wide), jnp.bfloat16),
            jax.ShapeDtypeStruct((rows, narrow), jnp.bfloat16),
            jax.ShapeDtypeStruct((rows, narrow), jnp.bfloat16),
            jax.ShapeDtypeStruct((8, HEAD_WIDTH), jnp.float32),
            jax.ShapeDtypeStruct((8, HEAD_WIDTH), jnp.float32),
        ),
        grid_spec=pltpu.PrefetchScalarGridSpec(
            num_scalar_prefetch=1,
            grid=(kv_heads,),
            in_specs=raw[:2]
            + table_specs
            + [columns(repeat), columns(1), columns(1), columns(1), columns(repeat)],
            out_specs=[
                columns(repeat),
                columns(1),
                columns(1),
                fixed(8, HEAD_WIDTH),
                fixed(8, HEAD_WIDTH),
            ],
            scratch_shapes=[
                pltpu.VMEM((rows // tile, repeat, own, tile), jnp.float32),
                pltpu.VMEM((rows // tile, repeat, own, tile), jnp.float32),
                pltpu.VMEM((repeat, own, HEAD_WIDTH), jnp.float32),
                pltpu.VMEM((rows, HEAD_WIDTH), jnp.float32),
                pltpu.VMEM((rows, HEAD_WIDTH), jnp.float32),
                pltpu.VMEM((repeat, own, 1), jnp.float32),
            ],
        ),
        compiler_params=pltpu.CompilerParams(vmem_limit_bytes=56 << 20),
        cost_estimate=pl.CostEstimate(
            flops=10 * rows * rows * wide, bytes_accessed=120_000_000, transcendentals=0
        ),
    )(order, qkv, qkv, *tables, *kept, grad)


def shift_perm(size, step):
    return [((place + step) % size, place) for place in range(size)]


def trade(values):
    return lax.ppermute(values, ("c", "h"), [(0, 0), (1, 2), (2, 1), (3, 3)])


def gather_tokens(own, *first):
    places = lax.axis_size("l")
    parts = [own] + [
        after(lax.ppermute(own, "l", shift_perm(places, step)), *first) for step in range(1, places)
    ]
    half = jnp.concatenate(parts, axis=0)
    return jnp.concatenate([half, lax.ppermute(half, "c", shift_perm(2, 1))], axis=0)


def scatter_tokens(partial):
    places = lax.axis_size("l")
    half = partial.shape[0] // 2
    rows = half // places
    other = lax.ppermute(partial[half:].astype(jnp.bfloat16), "c", shift_perm(2, 1))
    total = partial[:half] + other.astype(jnp.float32)
    own = total[:rows]
    for step in range(1, places):
        sent = total[step * rows : (step + 1) * rows].astype(jnp.bfloat16)
        own = own + lax.ppermute(sent, "l", shift_perm(places, -step)).astype(jnp.float32)
    return own


def after(value, *others):
    return lax.optimization_barrier((value,) + others)[0]


def core_halves(shard):
    core = lax.axis_index("c")
    half = shard.shape[-1] // 2
    first, second = shard[..., :half], shard[..., half:]
    mine = jnp.where(core == 0, first, second)
    other = lax.ppermute(jnp.where(core == 0, second, first), "c", shift_perm(2, 1))
    both = jnp.where(core == 0, jnp.stack([mine, other]), jnp.stack([other, mine]))
    return jnp.moveaxis(both, 0, -3).reshape(shard.shape[:-2] + (2 * shard.shape[-2], half))


def return_halves(near, far):
    core = lax.axis_index("c")
    far = lax.ppermute(far, "h", shift_perm(2, 1))
    sums = near.astype(jnp.float32) + far.astype(jnp.float32)
    rows = sums.shape[0] // 2
    first, second = sums[:rows], sums[rows:]
    mine = jnp.where(core == 0, first, second)
    sent = jnp.where(core == 0, second, first).astype(jnp.bfloat16)
    other = lax.ppermute(sent, "c", shift_perm(2, 1)).astype(jnp.float32)
    return mine, other


def columns_of(mine, other):
    core = lax.axis_index("c")
    return jnp.concatenate(
        [jnp.where(core == 0, mine, other), jnp.where(core == 0, other, mine)], axis=1
    )


def sum_over_d(partial):
    return lax.psum_scatter(partial.astype(jnp.bfloat16), "d", scatter_dimension=0, tiled=True)


def as_row(values):
    return values.reshape(1, -1)


def split(values):
    half = values.shape[1] // 2
    return values[:, :half], values[:, half:]


def scatter_weights(partial):
    core, upper = lax.axis_index("c"), lax.axis_index("h")
    rows = lax.psum_scatter(partial.astype(jnp.bfloat16), "d", scatter_dimension=0, tiled=True)
    half = rows.shape[0] // 2
    first, second = rows[:half], rows[half:]
    mine = jnp.where(core == 0, first, second)
    other = lax.ppermute(jnp.where(core == 0, second, first), "c", shift_perm(2, 1))
    same = core == upper
    far = lax.ppermute(jnp.where(same, other, mine), "h", shift_perm(2, 1))
    return jnp.where(same, mine, other).astype(jnp.float32) + far.astype(jnp.float32)


def per_device(
    tokens,
    segment_ids,
    attn_gain,
    q_weight,
    key_matrix,
    value_matrix,
    o_weight,
    q_gain,
    k_gain,
    mlp_gain,
    gate_weight,
    up_weight,
    down_weight,
    cotangent,
):
    width = attn_gain.shape[1] * lax.axis_size("d") * 2
    own_rows = tokens.shape[0]
    places = lax.axis_size("l")
    core, place = lax.axis_index("c"), lax.axis_index("l")
    q_cols, kv_cols, ff_cols = q_weight.shape[2], key_matrix.shape[2], gate_weight.shape[2]
    half_cols = ff_cols // 2

    gate_half = core_halves(gate_weight[0])
    up_half = core_halves(up_weight[0])
    mid_rows = jnp.concatenate([gate_half, up_half], axis=1)
    down_rows = core_halves(down_weight[0])
    mid_near = lax.all_gather(mid_rows, "d", axis=0, tiled=True)
    down_near = lax.all_gather(down_rows, "d", axis=0, tiled=True)

    cut = attn_gain.shape[1]
    head_cut = q_gain.shape[1]
    gains = jnp.concatenate([attn_gain[0], mlp_gain[0], q_gain[0], k_gain[0]]).astype(jnp.float32)
    gains = jnp.pad(gains, (0, 1024 - gains.shape[0])).reshape(8, 128)
    labels = trade(segment_ids)[0]
    order = jnp.stack(
        [
            ((core + core_step) % 2) * places + (place + step) % places
            for core_step in range(2)
            for step in range(places)
        ]
    )
    row_index = (order[:, None] * own_rows + jnp.arange(own_rows, dtype=jnp.int32)[None, :]).reshape(-1)
    labels = labels.reshape(2 * places, own_rows)[order].reshape(-1)
    cosine, sine, first_row = rotary_tables(labels, row_index)
    qkv_full, o_full, group, gains = enter(
        q_weight[0], key_matrix[0], value_matrix[0], o_weight[0], after(tokens, mid_rows), gains
    )
    mid_far = lax.ppermute(after(mid_rows, group), "h", shift_perm(2, 1))
    down_far = lax.ppermute(after(down_rows, group), "h", shift_perm(2, 1))
    cotangent = trade(after(cotangent, group))
    gains = gains.reshape(gains.shape[0], -1)
    attn_scale = gains[:, :cut].reshape(-1)
    mlp_scale = gains[:, cut : 2 * cut].reshape(-1)
    q_scale = gains[:, 2 * cut : 2 * cut + head_cut].reshape(-1)
    k_scale = gains[:, 2 * cut + head_cut : 2 * cut + 2 * head_cut].reshape(-1)

    stream = group[:own_rows]
    normed = rms_scale(group.astype(jnp.float32), attn_scale).astype(jnp.bfloat16)
    head_count, kv_heads = q_cols // HEAD_WIDTH, kv_cols // HEAD_WIDTH
    qkv = jnp.dot(normed, qkv_full, preferred_element_type=jnp.float32)
    tables = (cosine, sine, as_row(q_scale), as_row(k_scale), first_row)
    query_reduced, key_reduced, value_reduced, attended, totals = attention(
        qkv, tables, order, head_count, kv_heads
    )
    mid_far = lax.all_gather(after(mid_far, attended, down_near), "d", axis=0, tiled=True)

    def whole(values):
        return jax.ShapeDtypeStruct((own_rows, width), values)

    gain_sum = jax.ShapeDtypeStruct((1, width), jnp.float32)
    middle, normed_mid = exchange(
        1,
        contract_cols(attended, o_full).astype(jnp.bfloat16),
        (stream, as_row(mlp_scale)),
        (whole(jnp.float32),),
        middle_rows,
        True,
    )
    down_far = lax.all_gather(after(down_far, normed_mid), "d", axis=0, tiled=True)
    cotangent = after(cotangent, normed_mid)

    gate_near, up_near = split(jnp.dot(normed_mid, mid_near, preferred_element_type=jnp.float32))
    hidden_near = swiglu(gate_near, up_near).astype(jnp.bfloat16)
    gate_far, up_far = split(jnp.dot(normed_mid, mid_far, preferred_element_type=jnp.float32))
    hidden_far = swiglu(gate_far, up_far).astype(jnp.bfloat16)
    grad_rows = gather_tokens(cotangent, hidden_far)
    down_grads = sum_over_d(
        jnp.concatenate(
            [
                contract_rows(grad_rows, hidden_near).astype(jnp.bfloat16),
                contract_rows(grad_rows, hidden_far).astype(jnp.bfloat16),
            ],
            axis=1,
        )
    )

    def hidden_pull(gate, up, down):
        hidden_grad = jnp.dot(grad_rows, down, preferred_element_type=jnp.float32)
        _, pull_back = jax.vjp(swiglu, gate, up)
        gate_grad, up_grad = pull_back(hidden_grad)
        return jnp.concatenate(
            [gate_grad.astype(jnp.bfloat16), up_grad.astype(jnp.bfloat16)], axis=1
        )

    mid_back_near = hidden_pull(gate_near, up_near, down_near)
    mid_back_far = hidden_pull(gate_far, up_far, down_far)
    mid_grad_far = contract_rows(normed_mid, mid_back_far).astype(jnp.bfloat16)
    mid_sum_far = sum_over_d(mid_grad_far)
    normed_grad = (contract_cols(mid_back_near, mid_near) + contract_cols(mid_back_far, mid_far)).astype(
        jnp.bfloat16
    )
    gradient, mlp_gain_grad, grad_rows = exchange(
        2,
        after(normed_grad, mid_grad_far),
        (middle, cotangent, as_row(mlp_scale)),
        (whole(jnp.float32), gain_sum),
        middle_pull_rows,
        True,
    )
    mid_grad_near = contract_rows(normed_mid, after(mid_back_near, grad_rows)).astype(jnp.bfloat16)
    mid_sum_near = sum_over_d(mid_grad_near)

    grad_rows = after(grad_rows, mid_grad_near)
    out_grad = jnp.dot(grad_rows, o_full, preferred_element_type=jnp.float32).astype(jnp.bfloat16)
    o_wgrad = contract_rows(grad_rows, attended)
    query_back, key_back, value_back, q_gain_grad, k_gain_grad = attention_pull(
        qkv,
        tables,
        order,
        (query_reduced, key_reduced, value_reduced, totals),
        out_grad,
        head_count,
        kv_heads,
    )
    qkv_back = jnp.concatenate([query_back, key_back, value_back], axis=1)
    qkv_grad = contract_rows(normed, qkv_back).astype(jnp.bfloat16)
    attn_grad = scatter_weights(
        after(jnp.concatenate([qkv_grad, o_wgrad.astype(jnp.bfloat16)], axis=1), mid_sum_far)
    )
    gradient, moved, attn_gain_grad = exchange(
        3,
        contract_cols(after(qkv_back, qkv_grad), qkv_full).astype(jnp.bfloat16),
        (stream, gradient, as_row(attn_scale)),
        (whole(jnp.float32), whole(jnp.bfloat16), gain_sum),
        stream_pull_rows,
        False,
    )
    moved = trade(moved)
    gradient = jnp.where(core == lax.axis_index("h"), gradient, moved.astype(jnp.float32))

    hidden_near = after(hidden_near, attn_gain_grad)
    branch = scatter_tokens(
        contract_cols(hidden_near, down_near) + contract_cols(hidden_far, down_far)
    )
    activations = trade((middle + branch).astype(jnp.bfloat16))

    split_at = down_rows.shape[1]
    down_grad = columns_of(*return_halves(down_grads[:, :split_at], down_grads[:, split_at:]))
    mine, other = return_halves(mid_sum_near, mid_sum_far)
    gate_grad = columns_of(mine[:, :half_cols], other[:, :half_cols])
    up_grad = columns_of(mine[:, half_cols:], other[:, half_cols:])

    sums = lax.psum(
        jnp.concatenate([attn_gain_grad[0], mlp_gain_grad[0], q_gain_grad[0], k_gain_grad[0]]),
        ("d", "c", "h", "l"),
    )
    row = lax.axis_index("d") * 2 + core

    def owned(start, whole, part):
        return lax.dynamic_slice(sums[start : start + whole], (row * part,), (part,))[None]

    return (
        activations,
        gradient,
        owned(0, width, cut),
        attn_grad[None, :, :q_cols],
        attn_grad[None, :, q_cols : q_cols + kv_cols],
        attn_grad[None, :, q_cols + kv_cols : q_cols + 2 * kv_cols],
        attn_grad[None, :, q_cols + 2 * kv_cols :],
        owned(2 * width, HEAD_WIDTH, head_cut),
        owned(2 * width + HEAD_WIDTH, HEAD_WIDTH, head_cut),
        owned(width, width, cut),
        gate_grad[None],
        up_grad[None],
        down_grad[None],
    )


def solution(mesh):
    dp, tensor = mesh.shape["dp"], mesh.shape["tensor"]
    cut = Mesh(mesh.devices.reshape(dp // 2, 2, 2, tensor // 2), ("d", "c", "h", "l"))
    rows, cols = ("d", "c"), ("h", "l")
    tokens, labels = P(rows + cols, None), P(rows, None)
    gain, weight = P(None, rows), P(None, rows, cols)
    return jax.shard_map(
        per_device,
        mesh=cut,
        in_specs=(
            tokens,
            labels,
            gain,
            weight,
            weight,
            weight,
            weight,
            gain,
            gain,
            gain,
            weight,
            weight,
            weight,
            tokens,
        ),
        out_specs=(
            tokens,
            tokens,
            gain,
            weight,
            weight,
            weight,
            weight,
            gain,
            gain,
            gain,
            weight,
            weight,
            weight,
        ),
        check_vma=False,
    )
```

```python
import functools

import jax
import jax.numpy as jnp
from jax import lax
from jax.experimental import pallas as pl
from jax.experimental.pallas import tpu as pltpu
from jax.sharding import Mesh
from jax.sharding import PartitionSpec as P


HEAD_WIDTH = 128
NSEQ = 3


EPS = 1e-06
THETA = 1000000.0


def rms_scale(values, gain):
    return values * lax.rsqrt(jnp.mean(values * values, axis=-1, keepdims=True) + EPS) * gain


def swiglu(gate_raw, up_raw):
    return jax.nn.silu(gate_raw) * up_raw


def rotary_tables(sequence_labels, row_index):
    labels = jnp.arange(NSEQ, dtype=jnp.int32)
    starts = jnp.sum((sequence_labels[None, :] < labels[:, None]).astype(jnp.int32), axis=1)
    first_row = jnp.sum(
        jnp.where(sequence_labels[:, None] == labels[None, :], starts[None, :], 0), axis=1
    )
    position = (row_index - first_row).astype(jnp.float32)
    frequency = THETA ** (-(jnp.arange(HEAD_WIDTH // 2, dtype=jnp.float32) * (2.0 / HEAD_WIDTH)))
    angles = position[:, None] * frequency[None, :]
    sine = jnp.sin(angles)
    cosine = jnp.cos(angles)
    return (
        jnp.concatenate([cosine, cosine], axis=1),
        jnp.concatenate([-sine, sine], axis=1),
        first_row[:, None],
    )


def contract_rows(left, right):
    return lax.dot_general(
        left, right, (((0,), (0,)), ((), ())), preferred_element_type=jnp.float32
    )


def contract_cols(left, right):
    return lax.dot_general(
        left, right, (((1,), (1,)), ((), ())), preferred_element_type=jnp.float32
    )


MESH = pl.DeviceIdType.MESH
CHUNKS = 3


def remote(source, target, send_sem, recv_sem, **place):
    return pltpu.make_async_remote_copy(
        src_ref=source,
        dst_ref=target,
        send_sem=send_sem,
        recv_sem=recv_sem,
        device_id=place,
        device_id_type=MESH,
    )


def rows_at(index, size):
    return pl.ds(pl.multiple_of(index * size, size), size)


def hop_plan(nd, d):
    if nd == 4:
        side_x = d + 1 - 2 * lax.rem(d, 2)
        side_y = d + 2 - 4 * (d // 2)
        corner = side_x + side_y - d
        hops = (
            (0, d, side_x),
            (1, d, side_x),
            (0, d, side_y),
            (1, d, side_y),
            (0, side_x, side_y),
            (1, side_y, side_x),
        )
        sources = ((0, side_x), (1, side_x), (0, side_y), (1, side_y), (0, corner), (1, corner))
        return hops, sources, 4, ((0, 4), (3, 5))
    steps = [(part, step) for step in range(1, nd) for part in range(2)]
    hops = tuple((part, d, lax.rem(d + step, nd)) for part, step in steps)
    sources = tuple((part, lax.rem(d + nd - step, nd)) for part, step in steps)
    return hops, sources, len(hops), ()


def hop_count(nd):
    return 6 if nd == 4 else 2 * (nd - 1)


class Spread:
    def __init__(self, nd, d, block, send_sem, recv_sem):
        self.hops, self.sources, self.first, self.relayed = hop_plan(nd, d)
        self.block, self.send_sem, self.recv_sem = block, send_sem, recv_sem

    def copy(self, j, kind, part, of):
        at = self.block(j, of * 2 + part)
        return remote(
            at, at, self.send_sem.at[j, kind], self.recv_sem.at[j, kind], d=self.hops[kind][2]
        )

    def hop(self, j, kind):
        return self.copy(j, kind, *self.hops[kind][:2])

    def arrived(self, j, kind):
        return self.copy(j, kind, *self.sources[kind])

    def send(self, j, part):
        for kind in range(self.first):
            if self.hops[kind][0] == part:
                self.hop(j, kind).start()

    def relay(self, j):
        for after_kind, kind in self.relayed:
            self.arrived(j, after_kind).wait_recv()
            self.hop(j, kind).start()

    def finish(self, j):
        handled = {after_kind for after_kind, _ in self.relayed}
        for kind in range(len(self.hops)):
            if kind not in handled:
                self.arrived(j, kind).wait_recv()
            self.hop(j, kind).wait_send()


def entry_kernel(nd, tl, *refs):
    (q_ref, k_ref, v_ref, o_ref, tok_ref, gain_ref) = refs[:6]
    (qkv_full, o_full, tok_full, gain_full) = refs[6:10]
    (stage, tok_stage) = refs[10:12]
    (zs, zr, cs, li, lo, xs, xr, ts, tr, tli, tlo, ls, lr, fs, fr, gs, gr, gl) = refs[12:]
    d, c, h, l = (lax.axis_index(name) for name in ("d", "c", "h", "l"))
    same = c == h
    apart = c != h
    rows = q_ref.shape[0]
    own = tok_ref.shape[0]
    chunk = own // CHUNKS
    q_cols, kv_cols = q_ref.shape[1], k_ref.shape[1]
    weights = (
        (q_ref, qkv_full, 0, 0),
        (k_ref, qkv_full, q_cols, q_cols),
        (v_ref, qkv_full, q_cols + kv_cols, q_cols + kv_cols),
        (o_ref, o_full, 0, q_cols + 2 * kv_cols),
    )

    def block(j, row):
        source, full, start, _ = weights[j]
        return full.at[rows_at(row, rows), pl.ds(start, source.shape[1])]

    def held(j):
        source, _, _, start = weights[j]
        return stage.at[:, pl.ds(start, source.shape[1])]

    def from_far(j, part):
        return remote(block(j, d * 2 + part), block(j, d * 2 + part), zs.at[j], zr.at[j, part], h=1 - h)

    def to_far(j):
        return remote(weights[j][0], block(j, d * 2 + c), zs.at[j], zr.at[j, c], c=h, h=1 - h)

    def to_core(j):
        return remote(weights[j][0], block(j, d * 2 + c), cs.at[j], zr.at[j, c], c=h)

    def local_in(j):
        return pltpu.make_async_copy(weights[j][0], held(j), li.at[j])

    def local_out(j):
        return pltpu.make_async_copy(held(j), block(j, d * 2 + c), lo.at[j])

    def tokens_at(index, k):
        return tok_full.at[pl.ds(index * own + k * chunk, chunk)]

    def trade_tokens(k):
        return remote(tok_ref.at[pl.ds(k * chunk, chunk)], tokens_at(0, k), ts.at[k], tr.at[k], c=h, h=c)

    def along(step, k):
        return remote(
            tokens_at(0, k),
            tokens_at(tl - step, k),
            ls.at[(step - 1) * CHUNKS + k],
            lr.at[(tl - step - 1) * CHUNKS + k],
            l=lax.rem(l + step, tl),
        )

    def from_along(index, k):
        return remote(
            tokens_at(index, k),
            tokens_at(index, k),
            ls.at[(index - 1) * CHUNKS + k],
            lr.at[(index - 1) * CHUNKS + k],
            l=l,
        )

    def across(index, k):
        at = index * CHUNKS + k
        return remote(tokens_at(index, k), tokens_at(tl + index, k), fs.at[at], fr.at[at], c=1 - c)

    def gain_peer(step):
        place = lax.rem(d * 2 + c + step, 2 * nd)
        return place // 2, lax.rem(place, 2)

    def gains_to(step):
        to_d, to_c = gain_peer(step)
        return remote(
            gain_ref, gain_full.at[d * 2 + c], gs.at[step - 1], gr.at[2 * nd - step - 1], d=to_d, c=to_c
        )

    def gains_from(step):
        from_d, from_c = gain_peer(step)
        return remote(
            gain_ref, gain_full.at[from_d * 2 + from_c], gs.at[step - 1], gr.at[step - 1], d=from_d, c=from_c
        )

    def local_gains():
        return pltpu.make_async_copy(gain_ref, gain_full.at[d * 2 + c], gl)

    local_gains().start()
    for j in range(3):
        to_far(j).start()

        @pl.when(apart)
        def _():
            to_core(j).start()

    @pl.when(apart)
    def _():
        for k in range(CHUNKS):
            trade_tokens(k).start()

    to_far(3).start()

    @pl.when(apart)
    def _():
        to_core(3).start()

    @pl.when(same)
    def _():
        pltpu.make_async_copy(tok_ref, tok_stage, tli).start()
        for j in range(4):
            local_in(j).start()
        pltpu.make_async_copy(tok_ref, tok_stage, tli).wait()
        for k in range(CHUNKS):
            part = pl.ds(k * chunk, chunk)
            pltpu.make_async_copy(tok_stage.at[part], tokens_at(0, k), tlo.at[k]).start()
        for j in range(4):
            local_in(j).wait()
            local_out(j).start()

    for step in range(1, 2 * nd):
        gains_to(step).start()

    over_d = Spread(nd, d, block, xs, xr)

    def spread(j):
        for part in range(2):
            here = jnp.logical_and(same, c == part)

            @pl.when(here)
            def _():
                local_out(j).wait()

            @pl.when(jnp.logical_not(here))
            def _():
                from_far(j, part).wait_recv()

            over_d.send(j, part)

    relay = over_d.relay
    spread(0)
    spread(1)
    relay(0)
    spread(2)
    relay(1)
    for k in range(CHUNKS):

        @pl.when(same)
        def _():
            part = pl.ds(k * chunk, chunk)
            pltpu.make_async_copy(tok_stage.at[part], tokens_at(0, k), tlo.at[k]).wait()

        @pl.when(apart)
        def _():
            remote(tokens_at(0, k), tokens_at(0, k), ts.at[k], tr.at[k], c=1 - c, h=1 - h).wait_recv()

        for step in range(1, tl):
            along(step, k).start()
        across(0, k).start()
    relay(2)
    spread(3)
    for k in range(CHUNKS):
        for index in range(1, tl):
            from_along(index, k).wait_recv()
            across(index, k).start()
    relay(3)

    for j in range(4):
        over_d.finish(j)
        to_far(j).wait_send()
    for k in range(CHUNKS):
        for index in range(tl):
            across(index, k).wait()
        for step in range(1, tl):
            along(step, k).wait_send()
    for step in range(1, 2 * nd):
        gains_from(step).wait_recv()
        gains_to(step).wait_send()
    local_gains().wait()

    @pl.when(apart)
    def _():
        for j in range(4):
            to_core(j).wait_send()
        for k in range(CHUNKS):
            trade_tokens(k).wait_send()


def enter(q_weight, key_matrix, value_matrix, o_weight, tokens, gains):
    nd, tl = lax.axis_size("d"), lax.axis_size("l")
    rows, q_cols = q_weight.shape
    kv_cols = key_matrix.shape[1]
    own, width = tokens.shape
    hops = hop_count(nd)
    dma = pltpu.SemaphoreType.DMA
    return pl.pallas_call(
        functools.partial(entry_kernel, nd, tl),
        name="entry",
        out_shape=(
            jax.ShapeDtypeStruct((width, q_cols + 2 * kv_cols), jnp.bfloat16),
            jax.ShapeDtypeStruct((width, o_weight.shape[1]), jnp.bfloat16),
            jax.ShapeDtypeStruct((2 * tl * own, width), jnp.bfloat16),
            jax.ShapeDtypeStruct((2 * nd,) + gains.shape, jnp.float32),
        ),
        in_specs=[pl.BlockSpec(memory_space=pl.ANY)] * 6,
        out_specs=[pl.BlockSpec(memory_space=pl.ANY)] * 4,
        scratch_shapes=[
            pltpu.VMEM((rows, q_cols + 2 * kv_cols + o_weight.shape[1]), jnp.bfloat16),
            pltpu.VMEM((own, width), jnp.bfloat16),
            dma((4,)),
            dma((4, 2)),
            dma((4,)),
            dma((4,)),
            dma((4,)),
            dma((4, hops)),
            dma((4, hops)),
            dma((CHUNKS,)),
            dma((CHUNKS,)),
            dma,
            dma((CHUNKS,)),
            dma(((tl - 1) * CHUNKS,)),
            dma(((tl - 1) * CHUNKS,)),
            dma((tl * CHUNKS,)),
            dma((tl * CHUNKS,)),
            dma((2 * nd - 1,)),
            dma((2 * nd - 1,)),
            dma,
        ],
        compiler_params=pltpu.CompilerParams(has_side_effects=True),
        cost_estimate=pl.CostEstimate(flops=0, bytes_accessed=250_000_000, transcendentals=0),
    )(q_weight, key_matrix, value_matrix, o_weight, tokens, gains)


PIECES = 3


def exchange_kernel(nd, tl, epilogue, aux_count, out_count, gather, carry_weights, *refs):
    partial = refs[0]
    aux = refs[1 : 1 + aux_count]
    refs = refs[1 + aux_count :]
    if carry_weights:
        weight_rows, refs = refs[0], refs[1:]
    outs = refs[:out_count]
    rest = refs[out_count:]
    if gather:
        full, rest = rest[0], rest[1:]
    if carry_weights:
        weights, ws, wr, xs, xr, rest = rest[0], *rest[1:5], rest[5:]
    if gather:
        finished, ls, lr, fs, fr, keep, rest = rest[0], *rest[1:6], rest[6:]
    mine, other, sums, arrivals, cs, cr, loc, ss, sr = rest
    c, l = lax.axis_index("c"), lax.axis_index("l")
    d, h = lax.axis_index("d"), lax.axis_index("h")
    own = arrivals.shape[0] // (tl - 1)
    chunk = own // CHUNKS

    barrier = pltpu.get_barrier_semaphore()
    pl.semaphore_signal(barrier, inc=1, device_id={"c": 1 - c}, device_id_type=MESH)
    for step in range(1, tl):
        pl.semaphore_signal(
            barrier, inc=1, device_id={"l": lax.rem(l + step, tl)}, device_id_type=MESH
        )
    partners = tl
    if carry_weights:
        pl.semaphore_signal(barrier, inc=1, device_id={"h": 1 - h}, device_id_type=MESH)
        partners += 1
        for step in range(1, nd):
            pl.semaphore_signal(
                barrier, inc=1, device_id={"d": lax.rem(d + step, nd)}, device_id_type=MESH
            )
        partners += nd - 1
    pl.semaphore_wait(barrier, partners)

    def part(base, k):
        return rows_at(base * CHUNKS + k, chunk)

    def to_core(index, k):
        at = index * CHUNKS + k
        return remote(
            partial.at[part(tl + index, k)], other.at[part(index, k)], cs.at[at], cr.at[at], c=1 - c
        )

    def local(index, k):
        return pltpu.make_async_copy(
            partial.at[part(index, k)], mine.at[part(index, k)], loc.at[index * CHUNKS + k]
        )

    def along(step, k):
        at = (step - 1) * CHUNKS + k
        return remote(
            sums.at[part(step - 1, k)],
            arrivals.at[part(step - 1, k)],
            ss.at[at],
            sr.at[at],
            l=lax.rem(l + step, tl),
        )

    if carry_weights:
        half = weight_rows.shape[0] // 2
        piece = weight_rows.shape[1] // PIECES

        def block(j, row):
            return weights.at[rows_at(row, half), pl.ds(j * piece, piece)]

        def from_far(j, row_part):
            return remote(
                weight_rows.at[pl.ds(row_part * half, half), pl.ds(j * piece, piece)],
                block(j, d * 2 + row_part),
                ws.at[j, row_part],
                wr.at[j, row_part],
                h=1 - h,
            )

        over_d = Spread(nd, d, block, xs, xr)

        def spread(j):
            for row_part in range(2):
                from_far(j, row_part).wait_recv()
                over_d.send(j, row_part)

        for j in range(PIECES):
            for row_part in range(2):
                from_far(j, row_part).start()

    order = list(range(1, tl)) + [0]
    for index in order:
        for k in range(CHUNKS):
            to_core(index, k).start()
            local(index, k).start()

    def both(index, k):
        local(index, k).wait()
        to_core(index, k).wait_recv()
        at = part(index, k)
        return mine[at, :].astype(jnp.float32) + other[at, :].astype(jnp.float32)

    for step in range(1, tl):

        def pass_on(k, carry):
            sums[part(step - 1, k), :] = both(step, k).astype(jnp.bfloat16)
            along(step, k).start()
            return carry

        lax.fori_loop(0, CHUNKS, pass_on, 0)

    def gathered(index, k):
        return full.at[part(index, k)]

    def keep_own(k):
        return pltpu.make_async_copy(finished.at[part(0, k)], gathered(0, k), keep.at[k])

    def own_along(step, k):
        return remote(
            finished.at[part(0, k)],
            gathered(tl - step, k),
            ls.at[(step - 1) * CHUNKS + k],
            lr.at[(tl - step - 1) * CHUNKS + k],
            l=lax.rem(l + step, tl),
        )

    def from_along(index, k):
        at = (index - 1) * CHUNKS + k
        return remote(gathered(index, k), gathered(index, k), ls.at[at], lr.at[at], l=l)

    def across(index, k):
        source = finished.at[part(0, k)] if index == 0 else gathered(index, k)
        at = index * CHUNKS + k
        return remote(source, gathered(tl + index, k), fs.at[at], fr.at[at], c=1 - c)

    def finish(k, carry):
        total = both(0, k)
        for step in range(1, tl):
            along(step, k).wait_recv()
            total = total + arrivals[part(step - 1, k), :].astype(jnp.float32)
        row = epilogue(total, part(0, k), k, aux, outs)
        if gather:
            finished[part(0, k), :] = row
            keep_own(k).start()
            for step in range(1, tl):
                own_along(step, k).start()
            across(0, k).start()
        return carry

    if carry_weights:
        for k in range(CHUNKS):
            finish(k, 0)
            spread(k)
            if k:
                over_d.relay(k - 1)
    else:
        lax.fori_loop(0, CHUNKS, finish, 0)
    if gather:
        for k in range(CHUNKS):
            for index in range(1, tl):
                from_along(index, k).wait_recv()
                across(index, k).start()
        if carry_weights:
            over_d.relay(PIECES - 1)
        for k in range(CHUNKS):
            keep_own(k).wait()
            for index in range(tl):
                across(index, k).wait()
            for step in range(1, tl):
                own_along(step, k).wait_send()
    if carry_weights:
        for j in range(PIECES):
            over_d.finish(j)
            for row_part in range(2):
                from_far(j, row_part).wait_send()
    for k in range(CHUNKS):
        for index in range(tl):
            to_core(index, k).wait_send()
        for step in range(1, tl):
            along(step, k).wait_send()


def exchange(collective_id, partial, aux, outs, epilogue, gather, weight_rows=None):
    nd, tl = lax.axis_size("d"), lax.axis_size("l")
    total, width = partial.shape
    own = total // (2 * tl)
    dma = pltpu.SemaphoreType.DMA
    vmem = pl.BlockSpec(memory_space=pltpu.VMEM)
    anywhere = pl.BlockSpec(memory_space=pl.ANY)
    out_shape = list(outs)
    out_specs = [vmem] * len(outs)
    scratch = []
    given = ()
    if gather:
        out_shape.append(jax.ShapeDtypeStruct((total, width), jnp.bfloat16))
        out_specs.append(anywhere)
    if weight_rows is not None:
        given = (weight_rows,)
        rows, cols = weight_rows.shape
        out_shape.append(jax.ShapeDtypeStruct((nd * rows, cols), jnp.bfloat16))
        out_specs.append(anywhere)
        scratch += [
            dma((PIECES, 2)),
            dma((PIECES, 2)),
            dma((PIECES, hop_count(nd))),
            dma((PIECES, hop_count(nd))),
        ]
    if gather:
        scratch += [
            pltpu.VMEM((own, width), jnp.bfloat16),
            dma(((tl - 1) * CHUNKS,)),
            dma(((tl - 1) * CHUNKS,)),
            dma((tl * CHUNKS,)),
            dma((tl * CHUNKS,)),
            dma((CHUNKS,)),
        ]
    scratch += [
        pltpu.VMEM((tl * own, width), jnp.bfloat16),
        pltpu.VMEM((tl * own, width), jnp.bfloat16),
        pltpu.VMEM(((tl - 1) * own, width), jnp.bfloat16),
        pltpu.VMEM(((tl - 1) * own, width), jnp.bfloat16),
        dma((tl * CHUNKS,)),
        dma((tl * CHUNKS,)),
        dma((tl * CHUNKS,)),
        dma(((tl - 1) * CHUNKS,)),
        dma(((tl - 1) * CHUNKS,)),
    ]
    return pl.pallas_call(
        functools.partial(
            exchange_kernel, nd, tl, epilogue, len(aux), len(outs), gather, bool(given)
        ),
        out_shape=tuple(out_shape),
        in_specs=[anywhere] + [vmem] * len(aux) + [anywhere] * len(given),
        out_specs=out_specs,
        scratch_shapes=scratch,
        compiler_params=pltpu.CompilerParams(
            has_side_effects=True, collective_id=collective_id, vmem_limit_bytes=40 << 20
        ),
        cost_estimate=pl.CostEstimate(
            flops=0, bytes_accessed=200_000_000 if gather else 110_000_000, transcendentals=0
        ),
    )(partial, *aux, *given)


def middle_rows(total, rows, k, aux, outs):
    stream, gain = aux
    value = stream[rows, :].astype(jnp.float32) + total
    outs[0][rows, :] = value
    return rms_scale(value, gain[...]).astype(jnp.bfloat16)


def norm_pull(value, gain, grad):
    scale = lax.rsqrt(jnp.mean(value * value, axis=-1, keepdims=True) + EPS)
    scaled = grad * gain
    inner = jnp.mean(value * scaled, axis=-1, keepdims=True)
    return scale * scaled - value * (scale * scale * scale * inner), jnp.sum(
        grad * value * scale, axis=0, keepdims=True
    )


def add_rows(out, value, k):
    @pl.when(k == 0)
    def _():
        out[...] = value

    @pl.when(k > 0)
    def _():
        out[...] += value


def middle_pull_rows(total, rows, k, aux, outs):
    middle, cotangent, gain = aux
    pulled, gain_part = norm_pull(middle[rows, :], gain[...], total)
    value = cotangent[rows, :].astype(jnp.float32) + pulled
    outs[0][rows, :] = value
    add_rows(outs[1], gain_part, k)
    return value.astype(jnp.bfloat16)


def stream_pull_rows(total, rows, k, aux, outs):
    stream, gradient, gain = aux
    pulled, gain_part = norm_pull(stream[rows, :].astype(jnp.float32), gain[...], total)
    value = gradient[rows, :] + pulled
    outs[0][rows, :] = value
    outs[1][rows, :] = value.astype(jnp.bfloat16)
    add_rows(outs[2], gain_part, k)
    return None


def key_tile(rows):
    return next(size for size in (384, 256, 128) if rows % size == 0)


def turn(values):
    return pltpu.roll(values, HEAD_WIDTH // 2, 1)


def head_norm(values):
    return lax.rsqrt(jnp.mean(values * values, axis=-1, keepdims=True) + EPS)


def tile_mask(first, start, tile, row0, rows):
    keys = start + lax.broadcasted_iota(jnp.int32, (rows, tile), 1)
    last = row0 + lax.broadcasted_iota(jnp.int32, (rows, tile), 0)
    return jnp.logical_and(keys >= first, keys <= last)


def dot_last(left, right):
    return lax.dot_general(
        left, right, (((1,), (1,)), ((), ())), preferred_element_type=jnp.float32
    )


def attention_kernel(blocks, repeat, order_ref, *refs):
    q, k, v, cosine, sine, q_gain, k_gain, first = refs[:8]
    qr, kr, vb, out, total = refs[8:13]
    acc, den = refs[13:]
    rows = q.shape[0] // blocks
    tile = key_tile(q.shape[0])
    scale = HEAD_WIDTH**-0.5

    def rotated(values, gain, at):
        scaled = values * head_norm(values) * gain
        return (scaled * cosine[at, :] + turn(scaled) * sine[at, :]).astype(jnp.bfloat16)

    def prepare(i, carry):
        at, to = rows_at(i, rows), rows_at(order_ref[i], rows)
        for r in range(repeat):
            head = slice(r * HEAD_WIDTH, (r + 1) * HEAD_WIDTH)
            qr[at, head] = rotated(q[at, head], q_gain[...], at)
        kr[to, :] = rotated(k[at, :], k_gain[...], at)
        vb[to, :] = v[at, :].astype(jnp.bfloat16)
        return carry

    lax.fori_loop(0, blocks, prepare, 0)

    def attend(i, carry):
        at = rows_at(i, rows)
        row0 = order_ref[i] * rows
        acc[...] = jnp.zeros_like(acc)
        den[...] = jnp.zeros_like(den)

        def over_keys(t, inner):
            keys = rows_at(t, tile)
            mask = tile_mask(first[at, :], t * tile, tile, row0, rows)
            for r in range(repeat):
                head = slice(r * HEAD_WIDTH, (r + 1) * HEAD_WIDTH)
                scores = dot_last(qr[at, head], kr[keys, :]) * scale
                weights = jnp.where(mask, jnp.exp(scores), 0.0)
                den[r] += jnp.sum(weights, axis=-1, keepdims=True)
                acc[r] += jnp.dot(
                    weights.astype(jnp.bfloat16), vb[keys, :], preferred_element_type=jnp.float32
                )
            return inner

        lax.fori_loop(0, (row0 + rows + tile - 1) // tile, over_keys, 0)
        for r in range(repeat):
            head = slice(r * HEAD_WIDTH, (r + 1) * HEAD_WIDTH)
            out[at, head] = (acc[r] / den[r]).astype(jnp.bfloat16)
            total[at, r : r + 1] = den[r]
        return carry

    lax.fori_loop(0, blocks, attend, 0)


def attention_specs(rows, q_heads, kv_heads):
    repeat = q_heads // kv_heads

    def columns(width, start=0):
        return pl.BlockSpec((rows, width * HEAD_WIDTH), lambda g, order: (0, start // width + g))

    def fixed(*shape):
        return pl.BlockSpec(shape, lambda g, order: (0, 0))

    raw = [columns(repeat), columns(1, q_heads), columns(1, q_heads + kv_heads)]
    tables = [
        fixed(rows, HEAD_WIDTH),
        fixed(rows, HEAD_WIDTH),
        fixed(1, HEAD_WIDTH),
        fixed(1, HEAD_WIDTH),
        fixed(rows, 1),
    ]
    return repeat, columns, fixed, raw, tables


def attention(qkv, tables, order, q_heads, kv_heads):
    rows = qkv.shape[0]
    blocks = order.shape[0]
    repeat, columns, _, raw, table_specs = attention_specs(rows, q_heads, kv_heads)
    wide, narrow = q_heads * HEAD_WIDTH, kv_heads * HEAD_WIDTH
    return pl.pallas_call(
        functools.partial(attention_kernel, blocks, repeat),
        name="attention",
        out_shape=(
            jax.ShapeDtypeStruct((rows, wide), jnp.bfloat16),
            jax.ShapeDtypeStruct((rows, narrow), jnp.bfloat16),
            jax.ShapeDtypeStruct((rows, narrow), jnp.bfloat16),
            jax.ShapeDtypeStruct((rows, wide), jnp.bfloat16),
            jax.ShapeDtypeStruct((rows, narrow), jnp.float32),
        ),
        grid_spec=pltpu.PrefetchScalarGridSpec(
            num_scalar_prefetch=1,
            grid=(kv_heads,),
            in_specs=raw + table_specs,
            out_specs=[columns(repeat), columns(1), columns(1), columns(repeat), columns(1)],
            scratch_shapes=[
                pltpu.VMEM((repeat, rows // blocks, HEAD_WIDTH), jnp.float32),
                pltpu.VMEM((repeat, rows // blocks, 1), jnp.float32),
            ],
        ),
        compiler_params=pltpu.CompilerParams(vmem_limit_bytes=50 << 20),
        cost_estimate=pl.CostEstimate(
            flops=4 * rows * rows * wide, bytes_accessed=60_000_000, transcendentals=0
        ),
    )(order, qkv, qkv, qkv, *tables)


def attention_pull_kernel(blocks, repeat, order_ref, *refs):
    q, k, cosine, sine, q_gain, k_gain, first, qr, kr, vb, total, grad = refs[:12]
    dq, dk, dv, dq_gain, dk_gain = refs[12:17]
    shares, share_grads, dq_acc, dk_acc, dv_acc, inner_sum = refs[17:]
    rows = q.shape[0] // blocks
    tile = key_tile(q.shape[0])
    scale = HEAD_WIDTH**-0.5
    dk_acc[...] = jnp.zeros_like(dk_acc)
    dv_acc[...] = jnp.zeros_like(dv_acc)

    @pl.when(pl.program_id(0) == 0)
    def _():
        dq_gain[...] = jnp.zeros_like(dq_gain)
        dk_gain[...] = jnp.zeros_like(dk_gain)

    def pull(raw, gain, turned_grad, at, gain_out):
        scaled_grad = turned_grad * cosine[at, :] + turn(turned_grad * sine[at, :])
        r = head_norm(raw)
        gain_out[0:1, :] += jnp.sum(scaled_grad * raw * r, axis=0, keepdims=True)
        scaled = scaled_grad * gain
        inner = jnp.mean(raw * scaled, axis=-1, keepdims=True)
        return (r * scaled - raw * (r * r * r * inner)).astype(jnp.bfloat16)

    def over_rows(i, carry):
        at = rows_at(i, rows)
        row0 = order_ref[i] * rows
        tiles = (row0 + rows + tile - 1) // tile
        dq_acc[...] = jnp.zeros_like(dq_acc)
        inner_sum[...] = jnp.zeros_like(inner_sum)

        def first_pass(t, inner):
            keys = rows_at(t, tile)
            mask = tile_mask(first[at, :], t * tile, tile, row0, rows)
            for r in range(repeat):
                head = slice(r * HEAD_WIDTH, (r + 1) * HEAD_WIDTH)
                scores = dot_last(qr[at, head], kr[keys, :]) * scale
                share = jnp.where(mask, jnp.exp(scores), 0.0) * (1.0 / total[at, r : r + 1])
                share_grad = dot_last(grad[at, head], vb[keys, :])
                inner_sum[r] += jnp.sum(share * share_grad, axis=-1, keepdims=True)
                shares[t, r] = share
                share_grads[t, r] = share_grad
            return inner

        lax.fori_loop(0, tiles, first_pass, 0)

        def second_pass(t, inner):
            keys = rows_at(t, tile)
            for r in range(repeat):
                head = slice(r * HEAD_WIDTH, (r + 1) * HEAD_WIDTH)
                share = shares[t, r]
                score_grad = (share * (share_grads[t, r] - inner_sum[r])).astype(jnp.bfloat16)
                dq_acc[r] += jnp.dot(score_grad, kr[keys, :], preferred_element_type=jnp.float32)
                dk_acc[keys, :] += contract_rows(score_grad, qr[at, head])
                dv_acc[keys, :] += contract_rows(share.astype(jnp.bfloat16), grad[at, head])
            return inner

        lax.fori_loop(0, tiles, second_pass, 0)
        for r in range(repeat):
            head = slice(r * HEAD_WIDTH, (r + 1) * HEAD_WIDTH)
            dq[at, head] = pull(q[at, head], q_gain[...], dq_acc[r] * scale, at, dq_gain)
        return carry

    lax.fori_loop(0, blocks, over_rows, 0)

    def finish(i, carry):
        at, to = rows_at(i, rows), rows_at(order_ref[i], rows)
        dk[at, :] = pull(k[at, :], k_gain[...], dk_acc[to, :] * scale, at, dk_gain)
        dv[at, :] = dv_acc[to, :].astype(jnp.bfloat16)
        return carry

    lax.fori_loop(0, blocks, finish, 0)


def attention_pull(qkv, tables, order, kept, grad, q_heads, kv_heads):
    rows = qkv.shape[0]
    blocks = order.shape[0]
    repeat, columns, fixed, raw, table_specs = attention_specs(rows, q_heads, kv_heads)
    wide, narrow = q_heads * HEAD_WIDTH, kv_heads * HEAD_WIDTH
    own, tile = rows // blocks, key_tile(rows)
    return pl.pallas_call(
        functools.partial(attention_pull_kernel, blocks, repeat),
        name="attention_pull",
        out_shape=(
            jax.ShapeDtypeStruct((rows, wide), jnp.bfloat16),
            jax.ShapeDtypeStruct((rows, narrow), jnp.bfloat16),
            jax.ShapeDtypeStruct((rows, narrow), jnp.bfloat16),
            jax.ShapeDtypeStruct((8, HEAD_WIDTH), jnp.float32),
            jax.ShapeDtypeStruct((8, HEAD_WIDTH), jnp.float32),
        ),
        grid_spec=pltpu.PrefetchScalarGridSpec(
            num_scalar_prefetch=1,
            grid=(kv_heads,),
            in_specs=raw[:2]
            + table_specs
            + [columns(repeat), columns(1), columns(1), columns(1), columns(repeat)],
            out_specs=[
                columns(repeat),
                columns(1),
                columns(1),
                fixed(8, HEAD_WIDTH),
                fixed(8, HEAD_WIDTH),
            ],
            scratch_shapes=[
                pltpu.VMEM((rows // tile, repeat, own, tile), jnp.float32),
                pltpu.VMEM((rows // tile, repeat, own, tile), jnp.float32),
                pltpu.VMEM((repeat, own, HEAD_WIDTH), jnp.float32),
                pltpu.VMEM((rows, HEAD_WIDTH), jnp.float32),
                pltpu.VMEM((rows, HEAD_WIDTH), jnp.float32),
                pltpu.VMEM((repeat, own, 1), jnp.float32),
            ],
        ),
        compiler_params=pltpu.CompilerParams(vmem_limit_bytes=56 << 20),
        cost_estimate=pl.CostEstimate(
            flops=10 * rows * rows * wide, bytes_accessed=120_000_000, transcendentals=0
        ),
    )(order, qkv, qkv, *tables, *kept, grad)


def shift_perm(size, step):
    return [((place + step) % size, place) for place in range(size)]


def trade(values):
    return lax.ppermute(values, ("c", "h"), [(0, 0), (1, 2), (2, 1), (3, 3)])


def gather_tokens(own, *first):
    places = lax.axis_size("l")
    parts = [own] + [
        after(lax.ppermute(own, "l", shift_perm(places, step)), *first) for step in range(1, places)
    ]
    half = jnp.concatenate(parts, axis=0)
    return jnp.concatenate([half, lax.ppermute(half, "c", shift_perm(2, 1))], axis=0)


def scatter_tokens(partial, *first):
    places = lax.axis_size("l")
    half = partial.shape[0] // 2
    rows = half // places
    other = lax.ppermute(partial[half:].astype(jnp.bfloat16), "c", shift_perm(2, 1))
    total = partial[:half] + other.astype(jnp.float32)
    own = total[:rows]
    for step in range(1, places):
        sent = total[step * rows : (step + 1) * rows].astype(jnp.bfloat16)
        moved = lax.ppermute(sent, "l", shift_perm(places, -step))
        moved = after(moved, *first)
        own = own + moved.astype(jnp.float32)
    return own


def after(value, *others):
    return lax.optimization_barrier((value,) + others)[0]


def core_halves(shard):
    core = lax.axis_index("c")
    half = shard.shape[-1] // 2
    first, second = shard[..., :half], shard[..., half:]
    mine = jnp.where(core == 0, first, second)
    other = lax.ppermute(jnp.where(core == 0, second, first), "c", shift_perm(2, 1))
    both = jnp.where(core == 0, jnp.stack([mine, other]), jnp.stack([other, mine]))
    return jnp.moveaxis(both, 0, -3).reshape(shard.shape[:-2] + (2 * shard.shape[-2], half))


def return_halves(near, far):
    core = lax.axis_index("c")
    far = lax.ppermute(far, "h", shift_perm(2, 1))
    sums = near.astype(jnp.float32) + far.astype(jnp.float32)
    rows = sums.shape[0] // 2
    first, second = sums[:rows], sums[rows:]
    mine = jnp.where(core == 0, first, second)
    sent = jnp.where(core == 0, second, first).astype(jnp.bfloat16)
    other = lax.ppermute(sent, "c", shift_perm(2, 1)).astype(jnp.float32)
    return mine, other


def columns_of(mine, other):
    core = lax.axis_index("c")
    return jnp.concatenate(
        [jnp.where(core == 0, mine, other), jnp.where(core == 0, other, mine)], axis=1
    )


def sum_over_d(partial):
    return lax.psum_scatter(partial.astype(jnp.bfloat16), "d", scatter_dimension=0, tiled=True)


def as_row(values):
    return values.reshape(1, -1)


def split(values):
    half = values.shape[1] // 2
    return values[:, :half], values[:, half:]


def scatter_weights(partial):
    core, upper = lax.axis_index("c"), lax.axis_index("h")
    rows = lax.psum_scatter(partial.astype(jnp.bfloat16), "d", scatter_dimension=0, tiled=True)
    half = rows.shape[0] // 2
    first, second = rows[:half], rows[half:]
    mine = jnp.where(core == 0, first, second)
    other = lax.ppermute(jnp.where(core == 0, second, first), "c", shift_perm(2, 1))
    same = core == upper
    far = lax.ppermute(jnp.where(same, other, mine), "h", shift_perm(2, 1))
    return jnp.where(same, mine, other).astype(jnp.float32) + far.astype(jnp.float32)


def per_device(
    tokens,
    segment_ids,
    attn_gain,
    q_weight,
    key_matrix,
    value_matrix,
    o_weight,
    q_gain,
    k_gain,
    mlp_gain,
    gate_weight,
    up_weight,
    down_weight,
    cotangent,
):
    width = attn_gain.shape[1] * lax.axis_size("d") * 2
    own_rows = tokens.shape[0]
    places = lax.axis_size("l")
    core, place = lax.axis_index("c"), lax.axis_index("l")
    q_cols, kv_cols, ff_cols = q_weight.shape[2], key_matrix.shape[2], gate_weight.shape[2]
    half_cols = ff_cols // 2

    gate_half = core_halves(gate_weight[0])
    up_half = core_halves(up_weight[0])
    mid_rows = jnp.concatenate([gate_half, up_half], axis=1)
    down_rows = core_halves(down_weight[0])
    down_near = lax.all_gather(down_rows, "d", axis=0, tiled=True)

    cut = attn_gain.shape[1]
    head_cut = q_gain.shape[1]
    gains = jnp.concatenate([attn_gain[0], mlp_gain[0], q_gain[0], k_gain[0]]).astype(jnp.float32)
    gains = jnp.pad(gains, (0, 1024 - gains.shape[0])).reshape(8, 128)
    labels = trade(segment_ids)[0]
    order = jnp.stack(
        [
            ((core + core_step) % 2) * places + (place + step) % places
            for core_step in range(2)
            for step in range(places)
        ]
    )
    row_index = (order[:, None] * own_rows + jnp.arange(own_rows, dtype=jnp.int32)[None, :]).reshape(-1)
    labels = labels.reshape(2 * places, own_rows)[order].reshape(-1)
    cosine, sine, first_row = rotary_tables(labels, row_index)
    qkv_full, o_full, group, gains = enter(
        q_weight[0], key_matrix[0], value_matrix[0], o_weight[0], after(tokens, mid_rows), gains
    )
    mid_near = lax.all_gather(after(mid_rows, group), "d", axis=0, tiled=True)
    down_far = lax.ppermute(after(down_rows, group), "h", shift_perm(2, 1))
    cotangent = trade(after(cotangent, group))
    gains = gains.reshape(gains.shape[0], -1)
    attn_scale = gains[:, :cut].reshape(-1)
    mlp_scale = gains[:, cut : 2 * cut].reshape(-1)
    q_scale = gains[:, 2 * cut : 2 * cut + head_cut].reshape(-1)
    k_scale = gains[:, 2 * cut + head_cut : 2 * cut + 2 * head_cut].reshape(-1)

    stream = group[:own_rows]
    normed = rms_scale(group.astype(jnp.float32), attn_scale).astype(jnp.bfloat16)
    head_count, kv_heads = q_cols // HEAD_WIDTH, kv_cols // HEAD_WIDTH
    qkv = jnp.dot(normed, qkv_full, preferred_element_type=jnp.float32)
    tables = (cosine, sine, as_row(q_scale), as_row(k_scale), first_row)
    query_reduced, key_reduced, value_reduced, attended, totals = attention(
        qkv, tables, order, head_count, kv_heads
    )
    down_far = lax.all_gather(after(down_far, attended), "d", axis=0, tiled=True)

    def whole(values):
        return jax.ShapeDtypeStruct((own_rows, width), values)

    gain_sum = jax.ShapeDtypeStruct((1, width), jnp.float32)
    middle, normed_mid, mid_far = exchange(
        1,
        contract_cols(attended, o_full).astype(jnp.bfloat16),
        (stream, as_row(mlp_scale)),
        (whole(jnp.float32),),
        middle_rows,
        True,
        mid_rows,
    )
    cotangent = after(cotangent, normed_mid)

    gate_near, up_near = split(jnp.dot(normed_mid, mid_near, preferred_element_type=jnp.float32))
    hidden_near = swiglu(gate_near, up_near).astype(jnp.bfloat16)
    gate_far, up_far = split(jnp.dot(normed_mid, mid_far, preferred_element_type=jnp.float32))
    hidden_far = swiglu(gate_far, up_far).astype(jnp.bfloat16)
    branch = contract_cols(hidden_near, down_near) + contract_cols(hidden_far, down_far)
    grad_rows = gather_tokens(cotangent, branch)
    down_grads = sum_over_d(
        jnp.concatenate(
            [
                contract_rows(grad_rows, hidden_near).astype(jnp.bfloat16),
                contract_rows(grad_rows, hidden_far).astype(jnp.bfloat16),
            ],
            axis=1,
        )
    )

    def hidden_pull(gate, up, down):
        hidden_grad = jnp.dot(grad_rows, down, preferred_element_type=jnp.float32)
        _, pull_back = jax.vjp(swiglu, gate, up)
        gate_grad, up_grad = pull_back(hidden_grad)
        return jnp.concatenate(
            [gate_grad.astype(jnp.bfloat16), up_grad.astype(jnp.bfloat16)], axis=1
        )

    mid_back_near = hidden_pull(gate_near, up_near, down_near)
    mid_back_far = hidden_pull(gate_far, up_far, down_far)
    mid_grad_far = contract_rows(normed_mid, mid_back_far).astype(jnp.bfloat16)
    mid_sum_far = sum_over_d(mid_grad_far)
    normed_grad = (contract_cols(mid_back_near, mid_near) + contract_cols(mid_back_far, mid_far)).astype(
        jnp.bfloat16
    )
    gradient, mlp_gain_grad, grad_rows = exchange(
        2,
        after(normed_grad, mid_grad_far),
        (middle, cotangent, as_row(mlp_scale)),
        (whole(jnp.float32), gain_sum),
        middle_pull_rows,
        True,
    )
    mid_grad_near = contract_rows(normed_mid, after(mid_back_near, grad_rows)).astype(jnp.bfloat16)
    mid_sum_near = sum_over_d(mid_grad_near)

    grad_rows = after(grad_rows, mid_grad_near)
    out_grad = jnp.dot(grad_rows, o_full, preferred_element_type=jnp.float32).astype(jnp.bfloat16)
    o_wgrad = contract_rows(grad_rows, attended)
    query_back, key_back, value_back, q_gain_grad, k_gain_grad = attention_pull(
        qkv,
        tables,
        order,
        (query_reduced, key_reduced, value_reduced, totals),
        out_grad,
        head_count,
        kv_heads,
    )
    qkv_back = jnp.concatenate([query_back, key_back, value_back], axis=1)
    mid_sum_far = after(mid_sum_far, query_back)
    branch = scatter_tokens(branch, query_back)
    activations = trade((middle + branch).astype(jnp.bfloat16))
    qkv_grad = contract_rows(normed, qkv_back).astype(jnp.bfloat16)
    attn_grad = scatter_weights(
        after(jnp.concatenate([qkv_grad, o_wgrad.astype(jnp.bfloat16)], axis=1), mid_sum_far)
    )
    gradient, moved, attn_gain_grad = exchange(
        3,
        contract_cols(after(qkv_back, qkv_grad), qkv_full).astype(jnp.bfloat16),
        (stream, gradient, as_row(attn_scale)),
        (whole(jnp.float32), whole(jnp.bfloat16), gain_sum),
        stream_pull_rows,
        False,
    )
    moved = trade(moved)
    gradient = jnp.where(core == lax.axis_index("h"), gradient, moved.astype(jnp.float32))

    split_at = down_rows.shape[1]
    down_grad = columns_of(*return_halves(down_grads[:, :split_at], down_grads[:, split_at:]))
    mine, other = return_halves(mid_sum_near, mid_sum_far)
    gate_grad = columns_of(mine[:, :half_cols], other[:, :half_cols])
    up_grad = columns_of(mine[:, half_cols:], other[:, half_cols:])

    sums = lax.psum(
        jnp.concatenate([attn_gain_grad[0], mlp_gain_grad[0], q_gain_grad[0], k_gain_grad[0]]),
        ("d", "c", "h", "l"),
    )
    row = lax.axis_index("d") * 2 + core

    def owned(start, whole, part):
        return lax.dynamic_slice(sums[start : start + whole], (row * part,), (part,))[None]

    return (
        activations,
        gradient,
        owned(0, width, cut),
        attn_grad[None, :, :q_cols],
        attn_grad[None, :, q_cols : q_cols + kv_cols],
        attn_grad[None, :, q_cols + kv_cols : q_cols + 2 * kv_cols],
        attn_grad[None, :, q_cols + 2 * kv_cols :],
        owned(2 * width, HEAD_WIDTH, head_cut),
        owned(2 * width + HEAD_WIDTH, HEAD_WIDTH, head_cut),
        owned(width, width, cut),
        gate_grad[None],
        up_grad[None],
        down_grad[None],
    )


def solution(mesh):
    dp, tensor = mesh.shape["dp"], mesh.shape["tensor"]
    cut = Mesh(mesh.devices.reshape(dp // 2, 2, 2, tensor // 2), ("d", "c", "h", "l"))
    rows, cols = ("d", "c"), ("h", "l")
    tokens, labels = P(rows + cols, None), P(rows, None)
    gain, weight = P(None, rows), P(None, rows, cols)
    return jax.shard_map(
        per_device,
        mesh=cut,
        in_specs=(
            tokens,
            labels,
            gain,
            weight,
            weight,
            weight,
            weight,
            gain,
            gain,
            gain,
            weight,
            weight,
            weight,
            tokens,
        ),
        out_specs=(
            tokens,
            tokens,
            gain,
            weight,
            weight,
            weight,
            weight,
            gain,
            gain,
            gain,
            weight,
            weight,
            weight,
        ),
        check_vma=False,
    )
```

```python
import functools

import jax
import jax.numpy as jnp
from jax import lax
from jax.experimental import pallas as pl
from jax.experimental.pallas import tpu as pltpu
from jax.sharding import Mesh
from jax.sharding import PartitionSpec as P


HEAD_WIDTH = 128
NSEQ = 3


EPS = 1e-06
THETA = 1000000.0


def rms_scale(values, gain):
    return values * lax.rsqrt(jnp.mean(values * values, axis=-1, keepdims=True) + EPS) * gain


def swiglu(gate_raw, up_raw):
    return jax.nn.silu(gate_raw) * up_raw


def rotary_tables(sequence_labels, row_index):
    labels = jnp.arange(NSEQ, dtype=jnp.int32)
    starts = jnp.sum((sequence_labels[None, :] < labels[:, None]).astype(jnp.int32), axis=1)
    first_row = jnp.sum(
        jnp.where(sequence_labels[:, None] == labels[None, :], starts[None, :], 0), axis=1
    )
    position = (row_index - first_row).astype(jnp.float32)
    frequency = THETA ** (-(jnp.arange(HEAD_WIDTH // 2, dtype=jnp.float32) * (2.0 / HEAD_WIDTH)))
    angles = position[:, None] * frequency[None, :]
    sine = jnp.sin(angles)
    cosine = jnp.cos(angles)
    return (
        jnp.concatenate([cosine, cosine], axis=1),
        jnp.concatenate([-sine, sine], axis=1),
        first_row[:, None],
    )


def contract_rows(left, right):
    return lax.dot_general(
        left, right, (((0,), (0,)), ((), ())), preferred_element_type=jnp.float32
    )


def contract_cols(left, right):
    return lax.dot_general(
        left, right, (((1,), (1,)), ((), ())), preferred_element_type=jnp.float32
    )


MESH = pl.DeviceIdType.MESH
CHUNKS = 3


def remote(source, target, send_sem, recv_sem, **place):
    return pltpu.make_async_remote_copy(
        src_ref=source,
        dst_ref=target,
        send_sem=send_sem,
        recv_sem=recv_sem,
        device_id=place,
        device_id_type=MESH,
    )


def rows_at(index, size):
    return pl.ds(pl.multiple_of(index * size, size), size)


def hop_plan(nd, d):
    if nd == 4:
        side_x = d + 1 - 2 * lax.rem(d, 2)
        side_y = d + 2 - 4 * (d // 2)
        corner = side_x + side_y - d
        hops = (
            (0, d, side_x),
            (1, d, side_x),
            (0, d, side_y),
            (1, d, side_y),
            (0, side_x, side_y),
            (1, side_y, side_x),
        )
        sources = ((0, side_x), (1, side_x), (0, side_y), (1, side_y), (0, corner), (1, corner))
        return hops, sources, 4, ((0, 4), (3, 5))
    steps = [(part, step) for step in range(1, nd) for part in range(2)]
    hops = tuple((part, d, lax.rem(d + step, nd)) for part, step in steps)
    sources = tuple((part, lax.rem(d + nd - step, nd)) for part, step in steps)
    return hops, sources, len(hops), ()


def hop_count(nd):
    return 6 if nd == 4 else 2 * (nd - 1)


class Spread:
    def __init__(self, nd, d, block, send_sem, recv_sem):
        self.hops, self.sources, self.first, self.relayed = hop_plan(nd, d)
        self.block, self.send_sem, self.recv_sem = block, send_sem, recv_sem

    def copy(self, j, kind, part, of):
        at = self.block(j, of * 2 + part)
        return remote(
            at, at, self.send_sem.at[j, kind], self.recv_sem.at[j, kind], d=self.hops[kind][2]
        )

    def hop(self, j, kind):
        return self.copy(j, kind, *self.hops[kind][:2])

    def arrived(self, j, kind):
        return self.copy(j, kind, *self.sources[kind])

    def send(self, j, part):
        for kind in range(self.first):
            if self.hops[kind][0] == part:
                self.hop(j, kind).start()

    def relay(self, j):
        for after_kind, kind in self.relayed:
            self.arrived(j, after_kind).wait_recv()
            self.hop(j, kind).start()

    def finish(self, j):
        handled = {after_kind for after_kind, _ in self.relayed}
        for kind in range(len(self.hops)):
            if kind not in handled:
                self.arrived(j, kind).wait_recv()
            self.hop(j, kind).wait_send()


def entry_kernel(nd, tl, *refs):
    (q_ref, k_ref, v_ref, o_ref, tok_ref, gain_ref) = refs[:6]
    (qkv_full, o_full, tok_full, gain_full) = refs[6:10]
    (stage, tok_stage) = refs[10:12]
    (zs, zr, cs, li, lo, xs, xr, ts, tr, tli, tlo, ls, lr, fs, fr, gs, gr, gl) = refs[12:]
    d, c, h, l = (lax.axis_index(name) for name in ("d", "c", "h", "l"))
    same = c == h
    apart = c != h
    rows = q_ref.shape[0]
    own = tok_ref.shape[0]
    chunk = own // CHUNKS
    q_cols, kv_cols = q_ref.shape[1], k_ref.shape[1]
    weights = (
        (q_ref, qkv_full, 0, 0),
        (k_ref, qkv_full, q_cols, q_cols),
        (v_ref, qkv_full, q_cols + kv_cols, q_cols + kv_cols),
        (o_ref, o_full, 0, q_cols + 2 * kv_cols),
    )

    def block(j, row):
        source, full, start, _ = weights[j]
        return full.at[rows_at(row, rows), pl.ds(start, source.shape[1])]

    def held(j):
        source, _, _, start = weights[j]
        return stage.at[:, pl.ds(start, source.shape[1])]

    def from_far(j, part):
        return remote(block(j, d * 2 + part), block(j, d * 2 + part), zs.at[j], zr.at[j, part], h=1 - h)

    def to_far(j):
        return remote(weights[j][0], block(j, d * 2 + c), zs.at[j], zr.at[j, c], c=h, h=1 - h)

    def to_core(j):
        return remote(weights[j][0], block(j, d * 2 + c), cs.at[j], zr.at[j, c], c=h)

    def local_in(j):
        return pltpu.make_async_copy(weights[j][0], held(j), li.at[j])

    def local_out(j):
        return pltpu.make_async_copy(held(j), block(j, d * 2 + c), lo.at[j])

    def tokens_at(index, k):
        return tok_full.at[pl.ds(index * own + k * chunk, chunk)]

    def trade_tokens(k):
        return remote(tok_ref.at[pl.ds(k * chunk, chunk)], tokens_at(0, k), ts.at[k], tr.at[k], c=h, h=c)

    def along(step, k):
        return remote(
            tokens_at(0, k),
            tokens_at(tl - step, k),
            ls.at[(step - 1) * CHUNKS + k],
            lr.at[(tl - step - 1) * CHUNKS + k],
            l=lax.rem(l + step, tl),
        )

    def from_along(index, k):
        return remote(
            tokens_at(index, k),
            tokens_at(index, k),
            ls.at[(index - 1) * CHUNKS + k],
            lr.at[(index - 1) * CHUNKS + k],
            l=l,
        )

    def across(index, k):
        at = index * CHUNKS + k
        return remote(tokens_at(index, k), tokens_at(tl + index, k), fs.at[at], fr.at[at], c=1 - c)

    def gain_peer(step):
        place = lax.rem(d * 2 + c + step, 2 * nd)
        return place // 2, lax.rem(place, 2)

    def gains_to(step):
        to_d, to_c = gain_peer(step)
        return remote(
            gain_ref, gain_full.at[d * 2 + c], gs.at[step - 1], gr.at[2 * nd - step - 1], d=to_d, c=to_c
        )

    def gains_from(step):
        from_d, from_c = gain_peer(step)
        return remote(
            gain_ref, gain_full.at[from_d * 2 + from_c], gs.at[step - 1], gr.at[step - 1], d=from_d, c=from_c
        )

    def local_gains():
        return pltpu.make_async_copy(gain_ref, gain_full.at[d * 2 + c], gl)

    local_gains().start()

    @pl.when(apart)
    def _():
        for k in range(CHUNKS):
            trade_tokens(k).start()

    for j in range(4):
        to_far(j).start()

        @pl.when(apart)
        def _():
            to_core(j).start()

    @pl.when(same)
    def _():
        pltpu.make_async_copy(tok_ref, tok_stage, tli).start()
        for j in range(4):
            local_in(j).start()
        pltpu.make_async_copy(tok_ref, tok_stage, tli).wait()
        for k in range(CHUNKS):
            part = pl.ds(k * chunk, chunk)
            pltpu.make_async_copy(tok_stage.at[part], tokens_at(0, k), tlo.at[k]).start()
        for j in range(4):
            local_in(j).wait()
            local_out(j).start()

    for step in range(1, 2 * nd):
        gains_to(step).start()

    over_d = Spread(nd, d, block, xs, xr)

    def spread(j):
        for part in range(2):
            here = jnp.logical_and(same, c == part)

            @pl.when(here)
            def _():
                local_out(j).wait()

            @pl.when(jnp.logical_not(here))
            def _():
                from_far(j, part).wait_recv()

            over_d.send(j, part)

    relay = over_d.relay
    for k in range(CHUNKS):

        @pl.when(same)
        def _():
            part = pl.ds(k * chunk, chunk)
            pltpu.make_async_copy(tok_stage.at[part], tokens_at(0, k), tlo.at[k]).wait()

        @pl.when(apart)
        def _():
            remote(tokens_at(0, k), tokens_at(0, k), ts.at[k], tr.at[k], c=1 - c, h=1 - h).wait_recv()

        for step in range(1, tl):
            along(step, k).start()
        across(0, k).start()
    spread(0)
    spread(1)
    relay(0)
    spread(2)
    relay(1)
    for k in range(CHUNKS):
        for index in range(1, tl):
            from_along(index, k).wait_recv()
            across(index, k).start()
    relay(2)
    spread(3)
    relay(3)

    for j in range(4):
        over_d.finish(j)
        to_far(j).wait_send()
    for k in range(CHUNKS):
        for index in range(tl):
            across(index, k).wait()
        for step in range(1, tl):
            along(step, k).wait_send()
    for step in range(1, 2 * nd):
        gains_from(step).wait_recv()
        gains_to(step).wait_send()
    local_gains().wait()

    @pl.when(apart)
    def _():
        for j in range(4):
            to_core(j).wait_send()
        for k in range(CHUNKS):
            trade_tokens(k).wait_send()


def enter(q_weight, key_matrix, value_matrix, o_weight, tokens, gains):
    nd, tl = lax.axis_size("d"), lax.axis_size("l")
    rows, q_cols = q_weight.shape
    kv_cols = key_matrix.shape[1]
    own, width = tokens.shape
    hops = hop_count(nd)
    dma = pltpu.SemaphoreType.DMA
    return pl.pallas_call(
        functools.partial(entry_kernel, nd, tl),
        name="entry",
        out_shape=(
            jax.ShapeDtypeStruct((width, q_cols + 2 * kv_cols), jnp.bfloat16),
            jax.ShapeDtypeStruct((width, o_weight.shape[1]), jnp.bfloat16),
            jax.ShapeDtypeStruct((2 * tl * own, width), jnp.bfloat16),
            jax.ShapeDtypeStruct((2 * nd,) + gains.shape, jnp.float32),
        ),
        in_specs=[pl.BlockSpec(memory_space=pl.ANY)] * 6,
        out_specs=[pl.BlockSpec(memory_space=pl.ANY)] * 4,
        scratch_shapes=[
            pltpu.VMEM((rows, q_cols + 2 * kv_cols + o_weight.shape[1]), jnp.bfloat16),
            pltpu.VMEM((own, width), jnp.bfloat16),
            dma((4,)),
            dma((4, 2)),
            dma((4,)),
            dma((4,)),
            dma((4,)),
            dma((4, hops)),
            dma((4, hops)),
            dma((CHUNKS,)),
            dma((CHUNKS,)),
            dma,
            dma((CHUNKS,)),
            dma(((tl - 1) * CHUNKS,)),
            dma(((tl - 1) * CHUNKS,)),
            dma((tl * CHUNKS,)),
            dma((tl * CHUNKS,)),
            dma((2 * nd - 1,)),
            dma((2 * nd - 1,)),
            dma,
        ],
        compiler_params=pltpu.CompilerParams(has_side_effects=True),
        cost_estimate=pl.CostEstimate(flops=0, bytes_accessed=250_000_000, transcendentals=0),
    )(q_weight, key_matrix, value_matrix, o_weight, tokens, gains)


PIECES = 6


def exchange_kernel(nd, tl, epilogue, aux_count, out_count, gather, carry_weights, *refs):
    partial = refs[0]
    aux = refs[1 : 1 + aux_count]
    refs = refs[1 + aux_count :]
    if carry_weights:
        weight_rows, refs = refs[0], refs[1:]
    outs = refs[:out_count]
    rest = refs[out_count:]
    if gather:
        full, rest = rest[0], rest[1:]
    if carry_weights:
        weights, ws, wr, xs, xr, rest = rest[0], *rest[1:5], rest[5:]
    if gather:
        finished, ls, lr, fs, fr, keep, rest = rest[0], *rest[1:6], rest[6:]
    mine, other, sums, arrivals, cs, cr, loc, ss, sr = rest
    c, l = lax.axis_index("c"), lax.axis_index("l")
    d, h = lax.axis_index("d"), lax.axis_index("h")
    own = arrivals.shape[0] // (tl - 1)
    chunk = own // CHUNKS

    barrier = pltpu.get_barrier_semaphore()
    pl.semaphore_signal(barrier, inc=1, device_id={"c": 1 - c}, device_id_type=MESH)
    for step in range(1, tl):
        pl.semaphore_signal(
            barrier, inc=1, device_id={"l": lax.rem(l + step, tl)}, device_id_type=MESH
        )
    partners = tl
    if carry_weights:
        pl.semaphore_signal(barrier, inc=1, device_id={"h": 1 - h}, device_id_type=MESH)
        partners += 1
        for step in range(1, nd):
            pl.semaphore_signal(
                barrier, inc=1, device_id={"d": lax.rem(d + step, nd)}, device_id_type=MESH
            )
        partners += nd - 1
    pl.semaphore_wait(barrier, partners)

    def part(base, k):
        return rows_at(base * CHUNKS + k, chunk)

    def to_core(index, k):
        at = index * CHUNKS + k
        return remote(
            partial.at[part(tl + index, k)], other.at[part(index, k)], cs.at[at], cr.at[at], c=1 - c
        )

    def local(index, k):
        return pltpu.make_async_copy(
            partial.at[part(index, k)], mine.at[part(index, k)], loc.at[index * CHUNKS + k]
        )

    def along(step, k):
        at = (step - 1) * CHUNKS + k
        return remote(
            sums.at[part(step - 1, k)],
            arrivals.at[part(step - 1, k)],
            ss.at[at],
            sr.at[at],
            l=lax.rem(l + step, tl),
        )

    if carry_weights:
        half = weight_rows.shape[0] // 2
        piece = weight_rows.shape[1] // PIECES

        def block(j, row):
            return weights.at[rows_at(row, half), pl.ds(j * piece, piece)]

        def from_far(j, row_part):
            return remote(
                weight_rows.at[pl.ds(row_part * half, half), pl.ds(j * piece, piece)],
                block(j, d * 2 + row_part),
                ws.at[j, row_part],
                wr.at[j, row_part],
                h=1 - h,
            )

        over_d = Spread(nd, d, block, xs, xr)

        def spread(j):
            for row_part in range(2):
                from_far(j, row_part).wait_recv()
                over_d.send(j, row_part)

    order = list(range(1, tl)) + [0]
    for index in order:
        for k in range(CHUNKS):
            to_core(index, k).start()
            local(index, k).start()

    def both(index, k):
        local(index, k).wait()
        to_core(index, k).wait_recv()
        at = part(index, k)
        return mine[at, :].astype(jnp.float32) + other[at, :].astype(jnp.float32)

    for step in range(1, tl):

        def pass_on(k, carry):
            sums[part(step - 1, k), :] = both(step, k).astype(jnp.bfloat16)
            along(step, k).start()
            return carry

        lax.fori_loop(0, CHUNKS, pass_on, 0)

    if carry_weights:
        for j in range(PIECES):
            for row_part in range(2):
                from_far(j, row_part).start()

    def gathered(index, k):
        return full.at[part(index, k)]

    def keep_own(k):
        return pltpu.make_async_copy(finished.at[part(0, k)], gathered(0, k), keep.at[k])

    def own_along(step, k):
        return remote(
            finished.at[part(0, k)],
            gathered(tl - step, k),
            ls.at[(step - 1) * CHUNKS + k],
            lr.at[(tl - step - 1) * CHUNKS + k],
            l=lax.rem(l + step, tl),
        )

    def from_along(index, k):
        at = (index - 1) * CHUNKS + k
        return remote(gathered(index, k), gathered(index, k), ls.at[at], lr.at[at], l=l)

    def across(index, k):
        source = finished.at[part(0, k)] if index == 0 else gathered(index, k)
        at = index * CHUNKS + k
        return remote(source, gathered(tl + index, k), fs.at[at], fr.at[at], c=1 - c)

    def finish(k, carry):
        total = both(0, k)
        for step in range(1, tl):
            along(step, k).wait_recv()
            total = total + arrivals[part(step - 1, k), :].astype(jnp.float32)
        row = epilogue(total, part(0, k), k, aux, outs)
        if gather:
            finished[part(0, k), :] = row
            keep_own(k).start()
            for step in range(1, tl):
                own_along(step, k).start()
            across(0, k).start()
        return carry

    if carry_weights:
        for k in range(CHUNKS):
            finish(k, 0)
        for j in range(PIECES // 2):
            spread(j)
            if j:
                over_d.relay(j - 1)
    else:
        lax.fori_loop(0, CHUNKS, finish, 0)
    if gather:
        for k in range(CHUNKS):
            for index in range(1, tl):
                from_along(index, k).wait_recv()
                across(index, k).start()
        if carry_weights:
            for j in range(PIECES // 2, PIECES):
                spread(j)
                over_d.relay(j - 1)
            over_d.relay(PIECES - 1)
        for k in range(CHUNKS):
            keep_own(k).wait()
            for index in range(tl):
                across(index, k).wait()
            for step in range(1, tl):
                own_along(step, k).wait_send()
    if carry_weights:
        for j in range(PIECES):
            over_d.finish(j)
            for row_part in range(2):
                from_far(j, row_part).wait_send()
    for k in range(CHUNKS):
        for index in range(tl):
            to_core(index, k).wait_send()
        for step in range(1, tl):
            along(step, k).wait_send()


def exchange(collective_id, partial, aux, outs, epilogue, gather, weight_rows=None):
    nd, tl = lax.axis_size("d"), lax.axis_size("l")
    total, width = partial.shape
    own = total // (2 * tl)
    dma = pltpu.SemaphoreType.DMA
    vmem = pl.BlockSpec(memory_space=pltpu.VMEM)
    anywhere = pl.BlockSpec(memory_space=pl.ANY)
    out_shape = list(outs)
    out_specs = [vmem] * len(outs)
    scratch = []
    given = ()
    if gather:
        out_shape.append(jax.ShapeDtypeStruct((total, width), jnp.bfloat16))
        out_specs.append(anywhere)
    if weight_rows is not None:
        given = (weight_rows,)
        rows, cols = weight_rows.shape
        out_shape.append(jax.ShapeDtypeStruct((nd * rows, cols), jnp.bfloat16))
        out_specs.append(anywhere)
        scratch += [
            dma((PIECES, 2)),
            dma((PIECES, 2)),
            dma((PIECES, hop_count(nd))),
            dma((PIECES, hop_count(nd))),
        ]
    if gather:
        scratch += [
            pltpu.VMEM((own, width), jnp.bfloat16),
            dma(((tl - 1) * CHUNKS,)),
            dma(((tl - 1) * CHUNKS,)),
            dma((tl * CHUNKS,)),
            dma((tl * CHUNKS,)),
            dma((CHUNKS,)),
        ]
    scratch += [
        pltpu.VMEM((tl * own, width), jnp.bfloat16),
        pltpu.VMEM((tl * own, width), jnp.bfloat16),
        pltpu.VMEM(((tl - 1) * own, width), jnp.bfloat16),
        pltpu.VMEM(((tl - 1) * own, width), jnp.bfloat16),
        dma((tl * CHUNKS,)),
        dma((tl * CHUNKS,)),
        dma((tl * CHUNKS,)),
        dma(((tl - 1) * CHUNKS,)),
        dma(((tl - 1) * CHUNKS,)),
    ]
    return pl.pallas_call(
        functools.partial(
            exchange_kernel, nd, tl, epilogue, len(aux), len(outs), gather, bool(given)
        ),
        out_shape=tuple(out_shape),
        in_specs=[anywhere] + [vmem] * len(aux) + [anywhere] * len(given),
        out_specs=out_specs,
        scratch_shapes=scratch,
        compiler_params=pltpu.CompilerParams(
            has_side_effects=True, collective_id=collective_id, vmem_limit_bytes=40 << 20
        ),
        cost_estimate=pl.CostEstimate(
            flops=0, bytes_accessed=200_000_000 if gather else 110_000_000, transcendentals=0
        ),
    )(partial, *aux, *given)


def middle_rows(total, rows, k, aux, outs):
    stream, gain = aux
    value = stream[rows, :].astype(jnp.float32) + total
    outs[0][rows, :] = value
    return rms_scale(value, gain[...]).astype(jnp.bfloat16)


def norm_pull(value, gain, grad):
    scale = lax.rsqrt(jnp.mean(value * value, axis=-1, keepdims=True) + EPS)
    scaled = grad * gain
    inner = jnp.mean(value * scaled, axis=-1, keepdims=True)
    return scale * scaled - value * (scale * scale * scale * inner), jnp.sum(
        grad * value * scale, axis=0, keepdims=True
    )


def add_rows(out, value, k):
    @pl.when(k == 0)
    def _():
        out[...] = value

    @pl.when(k > 0)
    def _():
        out[...] += value


def middle_pull_rows(total, rows, k, aux, outs):
    middle, cotangent, gain = aux
    pulled, gain_part = norm_pull(middle[rows, :], gain[...], total)
    value = cotangent[rows, :].astype(jnp.float32) + pulled
    outs[0][rows, :] = value
    add_rows(outs[1], gain_part, k)
    return value.astype(jnp.bfloat16)


def stream_pull_rows(total, rows, k, aux, outs):
    stream, gradient, gain = aux
    pulled, gain_part = norm_pull(stream[rows, :].astype(jnp.float32), gain[...], total)
    value = gradient[rows, :] + pulled
    outs[0][rows, :] = value
    outs[1][rows, :] = value.astype(jnp.bfloat16)
    add_rows(outs[2], gain_part, k)
    return None


def key_tile(rows):
    return next(size for size in (384, 256, 128) if rows % size == 0)


def turn(values):
    return pltpu.roll(values, HEAD_WIDTH // 2, 1)


def head_norm(values):
    return lax.rsqrt(jnp.mean(values * values, axis=-1, keepdims=True) + EPS)


def tile_mask(first, start, tile, row0, rows):
    keys = start + lax.broadcasted_iota(jnp.int32, (rows, tile), 1)
    last = row0 + lax.broadcasted_iota(jnp.int32, (rows, tile), 0)
    return jnp.logical_and(keys >= first, keys <= last)


def dot_last(left, right):
    return lax.dot_general(
        left, right, (((1,), (1,)), ((), ())), preferred_element_type=jnp.float32
    )


def attention_kernel(blocks, repeat, order_ref, *refs):
    q, k, v, cosine, sine, q_gain, k_gain, first = refs[:8]
    qr, kr, vb, out, total = refs[8:13]
    acc, den = refs[13:]
    rows = q.shape[0] // blocks
    tile = key_tile(q.shape[0])
    scale = HEAD_WIDTH**-0.5

    def rotated(values, gain, at):
        scaled = values * head_norm(values) * gain
        return (scaled * cosine[at, :] + turn(scaled) * sine[at, :]).astype(jnp.bfloat16)

    def prepare(i, carry):
        at, to = rows_at(i, rows), rows_at(order_ref[i], rows)
        for r in range(repeat):
            head = slice(r * HEAD_WIDTH, (r + 1) * HEAD_WIDTH)
            qr[at, head] = rotated(q[at, head], q_gain[...], at)
        kr[to, :] = rotated(k[at, :], k_gain[...], at)
        vb[to, :] = v[at, :].astype(jnp.bfloat16)
        return carry

    lax.fori_loop(0, blocks, prepare, 0)

    def attend(i, carry):
        at = rows_at(i, rows)
        row0 = order_ref[i] * rows
        acc[...] = jnp.zeros_like(acc)
        den[...] = jnp.zeros_like(den)

        def over_keys(t, inner):
            keys = rows_at(t, tile)
            mask = tile_mask(first[at, :], t * tile, tile, row0, rows)
            for r in range(repeat):
                head = slice(r * HEAD_WIDTH, (r + 1) * HEAD_WIDTH)
                scores = dot_last(qr[at, head], kr[keys, :]) * scale
                weights = jnp.where(mask, jnp.exp(scores), 0.0)
                den[r] += jnp.sum(weights, axis=-1, keepdims=True)
                acc[r] += jnp.dot(
                    weights.astype(jnp.bfloat16), vb[keys, :], preferred_element_type=jnp.float32
                )
            return inner

        lax.fori_loop(0, (row0 + rows + tile - 1) // tile, over_keys, 0)
        for r in range(repeat):
            head = slice(r * HEAD_WIDTH, (r + 1) * HEAD_WIDTH)
            out[at, head] = (acc[r] / den[r]).astype(jnp.bfloat16)
            total[at, r : r + 1] = den[r]
        return carry

    lax.fori_loop(0, blocks, attend, 0)


def attention_specs(rows, q_heads, kv_heads):
    repeat = q_heads // kv_heads

    def columns(width, start=0):
        return pl.BlockSpec((rows, width * HEAD_WIDTH), lambda g, order: (0, start // width + g))

    def fixed(*shape):
        return pl.BlockSpec(shape, lambda g, order: (0, 0))

    raw = [columns(repeat), columns(1, q_heads), columns(1, q_heads + kv_heads)]
    tables = [
        fixed(rows, HEAD_WIDTH),
        fixed(rows, HEAD_WIDTH),
        fixed(1, HEAD_WIDTH),
        fixed(1, HEAD_WIDTH),
        fixed(rows, 1),
    ]
    return repeat, columns, fixed, raw, tables


def attention(qkv, tables, order, q_heads, kv_heads):
    rows = qkv.shape[0]
    blocks = order.shape[0]
    repeat, columns, _, raw, table_specs = attention_specs(rows, q_heads, kv_heads)
    wide, narrow = q_heads * HEAD_WIDTH, kv_heads * HEAD_WIDTH
    return pl.pallas_call(
        functools.partial(attention_kernel, blocks, repeat),
        name="attention",
        out_shape=(
            jax.ShapeDtypeStruct((rows, wide), jnp.bfloat16),
            jax.ShapeDtypeStruct((rows, narrow), jnp.bfloat16),
            jax.ShapeDtypeStruct((rows, narrow), jnp.bfloat16),
            jax.ShapeDtypeStruct((rows, wide), jnp.bfloat16),
            jax.ShapeDtypeStruct((rows, narrow), jnp.float32),
        ),
        grid_spec=pltpu.PrefetchScalarGridSpec(
            num_scalar_prefetch=1,
            grid=(kv_heads,),
            in_specs=raw + table_specs,
            out_specs=[columns(repeat), columns(1), columns(1), columns(repeat), columns(1)],
            scratch_shapes=[
                pltpu.VMEM((repeat, rows // blocks, HEAD_WIDTH), jnp.float32),
                pltpu.VMEM((repeat, rows // blocks, 1), jnp.float32),
            ],
        ),
        compiler_params=pltpu.CompilerParams(vmem_limit_bytes=50 << 20),
        cost_estimate=pl.CostEstimate(
            flops=4 * rows * rows * wide, bytes_accessed=60_000_000, transcendentals=0
        ),
    )(order, qkv, qkv, qkv, *tables)


def attention_pull_kernel(blocks, repeat, order_ref, *refs):
    q, k, cosine, sine, q_gain, k_gain, first, qr, kr, vb, total, grad = refs[:12]
    dq, dk, dv, dq_gain, dk_gain = refs[12:17]
    shares, share_grads, dq_acc, dk_acc, dv_acc, inner_sum = refs[17:]
    rows = q.shape[0] // blocks
    tile = key_tile(q.shape[0])
    scale = HEAD_WIDTH**-0.5
    dk_acc[...] = jnp.zeros_like(dk_acc)
    dv_acc[...] = jnp.zeros_like(dv_acc)

    @pl.when(pl.program_id(0) == 0)
    def _():
        dq_gain[...] = jnp.zeros_like(dq_gain)
        dk_gain[...] = jnp.zeros_like(dk_gain)

    def pull(raw, gain, turned_grad, at, gain_out):
        scaled_grad = turned_grad * cosine[at, :] + turn(turned_grad * sine[at, :])
        r = head_norm(raw)
        gain_out[0:1, :] += jnp.sum(scaled_grad * raw * r, axis=0, keepdims=True)
        scaled = scaled_grad * gain
        inner = jnp.mean(raw * scaled, axis=-1, keepdims=True)
        return (r * scaled - raw * (r * r * r * inner)).astype(jnp.bfloat16)

    def over_rows(i, carry):
        at = rows_at(i, rows)
        row0 = order_ref[i] * rows
        tiles = (row0 + rows + tile - 1) // tile
        dq_acc[...] = jnp.zeros_like(dq_acc)
        inner_sum[...] = jnp.zeros_like(inner_sum)

        def first_pass(t, inner):
            keys = rows_at(t, tile)
            mask = tile_mask(first[at, :], t * tile, tile, row0, rows)
            for r in range(repeat):
                head = slice(r * HEAD_WIDTH, (r + 1) * HEAD_WIDTH)
                scores = dot_last(qr[at, head], kr[keys, :]) * scale
                share = jnp.where(mask, jnp.exp(scores), 0.0) * (1.0 / total[at, r : r + 1])
                share_grad = dot_last(grad[at, head], vb[keys, :])
                inner_sum[r] += jnp.sum(share * share_grad, axis=-1, keepdims=True)
                shares[t, r] = share
                share_grads[t, r] = share_grad
            return inner

        lax.fori_loop(0, tiles, first_pass, 0)

        def second_pass(t, inner):
            keys = rows_at(t, tile)
            for r in range(repeat):
                head = slice(r * HEAD_WIDTH, (r + 1) * HEAD_WIDTH)
                share = shares[t, r]
                score_grad = (share * (share_grads[t, r] - inner_sum[r])).astype(jnp.bfloat16)
                dq_acc[r] += jnp.dot(score_grad, kr[keys, :], preferred_element_type=jnp.float32)
                dk_acc[keys, :] += contract_rows(score_grad, qr[at, head])
                dv_acc[keys, :] += contract_rows(share.astype(jnp.bfloat16), grad[at, head])
            return inner

        lax.fori_loop(0, tiles, second_pass, 0)
        for r in range(repeat):
            head = slice(r * HEAD_WIDTH, (r + 1) * HEAD_WIDTH)
            dq[at, head] = pull(q[at, head], q_gain[...], dq_acc[r] * scale, at, dq_gain)
        return carry

    lax.fori_loop(0, blocks, over_rows, 0)

    def finish(i, carry):
        at, to = rows_at(i, rows), rows_at(order_ref[i], rows)
        dk[at, :] = pull(k[at, :], k_gain[...], dk_acc[to, :] * scale, at, dk_gain)
        dv[at, :] = dv_acc[to, :].astype(jnp.bfloat16)
        return carry

    lax.fori_loop(0, blocks, finish, 0)


def attention_pull(qkv, tables, order, kept, grad, q_heads, kv_heads):
    rows = qkv.shape[0]
    blocks = order.shape[0]
    repeat, columns, fixed, raw, table_specs = attention_specs(rows, q_heads, kv_heads)
    wide, narrow = q_heads * HEAD_WIDTH, kv_heads * HEAD_WIDTH
    own, tile = rows // blocks, key_tile(rows)
    return pl.pallas_call(
        functools.partial(attention_pull_kernel, blocks, repeat),
        name="attention_pull",
        out_shape=(
            jax.ShapeDtypeStruct((rows, wide), jnp.bfloat16),
            jax.ShapeDtypeStruct((rows, narrow), jnp.bfloat16),
            jax.ShapeDtypeStruct((rows, narrow), jnp.bfloat16),
            jax.ShapeDtypeStruct((8, HEAD_WIDTH), jnp.float32),
            jax.ShapeDtypeStruct((8, HEAD_WIDTH), jnp.float32),
        ),
        grid_spec=pltpu.PrefetchScalarGridSpec(
            num_scalar_prefetch=1,
            grid=(kv_heads,),
            in_specs=raw[:2]
            + table_specs
            + [columns(repeat), columns(1), columns(1), columns(1), columns(repeat)],
            out_specs=[
                columns(repeat),
                columns(1),
                columns(1),
                fixed(8, HEAD_WIDTH),
                fixed(8, HEAD_WIDTH),
            ],
            scratch_shapes=[
                pltpu.VMEM((rows // tile, repeat, own, tile), jnp.float32),
                pltpu.VMEM((rows // tile, repeat, own, tile), jnp.float32),
                pltpu.VMEM((repeat, own, HEAD_WIDTH), jnp.float32),
                pltpu.VMEM((rows, HEAD_WIDTH), jnp.float32),
                pltpu.VMEM((rows, HEAD_WIDTH), jnp.float32),
                pltpu.VMEM((repeat, own, 1), jnp.float32),
            ],
        ),
        compiler_params=pltpu.CompilerParams(vmem_limit_bytes=56 << 20),
        cost_estimate=pl.CostEstimate(
            flops=10 * rows * rows * wide, bytes_accessed=120_000_000, transcendentals=0
        ),
    )(order, qkv, qkv, *tables, *kept, grad)


def shift_perm(size, step):
    return [((place + step) % size, place) for place in range(size)]


def trade(values):
    return lax.ppermute(values, ("c", "h"), [(0, 0), (1, 2), (2, 1), (3, 3)])


def gather_tokens(own, *first):
    places = lax.axis_size("l")
    moved = [lax.ppermute(own, "l", shift_perm(places, step)) for step in range(1, places)]
    parts = [own] + [after(part, *first) for part in moved]
    half = jnp.concatenate(parts, axis=0)
    return jnp.concatenate([half, lax.ppermute(half, "c", shift_perm(2, 1))], axis=0)


def scatter_tokens(partial, *first):
    places = lax.axis_size("l")
    half = partial.shape[0] // 2
    rows = half // places
    other = lax.ppermute(partial[half:].astype(jnp.bfloat16), "c", shift_perm(2, 1))
    total = partial[:half] + other.astype(jnp.float32)
    own = total[:rows]
    for step in range(1, places):
        sent = total[step * rows : (step + 1) * rows].astype(jnp.bfloat16)
        moved = lax.ppermute(sent, "l", shift_perm(places, -step))
        moved = after(moved, *first)
        own = own + moved.astype(jnp.float32)
    return own


def after(value, *others):
    return lax.optimization_barrier((value,) + others)[0]


def core_halves(shard):
    core = lax.axis_index("c")
    half = shard.shape[-1] // 2
    first, second = shard[..., :half], shard[..., half:]
    mine = jnp.where(core == 0, first, second)
    other = lax.ppermute(jnp.where(core == 0, second, first), "c", shift_perm(2, 1))
    both = jnp.where(core == 0, jnp.stack([mine, other]), jnp.stack([other, mine]))
    return jnp.moveaxis(both, 0, -3).reshape(shard.shape[:-2] + (2 * shard.shape[-2], half))


def return_halves(near, far):
    core = lax.axis_index("c")
    far = lax.ppermute(far, "h", shift_perm(2, 1))
    sums = near.astype(jnp.float32) + far.astype(jnp.float32)
    rows = sums.shape[0] // 2
    first, second = sums[:rows], sums[rows:]
    mine = jnp.where(core == 0, first, second)
    sent = jnp.where(core == 0, second, first).astype(jnp.bfloat16)
    other = lax.ppermute(sent, "c", shift_perm(2, 1)).astype(jnp.float32)
    return mine, other


def columns_of(mine, other):
    core = lax.axis_index("c")
    return jnp.concatenate(
        [jnp.where(core == 0, mine, other), jnp.where(core == 0, other, mine)], axis=1
    )


def sum_over_d(partial):
    return lax.psum_scatter(partial.astype(jnp.bfloat16), "d", scatter_dimension=0, tiled=True)


def as_row(values):
    return values.reshape(1, -1)


def split(values):
    half = values.shape[1] // 2
    return values[:, :half], values[:, half:]


def scatter_weights(partial):
    core, upper = lax.axis_index("c"), lax.axis_index("h")
    rows = sum_over_d(partial)
    half = rows.shape[0] // 2
    first, second = rows[:half], rows[half:]
    mine = jnp.where(core == 0, first, second)
    other = lax.ppermute(jnp.where(core == 0, second, first), "c", shift_perm(2, 1))
    same = core == upper
    far = lax.ppermute(jnp.where(same, other, mine), "h", shift_perm(2, 1))
    return jnp.where(same, mine, other).astype(jnp.float32) + far.astype(jnp.float32)


def per_device(
    tokens,
    segment_ids,
    attn_gain,
    q_weight,
    key_matrix,
    value_matrix,
    o_weight,
    q_gain,
    k_gain,
    mlp_gain,
    gate_weight,
    up_weight,
    down_weight,
    cotangent,
):
    width = attn_gain.shape[1] * lax.axis_size("d") * 2
    own_rows = tokens.shape[0]
    places = lax.axis_size("l")
    core, place = lax.axis_index("c"), lax.axis_index("l")
    q_cols, kv_cols, ff_cols = q_weight.shape[2], key_matrix.shape[2], gate_weight.shape[2]
    half_cols = ff_cols // 2

    gate_half = core_halves(gate_weight[0])
    up_half = core_halves(up_weight[0])
    mid_rows = jnp.concatenate([gate_half, up_half], axis=1)
    down_rows = core_halves(down_weight[0])
    down_near = lax.all_gather(down_rows, "d", axis=0, tiled=True)

    cut = attn_gain.shape[1]
    head_cut = q_gain.shape[1]
    gains = jnp.concatenate([attn_gain[0], mlp_gain[0], q_gain[0], k_gain[0]]).astype(jnp.float32)
    gains = jnp.pad(gains, (0, 1024 - gains.shape[0])).reshape(8, 128)
    labels = trade(segment_ids)[0]
    order = jnp.stack(
        [
            ((core + core_step) % 2) * places + (place + step) % places
            for core_step in range(2)
            for step in range(places)
        ]
    )
    row_index = (order[:, None] * own_rows + jnp.arange(own_rows, dtype=jnp.int32)[None, :]).reshape(-1)
    labels = labels.reshape(2 * places, own_rows)[order].reshape(-1)
    cosine, sine, first_row = rotary_tables(labels, row_index)
    qkv_full, o_full, group, gains = enter(
        q_weight[0], key_matrix[0], value_matrix[0], o_weight[0], after(tokens, mid_rows), gains
    )
    mid_near = lax.all_gather(after(mid_rows, group), "d", axis=0, tiled=True)
    down_far = lax.ppermute(after(down_rows, group), "h", shift_perm(2, 1))
    cotangent = trade(after(cotangent, group))
    gains = gains.reshape(gains.shape[0], -1)
    attn_scale = gains[:, :cut].reshape(-1)
    mlp_scale = gains[:, cut : 2 * cut].reshape(-1)
    q_scale = gains[:, 2 * cut : 2 * cut + head_cut].reshape(-1)
    k_scale = gains[:, 2 * cut + head_cut : 2 * cut + 2 * head_cut].reshape(-1)

    stream = group[:own_rows]
    normed = rms_scale(group.astype(jnp.float32), attn_scale).astype(jnp.bfloat16)
    head_count, kv_heads = q_cols // HEAD_WIDTH, kv_cols // HEAD_WIDTH
    qkv = jnp.dot(normed, qkv_full, preferred_element_type=jnp.float32)
    tables = (cosine, sine, as_row(q_scale), as_row(k_scale), first_row)
    query_reduced, key_reduced, value_reduced, attended, totals = attention(
        qkv, tables, order, head_count, kv_heads
    )
    down_far = lax.all_gather(after(down_far, attended), "d", axis=0, tiled=True)

    def whole(values):
        return jax.ShapeDtypeStruct((own_rows, width), values)

    gain_sum = jax.ShapeDtypeStruct((1, width), jnp.float32)
    middle, normed_mid, mid_far = exchange(
        1,
        contract_cols(attended, o_full).astype(jnp.bfloat16),
        (stream, as_row(mlp_scale)),
        (whole(jnp.float32),),
        middle_rows,
        True,
        mid_rows,
    )
    cotangent = after(cotangent, normed_mid)

    mid = jnp.dot(normed_mid, mid_near, preferred_element_type=jnp.float32)
    gate_near, up_near = split(mid)
    hidden_near = swiglu(gate_near, up_near).astype(jnp.bfloat16)
    mid = jnp.dot(normed_mid, mid_far, preferred_element_type=jnp.float32)
    gate_far, up_far = split(mid)
    hidden_far = swiglu(gate_far, up_far).astype(jnp.bfloat16)
    grad_rows = gather_tokens(cotangent, hidden_near, hidden_far)
    down_partial = jnp.concatenate(
        [
            contract_rows(grad_rows, hidden_near).astype(jnp.bfloat16),
            contract_rows(grad_rows, hidden_far).astype(jnp.bfloat16),
        ],
        axis=1,
    )
    down_grads = sum_over_d(down_partial)
    grad_rows = after(grad_rows, down_partial)

    def hidden_pull(gate, up, down):
        hidden_grad = jnp.dot(grad_rows, down, preferred_element_type=jnp.float32)
        _, pull_back = jax.vjp(swiglu, gate, up)
        gate_grad, up_grad = pull_back(hidden_grad)
        return jnp.concatenate(
            [gate_grad.astype(jnp.bfloat16), up_grad.astype(jnp.bfloat16)], axis=1
        )

    mid_back_near = hidden_pull(gate_near, up_near, down_near)
    mid_back_far = hidden_pull(gate_far, up_far, down_far)
    mid_grad_far = contract_rows(normed_mid, mid_back_far).astype(jnp.bfloat16)
    mid_sum_far = sum_over_d(mid_grad_far)
    normed_grad = (contract_cols(mid_back_near, mid_near) + contract_cols(mid_back_far, mid_far)).astype(
        jnp.bfloat16
    )
    gradient, mlp_gain_grad, grad_rows = exchange(
        2,
        after(normed_grad, mid_grad_far),
        (middle, cotangent, as_row(mlp_scale)),
        (whole(jnp.float32), gain_sum),
        middle_pull_rows,
        True,
    )
    mid_grad_near = contract_rows(normed_mid, after(mid_back_near, grad_rows)).astype(jnp.bfloat16)
    mid_sum_near = sum_over_d(mid_grad_near)

    grad_rows = after(grad_rows, mid_grad_near)
    out_grad = jnp.dot(grad_rows, o_full, preferred_element_type=jnp.float32).astype(jnp.bfloat16)
    o_wgrad = contract_rows(grad_rows, attended)
    query_back, key_back, value_back, q_gain_grad, k_gain_grad = attention_pull(
        qkv,
        tables,
        order,
        (query_reduced, key_reduced, value_reduced, totals),
        out_grad,
        head_count,
        kv_heads,
    )
    qkv_back = jnp.concatenate([query_back, key_back, value_back], axis=1)
    qkv_grad = contract_rows(normed, qkv_back).astype(jnp.bfloat16)
    attn_grad = scatter_weights(
        after(jnp.concatenate([qkv_grad, o_wgrad.astype(jnp.bfloat16)], axis=1), mid_sum_far)
    )
    gradient, moved, attn_gain_grad = exchange(
        3,
        contract_cols(after(qkv_back, qkv_grad), qkv_full).astype(jnp.bfloat16),
        (stream, gradient, as_row(attn_scale)),
        (whole(jnp.float32), whole(jnp.bfloat16), gain_sum),
        stream_pull_rows,
        False,
    )
    moved = trade(moved)
    gradient = jnp.where(core == lax.axis_index("h"), gradient, moved.astype(jnp.float32))

    hidden_near = after(hidden_near, attn_gain_grad)
    branch = scatter_tokens(
        contract_cols(hidden_near, down_near) + contract_cols(hidden_far, down_far)
    )
    activations = trade((middle + branch).astype(jnp.bfloat16))

    split_at = down_rows.shape[1]
    down_grad = columns_of(*return_halves(down_grads[:, :split_at], down_grads[:, split_at:]))
    mine, other = return_halves(mid_sum_near, mid_sum_far)
    gate_grad = columns_of(mine[:, :half_cols], other[:, :half_cols])
    up_grad = columns_of(mine[:, half_cols:], other[:, half_cols:])

    sums = lax.psum(
        jnp.concatenate([attn_gain_grad[0], mlp_gain_grad[0], q_gain_grad[0], k_gain_grad[0]]),
        ("d", "c", "h", "l"),
    )
    row = lax.axis_index("d") * 2 + core

    def owned(start, whole, part):
        return lax.dynamic_slice(sums[start : start + whole], (row * part,), (part,))[None]

    return (
        activations,
        gradient,
        owned(0, width, cut),
        attn_grad[None, :, :q_cols],
        attn_grad[None, :, q_cols : q_cols + kv_cols],
        attn_grad[None, :, q_cols + kv_cols : q_cols + 2 * kv_cols],
        attn_grad[None, :, q_cols + 2 * kv_cols :],
        owned(2 * width, HEAD_WIDTH, head_cut),
        owned(2 * width + HEAD_WIDTH, HEAD_WIDTH, head_cut),
        owned(width, width, cut),
        gate_grad[None],
        up_grad[None],
        down_grad[None],
    )


def solution(mesh):
    dp, tensor = mesh.shape["dp"], mesh.shape["tensor"]
    cut = Mesh(mesh.devices.reshape(dp // 2, 2, 2, tensor // 2), ("d", "c", "h", "l"))
    rows, cols = ("d", "c"), ("h", "l")
    tokens, labels = P(rows + cols, None), P(rows, None)
    gain, weight = P(None, rows), P(None, rows, cols)
    return jax.shard_map(
        per_device,
        mesh=cut,
        in_specs=(
            tokens,
            labels,
            gain,
            weight,
            weight,
            weight,
            weight,
            gain,
            gain,
            gain,
            weight,
            weight,
            weight,
            tokens,
        ),
        out_specs=(
            tokens,
            tokens,
            gain,
            weight,
            weight,
            weight,
            weight,
            gain,
            gain,
            gain,
            weight,
            weight,
            weight,
        ),
        check_vma=False,
    )
```

```python
import functools

import jax
import jax.numpy as jnp
from jax import lax
from jax.experimental import pallas as pl
from jax.experimental.pallas import tpu as pltpu
from jax.sharding import Mesh
from jax.sharding import PartitionSpec as P


HEAD_WIDTH = 128
NSEQ = 3


EPS = 1e-06
THETA = 1000000.0


def rms_scale(values, gain):
    return values * lax.rsqrt(jnp.mean(values * values, axis=-1, keepdims=True) + EPS) * gain


def swiglu(gate_raw, up_raw):
    return jax.nn.silu(gate_raw) * up_raw


def rotary_tables(sequence_labels, row_index):
    labels = jnp.arange(NSEQ, dtype=jnp.int32)
    starts = jnp.sum((sequence_labels[None, :] < labels[:, None]).astype(jnp.int32), axis=1)
    first_row = jnp.sum(
        jnp.where(sequence_labels[:, None] == labels[None, :], starts[None, :], 0), axis=1
    )
    position = (row_index - first_row).astype(jnp.float32)
    frequency = THETA ** (-(jnp.arange(HEAD_WIDTH // 2, dtype=jnp.float32) * (2.0 / HEAD_WIDTH)))
    angles = position[:, None] * frequency[None, :]
    sine = jnp.sin(angles)
    cosine = jnp.cos(angles)
    return (
        jnp.concatenate([cosine, cosine], axis=1),
        jnp.concatenate([-sine, sine], axis=1),
        first_row[:, None],
    )


def contract_rows(left, right):
    return lax.dot_general(
        left, right, (((0,), (0,)), ((), ())), preferred_element_type=jnp.float32
    )


def contract_cols(left, right):
    return lax.dot_general(
        left, right, (((1,), (1,)), ((), ())), preferred_element_type=jnp.float32
    )


MESH = pl.DeviceIdType.MESH
CHUNKS = 3


def remote(source, target, send_sem, recv_sem, **place):
    return pltpu.make_async_remote_copy(
        src_ref=source,
        dst_ref=target,
        send_sem=send_sem,
        recv_sem=recv_sem,
        device_id=place,
        device_id_type=MESH,
    )


def rows_at(index, size):
    return pl.ds(pl.multiple_of(index * size, size), size)


WEIGHTS = 5
ENTRY_START = (
    "w0", "t0", "w1", "w2", "t1", "w3", "w4", "t2",
)
ENTRY_ORDER = (
    "s0", "t0", "s1", "r0", "s2", "r1", "t1", "s3", "r2", "s4", "r3", "t2", "r4", "a0", "a1",
    "a2",
)


def hop_plan(nd, d):
    if nd == 4:
        side_x = d + 1 - 2 * lax.rem(d, 2)
        side_y = d + 2 - 4 * (d // 2)
        corner = side_x + side_y - d
        hops = (
            (0, d, side_x),
            (1, d, side_x),
            (0, d, side_y),
            (1, d, side_y),
            (0, side_x, side_y),
            (1, side_y, side_x),
        )
        sources = ((0, side_x), (1, side_x), (0, side_y), (1, side_y), (0, corner), (1, corner))
        return hops, sources, 4, ((0, 4), (3, 5))
    steps = [(part, step) for step in range(1, nd) for part in range(2)]
    hops = tuple((part, d, lax.rem(d + step, nd)) for part, step in steps)
    sources = tuple((part, lax.rem(d + nd - step, nd)) for part, step in steps)
    return hops, sources, len(hops), ()


def hop_count(nd):
    return 6 if nd == 4 else 2 * (nd - 1)


class Spread:
    def __init__(self, nd, d, block, send_sem, recv_sem):
        self.hops, self.sources, self.first, self.relayed = hop_plan(nd, d)
        self.block, self.send_sem, self.recv_sem = block, send_sem, recv_sem

    def copy(self, j, kind, part, of):
        at = self.block(j, of * 2 + part)
        return remote(
            at, at, self.send_sem.at[j, kind], self.recv_sem.at[j, kind], d=self.hops[kind][2]
        )

    def hop(self, j, kind):
        return self.copy(j, kind, *self.hops[kind][:2])

    def arrived(self, j, kind):
        return self.copy(j, kind, *self.sources[kind])

    def send(self, j, part):
        for kind in range(self.first):
            if self.hops[kind][0] == part:
                self.hop(j, kind).start()

    def relay(self, j):
        for after_kind, kind in self.relayed:
            self.arrived(j, after_kind).wait_recv()
            self.hop(j, kind).start()

    def finish(self, j):
        handled = {after_kind for after_kind, _ in self.relayed}
        for kind in range(len(self.hops)):
            if kind not in handled:
                self.arrived(j, kind).wait_recv()
            self.hop(j, kind).wait_send()


def entry_kernel(nd, tl, *refs):
    (q_ref, k_ref, v_ref, o_ref, tok_ref, gain_ref) = refs[:6]
    (qkv_full, o_full, tok_full, gain_full) = refs[6:10]
    (stage, tok_stage) = refs[10:12]
    (zs, zr, cs, li, lo, xs, xr, ts, tr, tli, tlo, ls, lr, fs, fr, gs, gr, gl) = refs[12:]
    d, c, h, l = (lax.axis_index(name) for name in ("d", "c", "h", "l"))
    same = c == h
    apart = c != h
    rows = q_ref.shape[0]
    own = tok_ref.shape[0]
    chunk = own // CHUNKS
    q_cols, kv_cols = q_ref.shape[1], k_ref.shape[1]
    o_half = o_ref.shape[1] // 2
    qkv_cols = q_cols + 2 * kv_cols
    weights = (
        (q_ref, qkv_full, 0, q_cols, 0),
        (k_ref, qkv_full, q_cols, kv_cols, q_cols),
        (v_ref, qkv_full, q_cols + kv_cols, kv_cols, q_cols + kv_cols),
        (o_ref.at[:, pl.ds(0, o_half)], o_full, 0, o_half, qkv_cols),
        (o_ref.at[:, pl.ds(o_half, o_half)], o_full, o_half, o_half, qkv_cols + o_half),
    )

    def block(j, row):
        _, full, start, cols, _ = weights[j]
        return full.at[rows_at(row, rows), pl.ds(start, cols)]

    def held(j):
        _, _, _, cols, start = weights[j]
        return stage.at[:, pl.ds(start, cols)]

    def from_far(j, part):
        return remote(block(j, d * 2 + part), block(j, d * 2 + part), zs.at[j], zr.at[j, part], h=1 - h)

    def to_far(j):
        return remote(weights[j][0], block(j, d * 2 + c), zs.at[j], zr.at[j, c], c=h, h=1 - h)

    def to_core(j):
        return remote(weights[j][0], block(j, d * 2 + c), cs.at[j], zr.at[j, c], c=h)

    def local_in(j):
        return pltpu.make_async_copy(weights[j][0], held(j), li.at[j])

    def local_out(j):
        return pltpu.make_async_copy(held(j), block(j, d * 2 + c), lo.at[j])

    def tokens_at(index, k):
        return tok_full.at[pl.ds(index * own + k * chunk, chunk)]

    def trade_tokens(k):
        return remote(tok_ref.at[pl.ds(k * chunk, chunk)], tokens_at(0, k), ts.at[k], tr.at[k], c=h, h=c)

    def along(step, k):
        return remote(
            tokens_at(0, k),
            tokens_at(tl - step, k),
            ls.at[(step - 1) * CHUNKS + k],
            lr.at[(tl - step - 1) * CHUNKS + k],
            l=lax.rem(l + step, tl),
        )

    def from_along(index, k):
        return remote(
            tokens_at(index, k),
            tokens_at(index, k),
            ls.at[(index - 1) * CHUNKS + k],
            lr.at[(index - 1) * CHUNKS + k],
            l=l,
        )

    def across(index, k):
        at = index * CHUNKS + k
        return remote(tokens_at(index, k), tokens_at(tl + index, k), fs.at[at], fr.at[at], c=1 - c)

    def gain_peer(step):
        place = lax.rem(d * 2 + c + step, 2 * nd)
        return place // 2, lax.rem(place, 2)

    def gains_to(step):
        to_d, to_c = gain_peer(step)
        return remote(
            gain_ref, gain_full.at[d * 2 + c], gs.at[step - 1], gr.at[2 * nd - step - 1], d=to_d, c=to_c
        )

    def gains_from(step):
        from_d, from_c = gain_peer(step)
        return remote(
            gain_ref, gain_full.at[from_d * 2 + from_c], gs.at[step - 1], gr.at[step - 1], d=from_d, c=from_c
        )

    def local_gains():
        return pltpu.make_async_copy(gain_ref, gain_full.at[d * 2 + c], gl)

    local_gains().start()

    def start_weights(j):
        to_far(j).start()

        @pl.when(apart)
        def _():
            to_core(j).start()

    def start_tokens(k):
        @pl.when(apart)
        def _():
            trade_tokens(k).start()

    for step in ENTRY_START:
        {"w": start_weights, "t": start_tokens}[step[0]](int(step[1:]))

    @pl.when(same)
    def _():
        pltpu.make_async_copy(tok_ref, tok_stage, tli).start()
        for j in range(WEIGHTS):
            local_in(j).start()
        pltpu.make_async_copy(tok_ref, tok_stage, tli).wait()
        for k in range(CHUNKS):
            part = pl.ds(k * chunk, chunk)
            pltpu.make_async_copy(tok_stage.at[part], tokens_at(0, k), tlo.at[k]).start()
        for j in range(WEIGHTS):
            local_in(j).wait()
            local_out(j).start()

    for step in range(1, 2 * nd):
        gains_to(step).start()

    over_d = Spread(nd, d, block, xs, xr)

    def spread(j):
        for part in range(2):
            here = jnp.logical_and(same, c == part)

            @pl.when(here)
            def _():
                local_out(j).wait()

            @pl.when(jnp.logical_not(here))
            def _():
                from_far(j, part).wait_recv()

            over_d.send(j, part)

    relay = over_d.relay

    def own_tokens(k):
        @pl.when(same)
        def _():
            part = pl.ds(k * chunk, chunk)
            pltpu.make_async_copy(tok_stage.at[part], tokens_at(0, k), tlo.at[k]).wait()

        @pl.when(apart)
        def _():
            remote(tokens_at(0, k), tokens_at(0, k), ts.at[k], tr.at[k], c=1 - c, h=1 - h).wait_recv()

        for step in range(1, tl):
            along(step, k).start()
        across(0, k).start()

    def pass_across(k):
        for index in range(1, tl):
            from_along(index, k).wait_recv()
            across(index, k).start()

    steps = {"t": own_tokens, "s": spread, "r": relay, "a": pass_across}
    for step in ENTRY_ORDER:
        steps[step[0]](int(step[1:]))

    for j in range(WEIGHTS):
        over_d.finish(j)
        to_far(j).wait_send()
    for k in range(CHUNKS):
        for index in range(tl):
            across(index, k).wait()
        for step in range(1, tl):
            along(step, k).wait_send()
    for step in range(1, 2 * nd):
        gains_from(step).wait_recv()
        gains_to(step).wait_send()
    local_gains().wait()

    @pl.when(apart)
    def _():
        for j in range(WEIGHTS):
            to_core(j).wait_send()
        for k in range(CHUNKS):
            trade_tokens(k).wait_send()


def enter(q_weight, key_matrix, value_matrix, o_weight, tokens, gains):
    nd, tl = lax.axis_size("d"), lax.axis_size("l")
    rows, q_cols = q_weight.shape
    kv_cols = key_matrix.shape[1]
    own, width = tokens.shape
    hops = hop_count(nd)
    dma = pltpu.SemaphoreType.DMA
    return pl.pallas_call(
        functools.partial(entry_kernel, nd, tl),
        name="entry",
        out_shape=(
            jax.ShapeDtypeStruct((width, q_cols + 2 * kv_cols), jnp.bfloat16),
            jax.ShapeDtypeStruct((width, o_weight.shape[1]), jnp.bfloat16),
            jax.ShapeDtypeStruct((2 * tl * own, width), jnp.bfloat16),
            jax.ShapeDtypeStruct((2 * nd,) + gains.shape, jnp.float32),
        ),
        in_specs=[pl.BlockSpec(memory_space=pl.ANY)] * 6,
        out_specs=[pl.BlockSpec(memory_space=pl.ANY)] * 4,
        scratch_shapes=[
            pltpu.VMEM((rows, q_cols + 2 * kv_cols + o_weight.shape[1]), jnp.bfloat16),
            pltpu.VMEM((own, width), jnp.bfloat16),
            dma((WEIGHTS,)),
            dma((WEIGHTS, 2)),
            dma((WEIGHTS,)),
            dma((WEIGHTS,)),
            dma((WEIGHTS,)),
            dma((WEIGHTS, hops)),
            dma((WEIGHTS, hops)),
            dma((CHUNKS,)),
            dma((CHUNKS,)),
            dma,
            dma((CHUNKS,)),
            dma(((tl - 1) * CHUNKS,)),
            dma(((tl - 1) * CHUNKS,)),
            dma((tl * CHUNKS,)),
            dma((tl * CHUNKS,)),
            dma((2 * nd - 1,)),
            dma((2 * nd - 1,)),
            dma,
        ],
        compiler_params=pltpu.CompilerParams(has_side_effects=True),
        cost_estimate=pl.CostEstimate(flops=0, bytes_accessed=250_000_000, transcendentals=0),
    )(q_weight, key_matrix, value_matrix, o_weight, tokens, gains)


PIECES = 6
SUM_ORDER = (
    "s0", "f0", "s1", "r0", "f1", "s2", "r1", "f2", "s3", "r2", "s4", "r3", "s5", "r4", "r5",
    "a0", "a1", "a2",
)


def exchange_kernel(nd, tl, epilogue, aux_count, out_count, gather, carry_weights, *refs):
    partial = refs[0]
    aux = refs[1 : 1 + aux_count]
    refs = refs[1 + aux_count :]
    if carry_weights:
        weight_rows, refs = refs[0], refs[1:]
    outs = refs[:out_count]
    rest = refs[out_count:]
    if gather:
        full, rest = rest[0], rest[1:]
    if carry_weights:
        weights, ws, wr, xs, xr, rest = rest[0], *rest[1:5], rest[5:]
    if gather:
        finished, ls, lr, fs, fr, keep, rest = rest[0], *rest[1:6], rest[6:]
    mine, other, sums, arrivals, cs, cr, loc, ss, sr = rest
    c, l = lax.axis_index("c"), lax.axis_index("l")
    d, h = lax.axis_index("d"), lax.axis_index("h")
    own = arrivals.shape[0] // (tl - 1)
    chunk = own // CHUNKS

    barrier = pltpu.get_barrier_semaphore()
    pl.semaphore_signal(barrier, inc=1, device_id={"c": 1 - c}, device_id_type=MESH)
    for step in range(1, tl):
        pl.semaphore_signal(
            barrier, inc=1, device_id={"l": lax.rem(l + step, tl)}, device_id_type=MESH
        )
    partners = tl
    if carry_weights:
        pl.semaphore_signal(barrier, inc=1, device_id={"h": 1 - h}, device_id_type=MESH)
        partners += 1
        for step in range(1, nd):
            pl.semaphore_signal(
                barrier, inc=1, device_id={"d": lax.rem(d + step, nd)}, device_id_type=MESH
            )
        partners += nd - 1
    pl.semaphore_wait(barrier, partners)

    def part(base, k):
        return rows_at(base * CHUNKS + k, chunk)

    def to_core(index, k):
        at = index * CHUNKS + k
        return remote(
            partial.at[part(tl + index, k)], other.at[part(index, k)], cs.at[at], cr.at[at], c=1 - c
        )

    def local(index, k):
        return pltpu.make_async_copy(
            partial.at[part(index, k)], mine.at[part(index, k)], loc.at[index * CHUNKS + k]
        )

    def along(step, k):
        at = (step - 1) * CHUNKS + k
        return remote(
            sums.at[part(step - 1, k)],
            arrivals.at[part(step - 1, k)],
            ss.at[at],
            sr.at[at],
            l=lax.rem(l + step, tl),
        )

    if carry_weights:
        half = weight_rows.shape[0] // 2
        piece = weight_rows.shape[1] // PIECES

        def block(j, row):
            return weights.at[rows_at(row, half), pl.ds(j * piece, piece)]

        def from_far(j, row_part):
            return remote(
                weight_rows.at[pl.ds(row_part * half, half), pl.ds(j * piece, piece)],
                block(j, d * 2 + row_part),
                ws.at[j, row_part],
                wr.at[j, row_part],
                h=1 - h,
            )

        over_d = Spread(nd, d, block, xs, xr)

        def spread(j):
            for row_part in range(2):
                from_far(j, row_part).wait_recv()
                over_d.send(j, row_part)

        for j in range(PIECES):
            for row_part in range(2):
                from_far(j, row_part).start()

    order = list(range(1, tl)) + [0]
    for index in order:
        for k in range(CHUNKS):
            to_core(index, k).start()
            local(index, k).start()

    def both(index, k):
        local(index, k).wait()
        to_core(index, k).wait_recv()
        at = part(index, k)
        return mine[at, :].astype(jnp.float32) + other[at, :].astype(jnp.float32)

    for step in range(1, tl):

        def pass_on(k, carry):
            sums[part(step - 1, k), :] = both(step, k).astype(jnp.bfloat16)
            along(step, k).start()
            return carry

        lax.fori_loop(0, CHUNKS, pass_on, 0)

    def gathered(index, k):
        return full.at[part(index, k)]

    def keep_own(k):
        return pltpu.make_async_copy(finished.at[part(0, k)], gathered(0, k), keep.at[k])

    def own_along(step, k):
        return remote(
            finished.at[part(0, k)],
            gathered(tl - step, k),
            ls.at[(step - 1) * CHUNKS + k],
            lr.at[(tl - step - 1) * CHUNKS + k],
            l=lax.rem(l + step, tl),
        )

    def from_along(index, k):
        at = (index - 1) * CHUNKS + k
        return remote(gathered(index, k), gathered(index, k), ls.at[at], lr.at[at], l=l)

    def across(index, k):
        source = finished.at[part(0, k)] if index == 0 else gathered(index, k)
        at = index * CHUNKS + k
        return remote(source, gathered(tl + index, k), fs.at[at], fr.at[at], c=1 - c)

    def finish(k, carry):
        total = both(0, k)
        for step in range(1, tl):
            along(step, k).wait_recv()
            total = total + arrivals[part(step - 1, k), :].astype(jnp.float32)
        row = epilogue(total, part(0, k), k, aux, outs)
        if gather:
            finished[part(0, k), :] = row
            keep_own(k).start()
            for step in range(1, tl):
                own_along(step, k).start()
            across(0, k).start()
        return carry

    def pass_across(k):
        for index in range(1, tl):
            from_along(index, k).wait_recv()
            across(index, k).start()

    if carry_weights:
        steps = {
            "s": spread,
            "r": over_d.relay,
            "f": lambda k: finish(k, 0),
            "a": pass_across,
        }
        for step in SUM_ORDER:
            steps[step[0]](int(step[1:]))
    else:
        lax.fori_loop(0, CHUNKS, finish, 0)
        if gather:
            for k in range(CHUNKS):
                pass_across(k)
    if gather:
        for k in range(CHUNKS):
            keep_own(k).wait()
            for index in range(tl):
                across(index, k).wait()
            for step in range(1, tl):
                own_along(step, k).wait_send()
    if carry_weights:
        for j in range(PIECES):
            over_d.finish(j)
            for row_part in range(2):
                from_far(j, row_part).wait_send()
    for k in range(CHUNKS):
        for index in range(tl):
            to_core(index, k).wait_send()
        for step in range(1, tl):
            along(step, k).wait_send()


def exchange(collective_id, partial, aux, outs, epilogue, gather, weight_rows=None):
    nd, tl = lax.axis_size("d"), lax.axis_size("l")
    total, width = partial.shape
    own = total // (2 * tl)
    dma = pltpu.SemaphoreType.DMA
    vmem = pl.BlockSpec(memory_space=pltpu.VMEM)
    anywhere = pl.BlockSpec(memory_space=pl.ANY)
    out_shape = list(outs)
    out_specs = [vmem] * len(outs)
    scratch = []
    given = ()
    if gather:
        out_shape.append(jax.ShapeDtypeStruct((total, width), jnp.bfloat16))
        out_specs.append(anywhere)
    if weight_rows is not None:
        given = (weight_rows,)
        rows, cols = weight_rows.shape
        out_shape.append(jax.ShapeDtypeStruct((nd * rows, cols), jnp.bfloat16))
        out_specs.append(anywhere)
        scratch += [
            dma((PIECES, 2)),
            dma((PIECES, 2)),
            dma((PIECES, hop_count(nd))),
            dma((PIECES, hop_count(nd))),
        ]
    if gather:
        scratch += [
            pltpu.VMEM((own, width), jnp.bfloat16),
            dma(((tl - 1) * CHUNKS,)),
            dma(((tl - 1) * CHUNKS,)),
            dma((tl * CHUNKS,)),
            dma((tl * CHUNKS,)),
            dma((CHUNKS,)),
        ]
    scratch += [
        pltpu.VMEM((tl * own, width), jnp.bfloat16),
        pltpu.VMEM((tl * own, width), jnp.bfloat16),
        pltpu.VMEM(((tl - 1) * own, width), jnp.bfloat16),
        pltpu.VMEM(((tl - 1) * own, width), jnp.bfloat16),
        dma((tl * CHUNKS,)),
        dma((tl * CHUNKS,)),
        dma((tl * CHUNKS,)),
        dma(((tl - 1) * CHUNKS,)),
        dma(((tl - 1) * CHUNKS,)),
    ]
    return pl.pallas_call(
        functools.partial(
            exchange_kernel, nd, tl, epilogue, len(aux), len(outs), gather, bool(given)
        ),
        out_shape=tuple(out_shape),
        in_specs=[anywhere] + [vmem] * len(aux) + [anywhere] * len(given),
        out_specs=out_specs,
        scratch_shapes=scratch,
        compiler_params=pltpu.CompilerParams(
            has_side_effects=True, collective_id=collective_id, vmem_limit_bytes=40 << 20
        ),
        cost_estimate=pl.CostEstimate(
            flops=0, bytes_accessed=200_000_000 if gather else 110_000_000, transcendentals=0
        ),
    )(partial, *aux, *given)


def gain_kernel(nd, tl, tiles, out, got, send_sem, recv_sem):
    d, c, h, l = (lax.axis_index(name) for name in ("d", "c", "h", "l"))
    count = 4 * nd * tl
    me = ((d * 2 + c) * 2 + h) * tl + l

    def to(step):
        place = lax.rem(me + step, count)
        to_l = lax.rem(place, tl)
        to_h = lax.rem(place // tl, 2)
        row = place // (2 * tl)
        return remote(
            tiles.at[row],
            got.at[step - 1],
            send_sem.at[step - 1],
            recv_sem.at[step - 1],
            d=row // 2,
            c=lax.rem(row, 2),
            h=to_h,
            l=to_l,
        )

    def start(step, carry):
        to(step).start()
        return carry

    def add(step, total):
        to(step).wait_recv()
        return total + got[step - 1]

    def drain(step, carry):
        to(step).wait_send()
        return carry

    lax.fori_loop(1, count, start, 0)
    out[...] = lax.fori_loop(1, count, add, tiles[d * 2 + c])
    lax.fori_loop(1, count, drain, 0)


def gain_total(tiles):
    nd, tl = lax.axis_size("d"), lax.axis_size("l")
    others = 4 * nd * tl - 1
    vmem = pl.BlockSpec(memory_space=pltpu.VMEM)
    return pl.pallas_call(
        functools.partial(gain_kernel, nd, tl),
        name="gain_total",
        out_shape=jax.ShapeDtypeStruct(tiles.shape[1:], jnp.float32),
        in_specs=[vmem],
        out_specs=vmem,
        scratch_shapes=[
            pltpu.VMEM((others,) + tiles.shape[1:], jnp.float32),
            pltpu.SemaphoreType.DMA((others,)),
            pltpu.SemaphoreType.DMA((others,)),
        ],
        compiler_params=pltpu.CompilerParams(has_side_effects=True),
        cost_estimate=pl.CostEstimate(flops=0, bytes_accessed=40_000_000, transcendentals=0),
    )(tiles)


def middle_rows(total, rows, k, aux, outs):
    stream, gain = aux
    value = stream[rows, :].astype(jnp.float32) + total
    outs[0][rows, :] = value
    return rms_scale(value, gain[...]).astype(jnp.bfloat16)


def norm_pull(value, gain, grad):
    scale = lax.rsqrt(jnp.mean(value * value, axis=-1, keepdims=True) + EPS)
    scaled = grad * gain
    inner = jnp.mean(value * scaled, axis=-1, keepdims=True)
    return scale * scaled - value * (scale * scale * scale * inner), jnp.sum(
        grad * value * scale, axis=0, keepdims=True
    )


def add_rows(out, value, k):
    @pl.when(k == 0)
    def _():
        out[...] = value

    @pl.when(k > 0)
    def _():
        out[...] += value


def middle_pull_rows(total, rows, k, aux, outs):
    middle, cotangent, gain = aux
    pulled, gain_part = norm_pull(middle[rows, :], gain[...], total)
    value = cotangent[rows, :].astype(jnp.float32) + pulled
    outs[0][rows, :] = value
    add_rows(outs[1], gain_part, k)
    return value.astype(jnp.bfloat16)


def stream_pull_rows(total, rows, k, aux, outs):
    stream, gradient, gain = aux
    pulled, gain_part = norm_pull(stream[rows, :].astype(jnp.float32), gain[...], total)
    value = gradient[rows, :] + pulled
    outs[0][rows, :] = value
    outs[1][rows, :] = value.astype(jnp.bfloat16)
    add_rows(outs[2], gain_part, k)
    return None


def key_tile(rows):
    return next(size for size in (384, 256, 128) if rows % size == 0)


def turn(values):
    return pltpu.roll(values, HEAD_WIDTH // 2, 1)


def head_norm(values):
    return lax.rsqrt(jnp.mean(values * values, axis=-1, keepdims=True) + EPS)


def tile_mask(first, start, tile, row0, rows):
    keys = start + lax.broadcasted_iota(jnp.int32, (rows, tile), 1)
    last = row0 + lax.broadcasted_iota(jnp.int32, (rows, tile), 0)
    return jnp.logical_and(keys >= first, keys <= last)


def dot_last(left, right):
    return lax.dot_general(
        left, right, (((1,), (1,)), ((), ())), preferred_element_type=jnp.float32
    )


def attention_kernel(blocks, repeat, order_ref, *refs):
    q, k, v, cosine, sine, q_gain, k_gain, first = refs[:8]
    qr, kr, vb, out, total = refs[8:13]
    acc, den = refs[13:]
    rows = q.shape[0] // blocks
    tile = key_tile(q.shape[0])
    scale = HEAD_WIDTH**-0.5

    def rotated(values, gain, at):
        scaled = values * head_norm(values) * gain
        return (scaled * cosine[at, :] + turn(scaled) * sine[at, :]).astype(jnp.bfloat16)

    def prepare(i, carry):
        at, to = rows_at(i, rows), rows_at(order_ref[i], rows)
        for r in range(repeat):
            head = slice(r * HEAD_WIDTH, (r + 1) * HEAD_WIDTH)
            qr[at, head] = rotated(q[at, head], q_gain[...], at)
        kr[to, :] = rotated(k[at, :], k_gain[...], at)
        vb[to, :] = v[at, :].astype(jnp.bfloat16)
        return carry

    lax.fori_loop(0, blocks, prepare, 0)

    def attend(i, carry):
        at = rows_at(i, rows)
        row0 = order_ref[i] * rows
        acc[...] = jnp.zeros_like(acc)
        den[...] = jnp.zeros_like(den)

        def over_keys(t, inner):
            keys = rows_at(t, tile)
            mask = tile_mask(first[at, :], t * tile, tile, row0, rows)
            for r in range(repeat):
                head = slice(r * HEAD_WIDTH, (r + 1) * HEAD_WIDTH)
                scores = dot_last(qr[at, head], kr[keys, :]) * scale
                weights = jnp.where(mask, jnp.exp(scores), 0.0)
                den[r] += jnp.sum(weights, axis=-1, keepdims=True)
                acc[r] += jnp.dot(
                    weights.astype(jnp.bfloat16), vb[keys, :], preferred_element_type=jnp.float32
                )
            return inner

        lax.fori_loop(0, (row0 + rows + tile - 1) // tile, over_keys, 0)
        for r in range(repeat):
            head = slice(r * HEAD_WIDTH, (r + 1) * HEAD_WIDTH)
            out[at, head] = (acc[r] / den[r]).astype(jnp.bfloat16)
            total[at, r : r + 1] = den[r]
        return carry

    lax.fori_loop(0, blocks, attend, 0)


def attention_specs(rows, q_heads, kv_heads):
    repeat = q_heads // kv_heads

    def columns(width, start=0):
        return pl.BlockSpec((rows, width * HEAD_WIDTH), lambda g, order: (0, start // width + g))

    def fixed(*shape):
        return pl.BlockSpec(shape, lambda g, order: (0, 0))

    raw = [columns(repeat), columns(1, q_heads), columns(1, q_heads + kv_heads)]
    tables = [
        fixed(rows, HEAD_WIDTH),
        fixed(rows, HEAD_WIDTH),
        fixed(1, HEAD_WIDTH),
        fixed(1, HEAD_WIDTH),
        fixed(rows, 1),
    ]
    return repeat, columns, fixed, raw, tables


def attention(qkv, tables, order, q_heads, kv_heads):
    rows = qkv.shape[0]
    blocks = order.shape[0]
    repeat, columns, _, raw, table_specs = attention_specs(rows, q_heads, kv_heads)
    wide, narrow = q_heads * HEAD_WIDTH, kv_heads * HEAD_WIDTH
    return pl.pallas_call(
        functools.partial(attention_kernel, blocks, repeat),
        name="attention",
        out_shape=(
            jax.ShapeDtypeStruct((rows, wide), jnp.bfloat16),
            jax.ShapeDtypeStruct((rows, narrow), jnp.bfloat16),
            jax.ShapeDtypeStruct((rows, narrow), jnp.bfloat16),
            jax.ShapeDtypeStruct((rows, wide), jnp.bfloat16),
            jax.ShapeDtypeStruct((rows, narrow), jnp.float32),
        ),
        grid_spec=pltpu.PrefetchScalarGridSpec(
            num_scalar_prefetch=1,
            grid=(kv_heads,),
            in_specs=raw + table_specs,
            out_specs=[columns(repeat), columns(1), columns(1), columns(repeat), columns(1)],
            scratch_shapes=[
                pltpu.VMEM((repeat, rows // blocks, HEAD_WIDTH), jnp.float32),
                pltpu.VMEM((repeat, rows // blocks, 1), jnp.float32),
            ],
        ),
        compiler_params=pltpu.CompilerParams(vmem_limit_bytes=50 << 20),
        cost_estimate=pl.CostEstimate(
            flops=4 * rows * rows * wide, bytes_accessed=60_000_000, transcendentals=0
        ),
    )(order, qkv, qkv, qkv, *tables)


def attention_pull_kernel(blocks, repeat, order_ref, *refs):
    q, k, cosine, sine, q_gain, k_gain, first, qr, kr, vb, total, grad = refs[:12]
    dq, dk, dv, dq_gain, dk_gain = refs[12:17]
    shares, share_grads, dq_acc, dk_acc, dv_acc, inner_sum = refs[17:]
    rows = q.shape[0] // blocks
    tile = key_tile(q.shape[0])
    scale = HEAD_WIDTH**-0.5
    dk_acc[...] = jnp.zeros_like(dk_acc)
    dv_acc[...] = jnp.zeros_like(dv_acc)

    @pl.when(pl.program_id(0) == 0)
    def _():
        dq_gain[...] = jnp.zeros_like(dq_gain)
        dk_gain[...] = jnp.zeros_like(dk_gain)

    def pull(raw, gain, turned_grad, at, gain_out):
        scaled_grad = turned_grad * cosine[at, :] + turn(turned_grad * sine[at, :])
        r = head_norm(raw)
        gain_out[0:1, :] += jnp.sum(scaled_grad * raw * r, axis=0, keepdims=True)
        scaled = scaled_grad * gain
        inner = jnp.mean(raw * scaled, axis=-1, keepdims=True)
        return (r * scaled - raw * (r * r * r * inner)).astype(jnp.bfloat16)

    def over_rows(i, carry):
        at = rows_at(i, rows)
        row0 = order_ref[i] * rows
        tiles = (row0 + rows + tile - 1) // tile
        dq_acc[...] = jnp.zeros_like(dq_acc)
        inner_sum[...] = jnp.zeros_like(inner_sum)

        def first_pass(t, inner):
            keys = rows_at(t, tile)
            mask = tile_mask(first[at, :], t * tile, tile, row0, rows)
            for r in range(repeat):
                head = slice(r * HEAD_WIDTH, (r + 1) * HEAD_WIDTH)
                scores = dot_last(qr[at, head], kr[keys, :]) * scale
                share = jnp.where(mask, jnp.exp(scores), 0.0) * (1.0 / total[at, r : r + 1])
                share_grad = dot_last(grad[at, head], vb[keys, :])
                inner_sum[r] += jnp.sum(share * share_grad, axis=-1, keepdims=True)
                shares[t, r] = share
                share_grads[t, r] = share_grad
            return inner

        lax.fori_loop(0, tiles, first_pass, 0)

        def second_pass(t, inner):
            keys = rows_at(t, tile)
            for r in range(repeat):
                head = slice(r * HEAD_WIDTH, (r + 1) * HEAD_WIDTH)
                share = shares[t, r]
                score_grad = (share * (share_grads[t, r] - inner_sum[r])).astype(jnp.bfloat16)
                dq_acc[r] += jnp.dot(score_grad, kr[keys, :], preferred_element_type=jnp.float32)
                dk_acc[keys, :] += contract_rows(score_grad, qr[at, head])
                dv_acc[keys, :] += contract_rows(share.astype(jnp.bfloat16), grad[at, head])
            return inner

        lax.fori_loop(0, tiles, second_pass, 0)
        for r in range(repeat):
            head = slice(r * HEAD_WIDTH, (r + 1) * HEAD_WIDTH)
            dq[at, head] = pull(q[at, head], q_gain[...], dq_acc[r] * scale, at, dq_gain)
        return carry

    lax.fori_loop(0, blocks, over_rows, 0)

    def finish(i, carry):
        at, to = rows_at(i, rows), rows_at(order_ref[i], rows)
        dk[at, :] = pull(k[at, :], k_gain[...], dk_acc[to, :] * scale, at, dk_gain)
        dv[at, :] = dv_acc[to, :].astype(jnp.bfloat16)
        return carry

    lax.fori_loop(0, blocks, finish, 0)


def attention_pull(qkv, tables, order, kept, grad, q_heads, kv_heads):
    rows = qkv.shape[0]
    blocks = order.shape[0]
    repeat, columns, fixed, raw, table_specs = attention_specs(rows, q_heads, kv_heads)
    wide, narrow = q_heads * HEAD_WIDTH, kv_heads * HEAD_WIDTH
    own, tile = rows // blocks, key_tile(rows)
    return pl.pallas_call(
        functools.partial(attention_pull_kernel, blocks, repeat),
        name="attention_pull",
        out_shape=(
            jax.ShapeDtypeStruct((rows, wide), jnp.bfloat16),
            jax.ShapeDtypeStruct((rows, narrow), jnp.bfloat16),
            jax.ShapeDtypeStruct((rows, narrow), jnp.bfloat16),
            jax.ShapeDtypeStruct((8, HEAD_WIDTH), jnp.float32),
            jax.ShapeDtypeStruct((8, HEAD_WIDTH), jnp.float32),
        ),
        grid_spec=pltpu.PrefetchScalarGridSpec(
            num_scalar_prefetch=1,
            grid=(kv_heads,),
            in_specs=raw[:2]
            + table_specs
            + [columns(repeat), columns(1), columns(1), columns(1), columns(repeat)],
            out_specs=[
                columns(repeat),
                columns(1),
                columns(1),
                fixed(8, HEAD_WIDTH),
                fixed(8, HEAD_WIDTH),
            ],
            scratch_shapes=[
                pltpu.VMEM((rows // tile, repeat, own, tile), jnp.float32),
                pltpu.VMEM((rows // tile, repeat, own, tile), jnp.float32),
                pltpu.VMEM((repeat, own, HEAD_WIDTH), jnp.float32),
                pltpu.VMEM((rows, HEAD_WIDTH), jnp.float32),
                pltpu.VMEM((rows, HEAD_WIDTH), jnp.float32),
                pltpu.VMEM((repeat, own, 1), jnp.float32),
            ],
        ),
        compiler_params=pltpu.CompilerParams(vmem_limit_bytes=56 << 20),
        cost_estimate=pl.CostEstimate(
            flops=10 * rows * rows * wide, bytes_accessed=120_000_000, transcendentals=0
        ),
    )(order, qkv, qkv, *tables, *kept, grad)


def shift_perm(size, step):
    return [((place + step) % size, place) for place in range(size)]


def trade(values):
    return lax.ppermute(values, ("c", "h"), [(0, 0), (1, 2), (2, 1), (3, 3)])


def gather_tokens(own, *first):
    places = lax.axis_size("l")
    moved = [lax.ppermute(own, "l", shift_perm(places, step)) for step in range(1, places)]
    parts = [own] + [after(part, *first) for part in moved]
    half = jnp.concatenate(parts, axis=0)
    return jnp.concatenate([half, lax.ppermute(half, "c", shift_perm(2, 1))], axis=0)


def scatter_tokens(partial, *first):
    places = lax.axis_size("l")
    half = partial.shape[0] // 2
    rows = half // places
    other = lax.ppermute(partial[half:].astype(jnp.bfloat16), "c", shift_perm(2, 1))
    total = partial[:half] + other.astype(jnp.float32)
    own = total[:rows]
    for step in range(1, places):
        sent = total[step * rows : (step + 1) * rows].astype(jnp.bfloat16)
        moved = lax.ppermute(sent, "l", shift_perm(places, -step))
        moved = after(moved, *first)
        own = own + moved.astype(jnp.float32)
    return own


def after(value, *others):
    return lax.optimization_barrier((value,) + others)[0]


def core_halves(shard):
    core = lax.axis_index("c")
    half = shard.shape[-1] // 2
    first, second = shard[..., :half], shard[..., half:]
    mine = jnp.where(core == 0, first, second)
    other = lax.ppermute(jnp.where(core == 0, second, first), "c", shift_perm(2, 1))
    both = jnp.where(core == 0, jnp.stack([mine, other]), jnp.stack([other, mine]))
    return jnp.moveaxis(both, 0, -3).reshape(shard.shape[:-2] + (2 * shard.shape[-2], half))


def return_halves(near, far):
    core = lax.axis_index("c")
    far = lax.ppermute(far, "h", shift_perm(2, 1))
    sums = near.astype(jnp.float32) + far.astype(jnp.float32)
    rows = sums.shape[0] // 2
    first, second = sums[:rows], sums[rows:]
    mine = jnp.where(core == 0, first, second)
    sent = jnp.where(core == 0, second, first).astype(jnp.bfloat16)
    other = lax.ppermute(sent, "c", shift_perm(2, 1)).astype(jnp.float32)
    return mine, other


def columns_of(mine, other):
    core = lax.axis_index("c")
    return jnp.concatenate(
        [jnp.where(core == 0, mine, other), jnp.where(core == 0, other, mine)], axis=1
    )


def sum_over_d(partial):
    return lax.psum_scatter(partial.astype(jnp.bfloat16), "d", scatter_dimension=0, tiled=True)


def as_row(values):
    return values.reshape(1, -1)


def split(values):
    half = values.shape[1] // 2
    return values[:, :half], values[:, half:]


def scatter_weights(partial):
    core, upper = lax.axis_index("c"), lax.axis_index("h")
    rows = sum_over_d(partial)
    half = rows.shape[0] // 2
    first, second = rows[:half], rows[half:]
    mine = jnp.where(core == 0, first, second)
    other = lax.ppermute(jnp.where(core == 0, second, first), "c", shift_perm(2, 1))
    same = core == upper
    far = lax.ppermute(jnp.where(same, other, mine), "h", shift_perm(2, 1))
    return jnp.where(same, mine, other).astype(jnp.float32) + far.astype(jnp.float32)


def per_device(
    tokens,
    segment_ids,
    attn_gain,
    q_weight,
    key_matrix,
    value_matrix,
    o_weight,
    q_gain,
    k_gain,
    mlp_gain,
    gate_weight,
    up_weight,
    down_weight,
    cotangent,
):
    width = attn_gain.shape[1] * lax.axis_size("d") * 2
    own_rows = tokens.shape[0]
    places = lax.axis_size("l")
    core, place = lax.axis_index("c"), lax.axis_index("l")
    q_cols, kv_cols, ff_cols = q_weight.shape[2], key_matrix.shape[2], gate_weight.shape[2]
    half_cols = ff_cols // 2

    gate_half = core_halves(gate_weight[0])
    up_half = core_halves(up_weight[0])
    mid_rows = jnp.concatenate([gate_half, up_half], axis=1)
    down_rows = core_halves(down_weight[0])
    down_near = lax.all_gather(down_rows, "d", axis=0, tiled=True)

    cut = attn_gain.shape[1]
    head_cut = q_gain.shape[1]
    gains = jnp.concatenate([attn_gain[0], mlp_gain[0], q_gain[0], k_gain[0]]).astype(jnp.float32)
    gains = jnp.pad(gains, (0, 1024 - gains.shape[0])).reshape(8, 128)
    labels = trade(segment_ids)[0]
    order = jnp.stack(
        [
            ((core + core_step) % 2) * places + (place + step) % places
            for core_step in range(2)
            for step in range(places)
        ]
    )
    row_index = (order[:, None] * own_rows + jnp.arange(own_rows, dtype=jnp.int32)[None, :]).reshape(-1)
    labels = labels.reshape(2 * places, own_rows)[order].reshape(-1)
    cosine, sine, first_row = rotary_tables(labels, row_index)
    qkv_full, o_full, group, gains = enter(
        q_weight[0], key_matrix[0], value_matrix[0], o_weight[0], after(tokens, mid_rows), gains
    )
    mid_near = lax.all_gather(after(mid_rows, group), "d", axis=0, tiled=True)
    down_far = lax.ppermute(after(down_rows, group), "h", shift_perm(2, 1))
    cotangent = trade(after(cotangent, group))
    gains = gains.reshape(gains.shape[0], -1)
    attn_scale = gains[:, :cut].reshape(-1)
    mlp_scale = gains[:, cut : 2 * cut].reshape(-1)
    q_scale = gains[:, 2 * cut : 2 * cut + head_cut].reshape(-1)
    k_scale = gains[:, 2 * cut + head_cut : 2 * cut + 2 * head_cut].reshape(-1)

    stream = group[:own_rows]
    normed = rms_scale(group.astype(jnp.float32), attn_scale).astype(jnp.bfloat16)
    head_count, kv_heads = q_cols // HEAD_WIDTH, kv_cols // HEAD_WIDTH
    qkv = jnp.dot(normed, qkv_full, preferred_element_type=jnp.float32)
    tables = (cosine, sine, as_row(q_scale), as_row(k_scale), first_row)
    query_reduced, key_reduced, value_reduced, attended, totals = attention(
        qkv, tables, order, head_count, kv_heads
    )
    down_far = lax.all_gather(after(down_far, attended), "d", axis=0, tiled=True)

    def whole(values):
        return jax.ShapeDtypeStruct((own_rows, width), values)

    gain_sum = jax.ShapeDtypeStruct((1, width), jnp.float32)
    middle, normed_mid, mid_far = exchange(
        1,
        contract_cols(attended, o_full).astype(jnp.bfloat16),
        (stream, as_row(mlp_scale)),
        (whole(jnp.float32),),
        middle_rows,
        True,
        mid_rows,
    )
    cotangent = after(cotangent, normed_mid)

    mid = jnp.dot(normed_mid, mid_near, preferred_element_type=jnp.float32)
    gate_near, up_near = split(mid)
    hidden_near = swiglu(gate_near, up_near).astype(jnp.bfloat16)
    mid = jnp.dot(normed_mid, mid_far, preferred_element_type=jnp.float32)
    gate_far, up_far = split(mid)
    hidden_far = swiglu(gate_far, up_far).astype(jnp.bfloat16)
    grad_rows = gather_tokens(cotangent, hidden_near, hidden_far)
    down_partial = jnp.concatenate(
        [
            contract_rows(grad_rows, hidden_near).astype(jnp.bfloat16),
            contract_rows(grad_rows, hidden_far).astype(jnp.bfloat16),
        ],
        axis=1,
    )
    down_grads = sum_over_d(down_partial)
    grad_rows = after(grad_rows, down_partial)

    def hidden_pull(gate, up, down):
        hidden_grad = jnp.dot(grad_rows, down, preferred_element_type=jnp.float32)
        _, pull_back = jax.vjp(swiglu, gate, up)
        gate_grad, up_grad = pull_back(hidden_grad)
        return jnp.concatenate(
            [gate_grad.astype(jnp.bfloat16), up_grad.astype(jnp.bfloat16)], axis=1
        )

    mid_back_near = hidden_pull(gate_near, up_near, down_near)
    mid_back_far = hidden_pull(gate_far, up_far, down_far)
    mid_grad_far = contract_rows(normed_mid, mid_back_far).astype(jnp.bfloat16)
    mid_sum_far = sum_over_d(mid_grad_far)
    normed_grad = (contract_cols(mid_back_near, mid_near) + contract_cols(mid_back_far, mid_far)).astype(
        jnp.bfloat16
    )
    gradient, mlp_gain_grad, grad_rows = exchange(
        2,
        after(normed_grad, mid_grad_far),
        (middle, cotangent, as_row(mlp_scale)),
        (whole(jnp.float32), gain_sum),
        middle_pull_rows,
        True,
    )
    mid_grad_near = contract_rows(normed_mid, after(mid_back_near, grad_rows)).astype(jnp.bfloat16)
    mid_sum_near = sum_over_d(mid_grad_near)

    grad_rows = after(grad_rows, mid_grad_near)
    out_grad = jnp.dot(grad_rows, o_full, preferred_element_type=jnp.float32).astype(jnp.bfloat16)
    o_wgrad = contract_rows(grad_rows, attended)
    query_back, key_back, value_back, q_gain_grad, k_gain_grad = attention_pull(
        qkv,
        tables,
        order,
        (query_reduced, key_reduced, value_reduced, totals),
        out_grad,
        head_count,
        kv_heads,
    )
    qkv_back = jnp.concatenate([query_back, key_back, value_back], axis=1)
    qkv_grad = contract_rows(normed, qkv_back).astype(jnp.bfloat16)
    attn_grad = scatter_weights(
        after(jnp.concatenate([qkv_grad, o_wgrad.astype(jnp.bfloat16)], axis=1), mid_sum_far)
    )
    gradient, moved, attn_gain_grad = exchange(
        3,
        contract_cols(after(qkv_back, qkv_grad), qkv_full).astype(jnp.bfloat16),
        (stream, gradient, as_row(attn_scale)),
        (whole(jnp.float32), whole(jnp.bfloat16), gain_sum),
        stream_pull_rows,
        False,
    )
    moved = trade(moved)
    gradient = jnp.where(core == lax.axis_index("h"), gradient, moved.astype(jnp.float32))

    hidden_near = after(hidden_near, attn_gain_grad)
    branch = scatter_tokens(
        contract_cols(hidden_near, down_near) + contract_cols(hidden_far, down_far)
    )
    activations = trade((middle + branch).astype(jnp.bfloat16))

    split_at = down_rows.shape[1]
    down_grad = columns_of(*return_halves(down_grads[:, :split_at], down_grads[:, split_at:]))
    mine, other = return_halves(mid_sum_near, mid_sum_far)
    gate_grad = columns_of(mine[:, :half_cols], other[:, :half_cols])
    up_grad = columns_of(mine[:, half_cols:], other[:, half_cols:])

    devices = gains.shape[0]
    sums = jnp.concatenate(
        [
            part.reshape(devices, -1)
            for part in (attn_gain_grad[0], mlp_gain_grad[0], q_gain_grad[0], k_gain_grad[0])
        ],
        axis=1,
    )
    sums = jnp.pad(sums, ((0, 0), (0, 1024 - sums.shape[1]))).reshape(devices, 8, 128)
    sums = gain_total(sums).reshape(1, -1)

    return (
        activations,
        gradient,
        sums[:, :cut],
        attn_grad[None, :, :q_cols],
        attn_grad[None, :, q_cols : q_cols + kv_cols],
        attn_grad[None, :, q_cols + kv_cols : q_cols + 2 * kv_cols],
        attn_grad[None, :, q_cols + 2 * kv_cols :],
        sums[:, 2 * cut : 2 * cut + head_cut],
        sums[:, 2 * cut + head_cut : 2 * cut + 2 * head_cut],
        sums[:, cut : 2 * cut],
        gate_grad[None],
        up_grad[None],
        down_grad[None],
    )


def solution(mesh):
    dp, tensor = mesh.shape["dp"], mesh.shape["tensor"]
    cut = Mesh(mesh.devices.reshape(dp // 2, 2, 2, tensor // 2), ("d", "c", "h", "l"))
    rows, cols = ("d", "c"), ("h", "l")
    tokens, labels = P(rows + cols, None), P(rows, None)
    gain, weight = P(None, rows), P(None, rows, cols)
    return jax.shard_map(
        per_device,
        mesh=cut,
        in_specs=(
            tokens,
            labels,
            gain,
            weight,
            weight,
            weight,
            weight,
            gain,
            gain,
            gain,
            weight,
            weight,
            weight,
            tokens,
        ),
        out_specs=(
            tokens,
            tokens,
            gain,
            weight,
            weight,
            weight,
            weight,
            gain,
            gain,
            gain,
            weight,
            weight,
            weight,
        ),
        check_vma=False,
    )
```

```python
import functools

import jax
import jax.numpy as jnp
from jax import lax
from jax.experimental import pallas as pl
from jax.experimental.pallas import tpu as pltpu
from jax.sharding import Mesh
from jax.sharding import PartitionSpec as P


HEAD_WIDTH = 128
NSEQ = 3


EPS = 1e-06
THETA = 1000000.0


def rms_scale(values, gain):
    return values * lax.rsqrt(jnp.mean(values * values, axis=-1, keepdims=True) + EPS) * gain


def swiglu(gate_raw, up_raw):
    return jax.nn.silu(gate_raw) * up_raw


def rotary_tables(sequence_labels, row_index):
    labels = jnp.arange(NSEQ, dtype=jnp.int32)
    starts = jnp.sum((sequence_labels[None, :] < labels[:, None]).astype(jnp.int32), axis=1)
    first_row = jnp.sum(
        jnp.where(sequence_labels[:, None] == labels[None, :], starts[None, :], 0), axis=1
    )
    position = (row_index - first_row).astype(jnp.float32)
    frequency = THETA ** (-(jnp.arange(HEAD_WIDTH // 2, dtype=jnp.float32) * (2.0 / HEAD_WIDTH)))
    angles = position[:, None] * frequency[None, :]
    sine = jnp.sin(angles)
    cosine = jnp.cos(angles)
    return (
        jnp.concatenate([cosine, cosine], axis=1),
        jnp.concatenate([-sine, sine], axis=1),
        first_row[:, None],
    )


def contract_rows(left, right):
    return lax.dot_general(
        left, right, (((0,), (0,)), ((), ())), preferred_element_type=jnp.float32
    )


def contract_cols(left, right):
    return lax.dot_general(
        left, right, (((1,), (1,)), ((), ())), preferred_element_type=jnp.float32
    )


MESH = pl.DeviceIdType.MESH
CHUNKS = 3


def remote(source, target, send_sem, recv_sem, **place):
    return pltpu.make_async_remote_copy(
        src_ref=source,
        dst_ref=target,
        send_sem=send_sem,
        recv_sem=recv_sem,
        device_id=place,
        device_id_type=MESH,
    )


def rows_at(index, size):
    return pl.ds(pl.multiple_of(index * size, size), size)


WEIGHTS = 5
ENTRY_START = (
    "w0", "t0", "w1", "w2", "t1", "w3", "w4", "t2",
)
ENTRY_ORDER = (
    "s0", "t0", "s1", "r0", "s2", "r1", "t1", "s3", "r2", "s4", "r3", "t2", "r4", "a0", "a1",
    "a2",
)


def hop_plan(nd, d):
    if nd == 4:
        side_x = d + 1 - 2 * lax.rem(d, 2)
        side_y = d + 2 - 4 * (d // 2)
        corner = side_x + side_y - d
        hops = (
            (0, d, side_x),
            (1, d, side_x),
            (0, d, side_y),
            (1, d, side_y),
            (0, side_x, side_y),
            (1, side_y, side_x),
        )
        sources = ((0, side_x), (1, side_x), (0, side_y), (1, side_y), (0, corner), (1, corner))
        return hops, sources, 4, ((0, 4), (3, 5))
    steps = [(part, step) for step in range(1, nd) for part in range(2)]
    hops = tuple((part, d, lax.rem(d + step, nd)) for part, step in steps)
    sources = tuple((part, lax.rem(d + nd - step, nd)) for part, step in steps)
    return hops, sources, len(hops), ()


def hop_count(nd):
    return 6 if nd == 4 else 2 * (nd - 1)


class Spread:
    def __init__(self, nd, d, block, send_sem, recv_sem, own=None):
        self.hops, self.sources, self.first, self.relayed = hop_plan(nd, d)
        self.block, self.send_sem, self.recv_sem = block, send_sem, recv_sem
        self.own = own or (lambda j, part: block(j, d * 2 + part))

    def copy(self, j, kind, source, part, of):
        return remote(
            source,
            self.block(j, of * 2 + part),
            self.send_sem.at[j, kind],
            self.recv_sem.at[j, kind],
            d=self.hops[kind][2],
        )

    def hop(self, j, kind):
        part, of, _ = self.hops[kind]
        source = self.own(j, part) if kind < self.first else self.block(j, of * 2 + part)
        return self.copy(j, kind, source, part, of)

    def arrived(self, j, kind):
        part, of = self.sources[kind]
        return self.copy(j, kind, self.block(j, of * 2 + part), part, of)

    def send(self, j, part):
        for kind in range(self.first):
            if self.hops[kind][0] == part:
                self.hop(j, kind).start()

    def relay(self, j):
        for after_kind, kind in self.relayed:
            self.arrived(j, after_kind).wait_recv()
            self.hop(j, kind).start()

    def finish(self, j):
        handled = {after_kind for after_kind, _ in self.relayed}
        for kind in range(len(self.hops)):
            if kind not in handled:
                self.arrived(j, kind).wait_recv()
            self.hop(j, kind).wait_send()


def entry_kernel(nd, tl, *refs):
    (q_ref, k_ref, v_ref, o_ref, gate_ref, up_ref, down_ref, tok_ref, cot_ref, gain_ref) = refs[:10]
    (qkv_full, o_full, mid_rows, down_rows, tok_full, cot_own, gain_full) = refs[10:17]
    (stage, half_stage, tok_stage, cot_stage) = refs[17:21]
    (zs, zr, cs, li, lo, xs, xr, ts, tr, tli, tlo, ls, lr, fs, fr) = refs[21:36]
    (gs, gr, gl, os, orv, oi, hs, hr, hi, ho) = refs[36:]
    d, c, h, l = (lax.axis_index(name) for name in ("d", "c", "h", "l"))
    same = c == h
    apart = c != h
    rows = q_ref.shape[0]
    own = tok_ref.shape[0]
    chunk = own // CHUNKS
    q_cols, kv_cols = q_ref.shape[1], k_ref.shape[1]
    o_half = o_ref.shape[1] // 2
    qkv_cols = q_cols + 2 * kv_cols
    weights = (
        (q_ref, qkv_full, 0, q_cols, 0),
        (k_ref, qkv_full, q_cols, kv_cols, q_cols),
        (v_ref, qkv_full, q_cols + kv_cols, kv_cols, q_cols + kv_cols),
        (o_ref.at[:, pl.ds(0, o_half)], o_full, 0, o_half, qkv_cols),
        (o_ref.at[:, pl.ds(o_half, o_half)], o_full, o_half, o_half, qkv_cols + o_half),
    )

    def block(j, row):
        _, full, start, cols, _ = weights[j]
        return full.at[rows_at(row, rows), pl.ds(start, cols)]

    def held(j):
        _, _, _, cols, start = weights[j]
        return stage.at[:, pl.ds(start, cols)]

    def from_far(j, part):
        return remote(block(j, d * 2 + part), block(j, d * 2 + part), zs.at[j], zr.at[j, part], h=1 - h)

    def to_far(j):
        return remote(weights[j][0], block(j, d * 2 + c), zs.at[j], zr.at[j, c], c=h, h=1 - h)

    def to_core(j):
        return remote(weights[j][0], block(j, d * 2 + c), cs.at[j], zr.at[j, c], c=h)

    def local_in(j):
        return pltpu.make_async_copy(weights[j][0], held(j), li.at[j])

    def local_out(j):
        return pltpu.make_async_copy(held(j), block(j, d * 2 + c), lo.at[j])

    def tokens_at(index, k):
        return tok_full.at[pl.ds(index * own + k * chunk, chunk)]

    def trade_tokens(k):
        return remote(tok_ref.at[pl.ds(k * chunk, chunk)], tokens_at(0, k), ts.at[k], tr.at[k], c=h, h=c)

    def along(step, k):
        return remote(
            tokens_at(0, k),
            tokens_at(tl - step, k),
            ls.at[(step - 1) * CHUNKS + k],
            lr.at[(tl - step - 1) * CHUNKS + k],
            l=lax.rem(l + step, tl),
        )

    def from_along(index, k):
        return remote(
            tokens_at(index, k),
            tokens_at(index, k),
            ls.at[(index - 1) * CHUNKS + k],
            lr.at[(index - 1) * CHUNKS + k],
            l=l,
        )

    def across(index, k):
        at = index * CHUNKS + k
        return remote(tokens_at(index, k), tokens_at(tl + index, k), fs.at[at], fr.at[at], c=1 - c)

    def gain_peer(step):
        place = lax.rem(d * 2 + c + step, 2 * nd)
        return place // 2, lax.rem(place, 2)

    def gains_to(step):
        to_d, to_c = gain_peer(step)
        return remote(
            gain_ref, gain_full.at[d * 2 + c], gs.at[step - 1], gr.at[2 * nd - step - 1], d=to_d, c=to_c
        )

    def gains_from(step):
        from_d, from_c = gain_peer(step)
        return remote(
            gain_ref, gain_full.at[from_d * 2 + from_c], gs.at[step - 1], gr.at[step - 1], d=from_d, c=from_c
        )

    def local_gains():
        return pltpu.make_async_copy(gain_ref, gain_full.at[d * 2 + c], gl)

    half = gate_ref.shape[1] // 2
    halves = ((gate_ref, mid_rows, 0), (up_ref, mid_rows, half), (down_ref, down_rows, 0))

    def columns_of_core(j, of):
        return halves[j][0].at[:, pl.ds(pl.multiple_of(of * half, half), half)]

    def half_at(j, of):
        return halves[j][1].at[rows_at(of, rows), pl.ds(halves[j][2], half)]

    def half_to_core(j):
        return remote(columns_of_core(j, 1 - c), half_at(j, c), hs.at[j], hr.at[j], c=1 - c)

    def half_from_core(j):
        return remote(half_at(j, 1 - c), half_at(j, 1 - c), hs.at[j], hr.at[j], c=1 - c)

    def half_in(j):
        return pltpu.make_async_copy(columns_of_core(j, c), half_stage.at[j], hi.at[j])

    def half_out(j):
        return pltpu.make_async_copy(half_stage.at[j], half_at(j, c), ho.at[j])

    local_gains().start()

    def start_weights(j):
        to_far(j).start()

        @pl.when(apart)
        def _():
            to_core(j).start()

    def start_tokens(k):
        @pl.when(apart)
        def _():
            trade_tokens(k).start()

    def trade_cotangent():
        return remote(cot_ref, cot_own, os, orv, c=h, h=c)

    def cotangent_in():
        return pltpu.make_async_copy(cot_ref, cot_stage, oi)

    def cotangent_out():
        return pltpu.make_async_copy(cot_stage, cot_own, oi)

    for step in ENTRY_START:
        {"w": start_weights, "t": start_tokens}[step[0]](int(step[1:]))

    @pl.when(apart)
    def _():
        trade_cotangent().start()

    @pl.when(same)
    def _():
        pltpu.make_async_copy(tok_ref, tok_stage, tli).start()
        for j in range(WEIGHTS):
            local_in(j).start()
        pltpu.make_async_copy(tok_ref, tok_stage, tli).wait()
        for k in range(CHUNKS):
            part = pl.ds(k * chunk, chunk)
            pltpu.make_async_copy(tok_stage.at[part], tokens_at(0, k), tlo.at[k]).start()
        for j in range(WEIGHTS):
            local_in(j).wait()
            local_out(j).start()
        cotangent_in().start()
        cotangent_in().wait()
        cotangent_out().start()

    for step in range(1, 2 * nd):
        gains_to(step).start()
    for j in range(3):
        half_in(j).start()
        half_to_core(j).start()
    for j in range(3):
        half_in(j).wait()
        half_out(j).start()

    over_d = Spread(nd, d, block, xs, xr)

    def spread(j):
        for part in range(2):
            here = jnp.logical_and(same, c == part)

            @pl.when(here)
            def _():
                local_out(j).wait()

            @pl.when(jnp.logical_not(here))
            def _():
                from_far(j, part).wait_recv()

            over_d.send(j, part)

    relay = over_d.relay

    def own_tokens(k):
        @pl.when(same)
        def _():
            part = pl.ds(k * chunk, chunk)
            pltpu.make_async_copy(tok_stage.at[part], tokens_at(0, k), tlo.at[k]).wait()

        @pl.when(apart)
        def _():
            remote(tokens_at(0, k), tokens_at(0, k), ts.at[k], tr.at[k], c=1 - c, h=1 - h).wait_recv()

        for step in range(1, tl):
            along(step, k).start()
        across(0, k).start()

    def pass_across(k):
        for index in range(1, tl):
            from_along(index, k).wait_recv()
            across(index, k).start()

    steps = {"t": own_tokens, "s": spread, "r": relay, "a": pass_across}
    for step in ENTRY_ORDER:
        steps[step[0]](int(step[1:]))

    for j in range(WEIGHTS):
        over_d.finish(j)
        to_far(j).wait_send()
    for k in range(CHUNKS):
        for index in range(tl):
            across(index, k).wait()
        for step in range(1, tl):
            along(step, k).wait_send()
    for step in range(1, 2 * nd):
        gains_from(step).wait_recv()
        gains_to(step).wait_send()
    local_gains().wait()
    for j in range(3):
        half_from_core(j).wait_recv()
        half_to_core(j).wait_send()
        half_out(j).wait()

    @pl.when(same)
    def _():
        cotangent_out().wait()

    @pl.when(apart)
    def _():
        trade_cotangent().wait()
        for j in range(WEIGHTS):
            to_core(j).wait_send()
        for k in range(CHUNKS):
            trade_tokens(k).wait_send()


def enter(q_weight, k_weight, v_weight, o_weight, gate, up, down, tokens, cotangent, gains):
    nd, tl = lax.axis_size("d"), lax.axis_size("l")
    rows, q_cols = q_weight.shape
    qkv_cols = q_cols + 2 * k_weight.shape[1]
    own, width = tokens.shape
    half = gate.shape[1] // 2
    dma = pltpu.SemaphoreType.DMA
    counts = (
        (WEIGHTS,),
        (WEIGHTS, 2),
        (WEIGHTS,),
        (WEIGHTS,),
        (WEIGHTS,),
        (WEIGHTS, hop_count(nd)),
        (WEIGHTS, hop_count(nd)),
        (CHUNKS,),
        (CHUNKS,),
        (),
        (CHUNKS,),
        ((tl - 1) * CHUNKS,),
        ((tl - 1) * CHUNKS,),
        (tl * CHUNKS,),
        (tl * CHUNKS,),
        (2 * nd - 1,),
        (2 * nd - 1,),
        (),
        (),
        (),
        (),
        (3,),
        (3,),
        (3,),
        (3,),
    )
    anywhere = pl.BlockSpec(memory_space=pl.ANY)

    def low(*shape):
        return jax.ShapeDtypeStruct(shape, jnp.bfloat16)

    return pl.pallas_call(
        functools.partial(entry_kernel, nd, tl),
        name="entry",
        out_shape=(
            low(width, qkv_cols),
            low(width, o_weight.shape[1]),
            low(2 * rows, 2 * half),
            low(2 * rows, half),
            low(2 * tl * own, width),
            low(own, width),
            jax.ShapeDtypeStruct((2 * nd,) + gains.shape, jnp.float32),
        ),
        in_specs=[anywhere] * 10,
        out_specs=[anywhere] * 7,
        scratch_shapes=[
            pltpu.VMEM((rows, qkv_cols + o_weight.shape[1]), jnp.bfloat16),
            pltpu.VMEM((3, rows, half), jnp.bfloat16),
            pltpu.VMEM((own, width), jnp.bfloat16),
            pltpu.VMEM((own, width), jnp.bfloat16),
        ]
        + [dma(count) if count else dma for count in counts],
        compiler_params=pltpu.CompilerParams(has_side_effects=True),
        cost_estimate=pl.CostEstimate(flops=0, bytes_accessed=250_000_000, transcendentals=0),
    )(q_weight, k_weight, v_weight, o_weight, gate, up, down, tokens, cotangent, gains)


PIECES = 6
SUM_ORDER = (
    "s3", "s4", "s5", "f0", "r3", "s0", "f1", "r4", "r0", "s1", "f2", "r5", "r1", "s2", "r2",
    "a0", "a1", "a2",
)


def exchange_kernel(nd, tl, epilogue, aux_count, out_count, gather, carry_weights, *refs):
    partial = refs[0]
    aux = refs[1 : 1 + aux_count]
    refs = refs[1 + aux_count :]
    if carry_weights:
        weight_rows, here_rows, refs = refs[0], refs[1], refs[2:]
    outs = refs[:out_count]
    rest = refs[out_count:]
    if gather:
        full, rest = rest[0], rest[1:]
    if carry_weights:
        weights, stage, ws, wr, xs, xr, hi, ho, rest = rest[0], *rest[1:8], rest[8:]
    if gather:
        finished, ls, lr, fs, fr, keep, rest = rest[0], *rest[1:6], rest[6:]
    mine, other, sums, arrivals, cs, cr, loc, ss, sr = rest
    c, l = lax.axis_index("c"), lax.axis_index("l")
    d, h = lax.axis_index("d"), lax.axis_index("h")
    own = arrivals.shape[0] // (tl - 1)
    chunk = own // CHUNKS

    barrier = pltpu.get_barrier_semaphore()
    pl.semaphore_signal(barrier, inc=1, device_id={"c": 1 - c}, device_id_type=MESH)
    for step in range(1, tl):
        pl.semaphore_signal(
            barrier, inc=1, device_id={"l": lax.rem(l + step, tl)}, device_id_type=MESH
        )
    partners = tl
    if carry_weights:
        pl.semaphore_signal(barrier, inc=1, device_id={"h": 1 - h}, device_id_type=MESH)
        partners += 1
        for step in range(1, nd):
            pl.semaphore_signal(
                barrier, inc=1, device_id={"d": lax.rem(d + step, nd)}, device_id_type=MESH
            )
        partners += nd - 1
    pl.semaphore_wait(barrier, partners)

    def part(base, k):
        return rows_at(base * CHUNKS + k, chunk)

    def to_core(index, k):
        at = index * CHUNKS + k
        return remote(
            partial.at[part(tl + index, k)], other.at[part(index, k)], cs.at[at], cr.at[at], c=1 - c
        )

    def local(index, k):
        return pltpu.make_async_copy(
            partial.at[part(index, k)], mine.at[part(index, k)], loc.at[index * CHUNKS + k]
        )

    def along(step, k):
        at = (step - 1) * CHUNKS + k
        return remote(
            sums.at[part(step - 1, k)],
            arrivals.at[part(step - 1, k)],
            ss.at[at],
            sr.at[at],
            l=lax.rem(l + step, tl),
        )

    if carry_weights:
        half = weight_rows.shape[0] // 2
        far_pieces = PIECES // 2
        piece = here_rows.shape[1] // far_pieces

        def block(j, row):
            return weights.at[rows_at(row, half), pl.ds(j * piece, piece)]

        def given(j, row_part):
            source = weight_rows if j < far_pieces else here_rows
            return source.at[pl.ds(row_part * half, half), pl.ds(j % far_pieces * piece, piece)]

        def held_here(j, row_part):
            return block(j, d * 2 + row_part) if j < far_pieces else given(j, row_part)

        def from_far(j, row_part):
            return remote(
                given(j, row_part),
                block(j, d * 2 + row_part),
                ws.at[j, row_part],
                wr.at[j, row_part],
                h=1 - h,
            )

        def here_in():
            return pltpu.make_async_copy(here_rows, stage, hi)

        def here_out():
            here = weights.at[rows_at(d, 2 * half), pl.ds(far_pieces * piece, far_pieces * piece)]
            return pltpu.make_async_copy(stage, here, ho)

        over_d = Spread(nd, d, block, xs, xr, held_here)

        def spread(j):
            for row_part in range(2):
                if j < far_pieces:
                    from_far(j, row_part).wait_recv()
                over_d.send(j, row_part)

        for j in range(far_pieces):
            for row_part in range(2):
                from_far(j, row_part).start()
        here_in().start()

    order = list(range(1, tl)) + [0]
    for index in order:
        for k in range(CHUNKS):
            to_core(index, k).start()
            local(index, k).start()

    def both(index, k):
        local(index, k).wait()
        to_core(index, k).wait_recv()
        at = part(index, k)
        return mine[at, :].astype(jnp.float32) + other[at, :].astype(jnp.float32)

    for step in range(1, tl):

        def pass_on(k, carry):
            sums[part(step - 1, k), :] = both(step, k).astype(jnp.bfloat16)
            along(step, k).start()
            return carry

        lax.fori_loop(0, CHUNKS, pass_on, 0)

    def gathered(index, k):
        return full.at[part(index, k)]

    def keep_own(k):
        return pltpu.make_async_copy(finished.at[part(0, k)], gathered(0, k), keep.at[k])

    def own_along(step, k):
        return remote(
            finished.at[part(0, k)],
            gathered(tl - step, k),
            ls.at[(step - 1) * CHUNKS + k],
            lr.at[(tl - step - 1) * CHUNKS + k],
            l=lax.rem(l + step, tl),
        )

    def from_along(index, k):
        at = (index - 1) * CHUNKS + k
        return remote(gathered(index, k), gathered(index, k), ls.at[at], lr.at[at], l=l)

    def across(index, k):
        source = finished.at[part(0, k)] if index == 0 else gathered(index, k)
        at = index * CHUNKS + k
        return remote(source, gathered(tl + index, k), fs.at[at], fr.at[at], c=1 - c)

    def finish(k, carry):
        total = both(0, k)
        for step in range(1, tl):
            along(step, k).wait_recv()
            total = total + arrivals[part(step - 1, k), :].astype(jnp.float32)
        row = epilogue(total, part(0, k), k, aux, outs)
        if gather:
            finished[part(0, k), :] = row
            keep_own(k).start()
            for step in range(1, tl):
                own_along(step, k).start()
            across(0, k).start()
        return carry

    def pass_across(k):
        for index in range(1, tl):
            from_along(index, k).wait_recv()
            across(index, k).start()

    if carry_weights:
        steps = {
            "s": spread,
            "r": over_d.relay,
            "f": lambda k: finish(k, 0),
            "a": pass_across,
        }
        here_in().wait()
        here_out().start()
        for step in SUM_ORDER:
            steps[step[0]](int(step[1:]))
    else:
        lax.fori_loop(0, CHUNKS, finish, 0)
        if gather:
            for k in range(CHUNKS):
                pass_across(k)
    if gather:
        for k in range(CHUNKS):
            keep_own(k).wait()
            for index in range(tl):
                across(index, k).wait()
            for step in range(1, tl):
                own_along(step, k).wait_send()
    if carry_weights:
        for j in range(PIECES):
            over_d.finish(j)
            if j < far_pieces:
                for row_part in range(2):
                    from_far(j, row_part).wait_send()
        here_out().wait()
    for k in range(CHUNKS):
        for index in range(tl):
            to_core(index, k).wait_send()
        for step in range(1, tl):
            along(step, k).wait_send()


def exchange(collective_id, partial, aux, outs, epilogue, gather, weight_rows=()):
    nd, tl = lax.axis_size("d"), lax.axis_size("l")
    total, width = partial.shape
    own = total // (2 * tl)
    dma = pltpu.SemaphoreType.DMA
    vmem = pl.BlockSpec(memory_space=pltpu.VMEM)
    anywhere = pl.BlockSpec(memory_space=pl.ANY)
    out_shape = list(outs)
    out_specs = [vmem] * len(outs)
    scratch = []
    if gather:
        out_shape.append(jax.ShapeDtypeStruct((total, width), jnp.bfloat16))
        out_specs.append(anywhere)
    if weight_rows:
        rows, cols = weight_rows[1].shape
        out_shape.append(jax.ShapeDtypeStruct((nd * rows, 2 * cols), jnp.bfloat16))
        out_specs.append(anywhere)
        scratch += [
            pltpu.VMEM((rows, cols), jnp.bfloat16),
            dma((PIECES, 2)),
            dma((PIECES, 2)),
            dma((PIECES, hop_count(nd))),
            dma((PIECES, hop_count(nd))),
            dma,
            dma,
        ]
    if gather:
        scratch += [
            pltpu.VMEM((own, width), jnp.bfloat16),
            dma(((tl - 1) * CHUNKS,)),
            dma(((tl - 1) * CHUNKS,)),
            dma((tl * CHUNKS,)),
            dma((tl * CHUNKS,)),
            dma((CHUNKS,)),
        ]
    scratch += [
        pltpu.VMEM((tl * own, width), jnp.bfloat16),
        pltpu.VMEM((tl * own, width), jnp.bfloat16),
        pltpu.VMEM(((tl - 1) * own, width), jnp.bfloat16),
        pltpu.VMEM(((tl - 1) * own, width), jnp.bfloat16),
        dma((tl * CHUNKS,)),
        dma((tl * CHUNKS,)),
        dma((tl * CHUNKS,)),
        dma(((tl - 1) * CHUNKS,)),
        dma(((tl - 1) * CHUNKS,)),
    ]
    return pl.pallas_call(
        functools.partial(
            exchange_kernel, nd, tl, epilogue, len(aux), len(outs), gather, bool(weight_rows)
        ),
        out_shape=tuple(out_shape),
        in_specs=[anywhere] + [vmem] * len(aux) + [anywhere] * len(weight_rows),
        out_specs=out_specs,
        scratch_shapes=scratch,
        compiler_params=pltpu.CompilerParams(
            has_side_effects=True, collective_id=collective_id, vmem_limit_bytes=40 << 20
        ),
        cost_estimate=pl.CostEstimate(
            flops=0, bytes_accessed=200_000_000 if gather else 110_000_000, transcendentals=0
        ),
    )(partial, *aux, *weight_rows)


def gain_kernel(nd, tl, tiles, out, got, send_sem, recv_sem):
    d, c, h, l = (lax.axis_index(name) for name in ("d", "c", "h", "l"))
    count = 4 * nd * tl
    me = ((d * 2 + c) * 2 + h) * tl + l

    def to(step):
        place = lax.rem(me + step, count)
        to_l = lax.rem(place, tl)
        to_h = lax.rem(place // tl, 2)
        row = place // (2 * tl)
        return remote(
            tiles.at[row],
            got.at[step - 1],
            send_sem.at[step - 1],
            recv_sem.at[step - 1],
            d=row // 2,
            c=lax.rem(row, 2),
            h=to_h,
            l=to_l,
        )

    def start(step, carry):
        to(step).start()
        return carry

    def add(step, total):
        to(step).wait_recv()
        return total + got[step - 1]

    def drain(step, carry):
        to(step).wait_send()
        return carry

    lax.fori_loop(1, count, start, 0)
    out[...] = lax.fori_loop(1, count, add, tiles[d * 2 + c])
    lax.fori_loop(1, count, drain, 0)


def gain_total(tiles):
    nd, tl = lax.axis_size("d"), lax.axis_size("l")
    others = 4 * nd * tl - 1
    vmem = pl.BlockSpec(memory_space=pltpu.VMEM)
    return pl.pallas_call(
        functools.partial(gain_kernel, nd, tl),
        name="gain_total",
        out_shape=jax.ShapeDtypeStruct(tiles.shape[1:], jnp.float32),
        in_specs=[vmem],
        out_specs=vmem,
        scratch_shapes=[
            pltpu.VMEM((others,) + tiles.shape[1:], jnp.float32),
            pltpu.SemaphoreType.DMA((others,)),
            pltpu.SemaphoreType.DMA((others,)),
        ],
        compiler_params=pltpu.CompilerParams(has_side_effects=True),
        cost_estimate=pl.CostEstimate(flops=0, bytes_accessed=40_000_000, transcendentals=0),
    )(tiles)


def middle_rows(total, rows, k, aux, outs):
    stream, gain = aux
    value = stream[rows, :].astype(jnp.float32) + total
    outs[0][rows, :] = value
    return rms_scale(value, gain[...]).astype(jnp.bfloat16)


def norm_pull(value, gain, grad):
    scale = lax.rsqrt(jnp.mean(value * value, axis=-1, keepdims=True) + EPS)
    scaled = grad * gain
    inner = jnp.mean(value * scaled, axis=-1, keepdims=True)
    return scale * scaled - value * (scale * scale * scale * inner), jnp.sum(
        grad * value * scale, axis=0, keepdims=True
    )


def add_rows(out, value, k):
    @pl.when(k == 0)
    def _():
        out[...] = value

    @pl.when(k > 0)
    def _():
        out[...] += value


def middle_pull_rows(total, rows, k, aux, outs):
    middle, cotangent, gain = aux
    pulled, gain_part = norm_pull(middle[rows, :], gain[...], total)
    value = cotangent[rows, :].astype(jnp.float32) + pulled
    outs[0][rows, :] = value
    add_rows(outs[1], gain_part, k)
    return value.astype(jnp.bfloat16)


def stream_pull_rows(total, rows, k, aux, outs):
    stream, gradient, gain = aux
    pulled, gain_part = norm_pull(stream[rows, :].astype(jnp.float32), gain[...], total)
    value = gradient[rows, :] + pulled
    outs[0][rows, :] = value
    outs[1][rows, :] = value.astype(jnp.bfloat16)
    add_rows(outs[2], gain_part, k)
    return None


def key_tile(rows):
    return next(size for size in (384, 256, 128) if rows % size == 0)


def turn(values):
    return pltpu.roll(values, HEAD_WIDTH // 2, 1)


def head_norm(values):
    return lax.rsqrt(jnp.mean(values * values, axis=-1, keepdims=True) + EPS)


def tile_mask(first, start, tile, row0, rows):
    keys = start + lax.broadcasted_iota(jnp.int32, (rows, tile), 1)
    last = row0 + lax.broadcasted_iota(jnp.int32, (rows, tile), 0)
    return jnp.logical_and(keys >= first, keys <= last)


def dot_last(left, right):
    return lax.dot_general(
        left, right, (((1,), (1,)), ((), ())), preferred_element_type=jnp.float32
    )


def attention_kernel(blocks, repeat, order_ref, *refs):
    q, k, v, cosine, sine, q_gain, k_gain, first = refs[:8]
    qr, kr, vb, out, total = refs[8:13]
    acc, den = refs[13:]
    rows = q.shape[0] // blocks
    tile = key_tile(q.shape[0])
    scale = HEAD_WIDTH**-0.5

    def rotated(values, gain, at):
        scaled = values * head_norm(values) * gain
        return (scaled * cosine[at, :] + turn(scaled) * sine[at, :]).astype(jnp.bfloat16)

    def prepare(i, carry):
        at, to = rows_at(i, rows), rows_at(order_ref[i], rows)
        for r in range(repeat):
            head = slice(r * HEAD_WIDTH, (r + 1) * HEAD_WIDTH)
            qr[at, head] = rotated(q[at, head], q_gain[...], at)
        kr[to, :] = rotated(k[at, :], k_gain[...], at)
        vb[to, :] = v[at, :].astype(jnp.bfloat16)
        return carry

    lax.fori_loop(0, blocks, prepare, 0)

    def attend(i, carry):
        at = rows_at(i, rows)
        row0 = order_ref[i] * rows
        acc[...] = jnp.zeros_like(acc)
        den[...] = jnp.zeros_like(den)

        def over_keys(t, inner):
            keys = rows_at(t, tile)
            mask = tile_mask(first[at, :], t * tile, tile, row0, rows)
            for r in range(repeat):
                head = slice(r * HEAD_WIDTH, (r + 1) * HEAD_WIDTH)
                scores = dot_last(qr[at, head], kr[keys, :]) * scale
                weights = jnp.where(mask, jnp.exp(scores), 0.0)
                den[r] += jnp.sum(weights, axis=-1, keepdims=True)
                acc[r] += jnp.dot(
                    weights.astype(jnp.bfloat16), vb[keys, :], preferred_element_type=jnp.float32
                )
            return inner

        lax.fori_loop(0, (row0 + rows + tile - 1) // tile, over_keys, 0)
        for r in range(repeat):
            head = slice(r * HEAD_WIDTH, (r + 1) * HEAD_WIDTH)
            out[at, head] = (acc[r] / den[r]).astype(jnp.bfloat16)
            total[at, r : r + 1] = den[r]
        return carry

    lax.fori_loop(0, blocks, attend, 0)


def attention_specs(rows, q_heads, kv_heads):
    repeat = q_heads // kv_heads

    def columns(width, start=0):
        return pl.BlockSpec((rows, width * HEAD_WIDTH), lambda g, order: (0, start // width + g))

    def fixed(*shape):
        return pl.BlockSpec(shape, lambda g, order: (0, 0))

    raw = [columns(repeat), columns(1, q_heads), columns(1, q_heads + kv_heads)]
    tables = [
        fixed(rows, HEAD_WIDTH),
        fixed(rows, HEAD_WIDTH),
        fixed(1, HEAD_WIDTH),
        fixed(1, HEAD_WIDTH),
        fixed(rows, 1),
    ]
    return repeat, columns, fixed, raw, tables


def attention(qkv, tables, order, q_heads, kv_heads):
    rows = qkv.shape[0]
    blocks = order.shape[0]
    repeat, columns, _, raw, table_specs = attention_specs(rows, q_heads, kv_heads)
    wide, narrow = q_heads * HEAD_WIDTH, kv_heads * HEAD_WIDTH
    return pl.pallas_call(
        functools.partial(attention_kernel, blocks, repeat),
        name="attention",
        out_shape=(
            jax.ShapeDtypeStruct((rows, wide), jnp.bfloat16),
            jax.ShapeDtypeStruct((rows, narrow), jnp.bfloat16),
            jax.ShapeDtypeStruct((rows, narrow), jnp.bfloat16),
            jax.ShapeDtypeStruct((rows, wide), jnp.bfloat16),
            jax.ShapeDtypeStruct((rows, narrow), jnp.float32),
        ),
        grid_spec=pltpu.PrefetchScalarGridSpec(
            num_scalar_prefetch=1,
            grid=(kv_heads,),
            in_specs=raw + table_specs,
            out_specs=[columns(repeat), columns(1), columns(1), columns(repeat), columns(1)],
            scratch_shapes=[
                pltpu.VMEM((repeat, rows // blocks, HEAD_WIDTH), jnp.float32),
                pltpu.VMEM((repeat, rows // blocks, 1), jnp.float32),
            ],
        ),
        compiler_params=pltpu.CompilerParams(vmem_limit_bytes=50 << 20),
        cost_estimate=pl.CostEstimate(
            flops=4 * rows * rows * wide, bytes_accessed=60_000_000, transcendentals=0
        ),
    )(order, qkv, qkv, qkv, *tables)


def attention_pull_kernel(blocks, repeat, order_ref, *refs):
    q, k, cosine, sine, q_gain, k_gain, first, qr, kr, vb, total, grad = refs[:12]
    dq, dk, dv, dq_gain, dk_gain = refs[12:17]
    shares, share_grads, dq_acc, dk_acc, dv_acc, inner_sum = refs[17:]
    rows = q.shape[0] // blocks
    tile = key_tile(q.shape[0])
    scale = HEAD_WIDTH**-0.5
    dk_acc[...] = jnp.zeros_like(dk_acc)
    dv_acc[...] = jnp.zeros_like(dv_acc)

    @pl.when(pl.program_id(0) == 0)
    def _():
        dq_gain[...] = jnp.zeros_like(dq_gain)
        dk_gain[...] = jnp.zeros_like(dk_gain)

    def pull(raw, gain, turned_grad, at, gain_out):
        scaled_grad = turned_grad * cosine[at, :] + turn(turned_grad * sine[at, :])
        r = head_norm(raw)
        gain_out[0:1, :] += jnp.sum(scaled_grad * raw * r, axis=0, keepdims=True)
        scaled = scaled_grad * gain
        inner = jnp.mean(raw * scaled, axis=-1, keepdims=True)
        return (r * scaled - raw * (r * r * r * inner)).astype(jnp.bfloat16)

    def over_rows(i, carry):
        at = rows_at(i, rows)
        row0 = order_ref[i] * rows
        tiles = (row0 + rows + tile - 1) // tile
        dq_acc[...] = jnp.zeros_like(dq_acc)
        inner_sum[...] = jnp.zeros_like(inner_sum)

        def first_pass(t, inner):
            keys = rows_at(t, tile)
            mask = tile_mask(first[at, :], t * tile, tile, row0, rows)
            for r in range(repeat):
                head = slice(r * HEAD_WIDTH, (r + 1) * HEAD_WIDTH)
                scores = dot_last(qr[at, head], kr[keys, :]) * scale
                share = jnp.where(mask, jnp.exp(scores), 0.0) * (1.0 / total[at, r : r + 1])
                share_grad = dot_last(grad[at, head], vb[keys, :])
                inner_sum[r] += jnp.sum(share * share_grad, axis=-1, keepdims=True)
                shares[t, r] = share
                share_grads[t, r] = share_grad
            return inner

        lax.fori_loop(0, tiles, first_pass, 0)

        def second_pass(t, inner):
            keys = rows_at(t, tile)
            for r in range(repeat):
                head = slice(r * HEAD_WIDTH, (r + 1) * HEAD_WIDTH)
                share = shares[t, r]
                score_grad = (share * (share_grads[t, r] - inner_sum[r])).astype(jnp.bfloat16)
                dq_acc[r] += jnp.dot(score_grad, kr[keys, :], preferred_element_type=jnp.float32)
                dk_acc[keys, :] += contract_rows(score_grad, qr[at, head])
                dv_acc[keys, :] += contract_rows(share.astype(jnp.bfloat16), grad[at, head])
            return inner

        lax.fori_loop(0, tiles, second_pass, 0)
        for r in range(repeat):
            head = slice(r * HEAD_WIDTH, (r + 1) * HEAD_WIDTH)
            dq[at, head] = pull(q[at, head], q_gain[...], dq_acc[r] * scale, at, dq_gain)
        return carry

    lax.fori_loop(0, blocks, over_rows, 0)

    def finish(i, carry):
        at, to = rows_at(i, rows), rows_at(order_ref[i], rows)
        dk[at, :] = pull(k[at, :], k_gain[...], dk_acc[to, :] * scale, at, dk_gain)
        dv[at, :] = dv_acc[to, :].astype(jnp.bfloat16)
        return carry

    lax.fori_loop(0, blocks, finish, 0)


def attention_pull(qkv, tables, order, kept, grad, q_heads, kv_heads):
    rows = qkv.shape[0]
    blocks = order.shape[0]
    repeat, columns, fixed, raw, table_specs = attention_specs(rows, q_heads, kv_heads)
    wide, narrow = q_heads * HEAD_WIDTH, kv_heads * HEAD_WIDTH
    own, tile = rows // blocks, key_tile(rows)
    return pl.pallas_call(
        functools.partial(attention_pull_kernel, blocks, repeat),
        name="attention_pull",
        out_shape=(
            jax.ShapeDtypeStruct((rows, wide), jnp.bfloat16),
            jax.ShapeDtypeStruct((rows, narrow), jnp.bfloat16),
            jax.ShapeDtypeStruct((rows, narrow), jnp.bfloat16),
            jax.ShapeDtypeStruct((8, HEAD_WIDTH), jnp.float32),
            jax.ShapeDtypeStruct((8, HEAD_WIDTH), jnp.float32),
        ),
        grid_spec=pltpu.PrefetchScalarGridSpec(
            num_scalar_prefetch=1,
            grid=(kv_heads,),
            in_specs=raw[:2]
            + table_specs
            + [columns(repeat), columns(1), columns(1), columns(1), columns(repeat)],
            out_specs=[
                columns(repeat),
                columns(1),
                columns(1),
                fixed(8, HEAD_WIDTH),
                fixed(8, HEAD_WIDTH),
            ],
            scratch_shapes=[
                pltpu.VMEM((rows // tile, repeat, own, tile), jnp.float32),
                pltpu.VMEM((rows // tile, repeat, own, tile), jnp.float32),
                pltpu.VMEM((repeat, own, HEAD_WIDTH), jnp.float32),
                pltpu.VMEM((rows, HEAD_WIDTH), jnp.float32),
                pltpu.VMEM((rows, HEAD_WIDTH), jnp.float32),
                pltpu.VMEM((repeat, own, 1), jnp.float32),
            ],
        ),
        compiler_params=pltpu.CompilerParams(vmem_limit_bytes=56 << 20),
        cost_estimate=pl.CostEstimate(
            flops=10 * rows * rows * wide, bytes_accessed=120_000_000, transcendentals=0
        ),
    )(order, qkv, qkv, *tables, *kept, grad)


def shift_perm(size, step):
    return [((place + step) % size, place) for place in range(size)]


def trade(values):
    return lax.ppermute(values, ("c", "h"), [(0, 0), (1, 2), (2, 1), (3, 3)])


def gather_along(own):
    places = lax.axis_size("l")
    return [own] + [lax.ppermute(own, "l", shift_perm(places, step)) for step in range(1, places)]


def gather_across(parts):
    half = jnp.concatenate(parts, axis=0)
    other = lax.ppermute(half, "c", shift_perm(2, 1))
    return jnp.concatenate([half, other], axis=0)


def scatter_tokens(partial, *first):
    places = lax.axis_size("l")
    half = partial.shape[0] // 2
    rows = half // places
    other = lax.ppermute(partial[half:].astype(jnp.bfloat16), "c", shift_perm(2, 1))
    total = partial[:half] + other.astype(jnp.float32)
    own = total[:rows]
    for step in range(1, places):
        sent = total[step * rows : (step + 1) * rows].astype(jnp.bfloat16)
        moved = lax.ppermute(sent, "l", shift_perm(places, -step))
        moved = after(moved, *first)
        own = own + moved.astype(jnp.float32)
    return own


def after(value, *others):
    return lax.optimization_barrier((value,) + others)[0]


def return_halves(near, far):
    core = lax.axis_index("c")
    far = lax.ppermute(far, "h", shift_perm(2, 1))
    sums = near.astype(jnp.float32) + far.astype(jnp.float32)
    rows = sums.shape[0] // 2
    first, second = sums[:rows], sums[rows:]
    mine = jnp.where(core == 0, first, second)
    sent = jnp.where(core == 0, second, first).astype(jnp.bfloat16)
    other = lax.ppermute(sent, "c", shift_perm(2, 1)).astype(jnp.float32)
    return mine, other


def columns_of(mine, other):
    core = lax.axis_index("c")
    return jnp.concatenate(
        [jnp.where(core == 0, mine, other), jnp.where(core == 0, other, mine)], axis=1
    )


def sum_over_d(partial):
    return lax.psum_scatter(partial.astype(jnp.bfloat16), "d", scatter_dimension=0, tiled=True)


def as_row(values):
    return values.reshape(1, -1)


def split(values):
    half = values.shape[1] // 2
    return values[:, :half], values[:, half:]


def return_blocks(rows):
    core, upper = lax.axis_index("c"), lax.axis_index("h")
    half = rows.shape[0] // 2
    first, second = rows[:half], rows[half:]
    mine = jnp.where(core == 0, first, second)
    other = lax.ppermute(jnp.where(core == 0, second, first), "c", shift_perm(2, 1))
    same = core == upper
    sent = jnp.where(same, other, mine)
    far = lax.ppermute(sent, "h", shift_perm(2, 1))
    return jnp.where(same, mine, other).astype(jnp.float32) + far.astype(jnp.float32), sent


def per_device(
    tokens,
    segment_ids,
    attn_gain,
    q_weight,
    key_matrix,
    value_matrix,
    o_weight,
    q_gain,
    k_gain,
    mlp_gain,
    gate_weight,
    up_weight,
    down_weight,
    cotangent,
):
    width = attn_gain.shape[1] * lax.axis_size("d") * 2
    own_rows = tokens.shape[0]
    places = lax.axis_size("l")
    core, place = lax.axis_index("c"), lax.axis_index("l")
    q_cols, kv_cols, ff_cols = q_weight.shape[2], key_matrix.shape[2], gate_weight.shape[2]
    half_cols = ff_cols // 2

    cut = attn_gain.shape[1]
    head_cut = q_gain.shape[1]
    gains = jnp.concatenate([attn_gain[0], mlp_gain[0], q_gain[0], k_gain[0]]).astype(jnp.float32)
    gains = jnp.pad(gains, (0, 1024 - gains.shape[0])).reshape(8, 128)
    labels = trade(segment_ids)[0]
    order = jnp.stack(
        [
            ((core + core_step) % 2) * places + (place + step) % places
            for core_step in range(2)
            for step in range(places)
        ]
    )
    row_index = (order[:, None] * own_rows + jnp.arange(own_rows, dtype=jnp.int32)[None, :]).reshape(-1)
    labels = labels.reshape(2 * places, own_rows)[order].reshape(-1)
    cosine, sine, first_row = rotary_tables(labels, row_index)
    qkv_full, o_full, mid_rows, down_rows, group, cotangent, gains = enter(
        q_weight[0],
        key_matrix[0],
        value_matrix[0],
        o_weight[0],
        gate_weight[0],
        up_weight[0],
        down_weight[0],
        after(tokens, cosine, sine, first_row),
        cotangent,
        gains,
    )
    mid_near = lax.all_gather(mid_rows, "d", axis=0, tiled=True)
    down_near = lax.all_gather(down_rows, "d", axis=0, tiled=True)
    up_far = lax.ppermute(mid_rows[:, half_cols:], "h", shift_perm(2, 1))
    down_far = lax.ppermute(down_rows, "h", shift_perm(2, 1))
    grad_half = gather_along(cotangent)
    gains = gains.reshape(gains.shape[0], -1)
    attn_scale = gains[:, :cut].reshape(-1)
    mlp_scale = gains[:, cut : 2 * cut].reshape(-1)
    q_scale = gains[:, 2 * cut : 2 * cut + head_cut].reshape(-1)
    k_scale = gains[:, 2 * cut + head_cut : 2 * cut + 2 * head_cut].reshape(-1)

    stream = group[:own_rows]
    normed = rms_scale(group.astype(jnp.float32), attn_scale).astype(jnp.bfloat16)
    head_count, kv_heads = q_cols // HEAD_WIDTH, kv_cols // HEAD_WIDTH
    qkv = jnp.dot(normed, qkv_full, preferred_element_type=jnp.float32)
    tables = (cosine, sine, as_row(q_scale), as_row(k_scale), first_row)
    query_reduced, key_reduced, value_reduced, attended, totals = attention(
        qkv, tables, order, head_count, kv_heads
    )

    grad_rows = gather_across([grad_half[0]] + [after(part, attended) for part in grad_half[1:]])

    def whole(values):
        return jax.ShapeDtypeStruct((own_rows, width), values)

    gain_sum = jax.ShapeDtypeStruct((1, width), jnp.float32)
    middle, normed_mid, mid_far = exchange(
        1,
        contract_cols(attended, o_full).astype(jnp.bfloat16),
        (stream, as_row(mlp_scale)),
        (whole(jnp.float32),),
        middle_rows,
        True,
        (mid_rows, after(up_far, attended)),
    )
    down_far = lax.all_gather(after(down_far, normed_mid), "d", axis=0, tiled=True)

    mid = jnp.dot(normed_mid, mid_near, preferred_element_type=jnp.float32)
    gate_near, up_near = split(mid)
    hidden_near = swiglu(gate_near, up_near).astype(jnp.bfloat16)
    mid = jnp.dot(normed_mid, mid_far, preferred_element_type=jnp.float32)
    gate_far, up_far = split(mid)
    hidden_far = swiglu(gate_far, up_far).astype(jnp.bfloat16)
    down_partial = jnp.concatenate(
        [
            contract_rows(grad_rows, hidden_near).astype(jnp.bfloat16),
            contract_rows(grad_rows, hidden_far).astype(jnp.bfloat16),
        ],
        axis=1,
    )
    down_grads = sum_over_d(down_partial)
    grad_rows = after(grad_rows, down_partial)

    def hidden_pull(gate, up, down):
        hidden_grad = jnp.dot(grad_rows, down, preferred_element_type=jnp.float32)
        _, pull_back = jax.vjp(swiglu, gate, up)
        gate_grad, up_grad = pull_back(hidden_grad)
        return jnp.concatenate(
            [gate_grad.astype(jnp.bfloat16), up_grad.astype(jnp.bfloat16)], axis=1
        )

    mid_back_near = hidden_pull(gate_near, up_near, down_near)
    mid_back_far = hidden_pull(gate_far, up_far, down_far)
    mid_grad_far = contract_rows(normed_mid, mid_back_far).astype(jnp.bfloat16)
    mid_sum_far = sum_over_d(mid_grad_far)
    normed_grad = (contract_cols(mid_back_near, mid_near) + contract_cols(mid_back_far, mid_far)).astype(
        jnp.bfloat16
    )
    gradient, mlp_gain_grad, grad_rows = exchange(
        2,
        after(normed_grad, mid_grad_far),
        (middle, cotangent, as_row(mlp_scale)),
        (whole(jnp.float32), gain_sum),
        middle_pull_rows,
        True,
    )
    mid_grad_near = contract_rows(normed_mid, after(mid_back_near, grad_rows)).astype(jnp.bfloat16)
    mid_sum_near = sum_over_d(mid_grad_near)

    hidden_near = after(hidden_near, mid_grad_near)
    branch = contract_cols(hidden_near, down_near) + contract_cols(hidden_far, down_far)
    grad_rows = after(grad_rows, branch)
    out_grad = jnp.dot(grad_rows, o_full, preferred_element_type=jnp.float32).astype(jnp.bfloat16)
    o_wgrad = contract_rows(grad_rows, attended)
    query_back, key_back, value_back, q_gain_grad, k_gain_grad = attention_pull(
        qkv,
        tables,
        order,
        (query_reduced, key_reduced, value_reduced, totals),
        out_grad,
        head_count,
        kv_heads,
    )
    qkv_back = jnp.concatenate([query_back, key_back, value_back], axis=1)
    qkv_grad = contract_rows(normed, qkv_back).astype(jnp.bfloat16)
    attn_partial = jnp.concatenate([qkv_grad, o_wgrad.astype(jnp.bfloat16)], axis=1)
    attn_rows = sum_over_d(after(attn_partial, mid_sum_far))
    branch = scatter_tokens(branch, qkv_grad)
    activations = trade((middle + branch).astype(jnp.bfloat16))
    gradient, moved, attn_gain_grad = exchange(
        3,
        contract_cols(after(qkv_back, qkv_grad), qkv_full).astype(jnp.bfloat16),
        (stream, gradient, as_row(attn_scale)),
        (whole(jnp.float32), whole(jnp.bfloat16), gain_sum),
        stream_pull_rows,
        False,
    )
    devices = gains.shape[0]
    sums = jnp.concatenate(
        [
            part.reshape(devices, -1)
            for part in (attn_gain_grad[0], mlp_gain_grad[0], q_gain_grad[0], k_gain_grad[0])
        ],
        axis=1,
    )
    sums = jnp.pad(sums, ((0, 0), (0, 1024 - sums.shape[1]))).reshape(devices, 8, 128)
    sums = gain_total(sums).reshape(1, -1)
    moved = trade(moved)
    gradient = jnp.where(core == lax.axis_index("h"), gradient, moved.astype(jnp.float32))


    attn_grad, attn_sent = return_blocks(after(attn_rows, attn_gain_grad))
    activations = after(activations, attn_sent)
    mid_sum_near = after(mid_sum_near, attn_sent)
    split_at = down_rows.shape[1]
    down_grad = columns_of(*return_halves(down_grads[:, :split_at], down_grads[:, split_at:]))
    mine, other = return_halves(mid_sum_near, mid_sum_far)
    gate_grad = columns_of(mine[:, :half_cols], other[:, :half_cols])
    up_grad = columns_of(mine[:, half_cols:], other[:, half_cols:])

    return (
        activations,
        gradient,
        sums[:, :cut],
        attn_grad[None, :, :q_cols],
        attn_grad[None, :, q_cols : q_cols + kv_cols],
        attn_grad[None, :, q_cols + kv_cols : q_cols + 2 * kv_cols],
        attn_grad[None, :, q_cols + 2 * kv_cols :],
        sums[:, 2 * cut : 2 * cut + head_cut],
        sums[:, 2 * cut + head_cut : 2 * cut + 2 * head_cut],
        sums[:, cut : 2 * cut],
        gate_grad[None],
        up_grad[None],
        down_grad[None],
    )


def solution(mesh):
    dp, tensor = mesh.shape["dp"], mesh.shape["tensor"]
    cut = Mesh(mesh.devices.reshape(dp // 2, 2, 2, tensor // 2), ("d", "c", "h", "l"))
    rows, cols = ("d", "c"), ("h", "l")
    tokens, labels = P(rows + cols, None), P(rows, None)
    gain, weight = P(None, rows), P(None, rows, cols)
    return jax.shard_map(
        per_device,
        mesh=cut,
        in_specs=(
            tokens,
            labels,
            gain,
            weight,
            weight,
            weight,
            weight,
            gain,
            gain,
            gain,
            weight,
            weight,
            weight,
            tokens,
        ),
        out_specs=(
            tokens,
            tokens,
            gain,
            weight,
            weight,
            weight,
            weight,
            gain,
            gain,
            gain,
            weight,
            weight,
            weight,
        ),
        check_vma=False,
    )
```

```python
import functools

import jax
import jax.numpy as jnp
from jax import lax
from jax.experimental import pallas as pl
from jax.experimental.pallas import tpu as pltpu
from jax.sharding import Mesh
from jax.sharding import PartitionSpec as P


HEAD_WIDTH = 128
NSEQ = 3


EPS = 1e-06
THETA = 1000000.0


def rms_scale(values, gain):
    return values * lax.rsqrt(jnp.mean(values * values, axis=-1, keepdims=True) + EPS) * gain


def swiglu(gate_raw, up_raw):
    return jax.nn.silu(gate_raw) * up_raw


def rotary_tables(sequence_labels, row_index):
    labels = jnp.arange(NSEQ, dtype=jnp.int32)
    starts = jnp.sum((sequence_labels[None, :] < labels[:, None]).astype(jnp.int32), axis=1)
    first_row = jnp.sum(
        jnp.where(sequence_labels[:, None] == labels[None, :], starts[None, :], 0), axis=1
    )
    position = (row_index - first_row).astype(jnp.float32)
    frequency = THETA ** (-(jnp.arange(HEAD_WIDTH // 2, dtype=jnp.float32) * (2.0 / HEAD_WIDTH)))
    angles = position[:, None] * frequency[None, :]
    sine = jnp.sin(angles)
    cosine = jnp.cos(angles)
    return (
        jnp.concatenate([cosine, cosine], axis=1),
        jnp.concatenate([-sine, sine], axis=1),
        first_row[:, None],
    )


def contract_rows(left, right):
    return lax.dot_general(
        left, right, (((0,), (0,)), ((), ())), preferred_element_type=jnp.float32
    )


def contract_cols(left, right):
    return lax.dot_general(
        left, right, (((1,), (1,)), ((), ())), preferred_element_type=jnp.float32
    )


MESH = pl.DeviceIdType.MESH
CHUNKS = 3


def remote(source, target, send_sem, recv_sem, **place):
    return pltpu.make_async_remote_copy(
        src_ref=source,
        dst_ref=target,
        send_sem=send_sem,
        recv_sem=recv_sem,
        device_id=place,
        device_id_type=MESH,
    )


def rows_at(index, size):
    return pl.ds(pl.multiple_of(index * size, size), size)


WEIGHTS = 5
ENTRY_START = (
    "w0", "t0", "w1", "w2", "t1", "w3", "w4", "t2",
)
ENTRY_ORDER = (
    "s0", "t0", "s1", "r0", "s2", "r1", "t1", "s3", "r2", "s4", "r3", "t2", "r4", "a0", "a1",
    "a2",
)


def hop_plan(nd, d):
    if nd == 4:
        side_x = d + 1 - 2 * lax.rem(d, 2)
        side_y = d + 2 - 4 * (d // 2)
        corner = side_x + side_y - d
        hops = (
            (0, d, side_x),
            (1, d, side_x),
            (0, d, side_y),
            (1, d, side_y),
            (0, side_x, side_y),
            (1, side_y, side_x),
        )
        sources = ((0, side_x), (1, side_x), (0, side_y), (1, side_y), (0, corner), (1, corner))
        return hops, sources, 4, ((0, 4), (3, 5))
    steps = [(part, step) for step in range(1, nd) for part in range(2)]
    hops = tuple((part, d, lax.rem(d + step, nd)) for part, step in steps)
    sources = tuple((part, lax.rem(d + nd - step, nd)) for part, step in steps)
    return hops, sources, len(hops), ()


def hop_count(nd):
    return 6 if nd == 4 else 2 * (nd - 1)


class Spread:
    def __init__(self, nd, d, block, send_sem, recv_sem, own=None):
        self.hops, self.sources, self.first, self.relayed = hop_plan(nd, d)
        self.block, self.send_sem, self.recv_sem = block, send_sem, recv_sem
        self.own = own or (lambda j, part: block(j, d * 2 + part))

    def copy(self, j, kind, source, part, of):
        return remote(
            source,
            self.block(j, of * 2 + part),
            self.send_sem.at[j, kind],
            self.recv_sem.at[j, kind],
            d=self.hops[kind][2],
        )

    def hop(self, j, kind):
        part, of, _ = self.hops[kind]
        source = self.own(j, part) if kind < self.first else self.block(j, of * 2 + part)
        return self.copy(j, kind, source, part, of)

    def arrived(self, j, kind):
        part, of = self.sources[kind]
        return self.copy(j, kind, self.block(j, of * 2 + part), part, of)

    def send(self, j, part):
        for kind in range(self.first):
            if self.hops[kind][0] == part:
                self.hop(j, kind).start()

    def relay(self, j):
        for after_kind, kind in self.relayed:
            self.arrived(j, after_kind).wait_recv()
            self.hop(j, kind).start()

    def finish(self, j):
        handled = {after_kind for after_kind, _ in self.relayed}
        for kind in range(len(self.hops)):
            if kind not in handled:
                self.arrived(j, kind).wait_recv()
            self.hop(j, kind).wait_send()


def entry_kernel(nd, tl, *refs):
    (q_ref, k_ref, v_ref, o_ref, gate_ref, up_ref, down_ref, tok_ref, cot_ref, gain_ref) = refs[:10]
    (qkv_full, o_full, mid_rows, down_rows, tok_full, cot_own, gain_full) = refs[10:17]
    (stage, half_stage, tok_stage, cot_stage) = refs[17:21]
    (zs, zr, cs, li, lo, xs, xr, ts, tr, tli, tlo, ls, lr, fs, fr) = refs[21:36]
    (gs, gr, gl, os, orv, oi, hs, hr, hi, ho) = refs[36:]
    d, c, h, l = (lax.axis_index(name) for name in ("d", "c", "h", "l"))
    same = c == h
    apart = c != h
    rows = q_ref.shape[0]
    own = tok_ref.shape[0]
    chunk = own // CHUNKS
    q_cols, kv_cols = q_ref.shape[1], k_ref.shape[1]
    o_half = o_ref.shape[1] // 2
    qkv_cols = q_cols + 2 * kv_cols
    weights = (
        (q_ref, qkv_full, 0, q_cols, 0),
        (k_ref, qkv_full, q_cols, kv_cols, q_cols),
        (v_ref, qkv_full, q_cols + kv_cols, kv_cols, q_cols + kv_cols),
        (o_ref.at[:, pl.ds(0, o_half)], o_full, 0, o_half, qkv_cols),
        (o_ref.at[:, pl.ds(o_half, o_half)], o_full, o_half, o_half, qkv_cols + o_half),
    )

    def block(j, row):
        _, full, start, cols, _ = weights[j]
        return full.at[rows_at(row, rows), pl.ds(start, cols)]

    def held(j):
        _, _, _, cols, start = weights[j]
        return stage.at[:, pl.ds(start, cols)]

    def from_far(j, part):
        return remote(block(j, d * 2 + part), block(j, d * 2 + part), zs.at[j], zr.at[j, part], h=1 - h)

    def to_far(j):
        return remote(weights[j][0], block(j, d * 2 + c), zs.at[j], zr.at[j, c], c=h, h=1 - h)

    def to_core(j):
        return remote(weights[j][0], block(j, d * 2 + c), cs.at[j], zr.at[j, c], c=h)

    def local_in(j):
        return pltpu.make_async_copy(weights[j][0], held(j), li.at[j])

    def local_out(j):
        return pltpu.make_async_copy(held(j), block(j, d * 2 + c), lo.at[j])

    def tokens_at(index, k):
        return tok_full.at[pl.ds(index * own + k * chunk, chunk)]

    def trade_tokens(k):
        return remote(tok_ref.at[pl.ds(k * chunk, chunk)], tokens_at(0, k), ts.at[k], tr.at[k], c=h, h=c)

    def along(step, k):
        return remote(
            tokens_at(0, k),
            tokens_at(tl - step, k),
            ls.at[(step - 1) * CHUNKS + k],
            lr.at[(tl - step - 1) * CHUNKS + k],
            l=lax.rem(l + step, tl),
        )

    def from_along(index, k):
        return remote(
            tokens_at(index, k),
            tokens_at(index, k),
            ls.at[(index - 1) * CHUNKS + k],
            lr.at[(index - 1) * CHUNKS + k],
            l=l,
        )

    def across(index, k):
        at = index * CHUNKS + k
        return remote(tokens_at(index, k), tokens_at(tl + index, k), fs.at[at], fr.at[at], c=1 - c)

    def gain_peer(step):
        place = lax.rem(d * 2 + c + step, 2 * nd)
        return place // 2, lax.rem(place, 2)

    def gains_to(step):
        to_d, to_c = gain_peer(step)
        return remote(
            gain_ref, gain_full.at[d * 2 + c], gs.at[step - 1], gr.at[2 * nd - step - 1], d=to_d, c=to_c
        )

    def gains_from(step):
        from_d, from_c = gain_peer(step)
        return remote(
            gain_ref, gain_full.at[from_d * 2 + from_c], gs.at[step - 1], gr.at[step - 1], d=from_d, c=from_c
        )

    def local_gains():
        return pltpu.make_async_copy(gain_ref, gain_full.at[d * 2 + c], gl)

    half = gate_ref.shape[1] // 2
    halves = ((gate_ref, mid_rows, 0), (up_ref, mid_rows, half), (down_ref, down_rows, 0))

    def columns_of_core(j, of):
        return halves[j][0].at[:, pl.ds(pl.multiple_of(of * half, half), half)]

    def half_at(j, of):
        return halves[j][1].at[rows_at(of, rows), pl.ds(halves[j][2], half)]

    def half_to_core(j):
        return remote(columns_of_core(j, 1 - c), half_at(j, c), hs.at[j], hr.at[j], c=1 - c)

    def half_from_core(j):
        return remote(half_at(j, 1 - c), half_at(j, 1 - c), hs.at[j], hr.at[j], c=1 - c)

    def half_in(j):
        return pltpu.make_async_copy(columns_of_core(j, c), half_stage.at[j], hi.at[j])

    def half_out(j):
        return pltpu.make_async_copy(half_stage.at[j], half_at(j, c), ho.at[j])

    local_gains().start()

    def start_weights(j):
        to_far(j).start()

        @pl.when(apart)
        def _():
            to_core(j).start()

    def start_tokens(k):
        @pl.when(apart)
        def _():
            trade_tokens(k).start()

    def trade_cotangent():
        return remote(cot_ref, cot_own, os, orv, c=h, h=c)

    def cotangent_in():
        return pltpu.make_async_copy(cot_ref, cot_stage, oi)

    def cotangent_out():
        return pltpu.make_async_copy(cot_stage, cot_own, oi)

    for step in ENTRY_START:
        {"w": start_weights, "t": start_tokens}[step[0]](int(step[1:]))

    @pl.when(apart)
    def _():
        trade_cotangent().start()

    @pl.when(same)
    def _():
        pltpu.make_async_copy(tok_ref, tok_stage, tli).start()
        for j in range(WEIGHTS):
            local_in(j).start()
        pltpu.make_async_copy(tok_ref, tok_stage, tli).wait()
        for k in range(CHUNKS):
            part = pl.ds(k * chunk, chunk)
            pltpu.make_async_copy(tok_stage.at[part], tokens_at(0, k), tlo.at[k]).start()
        for j in range(WEIGHTS):
            local_in(j).wait()
            local_out(j).start()
        cotangent_in().start()
        cotangent_in().wait()
        cotangent_out().start()

    for step in range(1, 2 * nd):
        gains_to(step).start()
    for j in range(3):
        half_in(j).start()
        half_to_core(j).start()
    for j in range(3):
        half_in(j).wait()
        half_out(j).start()

    over_d = Spread(nd, d, block, xs, xr)

    def spread(j):
        for part in range(2):
            here = jnp.logical_and(same, c == part)

            @pl.when(here)
            def _():
                local_out(j).wait()

            @pl.when(jnp.logical_not(here))
            def _():
                from_far(j, part).wait_recv()

            over_d.send(j, part)

    relay = over_d.relay

    def own_tokens(k):
        @pl.when(same)
        def _():
            part = pl.ds(k * chunk, chunk)
            pltpu.make_async_copy(tok_stage.at[part], tokens_at(0, k), tlo.at[k]).wait()

        @pl.when(apart)
        def _():
            remote(tokens_at(0, k), tokens_at(0, k), ts.at[k], tr.at[k], c=1 - c, h=1 - h).wait_recv()

        for step in range(1, tl):
            along(step, k).start()
        across(0, k).start()

    def pass_across(k):
        for index in range(1, tl):
            from_along(index, k).wait_recv()
            across(index, k).start()

    steps = {"t": own_tokens, "s": spread, "r": relay, "a": pass_across}
    for step in ENTRY_ORDER:
        steps[step[0]](int(step[1:]))

    for j in range(WEIGHTS):
        over_d.finish(j)
        to_far(j).wait_send()
    for k in range(CHUNKS):
        for index in range(tl):
            across(index, k).wait()
        for step in range(1, tl):
            along(step, k).wait_send()
    for step in range(1, 2 * nd):
        gains_from(step).wait_recv()
        gains_to(step).wait_send()
    local_gains().wait()
    for j in range(3):
        half_from_core(j).wait_recv()
        half_to_core(j).wait_send()
        half_out(j).wait()

    @pl.when(same)
    def _():
        cotangent_out().wait()

    @pl.when(apart)
    def _():
        trade_cotangent().wait()
        for j in range(WEIGHTS):
            to_core(j).wait_send()
        for k in range(CHUNKS):
            trade_tokens(k).wait_send()


def enter(q_weight, k_weight, v_weight, o_weight, gate, up, down, tokens, cotangent, gains):
    nd, tl = lax.axis_size("d"), lax.axis_size("l")
    rows, q_cols = q_weight.shape
    qkv_cols = q_cols + 2 * k_weight.shape[1]
    own, width = tokens.shape
    half = gate.shape[1] // 2
    dma = pltpu.SemaphoreType.DMA
    counts = (
        (WEIGHTS,),
        (WEIGHTS, 2),
        (WEIGHTS,),
        (WEIGHTS,),
        (WEIGHTS,),
        (WEIGHTS, hop_count(nd)),
        (WEIGHTS, hop_count(nd)),
        (CHUNKS,),
        (CHUNKS,),
        (),
        (CHUNKS,),
        ((tl - 1) * CHUNKS,),
        ((tl - 1) * CHUNKS,),
        (tl * CHUNKS,),
        (tl * CHUNKS,),
        (2 * nd - 1,),
        (2 * nd - 1,),
        (),
        (),
        (),
        (),
        (3,),
        (3,),
        (3,),
        (3,),
    )
    anywhere = pl.BlockSpec(memory_space=pl.ANY)

    def low(*shape):
        return jax.ShapeDtypeStruct(shape, jnp.bfloat16)

    return pl.pallas_call(
        functools.partial(entry_kernel, nd, tl),
        name="entry",
        out_shape=(
            low(width, qkv_cols),
            low(width, o_weight.shape[1]),
            low(2 * rows, 2 * half),
            low(2 * rows, half),
            low(2 * tl * own, width),
            low(own, width),
            jax.ShapeDtypeStruct((2 * nd,) + gains.shape, jnp.float32),
        ),
        in_specs=[anywhere] * 10,
        out_specs=[anywhere] * 7,
        scratch_shapes=[
            pltpu.VMEM((rows, qkv_cols + o_weight.shape[1]), jnp.bfloat16),
            pltpu.VMEM((3, rows, half), jnp.bfloat16),
            pltpu.VMEM((own, width), jnp.bfloat16),
            pltpu.VMEM((own, width), jnp.bfloat16),
        ]
        + [dma(count) if count else dma for count in counts],
        compiler_params=pltpu.CompilerParams(has_side_effects=True),
        cost_estimate=pl.CostEstimate(flops=0, bytes_accessed=250_000_000, transcendentals=0),
    )(q_weight, k_weight, v_weight, o_weight, gate, up, down, tokens, cotangent, gains)


PIECES = 6
SUM_ORDER = (
    "s3", "s4", "s5", "f0", "r3", "s0", "f1", "r4", "r0", "s1", "f2", "r5", "r1", "s2", "r2",
    "a0", "a1", "a2",
)


class Job:
    def __init__(self, inputs, shape, tiles, made):
        self.inputs, self.shape, self.tiles, self.made = inputs, shape, tiles, made

    def scratch(self):
        dma = pltpu.SemaphoreType.DMA
        return [pltpu.VMEM(value.shape, value.dtype) for value in self.inputs] + [
            pltpu.VMEM(self.shape, jnp.bfloat16),
            dma((len(self.inputs),)),
            dma((self.tiles,)),
        ]


class RunningJob:
    def __init__(self, job, given, result, scratch):
        self.job, self.given, self.result = job, given, result
        *self.held, self.product, self.in_sem, self.out_sem = scratch
        self.rows = job.shape[0] // job.tiles

    def copy_in(self, at):
        return pltpu.make_async_copy(self.given[at], self.held[at], self.in_sem.at[at])

    def copy_out(self, i):
        rows = rows_at(i, self.rows)
        return pltpu.make_async_copy(
            self.product.at[rows], self.result.at[rows], self.out_sem.at[i]
        )

    def fetch(self):
        for at in range(len(self.given)):
            self.copy_in(at).start()

    def run(self):
        for at in range(len(self.given)):
            self.copy_in(at).wait()

        def one(i, carry):
            self.product[rows_at(i, self.rows), :] = self.job.made(self.held, i, self.rows)
            self.copy_out(i).start()
            return carry

        lax.fori_loop(0, self.job.tiles, one, 0)

    def finish(self):
        for i in range(self.job.tiles):
            self.copy_out(i).wait()


def weight_grad_tile(held, i, rows):
    left, right = held
    return contract_rows(left[:, rows_at(i, rows)], right[...]).astype(jnp.bfloat16)


def down_tile(held, i, rows):
    near, far, down_near, down_far = held
    at = rows_at(i, rows)
    return (
        contract_cols(near[at, :], down_near[...]) + contract_cols(far[at, :], down_far[...])
    ).astype(jnp.bfloat16)


def exchange_kernel(
    nd, tl, epilogue, aux_count, out_count, gather, carry_weights, jobs, last, *refs
):
    partial = refs[0]
    aux = refs[1 : 1 + aux_count]
    refs = refs[1 + aux_count :]
    job_given = []
    for job in jobs:
        count = len(job.inputs)
        job_given.append(refs[:count])
        refs = refs[count:]
    if carry_weights:
        weight_rows, here_rows, refs = refs[0], refs[1], refs[2:]
    outs = refs[:out_count]
    rest = refs[out_count:]
    if gather:
        full, rest = rest[0], rest[1:]
    if carry_weights:
        weights, stage, ws, wr, xs, xr, hi, ho, rest = rest[0], *rest[1:8], rest[8:]
    job_results, rest = rest[: len(jobs)], rest[len(jobs) :]
    running = []
    for job, given, result in zip(jobs, job_given, job_results):
        count = len(job.inputs) + 3
        running.append(RunningJob(job, given, result, rest[:count]))
        rest = rest[count:]
    if last:
        low, back, gain_acc, tiles, got, ts, tr, gs, gr = rest[:9]
        rest = rest[9:]
    if gather:
        finished, ls, lr, fs, fr, keep, rest = rest[0], *rest[1:6], rest[6:]
    mine, other, sums, arrivals, cs, cr, loc, ss, sr = rest
    c, l = lax.axis_index("c"), lax.axis_index("l")
    d, h = lax.axis_index("d"), lax.axis_index("h")
    own = arrivals.shape[0] // (tl - 1)
    chunk = own // CHUNKS

    def greet():
        barrier = pltpu.get_barrier_semaphore()
        peers = [{"c": 1 - c}] + [{"l": lax.rem(l + step, tl)} for step in range(1, tl)]
        if carry_weights:
            peers += [{"h": 1 - h}] + [{"d": lax.rem(d + step, nd)} for step in range(1, nd)]
        for peer in peers:
            pl.semaphore_signal(barrier, inc=1, device_id=peer, device_id_type=MESH)
        pl.semaphore_wait(barrier, len(peers))

    if not last:
        greet()

    def part(base, k):
        return rows_at(base * CHUNKS + k, chunk)

    def to_core(index, k):
        at = index * CHUNKS + k
        return remote(
            partial.at[part(tl + index, k)], other.at[part(index, k)], cs.at[at], cr.at[at], c=1 - c
        )

    def local(index, k):
        return pltpu.make_async_copy(
            partial.at[part(index, k)], mine.at[part(index, k)], loc.at[index * CHUNKS + k]
        )

    def along(step, k):
        at = (step - 1) * CHUNKS + k
        return remote(
            sums.at[part(step - 1, k)],
            arrivals.at[part(step - 1, k)],
            ss.at[at],
            sr.at[at],
            l=lax.rem(l + step, tl),
        )

    if carry_weights:
        half = weight_rows.shape[0] // 2
        far_pieces = PIECES // 2
        piece = here_rows.shape[1] // far_pieces

        def block(j, row):
            return weights.at[rows_at(row, half), pl.ds(j * piece, piece)]

        def given(j, row_part):
            source = weight_rows if j < far_pieces else here_rows
            return source.at[pl.ds(row_part * half, half), pl.ds(j % far_pieces * piece, piece)]

        def held_here(j, row_part):
            return block(j, d * 2 + row_part) if j < far_pieces else given(j, row_part)

        def from_far(j, row_part):
            return remote(
                given(j, row_part),
                block(j, d * 2 + row_part),
                ws.at[j, row_part],
                wr.at[j, row_part],
                h=1 - h,
            )

        def here_in():
            return pltpu.make_async_copy(here_rows, stage, hi)

        def here_out():
            here = weights.at[rows_at(d, 2 * half), pl.ds(far_pieces * piece, far_pieces * piece)]
            return pltpu.make_async_copy(stage, here, ho)

        over_d = Spread(nd, d, block, xs, xr, held_here)

        def spread(j):
            for row_part in range(2):
                if j < far_pieces:
                    from_far(j, row_part).wait_recv()
                over_d.send(j, row_part)

        for j in range(far_pieces):
            for row_part in range(2):
                from_far(j, row_part).start()
        here_in().start()

    order = list(range(1, tl)) + [0]
    for index in order:
        for k in range(CHUNKS):
            to_core(index, k).start()
            local(index, k).start()

    def both(index, k):
        local(index, k).wait()
        to_core(index, k).wait_recv()
        at = part(index, k)
        return mine[at, :].astype(jnp.float32) + other[at, :].astype(jnp.float32)

    for step in range(1, tl):

        def pass_on(k, carry):
            sums[part(step - 1, k), :] = both(step, k).astype(jnp.bfloat16)
            along(step, k).start()
            return carry

        lax.fori_loop(0, CHUNKS, pass_on, 0)

    for job in running:
        job.fetch()
    if running:
        running[0].run()

    if last:
        apart = c != h
        count = 4 * nd * tl
        me = ((d * 2 + c) * 2 + h) * tl + l

        def to_owner(k):
            return remote(low.at[part(0, k)], back.at[part(0, k)], ts.at[k], tr.at[k], c=h, h=c)

        def gains_to(step):
            place = lax.rem(me + step, count)
            row = place // (2 * tl)
            return remote(
                tiles.at[row],
                got.at[step - 1],
                gs.at[step - 1],
                gr.at[step - 1],
                d=row // 2,
                c=lax.rem(row, 2),
                h=lax.rem(place // tl, 2),
                l=lax.rem(place, tl),
            )

        def start_gains(step, carry):
            gains_to(step).start()
            return carry

        def add_gains(step, total):
            gains_to(step).wait_recv()
            return total + got[step - 1]

        def drain_gains(step, carry):
            gains_to(step).wait_send()
            return carry

        def send_gains():
            cut = gain_acc.shape[1] // (2 * nd)
            lines = cut // 128
            tiles[...] = jnp.zeros_like(tiles)
            for row in range(2 * nd):
                for line in range(lines):
                    at = slice(row * cut + line * 128, row * cut + (line + 1) * 128)
                    tiles[row, line : line + 1, :] = gain_acc[:, at]
                    tiles[row, lines + line : lines + line + 1, :] = aux[3][:, at]
                tiles[row, 2 * lines : 2 * lines + 1, :] = aux[4][0:1, :]
                tiles[row, 2 * lines + 1 : 2 * lines + 2, :] = aux[5][0:1, :]
            lax.fori_loop(1, count, start_gains, 0)

    def gathered(index, k):
        return full.at[part(index, k)]

    def keep_own(k):
        return pltpu.make_async_copy(finished.at[part(0, k)], gathered(0, k), keep.at[k])

    def own_along(step, k):
        return remote(
            finished.at[part(0, k)],
            gathered(tl - step, k),
            ls.at[(step - 1) * CHUNKS + k],
            lr.at[(tl - step - 1) * CHUNKS + k],
            l=lax.rem(l + step, tl),
        )

    def from_along(index, k):
        at = (index - 1) * CHUNKS + k
        return remote(gathered(index, k), gathered(index, k), ls.at[at], lr.at[at], l=l)

    def across(index, k):
        source = finished.at[part(0, k)] if index == 0 else gathered(index, k)
        at = index * CHUNKS + k
        return remote(source, gathered(tl + index, k), fs.at[at], fr.at[at], c=1 - c)

    def finish(k, carry):
        total = both(0, k)
        for step in range(1, tl):
            along(step, k).wait_recv()
            total = total + arrivals[part(step - 1, k), :].astype(jnp.float32)
        kept = (outs[0], low, gain_acc) if last else outs
        row = epilogue(total, part(0, k), k, aux[:3], kept)
        if last:

            @pl.when(apart)
            def _():
                to_owner(k).start()

        if gather:
            finished[part(0, k), :] = row
            keep_own(k).start()
            for step in range(1, tl):
                own_along(step, k).start()
            across(0, k).start()
        return carry

    def pass_across(k):
        for index in range(1, tl):
            from_along(index, k).wait_recv()
            across(index, k).start()

    if carry_weights:
        steps = {
            "s": spread,
            "r": over_d.relay,
            "f": lambda k: finish(k, 0),
            "a": pass_across,
        }
        here_in().wait()
        here_out().start()
        for step in SUM_ORDER:
            steps[step[0]](int(step[1:]))
    else:
        lax.fori_loop(0, CHUNKS, finish, 0)
        for job in running[1:]:
            job.run()
        if gather:
            for k in range(CHUNKS):
                pass_across(k)
    if last:
        send_gains()

        @pl.when(apart)
        def _():
            for k in range(CHUNKS):
                to_owner(k).wait()
                outs[0][part(0, k), :] = back[part(0, k), :].astype(jnp.float32)

        outs[1][...] = lax.fori_loop(1, count, add_gains, tiles[d * 2 + c])
        lax.fori_loop(1, count, drain_gains, 0)
    for job in running:
        job.finish()
    if gather:
        for k in range(CHUNKS):
            keep_own(k).wait()
            for index in range(tl):
                across(index, k).wait()
            for step in range(1, tl):
                own_along(step, k).wait_send()
    if carry_weights:
        for j in range(PIECES):
            over_d.finish(j)
            if j < far_pieces:
                for row_part in range(2):
                    from_far(j, row_part).wait_send()
        here_out().wait()
    for k in range(CHUNKS):
        for index in range(tl):
            to_core(index, k).wait_send()
        for step in range(1, tl):
            along(step, k).wait_send()


def exchange(
    collective_id, partial, aux, outs, epilogue, gather, weight_rows=(), jobs=(), last=False
):
    nd, tl = lax.axis_size("d"), lax.axis_size("l")
    total, width = partial.shape
    own = total // (2 * tl)
    dma = pltpu.SemaphoreType.DMA
    vmem = pl.BlockSpec(memory_space=pltpu.VMEM)
    anywhere = pl.BlockSpec(memory_space=pl.ANY)
    out_shape = list(outs)
    out_specs = [vmem] * len(outs)
    scratch = []
    given = tuple(value for job in jobs for value in job.inputs)
    if gather:
        out_shape.append(jax.ShapeDtypeStruct((total, width), jnp.bfloat16))
        out_specs.append(anywhere)
    if weight_rows:
        rows, cols = weight_rows[1].shape
        out_shape.append(jax.ShapeDtypeStruct((nd * rows, 2 * cols), jnp.bfloat16))
        out_specs.append(anywhere)
        scratch += [
            pltpu.VMEM((rows, cols), jnp.bfloat16),
            dma((PIECES, 2)),
            dma((PIECES, 2)),
            dma((PIECES, hop_count(nd))),
            dma((PIECES, hop_count(nd))),
            dma,
            dma,
        ]
    for job in jobs:
        out_shape.append(jax.ShapeDtypeStruct(job.shape, jnp.bfloat16))
        out_specs.append(anywhere)
        scratch += job.scratch()
    if last:
        others = 4 * nd * tl - 1
        scratch += [
            pltpu.VMEM((own, width), jnp.bfloat16),
            pltpu.VMEM((own, width), jnp.bfloat16),
            pltpu.VMEM((1, width), jnp.float32),
            pltpu.VMEM((2 * nd, 8, 128), jnp.float32),
            pltpu.VMEM((others, 8, 128), jnp.float32),
            dma((CHUNKS,)),
            dma((CHUNKS,)),
            dma((others,)),
            dma((others,)),
        ]
    if gather:
        scratch += [
            pltpu.VMEM((own, width), jnp.bfloat16),
            dma(((tl - 1) * CHUNKS,)),
            dma(((tl - 1) * CHUNKS,)),
            dma((tl * CHUNKS,)),
            dma((tl * CHUNKS,)),
            dma((CHUNKS,)),
        ]
    scratch += [
        pltpu.VMEM((tl * own, width), jnp.bfloat16),
        pltpu.VMEM((tl * own, width), jnp.bfloat16),
        pltpu.VMEM(((tl - 1) * own, width), jnp.bfloat16),
        pltpu.VMEM(((tl - 1) * own, width), jnp.bfloat16),
        dma((tl * CHUNKS,)),
        dma((tl * CHUNKS,)),
        dma((tl * CHUNKS,)),
        dma(((tl - 1) * CHUNKS,)),
        dma(((tl - 1) * CHUNKS,)),
    ]
    return pl.pallas_call(
        functools.partial(
            exchange_kernel,
            nd,
            tl,
            epilogue,
            len(aux),
            len(outs),
            gather,
            bool(weight_rows),
            jobs,
            last,
        ),
        out_shape=tuple(out_shape),
        in_specs=[anywhere] + [vmem] * len(aux) + [anywhere] * (len(given) + len(weight_rows)),
        out_specs=out_specs,
        scratch_shapes=scratch,
        compiler_params=pltpu.CompilerParams(
            has_side_effects=True, collective_id=collective_id, vmem_limit_bytes=60 << 20
        ),
        cost_estimate=pl.CostEstimate(
            flops=0, bytes_accessed=200_000_000 if gather else 110_000_000, transcendentals=0
        ),
    )(partial, *aux, *given, *weight_rows)


def middle_rows(total, rows, k, aux, outs):
    stream, gain = aux
    value = stream[rows, :].astype(jnp.float32) + total
    outs[0][rows, :] = value
    return rms_scale(value, gain[...]).astype(jnp.bfloat16)


def norm_pull(value, gain, grad):
    scale = lax.rsqrt(jnp.mean(value * value, axis=-1, keepdims=True) + EPS)
    scaled = grad * gain
    inner = jnp.mean(value * scaled, axis=-1, keepdims=True)
    return scale * scaled - value * (scale * scale * scale * inner), jnp.sum(
        grad * value * scale, axis=0, keepdims=True
    )


def add_rows(out, value, k):
    @pl.when(k == 0)
    def _():
        out[...] = value

    @pl.when(k > 0)
    def _():
        out[...] += value


def middle_pull_rows(total, rows, k, aux, outs):
    middle, cotangent, gain = aux
    pulled, gain_part = norm_pull(middle[rows, :], gain[...], total)
    value = cotangent[rows, :].astype(jnp.float32) + pulled
    outs[0][rows, :] = value
    add_rows(outs[1], gain_part, k)
    return value.astype(jnp.bfloat16)


def stream_pull_rows(total, rows, k, aux, outs):
    stream, gradient, gain = aux
    pulled, gain_part = norm_pull(stream[rows, :].astype(jnp.float32), gain[...], total)
    value = gradient[rows, :] + pulled
    outs[0][rows, :] = value
    outs[1][rows, :] = value.astype(jnp.bfloat16)
    add_rows(outs[2], gain_part, k)
    return None


def key_tile(rows):
    return next(size for size in (384, 256, 128) if rows % size == 0)


def turn(values):
    return pltpu.roll(values, HEAD_WIDTH // 2, 1)


def head_norm(values):
    return lax.rsqrt(jnp.mean(values * values, axis=-1, keepdims=True) + EPS)


def tile_mask(first, start, tile, row0, rows):
    keys = start + lax.broadcasted_iota(jnp.int32, (rows, tile), 1)
    last = row0 + lax.broadcasted_iota(jnp.int32, (rows, tile), 0)
    return jnp.logical_and(keys >= first, keys <= last)


def dot_last(left, right):
    return lax.dot_general(
        left, right, (((1,), (1,)), ((), ())), preferred_element_type=jnp.float32
    )


def attention_kernel(blocks, repeat, order_ref, *refs):
    q, k, v, cosine, sine, q_gain, k_gain, first = refs[:8]
    qr, kr, vb, out, total = refs[8:13]
    acc, den = refs[13:]
    rows = q.shape[0] // blocks
    tile = key_tile(q.shape[0])
    scale = HEAD_WIDTH**-0.5

    def rotated(values, gain, at):
        scaled = values * head_norm(values) * gain
        return (scaled * cosine[at, :] + turn(scaled) * sine[at, :]).astype(jnp.bfloat16)

    def prepare(i, carry):
        at, to = rows_at(i, rows), rows_at(order_ref[i], rows)
        for r in range(repeat):
            head = slice(r * HEAD_WIDTH, (r + 1) * HEAD_WIDTH)
            qr[at, head] = rotated(q[at, head], q_gain[...], at)
        kr[to, :] = rotated(k[at, :], k_gain[...], at)
        vb[to, :] = v[at, :].astype(jnp.bfloat16)
        return carry

    lax.fori_loop(0, blocks, prepare, 0)

    def attend(i, carry):
        at = rows_at(i, rows)
        row0 = order_ref[i] * rows
        acc[...] = jnp.zeros_like(acc)
        den[...] = jnp.zeros_like(den)

        def over_keys(t, inner):
            keys = rows_at(t, tile)
            mask = tile_mask(first[at, :], t * tile, tile, row0, rows)
            for r in range(repeat):
                head = slice(r * HEAD_WIDTH, (r + 1) * HEAD_WIDTH)
                scores = dot_last(qr[at, head], kr[keys, :]) * scale
                weights = jnp.where(mask, jnp.exp(scores), 0.0)
                den[r] += jnp.sum(weights, axis=-1, keepdims=True)
                acc[r] += jnp.dot(
                    weights.astype(jnp.bfloat16), vb[keys, :], preferred_element_type=jnp.float32
                )
            return inner

        lax.fori_loop(0, (row0 + rows + tile - 1) // tile, over_keys, 0)
        for r in range(repeat):
            head = slice(r * HEAD_WIDTH, (r + 1) * HEAD_WIDTH)
            out[at, head] = (acc[r] / den[r]).astype(jnp.bfloat16)
            total[at, r : r + 1] = den[r]
        return carry

    lax.fori_loop(0, blocks, attend, 0)


def attention_specs(rows, q_heads, kv_heads):
    repeat = q_heads // kv_heads

    def columns(width, start=0):
        return pl.BlockSpec((rows, width * HEAD_WIDTH), lambda g, order: (0, start // width + g))

    def fixed(*shape):
        return pl.BlockSpec(shape, lambda g, order: (0, 0))

    raw = [columns(repeat), columns(1, q_heads), columns(1, q_heads + kv_heads)]
    tables = [
        fixed(rows, HEAD_WIDTH),
        fixed(rows, HEAD_WIDTH),
        fixed(1, HEAD_WIDTH),
        fixed(1, HEAD_WIDTH),
        fixed(rows, 1),
    ]
    return repeat, columns, fixed, raw, tables


def attention(qkv, tables, order, q_heads, kv_heads):
    rows = qkv.shape[0]
    blocks = order.shape[0]
    repeat, columns, _, raw, table_specs = attention_specs(rows, q_heads, kv_heads)
    wide, narrow = q_heads * HEAD_WIDTH, kv_heads * HEAD_WIDTH
    return pl.pallas_call(
        functools.partial(attention_kernel, blocks, repeat),
        name="attention",
        out_shape=(
            jax.ShapeDtypeStruct((rows, wide), jnp.bfloat16),
            jax.ShapeDtypeStruct((rows, narrow), jnp.bfloat16),
            jax.ShapeDtypeStruct((rows, narrow), jnp.bfloat16),
            jax.ShapeDtypeStruct((rows, wide), jnp.bfloat16),
            jax.ShapeDtypeStruct((rows, narrow), jnp.float32),
        ),
        grid_spec=pltpu.PrefetchScalarGridSpec(
            num_scalar_prefetch=1,
            grid=(kv_heads,),
            in_specs=raw + table_specs,
            out_specs=[columns(repeat), columns(1), columns(1), columns(repeat), columns(1)],
            scratch_shapes=[
                pltpu.VMEM((repeat, rows // blocks, HEAD_WIDTH), jnp.float32),
                pltpu.VMEM((repeat, rows // blocks, 1), jnp.float32),
            ],
        ),
        compiler_params=pltpu.CompilerParams(vmem_limit_bytes=50 << 20),
        cost_estimate=pl.CostEstimate(
            flops=4 * rows * rows * wide, bytes_accessed=60_000_000, transcendentals=0
        ),
    )(order, qkv, qkv, qkv, *tables)


def attention_pull_kernel(blocks, repeat, order_ref, *refs):
    q, k, cosine, sine, q_gain, k_gain, first, qr, kr, vb, total, grad = refs[:12]
    dq, dk, dv, dq_gain, dk_gain = refs[12:17]
    shares, share_grads, dq_acc, dk_acc, dv_acc, inner_sum = refs[17:]
    rows = q.shape[0] // blocks
    tile = key_tile(q.shape[0])
    scale = HEAD_WIDTH**-0.5
    dk_acc[...] = jnp.zeros_like(dk_acc)
    dv_acc[...] = jnp.zeros_like(dv_acc)

    @pl.when(pl.program_id(0) == 0)
    def _():
        dq_gain[...] = jnp.zeros_like(dq_gain)
        dk_gain[...] = jnp.zeros_like(dk_gain)

    def pull(raw, gain, turned_grad, at, gain_out):
        scaled_grad = turned_grad * cosine[at, :] + turn(turned_grad * sine[at, :])
        r = head_norm(raw)
        gain_out[0:1, :] += jnp.sum(scaled_grad * raw * r, axis=0, keepdims=True)
        scaled = scaled_grad * gain
        inner = jnp.mean(raw * scaled, axis=-1, keepdims=True)
        return (r * scaled - raw * (r * r * r * inner)).astype(jnp.bfloat16)

    def over_rows(i, carry):
        at = rows_at(i, rows)
        row0 = order_ref[i] * rows
        tiles = (row0 + rows + tile - 1) // tile
        dq_acc[...] = jnp.zeros_like(dq_acc)
        inner_sum[...] = jnp.zeros_like(inner_sum)

        def first_pass(t, inner):
            keys = rows_at(t, tile)
            mask = tile_mask(first[at, :], t * tile, tile, row0, rows)
            for r in range(repeat):
                head = slice(r * HEAD_WIDTH, (r + 1) * HEAD_WIDTH)
                scores = dot_last(qr[at, head], kr[keys, :]) * scale
                share = jnp.where(mask, jnp.exp(scores), 0.0) * (1.0 / total[at, r : r + 1])
                share_grad = dot_last(grad[at, head], vb[keys, :])
                inner_sum[r] += jnp.sum(share * share_grad, axis=-1, keepdims=True)
                shares[t, r] = share
                share_grads[t, r] = share_grad
            return inner

        lax.fori_loop(0, tiles, first_pass, 0)

        def second_pass(t, inner):
            keys = rows_at(t, tile)
            for r in range(repeat):
                head = slice(r * HEAD_WIDTH, (r + 1) * HEAD_WIDTH)
                share = shares[t, r]
                score_grad = (share * (share_grads[t, r] - inner_sum[r])).astype(jnp.bfloat16)
                dq_acc[r] += jnp.dot(score_grad, kr[keys, :], preferred_element_type=jnp.float32)
                dk_acc[keys, :] += contract_rows(score_grad, qr[at, head])
                dv_acc[keys, :] += contract_rows(share.astype(jnp.bfloat16), grad[at, head])
            return inner

        lax.fori_loop(0, tiles, second_pass, 0)
        for r in range(repeat):
            head = slice(r * HEAD_WIDTH, (r + 1) * HEAD_WIDTH)
            dq[at, head] = pull(q[at, head], q_gain[...], dq_acc[r] * scale, at, dq_gain)
        return carry

    lax.fori_loop(0, blocks, over_rows, 0)

    def finish(i, carry):
        at, to = rows_at(i, rows), rows_at(order_ref[i], rows)
        dk[at, :] = pull(k[at, :], k_gain[...], dk_acc[to, :] * scale, at, dk_gain)
        dv[at, :] = dv_acc[to, :].astype(jnp.bfloat16)
        return carry

    lax.fori_loop(0, blocks, finish, 0)


def attention_pull(qkv, tables, order, kept, grad, q_heads, kv_heads):
    rows = qkv.shape[0]
    blocks = order.shape[0]
    repeat, columns, fixed, raw, table_specs = attention_specs(rows, q_heads, kv_heads)
    wide, narrow = q_heads * HEAD_WIDTH, kv_heads * HEAD_WIDTH
    own, tile = rows // blocks, key_tile(rows)
    return pl.pallas_call(
        functools.partial(attention_pull_kernel, blocks, repeat),
        out_shape=(
            jax.ShapeDtypeStruct((rows, wide), jnp.bfloat16),
            jax.ShapeDtypeStruct((rows, narrow), jnp.bfloat16),
            jax.ShapeDtypeStruct((rows, narrow), jnp.bfloat16),
            jax.ShapeDtypeStruct((8, HEAD_WIDTH), jnp.float32),
            jax.ShapeDtypeStruct((8, HEAD_WIDTH), jnp.float32),
        ),
        grid_spec=pltpu.PrefetchScalarGridSpec(
            num_scalar_prefetch=1,
            grid=(kv_heads,),
            in_specs=raw[:2]
            + table_specs
            + [columns(repeat), columns(1), columns(1), columns(1), columns(repeat)],
            out_specs=[
                columns(repeat),
                columns(1),
                columns(1),
                fixed(8, HEAD_WIDTH),
                fixed(8, HEAD_WIDTH),
            ],
            scratch_shapes=[
                pltpu.VMEM((rows // tile, repeat, own, tile), jnp.float32),
                pltpu.VMEM((rows // tile, repeat, own, tile), jnp.float32),
                pltpu.VMEM((repeat, own, HEAD_WIDTH), jnp.float32),
                pltpu.VMEM((rows, HEAD_WIDTH), jnp.float32),
                pltpu.VMEM((rows, HEAD_WIDTH), jnp.float32),
                pltpu.VMEM((repeat, own, 1), jnp.float32),
            ],
        ),
        compiler_params=pltpu.CompilerParams(vmem_limit_bytes=56 << 20),
        cost_estimate=pl.CostEstimate(
            flops=10 * rows * rows * wide, bytes_accessed=120_000_000, transcendentals=0
        ),
    )(order, qkv, qkv, *tables, *kept, grad)


def shift_perm(size, step):
    return [((place + step) % size, place) for place in range(size)]


def trade(values):
    return lax.ppermute(values, ("c", "h"), [(0, 0), (1, 2), (2, 1), (3, 3)])


def gather_along(own):
    places = lax.axis_size("l")
    return [own] + [lax.ppermute(own, "l", shift_perm(places, step)) for step in range(1, places)]


def gather_across(parts):
    half = jnp.concatenate(parts, axis=0)
    other = lax.ppermute(half, "c", shift_perm(2, 1))
    return jnp.concatenate([half, other], axis=0)


def scatter_tokens(partial, *first):
    places = lax.axis_size("l")
    half = partial.shape[0] // 2
    rows = half // places
    other = lax.ppermute(partial[half:].astype(jnp.bfloat16), "c", shift_perm(2, 1))
    total = partial[:half] + other.astype(jnp.float32)
    own = total[:rows]
    for step in range(1, places):
        sent = total[step * rows : (step + 1) * rows].astype(jnp.bfloat16)
        moved = lax.ppermute(sent, "l", shift_perm(places, -step))
        moved = after(moved, *first)
        own = own + moved.astype(jnp.float32)
    return own


def after(value, *others):
    return lax.optimization_barrier((value,) + others)[0]


def return_halves(near, far):
    core = lax.axis_index("c")
    far = lax.ppermute(far, "h", shift_perm(2, 1))
    sums = near.astype(jnp.float32) + far.astype(jnp.float32)
    rows = sums.shape[0] // 2
    first, second = sums[:rows], sums[rows:]
    mine = jnp.where(core == 0, first, second)
    sent = jnp.where(core == 0, second, first).astype(jnp.bfloat16)
    other = lax.ppermute(sent, "c", shift_perm(2, 1)).astype(jnp.float32)
    return mine, other


def columns_of(mine, other):
    core = lax.axis_index("c")
    return jnp.concatenate(
        [jnp.where(core == 0, mine, other), jnp.where(core == 0, other, mine)], axis=1
    )


def sum_over_d(partial):
    return lax.psum_scatter(partial.astype(jnp.bfloat16), "d", scatter_dimension=0, tiled=True)


def as_row(values):
    return values.reshape(1, -1)


def split(values):
    half = values.shape[1] // 2
    return values[:, :half], values[:, half:]


def return_blocks(rows):
    core, upper = lax.axis_index("c"), lax.axis_index("h")
    half = rows.shape[0] // 2
    first, second = rows[:half], rows[half:]
    mine = jnp.where(core == 0, first, second)
    other = lax.ppermute(jnp.where(core == 0, second, first), "c", shift_perm(2, 1))
    same = core == upper
    sent = jnp.where(same, other, mine)
    far = lax.ppermute(sent, "h", shift_perm(2, 1))
    return jnp.where(same, mine, other).astype(jnp.float32) + far.astype(jnp.float32), sent


def per_device(
    tokens,
    segment_ids,
    attn_gain,
    q_weight,
    key_matrix,
    value_matrix,
    o_weight,
    q_gain,
    k_gain,
    mlp_gain,
    gate_weight,
    up_weight,
    down_weight,
    cotangent,
):
    width = attn_gain.shape[1] * lax.axis_size("d") * 2
    own_rows = tokens.shape[0]
    places = lax.axis_size("l")
    core, place = lax.axis_index("c"), lax.axis_index("l")
    q_cols, kv_cols, ff_cols = q_weight.shape[2], key_matrix.shape[2], gate_weight.shape[2]
    half_cols = ff_cols // 2

    cut = attn_gain.shape[1]
    head_cut = q_gain.shape[1]
    gains = jnp.concatenate([attn_gain[0], mlp_gain[0], q_gain[0], k_gain[0]]).astype(jnp.float32)
    gains = jnp.pad(gains, (0, 1024 - gains.shape[0])).reshape(8, 128)
    labels = trade(segment_ids)[0]
    order = jnp.stack(
        [
            ((core + core_step) % 2) * places + (place + step) % places
            for core_step in range(2)
            for step in range(places)
        ]
    )
    row_index = (order[:, None] * own_rows + jnp.arange(own_rows, dtype=jnp.int32)[None, :]).reshape(-1)
    labels = labels.reshape(2 * places, own_rows)[order].reshape(-1)
    cosine, sine, first_row = rotary_tables(labels, row_index)
    qkv_full, o_full, mid_rows, down_rows, group, cotangent, gains = enter(
        q_weight[0],
        key_matrix[0],
        value_matrix[0],
        o_weight[0],
        gate_weight[0],
        up_weight[0],
        down_weight[0],
        after(tokens, cosine, sine, first_row),
        cotangent,
        gains,
    )
    mid_near = lax.all_gather(mid_rows, "d", axis=0, tiled=True)
    down_near = lax.all_gather(down_rows, "d", axis=0, tiled=True)
    up_far = lax.ppermute(mid_rows[:, half_cols:], "h", shift_perm(2, 1))
    down_far = lax.ppermute(down_rows, "h", shift_perm(2, 1))
    grad_half = gather_along(cotangent)
    gains = gains.reshape(gains.shape[0], -1)
    attn_scale = gains[:, :cut].reshape(-1)
    mlp_scale = gains[:, cut : 2 * cut].reshape(-1)
    q_scale = gains[:, 2 * cut : 2 * cut + head_cut].reshape(-1)
    k_scale = gains[:, 2 * cut + head_cut : 2 * cut + 2 * head_cut].reshape(-1)

    stream = group[:own_rows]
    normed = rms_scale(group.astype(jnp.float32), attn_scale).astype(jnp.bfloat16)
    head_count, kv_heads = q_cols // HEAD_WIDTH, kv_cols // HEAD_WIDTH
    qkv = jnp.dot(normed, qkv_full, preferred_element_type=jnp.float32)
    tables = (cosine, sine, as_row(q_scale), as_row(k_scale), first_row)
    query_reduced, key_reduced, value_reduced, attended, totals = attention(
        qkv, tables, order, head_count, kv_heads
    )

    grad_rows = gather_across([grad_half[0]] + [after(part, attended) for part in grad_half[1:]])

    def whole(values):
        return jax.ShapeDtypeStruct((own_rows, width), values)

    gain_sum = jax.ShapeDtypeStruct((1, width), jnp.float32)
    middle, normed_mid, mid_far = exchange(
        1,
        contract_cols(attended, o_full).astype(jnp.bfloat16),
        (stream, as_row(mlp_scale)),
        (whole(jnp.float32),),
        middle_rows,
        True,
        (mid_rows, after(up_far, attended)),
    )
    down_far = lax.all_gather(after(down_far, normed_mid), "d", axis=0, tiled=True)

    mid = jnp.dot(normed_mid, mid_near, preferred_element_type=jnp.float32)
    gate_near, up_near = split(mid)
    hidden_near = swiglu(gate_near, up_near).astype(jnp.bfloat16)
    mid = jnp.dot(normed_mid, mid_far, preferred_element_type=jnp.float32)
    gate_far, up_far = split(mid)
    hidden_far = swiglu(gate_far, up_far).astype(jnp.bfloat16)
    down_grad_far = contract_rows(grad_rows, hidden_far).astype(jnp.bfloat16)
    down_sum_far = sum_over_d(down_grad_far)
    down_grad_near = contract_rows(grad_rows, hidden_near).astype(jnp.bfloat16)
    down_sum_near = sum_over_d(down_grad_near)
    grad_rows = after(grad_rows, down_grad_near, down_grad_far)

    def hidden_pull(gate, up, down):
        hidden_grad = jnp.dot(grad_rows, down, preferred_element_type=jnp.float32)
        _, pull_back = jax.vjp(swiglu, gate, up)
        gate_grad, up_grad = pull_back(hidden_grad)
        return jnp.concatenate(
            [gate_grad.astype(jnp.bfloat16), up_grad.astype(jnp.bfloat16)], axis=1
        )

    mid_back_near = hidden_pull(gate_near, up_near, down_near)
    mid_back_far = hidden_pull(gate_far, up_far, down_far)
    mid_grad_far = contract_rows(normed_mid, mid_back_far).astype(jnp.bfloat16)
    mid_sum_far = sum_over_d(mid_grad_far)
    normed_grad = contract_cols(mid_back_near, mid_near) + contract_cols(mid_back_far, mid_far)
    normed_grad = normed_grad.astype(jnp.bfloat16)
    gradient, mlp_gain_grad, grad_rows, mid_grad_near, branch = exchange(
        2,
        after(normed_grad, mid_grad_far),
        (middle, cotangent, as_row(mlp_scale)),
        (whole(jnp.float32), gain_sum),
        middle_pull_rows,
        True,
        jobs=(
            Job((normed_mid, mid_back_near), mid_near.shape, 8, weight_grad_tile),
            Job((hidden_near, hidden_far, down_near, down_far), normed_mid.shape, 4, down_tile),
        ),
    )
    mid_sum_near = sum_over_d(mid_grad_near)

    out_grad = jnp.dot(grad_rows, o_full, preferred_element_type=jnp.float32).astype(jnp.bfloat16)
    o_wgrad = contract_rows(grad_rows, attended)
    query_back, key_back, value_back, q_gain_grad, k_gain_grad = attention_pull(
        qkv,
        tables,
        order,
        (query_reduced, key_reduced, value_reduced, totals),
        out_grad,
        head_count,
        kv_heads,
    )
    qkv_back = jnp.concatenate([query_back, key_back, value_back], axis=1)
    qkv_grad = contract_rows(normed, qkv_back).astype(jnp.bfloat16)
    attn_partial = jnp.concatenate([qkv_grad, o_wgrad.astype(jnp.bfloat16)], axis=1)
    attn_rows = sum_over_d(after(attn_partial, mid_sum_far))
    branch = scatter_tokens(branch, qkv_grad)
    activations = trade((middle + branch).astype(jnp.bfloat16))
    gradient, sums = exchange(
        None,
        contract_cols(after(qkv_back, qkv_grad), qkv_full).astype(jnp.bfloat16),
        (stream, gradient, as_row(attn_scale), mlp_gain_grad, q_gain_grad, k_gain_grad),
        (whole(jnp.float32), jax.ShapeDtypeStruct((8, 128), jnp.float32)),
        stream_pull_rows,
        False,
        last=True,
    )
    lines = cut // 128
    head_at = (lax.axis_index("d") * 2 + core) * head_cut

    def head_gain(line):
        return lax.dynamic_slice(sums[line], (head_at,), (head_cut,))[None]

    attn_grad, attn_sent = return_blocks(after(attn_rows, sums))
    activations = after(activations, attn_sent)
    mid_sum_near = after(mid_sum_near, attn_sent)
    down_grad = columns_of(*return_halves(down_sum_near, down_sum_far))
    mine, other = return_halves(mid_sum_near, mid_sum_far)
    gate_grad = columns_of(mine[:, :half_cols], other[:, :half_cols])
    up_grad = columns_of(mine[:, half_cols:], other[:, half_cols:])

    return (
        activations,
        gradient,
        sums[:lines].reshape(1, cut),
        attn_grad[None, :, :q_cols],
        attn_grad[None, :, q_cols : q_cols + kv_cols],
        attn_grad[None, :, q_cols + kv_cols : q_cols + 2 * kv_cols],
        attn_grad[None, :, q_cols + 2 * kv_cols :],
        head_gain(2 * lines),
        head_gain(2 * lines + 1),
        sums[lines : 2 * lines].reshape(1, cut),
        gate_grad[None],
        up_grad[None],
        down_grad[None],
    )


def solution(mesh):
    dp, tensor = mesh.shape["dp"], mesh.shape["tensor"]
    cut = Mesh(mesh.devices.reshape(dp // 2, 2, 2, tensor // 2), ("d", "c", "h", "l"))
    rows, cols = ("d", "c"), ("h", "l")
    tokens, labels = P(rows + cols, None), P(rows, None)
    gain, weight = P(None, rows), P(None, rows, cols)
    return jax.shard_map(
        per_device,
        mesh=cut,
        in_specs=(
            tokens,
            labels,
            gain,
            weight,
            weight,
            weight,
            weight,
            gain,
            gain,
            gain,
            weight,
            weight,
            weight,
            tokens,
        ),
        out_specs=(
            tokens,
            tokens,
            gain,
            weight,
            weight,
            weight,
            weight,
            gain,
            gain,
            gain,
            weight,
            weight,
            weight,
        ),
        check_vma=False,
    )
```

```python
import functools

import jax
import jax.numpy as jnp
from jax import lax
from jax.experimental import pallas as pl
from jax.experimental.pallas import tpu as pltpu
from jax.sharding import Mesh
from jax.sharding import PartitionSpec as P


HEAD_WIDTH = 128
NSEQ = 3


EPS = 1e-06
THETA = 1000000.0


def rms_scale(values, gain):
    return values * lax.rsqrt(jnp.mean(values * values, axis=-1, keepdims=True) + EPS) * gain


def swiglu(gate_raw, up_raw):
    return jax.nn.silu(gate_raw) * up_raw


def rotary_tables(sequence_labels, row_index):
    labels = jnp.arange(NSEQ, dtype=jnp.int32)
    starts = jnp.sum((sequence_labels[None, :] < labels[:, None]).astype(jnp.int32), axis=1)
    first_row = jnp.sum(
        jnp.where(sequence_labels[:, None] == labels[None, :], starts[None, :], 0), axis=1
    )
    position = (row_index - first_row).astype(jnp.float32)
    frequency = THETA ** (-(jnp.arange(HEAD_WIDTH // 2, dtype=jnp.float32) * (2.0 / HEAD_WIDTH)))
    angles = position[:, None] * frequency[None, :]
    sine = jnp.sin(angles)
    cosine = jnp.cos(angles)
    return (
        jnp.concatenate([cosine, cosine], axis=1),
        jnp.concatenate([-sine, sine], axis=1),
        first_row[:, None],
    )


def contract_rows(left, right):
    return lax.dot_general(
        left, right, (((0,), (0,)), ((), ())), preferred_element_type=jnp.float32
    )


def contract_cols(left, right):
    return lax.dot_general(
        left, right, (((1,), (1,)), ((), ())), preferred_element_type=jnp.float32
    )


MESH = pl.DeviceIdType.MESH
CHUNKS = 3


def remote(source, target, send_sem, recv_sem, **place):
    return pltpu.make_async_remote_copy(
        src_ref=source,
        dst_ref=target,
        send_sem=send_sem,
        recv_sem=recv_sem,
        device_id=place,
        device_id_type=MESH,
    )


def rows_at(index, size):
    return pl.ds(pl.multiple_of(index * size, size), size)


WEIGHTS = 5
ENTRY_START = (
    "w0", "t0", "w1", "w2", "t1", "w3", "w4", "t2",
)
ENTRY_ORDER = (
    "s0", "t0", "s1", "r0", "s2", "r1", "t1", "s3", "r2", "s4", "r3", "t2", "r4", "a0", "a1",
    "a2",
)


def hop_plan(nd, d):
    if nd == 4:
        side_x = d + 1 - 2 * lax.rem(d, 2)
        side_y = d + 2 - 4 * (d // 2)
        corner = side_x + side_y - d
        hops = (
            (0, d, side_x),
            (1, d, side_x),
            (0, d, side_y),
            (1, d, side_y),
            (0, side_x, side_y),
            (1, side_y, side_x),
        )
        sources = ((0, side_x), (1, side_x), (0, side_y), (1, side_y), (0, corner), (1, corner))
        return hops, sources, 4, ((0, 4), (3, 5))
    steps = [(part, step) for step in range(1, nd) for part in range(2)]
    hops = tuple((part, d, lax.rem(d + step, nd)) for part, step in steps)
    sources = tuple((part, lax.rem(d + nd - step, nd)) for part, step in steps)
    return hops, sources, len(hops), ()


def hop_count(nd):
    return 6 if nd == 4 else 2 * (nd - 1)


class Spread:
    def __init__(self, nd, d, block, send_sem, recv_sem, own=None):
        self.hops, self.sources, self.first, self.relayed = hop_plan(nd, d)
        self.block, self.send_sem, self.recv_sem = block, send_sem, recv_sem
        self.own = own or (lambda j, part: block(j, d * 2 + part))

    def copy(self, j, kind, source, part, of):
        return remote(
            source,
            self.block(j, of * 2 + part),
            self.send_sem.at[j, kind],
            self.recv_sem.at[j, kind],
            d=self.hops[kind][2],
        )

    def hop(self, j, kind):
        part, of, _ = self.hops[kind]
        source = self.own(j, part) if kind < self.first else self.block(j, of * 2 + part)
        return self.copy(j, kind, source, part, of)

    def arrived(self, j, kind):
        part, of = self.sources[kind]
        return self.copy(j, kind, self.block(j, of * 2 + part), part, of)

    def send(self, j, part):
        for kind in range(self.first):
            if self.hops[kind][0] == part:
                self.hop(j, kind).start()

    def relay(self, j):
        for after_kind, kind in self.relayed:
            self.arrived(j, after_kind).wait_recv()
            self.hop(j, kind).start()

    def finish(self, j):
        handled = {after_kind for after_kind, _ in self.relayed}
        for kind in range(len(self.hops)):
            if kind not in handled:
                self.arrived(j, kind).wait_recv()
            self.hop(j, kind).wait_send()


def entry_kernel(nd, tl, *refs):
    (q_ref, k_ref, v_ref, o_ref, gate_ref, up_ref, down_ref, tok_ref, cot_ref, gain_ref) = refs[:10]
    (qkv_full, o_full, mid_rows, down_rows, tok_full, cot_own, gain_full) = refs[10:17]
    (stage, half_stage, tok_stage, cot_stage) = refs[17:21]
    (zs, zr, cs, li, lo, xs, xr, ts, tr, tli, tlo, ls, lr, fs, fr) = refs[21:36]
    (gs, gr, gl, os, orv, oi, hs, hr, hi, ho) = refs[36:]
    d, c, h, l = (lax.axis_index(name) for name in ("d", "c", "h", "l"))
    same = c == h
    apart = c != h
    rows = q_ref.shape[0]
    own = tok_ref.shape[0]
    chunk = own // CHUNKS
    q_cols, kv_cols = q_ref.shape[1], k_ref.shape[1]
    o_half = o_ref.shape[1] // 2
    qkv_cols = q_cols + 2 * kv_cols
    weights = (
        (q_ref, qkv_full, 0, q_cols, 0),
        (k_ref, qkv_full, q_cols, kv_cols, q_cols),
        (v_ref, qkv_full, q_cols + kv_cols, kv_cols, q_cols + kv_cols),
        (o_ref.at[:, pl.ds(0, o_half)], o_full, 0, o_half, qkv_cols),
        (o_ref.at[:, pl.ds(o_half, o_half)], o_full, o_half, o_half, qkv_cols + o_half),
    )

    def block(j, row):
        _, full, start, cols, _ = weights[j]
        return full.at[rows_at(row, rows), pl.ds(start, cols)]

    def held(j):
        _, _, _, cols, start = weights[j]
        return stage.at[:, pl.ds(start, cols)]

    def from_far(j, part):
        return remote(block(j, d * 2 + part), block(j, d * 2 + part), zs.at[j], zr.at[j, part], h=1 - h)

    def to_far(j):
        return remote(weights[j][0], block(j, d * 2 + c), zs.at[j], zr.at[j, c], c=h, h=1 - h)

    def to_core(j):
        return remote(weights[j][0], block(j, d * 2 + c), cs.at[j], zr.at[j, c], c=h)

    def local_in(j):
        return pltpu.make_async_copy(weights[j][0], held(j), li.at[j])

    def local_out(j):
        return pltpu.make_async_copy(held(j), block(j, d * 2 + c), lo.at[j])

    def tokens_at(index, k):
        return tok_full.at[pl.ds(index * own + k * chunk, chunk)]

    def trade_tokens(k):
        return remote(tok_ref.at[pl.ds(k * chunk, chunk)], tokens_at(0, k), ts.at[k], tr.at[k], c=h, h=c)

    def along(step, k):
        return remote(
            tokens_at(0, k),
            tokens_at(tl - step, k),
            ls.at[(step - 1) * CHUNKS + k],
            lr.at[(tl - step - 1) * CHUNKS + k],
            l=lax.rem(l + step, tl),
        )

    def from_along(index, k):
        return remote(
            tokens_at(index, k),
            tokens_at(index, k),
            ls.at[(index - 1) * CHUNKS + k],
            lr.at[(index - 1) * CHUNKS + k],
            l=l,
        )

    def across(index, k):
        at = index * CHUNKS + k
        return remote(tokens_at(index, k), tokens_at(tl + index, k), fs.at[at], fr.at[at], c=1 - c)

    def gain_peer(step):
        place = lax.rem(d * 2 + c + step, 2 * nd)
        return place // 2, lax.rem(place, 2)

    def gains_to(step):
        to_d, to_c = gain_peer(step)
        return remote(
            gain_ref, gain_full.at[d * 2 + c], gs.at[step - 1], gr.at[2 * nd - step - 1], d=to_d, c=to_c
        )

    def gains_from(step):
        from_d, from_c = gain_peer(step)
        return remote(
            gain_ref, gain_full.at[from_d * 2 + from_c], gs.at[step - 1], gr.at[step - 1], d=from_d, c=from_c
        )

    def local_gains():
        return pltpu.make_async_copy(gain_ref, gain_full.at[d * 2 + c], gl)

    half = gate_ref.shape[1] // 2
    halves = ((gate_ref, mid_rows, 0), (up_ref, mid_rows, half), (down_ref, down_rows, 0))

    def columns_of_core(j, of):
        return halves[j][0].at[:, pl.ds(pl.multiple_of(of * half, half), half)]

    def half_at(j, of):
        return halves[j][1].at[rows_at(of, rows), pl.ds(halves[j][2], half)]

    def half_to_core(j):
        return remote(columns_of_core(j, 1 - c), half_at(j, c), hs.at[j], hr.at[j], c=1 - c)

    def half_from_core(j):
        return remote(half_at(j, 1 - c), half_at(j, 1 - c), hs.at[j], hr.at[j], c=1 - c)

    def half_in(j):
        return pltpu.make_async_copy(columns_of_core(j, c), half_stage.at[j], hi.at[j])

    def half_out(j):
        return pltpu.make_async_copy(half_stage.at[j], half_at(j, c), ho.at[j])

    local_gains().start()

    def start_weights(j):
        to_far(j).start()

        @pl.when(apart)
        def _():
            to_core(j).start()

    def start_tokens(k):
        @pl.when(apart)
        def _():
            trade_tokens(k).start()

    def trade_cotangent():
        return remote(cot_ref, cot_own, os, orv, c=h, h=c)

    def cotangent_in():
        return pltpu.make_async_copy(cot_ref, cot_stage, oi)

    def cotangent_out():
        return pltpu.make_async_copy(cot_stage, cot_own, oi)

    for step in ENTRY_START:
        {"w": start_weights, "t": start_tokens}[step[0]](int(step[1:]))

    @pl.when(apart)
    def _():
        trade_cotangent().start()

    @pl.when(same)
    def _():
        pltpu.make_async_copy(tok_ref, tok_stage, tli).start()
        for j in range(WEIGHTS):
            local_in(j).start()
        pltpu.make_async_copy(tok_ref, tok_stage, tli).wait()
        for k in range(CHUNKS):
            part = pl.ds(k * chunk, chunk)
            pltpu.make_async_copy(tok_stage.at[part], tokens_at(0, k), tlo.at[k]).start()
        for j in range(WEIGHTS):
            local_in(j).wait()
            local_out(j).start()
        cotangent_in().start()
        cotangent_in().wait()
        cotangent_out().start()

    for step in range(1, 2 * nd):
        gains_to(step).start()
    for j in range(3):
        half_in(j).start()
        half_to_core(j).start()
    for j in range(3):
        half_in(j).wait()
        half_out(j).start()

    over_d = Spread(nd, d, block, xs, xr)

    def spread(j):
        for part in range(2):
            here = jnp.logical_and(same, c == part)

            @pl.when(here)
            def _():
                local_out(j).wait()

            @pl.when(jnp.logical_not(here))
            def _():
                from_far(j, part).wait_recv()

            over_d.send(j, part)

    relay = over_d.relay

    def own_tokens(k):
        @pl.when(same)
        def _():
            part = pl.ds(k * chunk, chunk)
            pltpu.make_async_copy(tok_stage.at[part], tokens_at(0, k), tlo.at[k]).wait()

        @pl.when(apart)
        def _():
            remote(tokens_at(0, k), tokens_at(0, k), ts.at[k], tr.at[k], c=1 - c, h=1 - h).wait_recv()

        for step in range(1, tl):
            along(step, k).start()
        across(0, k).start()

    def pass_across(k):
        for index in range(1, tl):
            from_along(index, k).wait_recv()
            across(index, k).start()

    steps = {"t": own_tokens, "s": spread, "r": relay, "a": pass_across}
    for step in ENTRY_ORDER:
        steps[step[0]](int(step[1:]))

    for j in range(WEIGHTS):
        over_d.finish(j)
        to_far(j).wait_send()
    for k in range(CHUNKS):
        for index in range(tl):
            across(index, k).wait()
        for step in range(1, tl):
            along(step, k).wait_send()
    for step in range(1, 2 * nd):
        gains_from(step).wait_recv()
        gains_to(step).wait_send()
    local_gains().wait()
    for j in range(3):
        half_from_core(j).wait_recv()
        half_to_core(j).wait_send()
        half_out(j).wait()

    @pl.when(same)
    def _():
        cotangent_out().wait()

    @pl.when(apart)
    def _():
        trade_cotangent().wait()
        for j in range(WEIGHTS):
            to_core(j).wait_send()
        for k in range(CHUNKS):
            trade_tokens(k).wait_send()


def enter(q_weight, k_weight, v_weight, o_weight, gate, up, down, tokens, cotangent, gains):
    nd, tl = lax.axis_size("d"), lax.axis_size("l")
    rows, q_cols = q_weight.shape
    qkv_cols = q_cols + 2 * k_weight.shape[1]
    own, width = tokens.shape
    half = gate.shape[1] // 2
    dma = pltpu.SemaphoreType.DMA
    counts = (
        (WEIGHTS,),
        (WEIGHTS, 2),
        (WEIGHTS,),
        (WEIGHTS,),
        (WEIGHTS,),
        (WEIGHTS, hop_count(nd)),
        (WEIGHTS, hop_count(nd)),
        (CHUNKS,),
        (CHUNKS,),
        (),
        (CHUNKS,),
        ((tl - 1) * CHUNKS,),
        ((tl - 1) * CHUNKS,),
        (tl * CHUNKS,),
        (tl * CHUNKS,),
        (2 * nd - 1,),
        (2 * nd - 1,),
        (),
        (),
        (),
        (),
        (3,),
        (3,),
        (3,),
        (3,),
    )
    anywhere = pl.BlockSpec(memory_space=pl.ANY)

    def low(*shape):
        return jax.ShapeDtypeStruct(shape, jnp.bfloat16)

    return pl.pallas_call(
        functools.partial(entry_kernel, nd, tl),
        name="entry",
        out_shape=(
            low(width, qkv_cols),
            low(width, o_weight.shape[1]),
            low(2 * rows, 2 * half),
            low(2 * rows, half),
            low(2 * tl * own, width),
            low(own, width),
            jax.ShapeDtypeStruct((2 * nd,) + gains.shape, jnp.float32),
        ),
        in_specs=[anywhere] * 10,
        out_specs=[anywhere] * 7,
        scratch_shapes=[
            pltpu.VMEM((rows, qkv_cols + o_weight.shape[1]), jnp.bfloat16),
            pltpu.VMEM((3, rows, half), jnp.bfloat16),
            pltpu.VMEM((own, width), jnp.bfloat16),
            pltpu.VMEM((own, width), jnp.bfloat16),
        ]
        + [dma(count) if count else dma for count in counts],
        compiler_params=pltpu.CompilerParams(has_side_effects=True),
        cost_estimate=pl.CostEstimate(flops=0, bytes_accessed=250_000_000, transcendentals=0),
    )(q_weight, k_weight, v_weight, o_weight, gate, up, down, tokens, cotangent, gains)


PIECES = 6
RETURN_AHEAD = 2
RETURN_ORDER = (
    "m0", "w2", "f0", "m1", "w3", "f1", "h0", "m2", "w4", "f2", "g0", "h1", "m3", "w5", "h2", "m4",
    "h3", "m5", "h4", "h5",
)
SUM_ORDER = (
    "s3", "s4", "s5", "f0", "r3", "s0", "f1", "r4", "r0", "s1", "f2", "r5", "r1", "s2", "r2",
    "a0", "a1", "a2",
)


class Return:
    def __init__(self, nd, pieces, out, scratch):
        self.nd, self.pieces, self.out = nd, pieces, out
        self.held, self.first, self.mixed, self.second, self.sums, self.parts = scratch[:6]
        (self.load, self.fs, self.fr, self.ss, self.sr, self.ps, self.pr) = scratch[6:]
        self.d, self.c, self.h = (lax.axis_index(name) for name in ("d", "c", "h"))
        self.rows = out.shape[0]
        d = self.d
        if nd == 4:
            side_x = d + 1 - 2 * lax.rem(d, 2)
            side_y = d + 2 - 4 * (d // 2)
            corner = side_x + side_y - d
            self.blocks = ((d, 0), (side_y, 0), (d, 1), (side_x, 1))
            self.sends = (
                (side_x, 0, side_x),
                (corner, 0, side_x),
                (side_y, 1, side_y),
                (corner, 1, side_y),
            )
            self.mixes = ((1, side_y), (3, side_x))
        else:
            self.blocks = ((d, 0), (d, 1))
            self.sends = tuple(
                (lax.rem(d + step, nd), part, lax.rem(d + step, nd))
                for step in range(1, nd)
                for part in range(2)
            )
            self.mixes = ()

    @staticmethod
    def scratch(nd, count, rows, cols):
        dma = pltpu.SemaphoreType.DMA
        blocks, sends, mixes = (4, 4, 2) if nd == 4 else (2, 2 * (nd - 1), 1)

        def buffer(number):
            return pltpu.VMEM((count, number, rows, cols), jnp.bfloat16)

        return [
            buffer(blocks),
            buffer(sends),
            buffer(mixes),
            buffer(mixes),
            buffer(2),
            buffer(2),
            dma((count, blocks)),
            dma((count, sends)),
            dma((count, sends)),
            dma((count, mixes)),
            dma((count, mixes)),
            dma((count, 2)),
            dma((count, 2)),
        ]

    def source(self, j, of, part):
        ref, start = self.pieces[j]
        cols = self.held.shape[3]
        return ref.at[rows_at(of * 2 + part, self.rows), pl.ds(start, cols)]

    def loading(self, j, at):
        return pltpu.make_async_copy(
            self.source(j, *self.blocks[at]), self.held.at[j, at], self.load.at[j, at]
        )

    def sending(self, j, at):
        of, part, to = self.sends[at]
        return remote(
            self.source(j, of, part), self.first.at[j, at], self.fs.at[j, at], self.fr.at[j, at], d=to
        )

    def mixing(self, j, at):
        return remote(
            self.mixed.at[j, at],
            self.second.at[j, at],
            self.ss.at[j, at],
            self.sr.at[j, at],
            d=self.mixes[at][1],
        )

    def handing(self, j, part):
        return remote(
            self.sums.at[j, part],
            self.parts.at[j, self.h],
            self.ps.at[j, part],
            self.pr.at[j, self.h],
            c=part,
            h=self.c,
        )

    def stays(self, part):
        return jnp.logical_and(self.c == part, self.h == self.c)

    def start(self, j):
        for at in range(len(self.sends)):
            self.sending(j, at).start()
        for at in range(len(self.blocks)):
            self.loading(j, at).start()

    def value(self, ref, j, at):
        return ref[j, at].astype(jnp.float32)

    def mix(self, j):
        for at, (block, _) in enumerate(self.mixes):
            self.loading(j, block).wait()
            self.sending(j, block).wait_recv()
            total = self.value(self.held, j, block) + self.value(self.first, j, block)
            self.mixed[j, at] = total.astype(jnp.bfloat16)
            self.mixing(j, at).start()

    def hand(self, j):
        for part in range(2):
            own = 2 * part if self.mixes else part
            self.loading(j, own).wait()
            total = self.value(self.held, j, own)
            for at in [own] if self.mixes else range(part, len(self.sends), 2):
                self.sending(j, at).wait_recv()
                total = total + self.value(self.first, j, at)
            if self.mixes:
                self.mixing(j, part).wait_recv()
                total = total + self.value(self.second, j, part)
            self.sums[j, part] = total.astype(jnp.bfloat16)

            @pl.when(self.stays(part))
            def _():
                self.parts[j, self.h] = self.sums[j, part]

            @pl.when(jnp.logical_not(self.stays(part)))
            def _():
                self.handing(j, part).start()

    def arriving(self, j, of_h):
        return remote(
            self.parts.at[j, of_h], self.parts.at[j, of_h], self.ps.at[j, 0], self.pr.at[j, of_h], h=1 - self.h
        )

    def finish(self, j):
        for of_h in range(2):

            @pl.when(jnp.logical_not(jnp.logical_and(self.c == self.h, self.h == of_h)))
            def _():
                self.arriving(j, of_h).wait_recv()

        cols = self.held.shape[3]
        total = self.value(self.parts, j, 0) + self.value(self.parts, j, 1)
        self.out[:, j * cols : (j + 1) * cols] = total
        for at in range(len(self.sends)):
            self.sending(j, at).wait_send()
        for at in range(len(self.mixes)):
            self.mixing(j, at).wait_send()
        for part in range(2):

            @pl.when(jnp.logical_not(self.stays(part)))
            def _():
                self.handing(j, part).wait_send()


class Job:
    def __init__(self, inputs, shape, tiles, made):
        self.inputs, self.shape, self.tiles, self.made = inputs, shape, tiles, made

    def scratch(self):
        dma = pltpu.SemaphoreType.DMA
        return [pltpu.VMEM(value.shape, value.dtype) for value in self.inputs] + [
            pltpu.VMEM(self.shape, jnp.bfloat16),
            dma((len(self.inputs),)),
            dma((self.tiles,)),
        ]


class RunningJob:
    def __init__(self, job, given, result, scratch):
        self.job, self.given, self.result = job, given, result
        *self.held, self.product, self.in_sem, self.out_sem = scratch
        self.rows = job.shape[0] // job.tiles

    def copy_in(self, at):
        return pltpu.make_async_copy(self.given[at], self.held[at], self.in_sem.at[at])

    def copy_out(self, i):
        rows = rows_at(i, self.rows)
        return pltpu.make_async_copy(
            self.product.at[rows], self.result.at[rows], self.out_sem.at[i]
        )

    def fetch(self):
        for at in range(len(self.given)):
            self.copy_in(at).start()

    def run(self):
        for at in range(len(self.given)):
            self.copy_in(at).wait()

        def one(i, carry):
            self.product[rows_at(i, self.rows), :] = self.job.made(self.held, i, self.rows)
            self.copy_out(i).start()
            return carry

        lax.fori_loop(0, self.job.tiles, one, 0)

    def finish(self):
        for i in range(self.job.tiles):
            self.copy_out(i).wait()


def weight_grad_tile(held, i, rows):
    left, right = held
    return contract_rows(left[:, rows_at(i, rows)], right[...]).astype(jnp.bfloat16)


def down_tile(held, i, rows):
    near, far, down_near, down_far = held
    at = rows_at(i, rows)
    return (
        contract_cols(near[at, :], down_near[...]) + contract_cols(far[at, :], down_far[...])
    ).astype(jnp.bfloat16)


def exchange_kernel(
    nd, tl, epilogue, aux_count, out_count, gather, carry_weights, jobs, last, *refs
):
    partial = refs[0]
    aux = refs[1 : 1 + aux_count]
    refs = refs[1 + aux_count :]
    job_given = []
    for job in jobs:
        count = len(job.inputs)
        job_given.append(refs[:count])
        refs = refs[count:]
    if carry_weights:
        weight_rows, here_rows, refs = refs[0], refs[1], refs[2:]
    gradients, refs = refs[:last], refs[last:]
    outs = refs[:out_count]
    rest = refs[out_count:]
    if gather:
        full, rest = rest[0], rest[1:]
    if carry_weights:
        weights, stage, ws, wr, xs, xr, hi, ho, rest = rest[0], *rest[1:8], rest[8:]
    job_results, rest = rest[: len(jobs)], rest[len(jobs) :]
    running = []
    for job, given, result in zip(jobs, job_given, job_results):
        count = len(job.inputs) + 3
        running.append(RunningJob(job, given, result, rest[:count]))
        rest = rest[count:]
    if last:
        low, back, gain_acc, tiles, got, ts, tr, gs, gr = rest[:9]
        returned, rest = rest[9:22], rest[22:]
        cols = returned[0].shape[3]
        pieces = [
            (array, start) for array in gradients for start in range(0, array.shape[1], cols)
        ]
        back_home = Return(nd, pieces, outs[2], returned)
    if gather:
        finished, ls, lr, fs, fr, keep, rest = rest[0], *rest[1:6], rest[6:]
    mine, other, sums, arrivals, cs, cr, loc, ss, sr = rest
    c, l = lax.axis_index("c"), lax.axis_index("l")
    d, h = lax.axis_index("d"), lax.axis_index("h")
    own = arrivals.shape[0] // (tl - 1)
    chunk = own // CHUNKS

    def greet():
        barrier = pltpu.get_barrier_semaphore()
        peers = [{"c": 1 - c}] + [{"l": lax.rem(l + step, tl)} for step in range(1, tl)]
        if carry_weights:
            peers += [{"h": 1 - h}] + [{"d": lax.rem(d + step, nd)} for step in range(1, nd)]
        for peer in peers:
            pl.semaphore_signal(barrier, inc=1, device_id=peer, device_id_type=MESH)
        pl.semaphore_wait(barrier, len(peers))

    if not last:
        greet()

    def part(base, k):
        return rows_at(base * CHUNKS + k, chunk)

    def to_core(index, k):
        at = index * CHUNKS + k
        return remote(
            partial.at[part(tl + index, k)], other.at[part(index, k)], cs.at[at], cr.at[at], c=1 - c
        )

    def local(index, k):
        return pltpu.make_async_copy(
            partial.at[part(index, k)], mine.at[part(index, k)], loc.at[index * CHUNKS + k]
        )

    def along(step, k):
        at = (step - 1) * CHUNKS + k
        return remote(
            sums.at[part(step - 1, k)],
            arrivals.at[part(step - 1, k)],
            ss.at[at],
            sr.at[at],
            l=lax.rem(l + step, tl),
        )

    if carry_weights:
        half = weight_rows.shape[0] // 2
        far_pieces = PIECES // 2
        piece = here_rows.shape[1] // far_pieces

        def block(j, row):
            return weights.at[rows_at(row, half), pl.ds(j * piece, piece)]

        def given(j, row_part):
            source = weight_rows if j < far_pieces else here_rows
            return source.at[pl.ds(row_part * half, half), pl.ds(j % far_pieces * piece, piece)]

        def held_here(j, row_part):
            return block(j, d * 2 + row_part) if j < far_pieces else given(j, row_part)

        def from_far(j, row_part):
            return remote(
                given(j, row_part),
                block(j, d * 2 + row_part),
                ws.at[j, row_part],
                wr.at[j, row_part],
                h=1 - h,
            )

        def here_in():
            return pltpu.make_async_copy(here_rows, stage, hi)

        def here_out():
            here = weights.at[rows_at(d, 2 * half), pl.ds(far_pieces * piece, far_pieces * piece)]
            return pltpu.make_async_copy(stage, here, ho)

        over_d = Spread(nd, d, block, xs, xr, held_here)

        def spread(j):
            for row_part in range(2):
                if j < far_pieces:
                    from_far(j, row_part).wait_recv()
                over_d.send(j, row_part)

        for j in range(far_pieces):
            for row_part in range(2):
                from_far(j, row_part).start()
        here_in().start()

    order = list(range(1, tl)) + [0]
    for index in order:
        for k in range(CHUNKS):
            to_core(index, k).start()
            local(index, k).start()

    if last:
        for j in range(RETURN_AHEAD):
            back_home.start(j)

    def both(index, k):
        local(index, k).wait()
        to_core(index, k).wait_recv()
        at = part(index, k)
        return mine[at, :].astype(jnp.float32) + other[at, :].astype(jnp.float32)

    for step in range(1, tl):

        def pass_on(k, carry):
            sums[part(step - 1, k), :] = both(step, k).astype(jnp.bfloat16)
            along(step, k).start()
            return carry

        lax.fori_loop(0, CHUNKS, pass_on, 0)

    for job in running:
        job.fetch()
    if running:
        running[0].run()

    if last:
        apart = c != h
        count = 4 * nd * tl
        me = ((d * 2 + c) * 2 + h) * tl + l

        def to_owner(k):
            return remote(low.at[part(0, k)], back.at[part(0, k)], ts.at[k], tr.at[k], c=h, h=c)

        def gains_to(step):
            place = lax.rem(me + step, count)
            row = place // (2 * tl)
            return remote(
                tiles.at[row],
                got.at[step - 1],
                gs.at[step - 1],
                gr.at[step - 1],
                d=row // 2,
                c=lax.rem(row, 2),
                h=lax.rem(place // tl, 2),
                l=lax.rem(place, tl),
            )

        def start_gains(step, carry):
            gains_to(step).start()
            return carry

        def add_gains(step, total):
            gains_to(step).wait_recv()
            return total + got[step - 1]

        def drain_gains(step, carry):
            gains_to(step).wait_send()
            return carry

        def send_gains(_):
            cut = gain_acc.shape[1] // (2 * nd)
            lines = cut // 128
            tiles[...] = jnp.zeros_like(tiles)
            for row in range(2 * nd):
                for line in range(lines):
                    at = slice(row * cut + line * 128, row * cut + (line + 1) * 128)
                    tiles[row, line : line + 1, :] = gain_acc[:, at]
                    tiles[row, lines + line : lines + line + 1, :] = aux[3][:, at]
                tiles[row, 2 * lines : 2 * lines + 1, :] = aux[4][0:1, :]
                tiles[row, 2 * lines + 1 : 2 * lines + 2, :] = aux[5][0:1, :]
            lax.fori_loop(1, count, start_gains, 0)

    def gathered(index, k):
        return full.at[part(index, k)]

    def keep_own(k):
        return pltpu.make_async_copy(finished.at[part(0, k)], gathered(0, k), keep.at[k])

    def own_along(step, k):
        return remote(
            finished.at[part(0, k)],
            gathered(tl - step, k),
            ls.at[(step - 1) * CHUNKS + k],
            lr.at[(tl - step - 1) * CHUNKS + k],
            l=lax.rem(l + step, tl),
        )

    def from_along(index, k):
        at = (index - 1) * CHUNKS + k
        return remote(gathered(index, k), gathered(index, k), ls.at[at], lr.at[at], l=l)

    def across(index, k):
        source = finished.at[part(0, k)] if index == 0 else gathered(index, k)
        at = index * CHUNKS + k
        return remote(source, gathered(tl + index, k), fs.at[at], fr.at[at], c=1 - c)

    def finish(k, carry):
        total = both(0, k)
        for step in range(1, tl):
            along(step, k).wait_recv()
            total = total + arrivals[part(step - 1, k), :].astype(jnp.float32)
        kept = (outs[0], low, gain_acc) if last else outs
        row = epilogue(total, part(0, k), k, aux[:3], kept)
        if last:

            @pl.when(apart)
            def _():
                to_owner(k).start()

        if gather:
            finished[part(0, k), :] = row
            keep_own(k).start()
            for step in range(1, tl):
                own_along(step, k).start()
            across(0, k).start()
        return carry

    def pass_across(k):
        for index in range(1, tl):
            from_along(index, k).wait_recv()
            across(index, k).start()

    if carry_weights:
        steps = {
            "s": spread,
            "r": over_d.relay,
            "f": lambda k: finish(k, 0),
            "a": pass_across,
        }
        here_in().wait()
        here_out().start()
        for step in SUM_ORDER:
            steps[step[0]](int(step[1:]))
    elif last:
        steps = {
            "w": back_home.start,
            "m": back_home.mix,
            "h": back_home.hand,
            "f": lambda k: finish(k, 0),
            "g": send_gains,
        }
        for step in RETURN_ORDER:
            steps[step[0]](int(step[1:]))
    else:
        lax.fori_loop(0, CHUNKS, finish, 0)
        for job in running[1:]:
            job.run()
        if gather:
            for k in range(CHUNKS):
                pass_across(k)
    if last:
        @pl.when(apart)
        def _():
            for k in range(CHUNKS):
                to_owner(k).wait()
                outs[0][part(0, k), :] = back[part(0, k), :].astype(jnp.float32)

        outs[1][...] = lax.fori_loop(1, count, add_gains, tiles[d * 2 + c])
        lax.fori_loop(1, count, drain_gains, 0)
        for j in range(len(pieces)):
            back_home.finish(j)
    for job in running:
        job.finish()
    if gather:
        for k in range(CHUNKS):
            keep_own(k).wait()
            for index in range(tl):
                across(index, k).wait()
            for step in range(1, tl):
                own_along(step, k).wait_send()
    if carry_weights:
        for j in range(PIECES):
            over_d.finish(j)
            if j < far_pieces:
                for row_part in range(2):
                    from_far(j, row_part).wait_send()
        here_out().wait()
    for k in range(CHUNKS):
        for index in range(tl):
            to_core(index, k).wait_send()
        for step in range(1, tl):
            along(step, k).wait_send()


def exchange(collective_id, partial, aux, outs, epilogue, gather, weight_rows=(), jobs=(), last=()):
    nd, tl = lax.axis_size("d"), lax.axis_size("l")
    total, width = partial.shape
    own = total // (2 * tl)
    dma = pltpu.SemaphoreType.DMA
    vmem = pl.BlockSpec(memory_space=pltpu.VMEM)
    anywhere = pl.BlockSpec(memory_space=pl.ANY)
    out_shape = list(outs)
    out_specs = [vmem] * len(outs)
    scratch = []
    given = tuple(value for job in jobs for value in job.inputs)
    if gather:
        out_shape.append(jax.ShapeDtypeStruct((total, width), jnp.bfloat16))
        out_specs.append(anywhere)
    if weight_rows:
        rows, cols = weight_rows[1].shape
        out_shape.append(jax.ShapeDtypeStruct((nd * rows, 2 * cols), jnp.bfloat16))
        out_specs.append(anywhere)
        scratch += [
            pltpu.VMEM((rows, cols), jnp.bfloat16),
            dma((PIECES, 2)),
            dma((PIECES, 2)),
            dma((PIECES, hop_count(nd))),
            dma((PIECES, hop_count(nd))),
            dma,
            dma,
        ]
    for job in jobs:
        out_shape.append(jax.ShapeDtypeStruct(job.shape, jnp.bfloat16))
        out_specs.append(anywhere)
        scratch += job.scratch()
    if last:
        others = 4 * nd * tl - 1
        scratch += [
            pltpu.VMEM((own, width), jnp.bfloat16),
            pltpu.VMEM((own, width), jnp.bfloat16),
            pltpu.VMEM((1, width), jnp.float32),
            pltpu.VMEM((2 * nd, 8, 128), jnp.float32),
            pltpu.VMEM((others, 8, 128), jnp.float32),
            dma((CHUNKS,)),
            dma((CHUNKS,)),
            dma((others,)),
            dma((others,)),
        ]
        cols = min(array.shape[1] for array in last) // 2
        count = sum(array.shape[1] for array in last) // cols
        scratch += Return.scratch(nd, count, outs[2].shape[0], cols)
    if gather:
        scratch += [
            pltpu.VMEM((own, width), jnp.bfloat16),
            dma(((tl - 1) * CHUNKS,)),
            dma(((tl - 1) * CHUNKS,)),
            dma((tl * CHUNKS,)),
            dma((tl * CHUNKS,)),
            dma((CHUNKS,)),
        ]
    scratch += [
        pltpu.VMEM((tl * own, width), jnp.bfloat16),
        pltpu.VMEM((tl * own, width), jnp.bfloat16),
        pltpu.VMEM(((tl - 1) * own, width), jnp.bfloat16),
        pltpu.VMEM(((tl - 1) * own, width), jnp.bfloat16),
        dma((tl * CHUNKS,)),
        dma((tl * CHUNKS,)),
        dma((tl * CHUNKS,)),
        dma(((tl - 1) * CHUNKS,)),
        dma(((tl - 1) * CHUNKS,)),
    ]
    return pl.pallas_call(
        functools.partial(
            exchange_kernel,
            nd,
            tl,
            epilogue,
            len(aux),
            len(outs),
            gather,
            bool(weight_rows),
            jobs,
            len(last),
        ),
        out_shape=tuple(out_shape),
        in_specs=[anywhere] + [vmem] * len(aux) + [anywhere] * (len(given) + len(weight_rows) + len(last)),
        out_specs=out_specs,
        scratch_shapes=scratch,
        compiler_params=pltpu.CompilerParams(
            has_side_effects=True, collective_id=collective_id, vmem_limit_bytes=60 << 20
        ),
        cost_estimate=pl.CostEstimate(
            flops=0, bytes_accessed=200_000_000 if gather else 110_000_000, transcendentals=0
        ),
    )(partial, *aux, *given, *weight_rows, *last)


def middle_rows(total, rows, k, aux, outs):
    stream, gain = aux
    value = stream[rows, :].astype(jnp.float32) + total
    outs[0][rows, :] = value
    return rms_scale(value, gain[...]).astype(jnp.bfloat16)


def norm_pull(value, gain, grad):
    scale = lax.rsqrt(jnp.mean(value * value, axis=-1, keepdims=True) + EPS)
    scaled = grad * gain
    inner = jnp.mean(value * scaled, axis=-1, keepdims=True)
    return scale * scaled - value * (scale * scale * scale * inner), jnp.sum(
        grad * value * scale, axis=0, keepdims=True
    )


def add_rows(out, value, k):
    @pl.when(k == 0)
    def _():
        out[...] = value

    @pl.when(k > 0)
    def _():
        out[...] += value


def middle_pull_rows(total, rows, k, aux, outs):
    middle, cotangent, gain = aux
    pulled, gain_part = norm_pull(middle[rows, :], gain[...], total)
    value = cotangent[rows, :].astype(jnp.float32) + pulled
    outs[0][rows, :] = value
    add_rows(outs[1], gain_part, k)
    return value.astype(jnp.bfloat16)


def stream_pull_rows(total, rows, k, aux, outs):
    stream, gradient, gain = aux
    pulled, gain_part = norm_pull(stream[rows, :].astype(jnp.float32), gain[...], total)
    value = gradient[rows, :] + pulled
    outs[0][rows, :] = value
    outs[1][rows, :] = value.astype(jnp.bfloat16)
    add_rows(outs[2], gain_part, k)
    return None


def key_tile(rows):
    return next(size for size in (384, 256, 128) if rows % size == 0)


def turn(values):
    return pltpu.roll(values, HEAD_WIDTH // 2, 1)


def head_norm(values):
    return lax.rsqrt(jnp.mean(values * values, axis=-1, keepdims=True) + EPS)


def tile_mask(first, start, tile, row0, rows):
    keys = start + lax.broadcasted_iota(jnp.int32, (rows, tile), 1)
    last = row0 + lax.broadcasted_iota(jnp.int32, (rows, tile), 0)
    return jnp.logical_and(keys >= first, keys <= last)


def dot_last(left, right):
    return lax.dot_general(
        left, right, (((1,), (1,)), ((), ())), preferred_element_type=jnp.float32
    )


def attention_kernel(blocks, repeat, order_ref, *refs):
    q, k, v, cosine, sine, q_gain, k_gain, first = refs[:8]
    qr, kr, vb, out, total = refs[8:13]
    acc, den = refs[13:]
    rows = q.shape[0] // blocks
    tile = key_tile(q.shape[0])
    scale = HEAD_WIDTH**-0.5

    def rotated(values, gain, at):
        scaled = values * head_norm(values) * gain
        return (scaled * cosine[at, :] + turn(scaled) * sine[at, :]).astype(jnp.bfloat16)

    def prepare(i, carry):
        at, to = rows_at(i, rows), rows_at(order_ref[i], rows)
        for r in range(repeat):
            head = slice(r * HEAD_WIDTH, (r + 1) * HEAD_WIDTH)
            qr[at, head] = rotated(q[at, head], q_gain[...], at)
        kr[to, :] = rotated(k[at, :], k_gain[...], at)
        vb[to, :] = v[at, :].astype(jnp.bfloat16)
        return carry

    lax.fori_loop(0, blocks, prepare, 0)

    def attend(i, carry):
        at = rows_at(i, rows)
        row0 = order_ref[i] * rows
        acc[...] = jnp.zeros_like(acc)
        den[...] = jnp.zeros_like(den)

        def over_keys(t, inner):
            keys = rows_at(t, tile)
            mask = tile_mask(first[at, :], t * tile, tile, row0, rows)
            for r in range(repeat):
                head = slice(r * HEAD_WIDTH, (r + 1) * HEAD_WIDTH)
                scores = dot_last(qr[at, head], kr[keys, :]) * scale
                weights = jnp.where(mask, jnp.exp(scores), 0.0)
                den[r] += jnp.sum(weights, axis=-1, keepdims=True)
                acc[r] += jnp.dot(
                    weights.astype(jnp.bfloat16), vb[keys, :], preferred_element_type=jnp.float32
                )
            return inner

        lax.fori_loop(0, (row0 + rows + tile - 1) // tile, over_keys, 0)
        for r in range(repeat):
            head = slice(r * HEAD_WIDTH, (r + 1) * HEAD_WIDTH)
            out[at, head] = (acc[r] / den[r]).astype(jnp.bfloat16)
            total[at, r : r + 1] = den[r]
        return carry

    lax.fori_loop(0, blocks, attend, 0)


def attention_specs(rows, q_heads, kv_heads):
    repeat = q_heads // kv_heads

    def columns(width, start=0):
        return pl.BlockSpec((rows, width * HEAD_WIDTH), lambda g, order: (0, start // width + g))

    def fixed(*shape):
        return pl.BlockSpec(shape, lambda g, order: (0, 0))

    raw = [columns(repeat), columns(1, q_heads), columns(1, q_heads + kv_heads)]
    tables = [
        fixed(rows, HEAD_WIDTH),
        fixed(rows, HEAD_WIDTH),
        fixed(1, HEAD_WIDTH),
        fixed(1, HEAD_WIDTH),
        fixed(rows, 1),
    ]
    return repeat, columns, fixed, raw, tables


def attention(qkv, tables, order, q_heads, kv_heads):
    rows = qkv.shape[0]
    blocks = order.shape[0]
    repeat, columns, _, raw, table_specs = attention_specs(rows, q_heads, kv_heads)
    wide, narrow = q_heads * HEAD_WIDTH, kv_heads * HEAD_WIDTH
    return pl.pallas_call(
        functools.partial(attention_kernel, blocks, repeat),
        name="attention",
        out_shape=(
            jax.ShapeDtypeStruct((rows, wide), jnp.bfloat16),
            jax.ShapeDtypeStruct((rows, narrow), jnp.bfloat16),
            jax.ShapeDtypeStruct((rows, narrow), jnp.bfloat16),
            jax.ShapeDtypeStruct((rows, wide), jnp.bfloat16),
            jax.ShapeDtypeStruct((rows, narrow), jnp.float32),
        ),
        grid_spec=pltpu.PrefetchScalarGridSpec(
            num_scalar_prefetch=1,
            grid=(kv_heads,),
            in_specs=raw + table_specs,
            out_specs=[columns(repeat), columns(1), columns(1), columns(repeat), columns(1)],
            scratch_shapes=[
                pltpu.VMEM((repeat, rows // blocks, HEAD_WIDTH), jnp.float32),
                pltpu.VMEM((repeat, rows // blocks, 1), jnp.float32),
            ],
        ),
        compiler_params=pltpu.CompilerParams(vmem_limit_bytes=50 << 20),
        cost_estimate=pl.CostEstimate(
            flops=4 * rows * rows * wide, bytes_accessed=60_000_000, transcendentals=0
        ),
    )(order, qkv, qkv, qkv, *tables)


def attention_pull_kernel(blocks, repeat, order_ref, *refs):
    q, k, cosine, sine, q_gain, k_gain, first, qr, kr, vb, total, grad = refs[:12]
    dq, dk, dv, dq_gain, dk_gain = refs[12:17]
    shares, share_grads, dq_acc, dk_acc, dv_acc, inner_sum = refs[17:]
    rows = q.shape[0] // blocks
    tile = key_tile(q.shape[0])
    scale = HEAD_WIDTH**-0.5
    dk_acc[...] = jnp.zeros_like(dk_acc)
    dv_acc[...] = jnp.zeros_like(dv_acc)

    @pl.when(pl.program_id(0) == 0)
    def _():
        dq_gain[...] = jnp.zeros_like(dq_gain)
        dk_gain[...] = jnp.zeros_like(dk_gain)

    def pull(raw, gain, turned_grad, at, gain_out):
        scaled_grad = turned_grad * cosine[at, :] + turn(turned_grad * sine[at, :])
        r = head_norm(raw)
        gain_out[0:1, :] += jnp.sum(scaled_grad * raw * r, axis=0, keepdims=True)
        scaled = scaled_grad * gain
        inner = jnp.mean(raw * scaled, axis=-1, keepdims=True)
        return (r * scaled - raw * (r * r * r * inner)).astype(jnp.bfloat16)

    def over_rows(i, carry):
        at = rows_at(i, rows)
        row0 = order_ref[i] * rows
        tiles = (row0 + rows + tile - 1) // tile
        dq_acc[...] = jnp.zeros_like(dq_acc)
        inner_sum[...] = jnp.zeros_like(inner_sum)

        def first_pass(t, inner):
            keys = rows_at(t, tile)
            mask = tile_mask(first[at, :], t * tile, tile, row0, rows)
            for r in range(repeat):
                head = slice(r * HEAD_WIDTH, (r + 1) * HEAD_WIDTH)
                scores = dot_last(qr[at, head], kr[keys, :]) * scale
                share = jnp.where(mask, jnp.exp(scores), 0.0) * (1.0 / total[at, r : r + 1])
                share_grad = dot_last(grad[at, head], vb[keys, :])
                inner_sum[r] += jnp.sum(share * share_grad, axis=-1, keepdims=True)
                shares[t, r] = share
                share_grads[t, r] = share_grad
            return inner

        lax.fori_loop(0, tiles, first_pass, 0)

        def second_pass(t, inner):
            keys = rows_at(t, tile)
            for r in range(repeat):
                head = slice(r * HEAD_WIDTH, (r + 1) * HEAD_WIDTH)
                share = shares[t, r]
                score_grad = (share * (share_grads[t, r] - inner_sum[r])).astype(jnp.bfloat16)
                dq_acc[r] += jnp.dot(score_grad, kr[keys, :], preferred_element_type=jnp.float32)
                dk_acc[keys, :] += contract_rows(score_grad, qr[at, head])
                dv_acc[keys, :] += contract_rows(share.astype(jnp.bfloat16), grad[at, head])
            return inner

        lax.fori_loop(0, tiles, second_pass, 0)
        for r in range(repeat):
            head = slice(r * HEAD_WIDTH, (r + 1) * HEAD_WIDTH)
            dq[at, head] = pull(q[at, head], q_gain[...], dq_acc[r] * scale, at, dq_gain)
        return carry

    lax.fori_loop(0, blocks, over_rows, 0)

    def finish(i, carry):
        at, to = rows_at(i, rows), rows_at(order_ref[i], rows)
        dk[at, :] = pull(k[at, :], k_gain[...], dk_acc[to, :] * scale, at, dk_gain)
        dv[at, :] = dv_acc[to, :].astype(jnp.bfloat16)
        return carry

    lax.fori_loop(0, blocks, finish, 0)


def attention_pull(qkv, tables, order, kept, grad, q_heads, kv_heads):
    rows = qkv.shape[0]
    blocks = order.shape[0]
    repeat, columns, fixed, raw, table_specs = attention_specs(rows, q_heads, kv_heads)
    wide, narrow = q_heads * HEAD_WIDTH, kv_heads * HEAD_WIDTH
    own, tile = rows // blocks, key_tile(rows)
    return pl.pallas_call(
        functools.partial(attention_pull_kernel, blocks, repeat),
        out_shape=(
            jax.ShapeDtypeStruct((rows, wide), jnp.bfloat16),
            jax.ShapeDtypeStruct((rows, narrow), jnp.bfloat16),
            jax.ShapeDtypeStruct((rows, narrow), jnp.bfloat16),
            jax.ShapeDtypeStruct((8, HEAD_WIDTH), jnp.float32),
            jax.ShapeDtypeStruct((8, HEAD_WIDTH), jnp.float32),
        ),
        grid_spec=pltpu.PrefetchScalarGridSpec(
            num_scalar_prefetch=1,
            grid=(kv_heads,),
            in_specs=raw[:2]
            + table_specs
            + [columns(repeat), columns(1), columns(1), columns(1), columns(repeat)],
            out_specs=[
                columns(repeat),
                columns(1),
                columns(1),
                fixed(8, HEAD_WIDTH),
                fixed(8, HEAD_WIDTH),
            ],
            scratch_shapes=[
                pltpu.VMEM((rows // tile, repeat, own, tile), jnp.float32),
                pltpu.VMEM((rows // tile, repeat, own, tile), jnp.float32),
                pltpu.VMEM((repeat, own, HEAD_WIDTH), jnp.float32),
                pltpu.VMEM((rows, HEAD_WIDTH), jnp.float32),
                pltpu.VMEM((rows, HEAD_WIDTH), jnp.float32),
                pltpu.VMEM((repeat, own, 1), jnp.float32),
            ],
        ),
        compiler_params=pltpu.CompilerParams(vmem_limit_bytes=56 << 20),
        cost_estimate=pl.CostEstimate(
            flops=10 * rows * rows * wide, bytes_accessed=120_000_000, transcendentals=0
        ),
    )(order, qkv, qkv, *tables, *kept, grad)


def shift_perm(size, step):
    return [((place + step) % size, place) for place in range(size)]


def trade(values):
    return lax.ppermute(values, ("c", "h"), [(0, 0), (1, 2), (2, 1), (3, 3)])


def gather_along(own):
    places = lax.axis_size("l")
    return [own] + [lax.ppermute(own, "l", shift_perm(places, step)) for step in range(1, places)]


def gather_across(parts):
    half = jnp.concatenate(parts, axis=0)
    other = lax.ppermute(half, "c", shift_perm(2, 1))
    return jnp.concatenate([half, other], axis=0)


def scatter_tokens(partial, *first):
    places = lax.axis_size("l")
    half = partial.shape[0] // 2
    rows = half // places
    other = lax.ppermute(partial[half:].astype(jnp.bfloat16), "c", shift_perm(2, 1))
    total = partial[:half] + other.astype(jnp.float32)
    own = total[:rows]
    for step in range(1, places):
        sent = total[step * rows : (step + 1) * rows].astype(jnp.bfloat16)
        moved = lax.ppermute(sent, "l", shift_perm(places, -step))
        moved = after(moved, *first)
        own = own + moved.astype(jnp.float32)
    return own


def after(value, *others):
    return lax.optimization_barrier((value,) + others)[0]


def return_halves(near, far):
    core = lax.axis_index("c")
    far = lax.ppermute(far, "h", shift_perm(2, 1))
    sums = near.astype(jnp.float32) + far.astype(jnp.float32)
    rows = sums.shape[0] // 2
    first, second = sums[:rows], sums[rows:]
    mine = jnp.where(core == 0, first, second)
    sent = jnp.where(core == 0, second, first).astype(jnp.bfloat16)
    other = lax.ppermute(sent, "c", shift_perm(2, 1)).astype(jnp.float32)
    return mine, other


def columns_of(mine, other):
    core = lax.axis_index("c")
    return jnp.concatenate(
        [jnp.where(core == 0, mine, other), jnp.where(core == 0, other, mine)], axis=1
    )


def sum_over_d(partial):
    return lax.psum_scatter(partial.astype(jnp.bfloat16), "d", scatter_dimension=0, tiled=True)


def as_row(values):
    return values.reshape(1, -1)


def split(values):
    half = values.shape[1] // 2
    return values[:, :half], values[:, half:]


def per_device(
    tokens,
    segment_ids,
    attn_gain,
    q_weight,
    key_matrix,
    value_matrix,
    o_weight,
    q_gain,
    k_gain,
    mlp_gain,
    gate_weight,
    up_weight,
    down_weight,
    cotangent,
):
    width = attn_gain.shape[1] * lax.axis_size("d") * 2
    own_rows = tokens.shape[0]
    places = lax.axis_size("l")
    core, place = lax.axis_index("c"), lax.axis_index("l")
    q_cols, kv_cols, ff_cols = q_weight.shape[2], key_matrix.shape[2], gate_weight.shape[2]
    half_cols = ff_cols // 2

    cut = attn_gain.shape[1]
    head_cut = q_gain.shape[1]
    gains = jnp.concatenate([attn_gain[0], mlp_gain[0], q_gain[0], k_gain[0]]).astype(jnp.float32)
    gains = jnp.pad(gains, (0, 1024 - gains.shape[0])).reshape(8, 128)
    labels = trade(segment_ids)[0]
    order = jnp.stack(
        [
            ((core + core_step) % 2) * places + (place + step) % places
            for core_step in range(2)
            for step in range(places)
        ]
    )
    row_index = (order[:, None] * own_rows + jnp.arange(own_rows, dtype=jnp.int32)[None, :]).reshape(-1)
    labels = labels.reshape(2 * places, own_rows)[order].reshape(-1)
    cosine, sine, first_row = rotary_tables(labels, row_index)
    qkv_full, o_full, mid_rows, down_rows, group, cotangent, gains = enter(
        q_weight[0],
        key_matrix[0],
        value_matrix[0],
        o_weight[0],
        gate_weight[0],
        up_weight[0],
        down_weight[0],
        after(tokens, cosine, sine, first_row),
        cotangent,
        gains,
    )
    mid_near = lax.all_gather(mid_rows, "d", axis=0, tiled=True)
    down_near = lax.all_gather(down_rows, "d", axis=0, tiled=True)
    up_far = lax.ppermute(mid_rows[:, half_cols:], "h", shift_perm(2, 1))
    down_far = lax.ppermute(down_rows, "h", shift_perm(2, 1))
    grad_half = gather_along(cotangent)
    gains = gains.reshape(gains.shape[0], -1)
    attn_scale = gains[:, :cut].reshape(-1)
    mlp_scale = gains[:, cut : 2 * cut].reshape(-1)
    q_scale = gains[:, 2 * cut : 2 * cut + head_cut].reshape(-1)
    k_scale = gains[:, 2 * cut + head_cut : 2 * cut + 2 * head_cut].reshape(-1)

    stream = group[:own_rows]
    normed = rms_scale(group.astype(jnp.float32), attn_scale).astype(jnp.bfloat16)
    head_count, kv_heads = q_cols // HEAD_WIDTH, kv_cols // HEAD_WIDTH
    qkv = jnp.dot(normed, qkv_full, preferred_element_type=jnp.float32)
    tables = (cosine, sine, as_row(q_scale), as_row(k_scale), first_row)
    query_reduced, key_reduced, value_reduced, attended, totals = attention(
        qkv, tables, order, head_count, kv_heads
    )

    grad_rows = gather_across([grad_half[0]] + [after(part, attended) for part in grad_half[1:]])

    def whole(values):
        return jax.ShapeDtypeStruct((own_rows, width), values)

    gain_sum = jax.ShapeDtypeStruct((1, width), jnp.float32)
    middle, normed_mid, mid_far = exchange(
        1,
        contract_cols(attended, o_full).astype(jnp.bfloat16),
        (stream, as_row(mlp_scale)),
        (whole(jnp.float32),),
        middle_rows,
        True,
        (mid_rows, after(up_far, attended)),
    )
    down_far = lax.all_gather(after(down_far, normed_mid), "d", axis=0, tiled=True)

    mid = jnp.dot(normed_mid, mid_near, preferred_element_type=jnp.float32)
    gate_near, up_near = split(mid)
    hidden_near = swiglu(gate_near, up_near).astype(jnp.bfloat16)
    mid = jnp.dot(normed_mid, mid_far, preferred_element_type=jnp.float32)
    gate_far, up_far = split(mid)
    hidden_far = swiglu(gate_far, up_far).astype(jnp.bfloat16)
    down_grad_far = contract_rows(grad_rows, hidden_far).astype(jnp.bfloat16)
    down_sum_far = sum_over_d(down_grad_far)
    down_grad_near = contract_rows(grad_rows, hidden_near).astype(jnp.bfloat16)
    down_sum_near = sum_over_d(down_grad_near)
    grad_rows = after(grad_rows, down_grad_near, down_grad_far)

    def hidden_pull(gate, up, down):
        hidden_grad = jnp.dot(grad_rows, down, preferred_element_type=jnp.float32)
        _, pull_back = jax.vjp(swiglu, gate, up)
        gate_grad, up_grad = pull_back(hidden_grad)
        return jnp.concatenate(
            [gate_grad.astype(jnp.bfloat16), up_grad.astype(jnp.bfloat16)], axis=1
        )

    mid_back_near = hidden_pull(gate_near, up_near, down_near)
    mid_back_far = hidden_pull(gate_far, up_far, down_far)
    mid_grad_far = contract_rows(normed_mid, mid_back_far).astype(jnp.bfloat16)
    mid_sum_far = sum_over_d(mid_grad_far)
    normed_grad = contract_cols(mid_back_near, mid_near) + contract_cols(mid_back_far, mid_far)
    normed_grad = normed_grad.astype(jnp.bfloat16)
    gradient, mlp_gain_grad, grad_rows, mid_grad_near, branch = exchange(
        2,
        after(normed_grad, mid_grad_far),
        (middle, cotangent, as_row(mlp_scale)),
        (whole(jnp.float32), gain_sum),
        middle_pull_rows,
        True,
        jobs=(
            Job((normed_mid, mid_back_near), mid_near.shape, 8, weight_grad_tile),
            Job((hidden_near, hidden_far, down_near, down_far), normed_mid.shape, 4, down_tile),
        ),
    )
    mid_sum_near = sum_over_d(mid_grad_near)

    out_grad = jnp.dot(grad_rows, o_full, preferred_element_type=jnp.float32).astype(jnp.bfloat16)
    o_wgrad = contract_rows(grad_rows, attended)
    query_back, key_back, value_back, q_gain_grad, k_gain_grad = attention_pull(
        qkv,
        tables,
        order,
        (query_reduced, key_reduced, value_reduced, totals),
        out_grad,
        head_count,
        kv_heads,
    )
    qkv_back = jnp.concatenate([query_back, key_back, value_back], axis=1)
    qkv_grad = contract_rows(normed, qkv_back).astype(jnp.bfloat16)
    o_wgrad = o_wgrad.astype(jnp.bfloat16)
    branch = scatter_tokens(branch, qkv_grad)
    activations = trade((middle + branch).astype(jnp.bfloat16))
    gradient, sums, attn_grad = exchange(
        None,
        contract_cols(after(qkv_back, qkv_grad), qkv_full).astype(jnp.bfloat16),
        (stream, gradient, as_row(attn_scale), mlp_gain_grad, q_gain_grad, k_gain_grad),
        (
            whole(jnp.float32),
            jax.ShapeDtypeStruct((8, 128), jnp.float32),
            jax.ShapeDtypeStruct((q_weight.shape[1], 2 * q_cols + 2 * kv_cols), jnp.float32),
        ),
        stream_pull_rows,
        False,
        last=(qkv_grad, o_wgrad),
    )
    lines = cut // 128
    head_at = (lax.axis_index("d") * 2 + core) * head_cut

    def head_gain(line):
        return lax.dynamic_slice(sums[line], (head_at,), (head_cut,))[None]

    mid_sum_near = after(mid_sum_near, sums)
    down_sum_near = after(down_sum_near, sums)
    down_grad = columns_of(*return_halves(down_sum_near, down_sum_far))
    mine, other = return_halves(mid_sum_near, mid_sum_far)
    gate_grad = columns_of(mine[:, :half_cols], other[:, :half_cols])
    up_grad = columns_of(mine[:, half_cols:], other[:, half_cols:])

    return (
        activations,
        gradient,
        sums[:lines].reshape(1, cut),
        attn_grad[None, :, :q_cols],
        attn_grad[None, :, q_cols : q_cols + kv_cols],
        attn_grad[None, :, q_cols + kv_cols : q_cols + 2 * kv_cols],
        attn_grad[None, :, q_cols + 2 * kv_cols :],
        head_gain(2 * lines),
        head_gain(2 * lines + 1),
        sums[lines : 2 * lines].reshape(1, cut),
        gate_grad[None],
        up_grad[None],
        down_grad[None],
    )


def solution(mesh):
    dp, tensor = mesh.shape["dp"], mesh.shape["tensor"]
    cut = Mesh(mesh.devices.reshape(dp // 2, 2, 2, tensor // 2), ("d", "c", "h", "l"))
    rows, cols = ("d", "c"), ("h", "l")
    tokens, labels = P(rows + cols, None), P(rows, None)
    gain, weight = P(None, rows), P(None, rows, cols)
    return jax.shard_map(
        per_device,
        mesh=cut,
        in_specs=(
            tokens,
            labels,
            gain,
            weight,
            weight,
            weight,
            weight,
            gain,
            gain,
            gain,
            weight,
            weight,
            weight,
            tokens,
        ),
        out_specs=(
            tokens,
            tokens,
            gain,
            weight,
            weight,
            weight,
            weight,
            gain,
            gain,
            gain,
            weight,
            weight,
            weight,
        ),
        check_vma=False,
    )
```

```python
import functools
import math

import jax
import jax.numpy as jnp
from jax import lax
from jax.experimental import pallas as pl
from jax.experimental.pallas import tpu as pltpu
from jax.sharding import Mesh
from jax.sharding import PartitionSpec as P


HEAD_WIDTH = 128
NSEQ = 3


EPS = 1e-06
THETA = 1000000.0


def rms_scale(values, gain):
    return values * lax.rsqrt(jnp.mean(values * values, axis=-1, keepdims=True) + EPS) * gain


def swiglu(gate_raw, up_raw):
    return jax.nn.silu(gate_raw) * up_raw


def rotary_tables(sequence_labels, row_index):
    labels = jnp.arange(NSEQ, dtype=jnp.int32)
    starts = jnp.sum((sequence_labels[None, :] < labels[:, None]).astype(jnp.int32), axis=1)
    first_row = jnp.sum(
        jnp.where(sequence_labels[:, None] == labels[None, :], starts[None, :], 0), axis=1
    )
    position = (row_index - first_row).astype(jnp.float32)
    frequency = THETA ** (-(jnp.arange(HEAD_WIDTH // 2, dtype=jnp.float32) * (2.0 / HEAD_WIDTH)))
    angles = position[:, None] * frequency[None, :]
    sine = jnp.sin(angles)
    cosine = jnp.cos(angles)
    return (
        jnp.concatenate([cosine, cosine], axis=1),
        jnp.concatenate([-sine, sine], axis=1),
        first_row[:, None],
    )


def contract_rows(left, right):
    return lax.dot_general(
        left, right, (((0,), (0,)), ((), ())), preferred_element_type=jnp.float32
    )


def contract_cols(left, right):
    return lax.dot_general(
        left, right, (((1,), (1,)), ((), ())), preferred_element_type=jnp.float32
    )


MESH = pl.DeviceIdType.MESH
CHUNKS = 3


def remote(source, target, send_sem, recv_sem, **place):
    return pltpu.make_async_remote_copy(
        src_ref=source,
        dst_ref=target,
        send_sem=send_sem,
        recv_sem=recv_sem,
        device_id=place,
        device_id_type=MESH,
    )


def rows_at(index, size):
    return pl.ds(pl.multiple_of(index * size, size), size)


WEIGHTS = 5
ENTRY_START = (
    "w0", "t0", "w1", "w2", "t1", "w3", "w4", "t2",
)
ENTRY_ORDER = (
    "s0", "t0", "s1", "r0", "s2", "r1", "t1", "s3", "r2", "s4", "r3", "t2", "r4", "a0", "a1",
    "a2",
)


def hop_plan(nd, d):
    if nd == 4:
        side_x = d + 1 - 2 * lax.rem(d, 2)
        side_y = d + 2 - 4 * (d // 2)
        corner = side_x + side_y - d
        hops = (
            (0, d, side_x),
            (1, d, side_x),
            (0, d, side_y),
            (1, d, side_y),
            (0, side_x, side_y),
            (1, side_y, side_x),
        )
        sources = ((0, side_x), (1, side_x), (0, side_y), (1, side_y), (0, corner), (1, corner))
        return hops, sources, 4, ((0, 4), (3, 5))
    steps = [(part, step) for step in range(1, nd) for part in range(2)]
    hops = tuple((part, d, lax.rem(d + step, nd)) for part, step in steps)
    sources = tuple((part, lax.rem(d + nd - step, nd)) for part, step in steps)
    return hops, sources, len(hops), ()


def hop_count(nd):
    return 6 if nd == 4 else 2 * (nd - 1)


class Spread:
    def __init__(self, nd, d, block, send_sem, recv_sem, own=None):
        self.hops, self.sources, self.first, self.relayed = hop_plan(nd, d)
        self.block, self.send_sem, self.recv_sem = block, send_sem, recv_sem
        self.own = own or (lambda j, part: block(j, d * 2 + part))

    def copy(self, j, kind, source, part, of):
        return remote(
            source,
            self.block(j, of * 2 + part),
            self.send_sem.at[j, kind],
            self.recv_sem.at[j, kind],
            d=self.hops[kind][2],
        )

    def hop(self, j, kind):
        part, of, _ = self.hops[kind]
        source = self.own(j, part) if kind < self.first else self.block(j, of * 2 + part)
        return self.copy(j, kind, source, part, of)

    def arrived(self, j, kind):
        part, of = self.sources[kind]
        return self.copy(j, kind, self.block(j, of * 2 + part), part, of)

    def send(self, j, part):
        for kind in range(self.first):
            if self.hops[kind][0] == part:
                self.hop(j, kind).start()

    def relay(self, j):
        for after_kind, kind in self.relayed:
            self.arrived(j, after_kind).wait_recv()
            self.hop(j, kind).start()

    def finish(self, j):
        handled = {after_kind for after_kind, _ in self.relayed}
        for kind in range(len(self.hops)):
            if kind not in handled:
                self.arrived(j, kind).wait_recv()
            self.hop(j, kind).wait_send()


def entry_kernel(nd, tl, *refs):
    (q_ref, k_ref, v_ref, o_ref, gate_ref, up_ref, down_ref, tok_ref, cot_ref, gain_ref) = refs[:10]
    (qkv_full, o_full, mid_rows, down_rows, tok_full, cot_own, gain_full) = refs[10:17]
    (stage, half_stage, tok_stage, cot_stage) = refs[17:21]
    (zs, zr, cs, li, lo, xs, xr, ts, tr, tli, tlo, ls, lr, fs, fr) = refs[21:36]
    (gs, gr, gl, os, orv, oi, hs, hr, hi, ho) = refs[36:]
    d, c, h, l = (lax.axis_index(name) for name in ("d", "c", "h", "l"))
    same = c == h
    apart = c != h
    rows = q_ref.shape[0]
    own = tok_ref.shape[0]
    chunk = own // CHUNKS
    q_cols, kv_cols = q_ref.shape[1], k_ref.shape[1]
    o_half = o_ref.shape[1] // 2
    qkv_cols = q_cols + 2 * kv_cols
    weights = (
        (q_ref, qkv_full, 0, q_cols, 0),
        (k_ref, qkv_full, q_cols, kv_cols, q_cols),
        (v_ref, qkv_full, q_cols + kv_cols, kv_cols, q_cols + kv_cols),
        (o_ref.at[:, pl.ds(0, o_half)], o_full, 0, o_half, qkv_cols),
        (o_ref.at[:, pl.ds(o_half, o_half)], o_full, o_half, o_half, qkv_cols + o_half),
    )

    def block(j, row):
        _, full, start, cols, _ = weights[j]
        return full.at[rows_at(row, rows), pl.ds(start, cols)]

    def held(j):
        _, _, _, cols, start = weights[j]
        return stage.at[:, pl.ds(start, cols)]

    def from_far(j, part):
        return remote(block(j, d * 2 + part), block(j, d * 2 + part), zs.at[j], zr.at[j, part], h=1 - h)

    def to_far(j):
        return remote(weights[j][0], block(j, d * 2 + c), zs.at[j], zr.at[j, c], c=h, h=1 - h)

    def to_core(j):
        return remote(weights[j][0], block(j, d * 2 + c), cs.at[j], zr.at[j, c], c=h)

    def local_in(j):
        return pltpu.make_async_copy(weights[j][0], held(j), li.at[j])

    def local_out(j):
        return pltpu.make_async_copy(held(j), block(j, d * 2 + c), lo.at[j])

    def tokens_at(index, k):
        return tok_full.at[pl.ds(index * own + k * chunk, chunk)]

    def trade_tokens(k):
        return remote(tok_ref.at[pl.ds(k * chunk, chunk)], tokens_at(0, k), ts.at[k], tr.at[k], c=h, h=c)

    def along(step, k):
        return remote(
            tokens_at(0, k),
            tokens_at(tl - step, k),
            ls.at[(step - 1) * CHUNKS + k],
            lr.at[(tl - step - 1) * CHUNKS + k],
            l=lax.rem(l + step, tl),
        )

    def from_along(index, k):
        return remote(
            tokens_at(index, k),
            tokens_at(index, k),
            ls.at[(index - 1) * CHUNKS + k],
            lr.at[(index - 1) * CHUNKS + k],
            l=l,
        )

    def across(index, k):
        at = index * CHUNKS + k
        return remote(tokens_at(index, k), tokens_at(tl + index, k), fs.at[at], fr.at[at], c=1 - c)

    def gain_peer(step):
        place = lax.rem(d * 2 + c + step, 2 * nd)
        return place // 2, lax.rem(place, 2)

    def gains_to(step):
        to_d, to_c = gain_peer(step)
        return remote(
            gain_ref, gain_full.at[d * 2 + c], gs.at[step - 1], gr.at[2 * nd - step - 1], d=to_d, c=to_c
        )

    def gains_from(step):
        from_d, from_c = gain_peer(step)
        return remote(
            gain_ref, gain_full.at[from_d * 2 + from_c], gs.at[step - 1], gr.at[step - 1], d=from_d, c=from_c
        )

    def local_gains():
        return pltpu.make_async_copy(gain_ref, gain_full.at[d * 2 + c], gl)

    half = gate_ref.shape[1] // 2
    halves = ((gate_ref, mid_rows, 0), (up_ref, mid_rows, half), (down_ref, down_rows, 0))

    def columns_of_core(j, of):
        return halves[j][0].at[:, pl.ds(pl.multiple_of(of * half, half), half)]

    def half_at(j, of):
        return halves[j][1].at[rows_at(of, rows), pl.ds(halves[j][2], half)]

    def half_to_core(j):
        return remote(columns_of_core(j, 1 - c), half_at(j, c), hs.at[j], hr.at[j], c=1 - c)

    def half_from_core(j):
        return remote(half_at(j, 1 - c), half_at(j, 1 - c), hs.at[j], hr.at[j], c=1 - c)

    def half_in(j):
        return pltpu.make_async_copy(columns_of_core(j, c), half_stage.at[j], hi.at[j])

    def half_out(j):
        return pltpu.make_async_copy(half_stage.at[j], half_at(j, c), ho.at[j])

    local_gains().start()

    def start_weights(j):
        to_far(j).start()

        @pl.when(apart)
        def _():
            to_core(j).start()

    def start_tokens(k):
        @pl.when(apart)
        def _():
            trade_tokens(k).start()

    def trade_cotangent():
        return remote(cot_ref, cot_own, os, orv, c=h, h=c)

    def cotangent_in():
        return pltpu.make_async_copy(cot_ref, cot_stage, oi)

    def cotangent_out():
        return pltpu.make_async_copy(cot_stage, cot_own, oi)

    for step in ENTRY_START:
        {"w": start_weights, "t": start_tokens}[step[0]](int(step[1:]))

    @pl.when(apart)
    def _():
        trade_cotangent().start()

    @pl.when(same)
    def _():
        pltpu.make_async_copy(tok_ref, tok_stage, tli).start()
        for j in range(WEIGHTS):
            local_in(j).start()
        pltpu.make_async_copy(tok_ref, tok_stage, tli).wait()
        for k in range(CHUNKS):
            part = pl.ds(k * chunk, chunk)
            pltpu.make_async_copy(tok_stage.at[part], tokens_at(0, k), tlo.at[k]).start()
        for j in range(WEIGHTS):
            local_in(j).wait()
            local_out(j).start()
        cotangent_in().start()
        cotangent_in().wait()
        cotangent_out().start()

    for step in range(1, 2 * nd):
        gains_to(step).start()
    for j in range(3):
        half_in(j).start()
        half_to_core(j).start()
    for j in range(3):
        half_in(j).wait()
        half_out(j).start()

    over_d = Spread(nd, d, block, xs, xr)

    def spread(j):
        for part in range(2):
            here = jnp.logical_and(same, c == part)

            @pl.when(here)
            def _():
                local_out(j).wait()

            @pl.when(jnp.logical_not(here))
            def _():
                from_far(j, part).wait_recv()

            over_d.send(j, part)

    relay = over_d.relay

    def own_tokens(k):
        @pl.when(same)
        def _():
            part = pl.ds(k * chunk, chunk)
            pltpu.make_async_copy(tok_stage.at[part], tokens_at(0, k), tlo.at[k]).wait()

        @pl.when(apart)
        def _():
            remote(tokens_at(0, k), tokens_at(0, k), ts.at[k], tr.at[k], c=1 - c, h=1 - h).wait_recv()

        for step in range(1, tl):
            along(step, k).start()
        across(0, k).start()

    def pass_across(k):
        for index in range(1, tl):
            from_along(index, k).wait_recv()
            across(index, k).start()

    steps = {"t": own_tokens, "s": spread, "r": relay, "a": pass_across}
    for step in ENTRY_ORDER:
        steps[step[0]](int(step[1:]))

    for j in range(WEIGHTS):
        over_d.finish(j)
        to_far(j).wait_send()
    for k in range(CHUNKS):
        for index in range(tl):
            across(index, k).wait()
        for step in range(1, tl):
            along(step, k).wait_send()
    for step in range(1, 2 * nd):
        gains_from(step).wait_recv()
        gains_to(step).wait_send()
    local_gains().wait()
    for j in range(3):
        half_from_core(j).wait_recv()
        half_to_core(j).wait_send()
        half_out(j).wait()

    @pl.when(same)
    def _():
        cotangent_out().wait()

    @pl.when(apart)
    def _():
        trade_cotangent().wait()
        for j in range(WEIGHTS):
            to_core(j).wait_send()
        for k in range(CHUNKS):
            trade_tokens(k).wait_send()


def enter(q_weight, k_weight, v_weight, o_weight, gate, up, down, tokens, cotangent, gains):
    nd, tl = lax.axis_size("d"), lax.axis_size("l")
    rows, q_cols = q_weight.shape
    qkv_cols = q_cols + 2 * k_weight.shape[1]
    own, width = tokens.shape
    half = gate.shape[1] // 2
    dma = pltpu.SemaphoreType.DMA
    counts = (
        (WEIGHTS,),
        (WEIGHTS, 2),
        (WEIGHTS,),
        (WEIGHTS,),
        (WEIGHTS,),
        (WEIGHTS, hop_count(nd)),
        (WEIGHTS, hop_count(nd)),
        (CHUNKS,),
        (CHUNKS,),
        (),
        (CHUNKS,),
        ((tl - 1) * CHUNKS,),
        ((tl - 1) * CHUNKS,),
        (tl * CHUNKS,),
        (tl * CHUNKS,),
        (2 * nd - 1,),
        (2 * nd - 1,),
        (),
        (),
        (),
        (),
        (3,),
        (3,),
        (3,),
        (3,),
    )
    anywhere = pl.BlockSpec(memory_space=pl.ANY)

    def low(*shape):
        return jax.ShapeDtypeStruct(shape, jnp.bfloat16)

    return pl.pallas_call(
        functools.partial(entry_kernel, nd, tl),
        name="entry",
        out_shape=(
            low(width, qkv_cols),
            low(width, o_weight.shape[1]),
            low(2 * rows, 2 * half),
            low(2 * rows, half),
            low(2 * tl * own, width),
            low(own, width),
            jax.ShapeDtypeStruct((2 * nd,) + gains.shape, jnp.float32),
        ),
        in_specs=[anywhere] * 10,
        out_specs=[anywhere] * 7,
        scratch_shapes=[
            pltpu.VMEM((rows, qkv_cols + o_weight.shape[1]), jnp.bfloat16),
            pltpu.VMEM((3, rows, half), jnp.bfloat16),
            pltpu.VMEM((own, width), jnp.bfloat16),
            pltpu.VMEM((own, width), jnp.bfloat16),
        ]
        + [dma(count) if count else dma for count in counts],
        compiler_params=pltpu.CompilerParams(has_side_effects=True),
        cost_estimate=pl.CostEstimate(flops=0, bytes_accessed=250_000_000, transcendentals=0),
    )(q_weight, k_weight, v_weight, o_weight, gate, up, down, tokens, cotangent, gains)


PIECES = 6
RETURN_AHEAD = 2
RETURN_ORDER = (
    "m0", "w2", "f0", "m1", "w3", "f1", "h0", "m2", "w4", "f2", "g0", "h1", "m3", "w5", "h2", "m4",
    "h3", "m5", "h4", "h5",
)
SUM_ORDER = (
    "s3", "s4", "s5", "f0", "r3", "s0", "f1", "r4", "r0", "s1", "f2", "r5", "r1", "s2", "r2",
    "a0", "a1", "a2",
)


class Return:
    def __init__(self, nd, pieces, out, scratch):
        self.nd, self.pieces, self.out = nd, pieces, out
        self.held, self.first, self.mixed, self.second, self.sums, self.parts = scratch[:6]
        (self.load, self.fs, self.fr, self.ss, self.sr, self.ps, self.pr) = scratch[6:]
        self.d, self.c, self.h = (lax.axis_index(name) for name in ("d", "c", "h"))
        self.rows = out.shape[0]
        d = self.d
        if nd == 4:
            side_x = d + 1 - 2 * lax.rem(d, 2)
            side_y = d + 2 - 4 * (d // 2)
            corner = side_x + side_y - d
            self.blocks = ((d, 0), (side_y, 0), (d, 1), (side_x, 1))
            self.sends = (
                (side_x, 0, side_x),
                (corner, 0, side_x),
                (side_y, 1, side_y),
                (corner, 1, side_y),
            )
            self.mixes = ((1, side_y), (3, side_x))
        else:
            self.blocks = ((d, 0), (d, 1))
            self.sends = tuple(
                (lax.rem(d + step, nd), part, lax.rem(d + step, nd))
                for step in range(1, nd)
                for part in range(2)
            )
            self.mixes = ()

    @staticmethod
    def scratch(nd, count, rows, cols):
        dma = pltpu.SemaphoreType.DMA
        blocks, sends, mixes = (4, 4, 2) if nd == 4 else (2, 2 * (nd - 1), 1)

        def buffer(number):
            return pltpu.VMEM((count, number, rows, cols), jnp.bfloat16)

        return [
            buffer(blocks),
            buffer(sends),
            buffer(mixes),
            buffer(mixes),
            buffer(2),
            buffer(2),
            dma((count, blocks)),
            dma((count, sends)),
            dma((count, sends)),
            dma((count, mixes)),
            dma((count, mixes)),
            dma((count, 2)),
            dma((count, 2)),
        ]

    def source(self, j, of, part):
        ref, start = self.pieces[j]
        cols = self.held.shape[3]
        return ref.at[rows_at(of * 2 + part, self.rows), pl.ds(start, cols)]

    def loading(self, j, at):
        return pltpu.make_async_copy(
            self.source(j, *self.blocks[at]), self.held.at[j, at], self.load.at[j, at]
        )

    def sending(self, j, at):
        of, part, to = self.sends[at]
        return remote(
            self.source(j, of, part), self.first.at[j, at], self.fs.at[j, at], self.fr.at[j, at], d=to
        )

    def mixing(self, j, at):
        return remote(
            self.mixed.at[j, at],
            self.second.at[j, at],
            self.ss.at[j, at],
            self.sr.at[j, at],
            d=self.mixes[at][1],
        )

    def handing(self, j, part):
        return remote(
            self.sums.at[j, part],
            self.parts.at[j, self.h],
            self.ps.at[j, part],
            self.pr.at[j, self.h],
            c=part,
            h=self.c,
        )

    def stays(self, part):
        return jnp.logical_and(self.c == part, self.h == self.c)

    def start(self, j):
        for at in range(len(self.sends)):
            self.sending(j, at).start()
        for at in range(len(self.blocks)):
            self.loading(j, at).start()

    def value(self, ref, j, at):
        return ref[j, at].astype(jnp.float32)

    def mix(self, j):
        for at, (block, _) in enumerate(self.mixes):
            self.loading(j, block).wait()
            self.sending(j, block).wait_recv()
            total = self.value(self.held, j, block) + self.value(self.first, j, block)
            self.mixed[j, at] = total.astype(jnp.bfloat16)
            self.mixing(j, at).start()

    def hand(self, j):
        for part in range(2):
            own = 2 * part if self.mixes else part
            self.loading(j, own).wait()
            total = self.value(self.held, j, own)
            for at in [own] if self.mixes else range(part, len(self.sends), 2):
                self.sending(j, at).wait_recv()
                total = total + self.value(self.first, j, at)
            if self.mixes:
                self.mixing(j, part).wait_recv()
                total = total + self.value(self.second, j, part)
            self.sums[j, part] = total.astype(jnp.bfloat16)

            @pl.when(self.stays(part))
            def _():
                self.parts[j, self.h] = self.sums[j, part]

            @pl.when(jnp.logical_not(self.stays(part)))
            def _():
                self.handing(j, part).start()

    def arriving(self, j, of_h):
        return remote(
            self.parts.at[j, of_h], self.parts.at[j, of_h], self.ps.at[j, 0], self.pr.at[j, of_h], h=1 - self.h
        )

    def finish(self, j):
        for of_h in range(2):

            @pl.when(jnp.logical_not(jnp.logical_and(self.c == self.h, self.h == of_h)))
            def _():
                self.arriving(j, of_h).wait_recv()

        cols = self.held.shape[3]
        total = self.value(self.parts, j, 0) + self.value(self.parts, j, 1)
        self.out[:, j * cols : (j + 1) * cols] = total
        for at in range(len(self.sends)):
            self.sending(j, at).wait_send()
        for at in range(len(self.mixes)):
            self.mixing(j, at).wait_send()
        for part in range(2):

            @pl.when(jnp.logical_not(self.stays(part)))
            def _():
                self.handing(j, part).wait_send()


class Job:
    def __init__(self, inputs, shape, tiles, made):
        self.inputs, self.shape, self.tiles, self.made = inputs, shape, tiles, made

    def scratch(self):
        dma = pltpu.SemaphoreType.DMA
        return [pltpu.VMEM(value.shape, value.dtype) for value in self.inputs] + [
            pltpu.VMEM(self.shape, jnp.bfloat16),
            dma((len(self.inputs),)),
            dma((self.tiles,)),
        ]


class RunningJob:
    def __init__(self, job, given, result, scratch):
        self.job, self.given, self.result = job, given, result
        *self.held, self.product, self.in_sem, self.out_sem = scratch
        self.rows = job.shape[0] // job.tiles

    def copy_in(self, at):
        return pltpu.make_async_copy(self.given[at], self.held[at], self.in_sem.at[at])

    def copy_out(self, i):
        rows = rows_at(i, self.rows)
        return pltpu.make_async_copy(
            self.product.at[rows], self.result.at[rows], self.out_sem.at[i]
        )

    def fetch(self):
        for at in range(len(self.given)):
            self.copy_in(at).start()

    def run(self):
        for at in range(len(self.given)):
            self.copy_in(at).wait()

        def one(i, carry):
            self.product[rows_at(i, self.rows), :] = self.job.made(self.held, i, self.rows)
            self.copy_out(i).start()
            return carry

        lax.fori_loop(0, self.job.tiles, one, 0)

    def finish(self):
        for i in range(self.job.tiles):
            self.copy_out(i).wait()


def weight_grad_tile(held, i, rows):
    left, right = held
    return contract_rows(left[:, rows_at(i, rows)], right[...]).astype(jnp.bfloat16)


def down_tile(held, i, rows):
    near, far, down_near, down_far = held
    at = rows_at(i, rows)
    return (
        contract_cols(near[at, :], down_near[...]) + contract_cols(far[at, :], down_far[...])
    ).astype(jnp.bfloat16)


def exchange_kernel(
    nd, tl, epilogue, aux_count, out_count, gather, carry_weights, jobs, last, *refs
):
    partial = refs[0]
    aux = refs[1 : 1 + aux_count]
    refs = refs[1 + aux_count :]
    job_given = []
    for job in jobs:
        count = len(job.inputs)
        job_given.append(refs[:count])
        refs = refs[count:]
    if carry_weights:
        weight_rows, here_rows, refs = refs[0], refs[1], refs[2:]
    gradients, refs = refs[:last], refs[last:]
    outs = refs[:out_count]
    rest = refs[out_count:]
    if gather:
        full, rest = rest[0], rest[1:]
    if carry_weights:
        weights, stage, ws, wr, xs, xr, hi, ho, rest = rest[0], *rest[1:8], rest[8:]
    job_results, rest = rest[: len(jobs)], rest[len(jobs) :]
    running = []
    for job, given, result in zip(jobs, job_given, job_results):
        count = len(job.inputs) + 3
        running.append(RunningJob(job, given, result, rest[:count]))
        rest = rest[count:]
    if last:
        low, back, gain_acc, tiles, got, ts, tr, gs, gr = rest[:9]
        returned, rest = rest[9:22], rest[22:]
        cols = returned[0].shape[3]
        pieces = [
            (array, start) for array in gradients for start in range(0, array.shape[1], cols)
        ]
        back_home = Return(nd, pieces, outs[2], returned)
    if gather:
        finished, ls, lr, fs, fr, keep, rest = rest[0], *rest[1:6], rest[6:]
    mine, other, sums, arrivals, cs, cr, loc, ss, sr = rest
    c, l = lax.axis_index("c"), lax.axis_index("l")
    d, h = lax.axis_index("d"), lax.axis_index("h")
    own = arrivals.shape[0] // (tl - 1)
    chunk = own // CHUNKS

    def greet():
        barrier = pltpu.get_barrier_semaphore()
        peers = [{"c": 1 - c}] + [{"l": lax.rem(l + step, tl)} for step in range(1, tl)]
        if carry_weights:
            peers += [{"h": 1 - h}] + [{"d": lax.rem(d + step, nd)} for step in range(1, nd)]
        for peer in peers:
            pl.semaphore_signal(barrier, inc=1, device_id=peer, device_id_type=MESH)
        pl.semaphore_wait(barrier, len(peers))

    if not last:
        greet()

    def part(base, k):
        return rows_at(base * CHUNKS + k, chunk)

    def to_core(index, k):
        at = index * CHUNKS + k
        return remote(
            partial.at[part(tl + index, k)], other.at[part(index, k)], cs.at[at], cr.at[at], c=1 - c
        )

    def local(index, k):
        return pltpu.make_async_copy(
            partial.at[part(index, k)], mine.at[part(index, k)], loc.at[index * CHUNKS + k]
        )

    def along(step, k):
        at = (step - 1) * CHUNKS + k
        return remote(
            sums.at[part(step - 1, k)],
            arrivals.at[part(step - 1, k)],
            ss.at[at],
            sr.at[at],
            l=lax.rem(l + step, tl),
        )

    if carry_weights:
        half = weight_rows.shape[0] // 2
        far_pieces = PIECES // 2
        piece = here_rows.shape[1] // far_pieces

        def block(j, row):
            return weights.at[rows_at(row, half), pl.ds(j * piece, piece)]

        def given(j, row_part):
            source = weight_rows if j < far_pieces else here_rows
            return source.at[pl.ds(row_part * half, half), pl.ds(j % far_pieces * piece, piece)]

        def held_here(j, row_part):
            return block(j, d * 2 + row_part) if j < far_pieces else given(j, row_part)

        def from_far(j, row_part):
            return remote(
                given(j, row_part),
                block(j, d * 2 + row_part),
                ws.at[j, row_part],
                wr.at[j, row_part],
                h=1 - h,
            )

        def here_in():
            return pltpu.make_async_copy(here_rows, stage, hi)

        def here_out():
            here = weights.at[rows_at(d, 2 * half), pl.ds(far_pieces * piece, far_pieces * piece)]
            return pltpu.make_async_copy(stage, here, ho)

        over_d = Spread(nd, d, block, xs, xr, held_here)

        def spread(j):
            for row_part in range(2):
                if j < far_pieces:
                    from_far(j, row_part).wait_recv()
                over_d.send(j, row_part)

        for j in range(far_pieces):
            for row_part in range(2):
                from_far(j, row_part).start()
        here_in().start()

    order = list(range(1, tl)) + [0]
    for index in order:
        for k in range(CHUNKS):
            to_core(index, k).start()
            local(index, k).start()

    if last:
        for j in range(RETURN_AHEAD):
            back_home.start(j)

    def both(index, k):
        local(index, k).wait()
        to_core(index, k).wait_recv()
        at = part(index, k)
        return mine[at, :].astype(jnp.float32) + other[at, :].astype(jnp.float32)

    for step in range(1, tl):

        def pass_on(k, carry):
            sums[part(step - 1, k), :] = both(step, k).astype(jnp.bfloat16)
            along(step, k).start()
            return carry

        lax.fori_loop(0, CHUNKS, pass_on, 0)

    for job in running:
        job.fetch()
    for job in running[:-1]:
        job.run()

    if last:
        apart = c != h
        count = 4 * nd * tl
        me = ((d * 2 + c) * 2 + h) * tl + l

        def to_owner(k):
            return remote(low.at[part(0, k)], back.at[part(0, k)], ts.at[k], tr.at[k], c=h, h=c)

        def gains_to(step):
            place = lax.rem(me + step, count)
            row = place // (2 * tl)
            return remote(
                tiles.at[row],
                got.at[step - 1],
                gs.at[step - 1],
                gr.at[step - 1],
                d=row // 2,
                c=lax.rem(row, 2),
                h=lax.rem(place // tl, 2),
                l=lax.rem(place, tl),
            )

        def start_gains(step, carry):
            gains_to(step).start()
            return carry

        def add_gains(step, total):
            gains_to(step).wait_recv()
            return total + got[step - 1]

        def drain_gains(step, carry):
            gains_to(step).wait_send()
            return carry

        def send_gains(_):
            cut = gain_acc.shape[1] // (2 * nd)
            lines = cut // 128
            tiles[...] = jnp.zeros_like(tiles)
            for row in range(2 * nd):
                for line in range(lines):
                    at = slice(row * cut + line * 128, row * cut + (line + 1) * 128)
                    tiles[row, line : line + 1, :] = gain_acc[:, at]
                    tiles[row, lines + line : lines + line + 1, :] = aux[3][:, at]
                tiles[row, 2 * lines : 2 * lines + 1, :] = aux[4][0:1, :]
                tiles[row, 2 * lines + 1 : 2 * lines + 2, :] = aux[5][0:1, :]
            lax.fori_loop(1, count, start_gains, 0)

    def gathered(index, k):
        return full.at[part(index, k)]

    def keep_own(k):
        return pltpu.make_async_copy(finished.at[part(0, k)], gathered(0, k), keep.at[k])

    def own_along(step, k):
        return remote(
            finished.at[part(0, k)],
            gathered(tl - step, k),
            ls.at[(step - 1) * CHUNKS + k],
            lr.at[(tl - step - 1) * CHUNKS + k],
            l=lax.rem(l + step, tl),
        )

    def from_along(index, k):
        at = (index - 1) * CHUNKS + k
        return remote(gathered(index, k), gathered(index, k), ls.at[at], lr.at[at], l=l)

    def across(index, k):
        source = finished.at[part(0, k)] if index == 0 else gathered(index, k)
        at = index * CHUNKS + k
        return remote(source, gathered(tl + index, k), fs.at[at], fr.at[at], c=1 - c)

    def finish(k, carry):
        total = both(0, k)
        for step in range(1, tl):
            along(step, k).wait_recv()
            total = total + arrivals[part(step - 1, k), :].astype(jnp.float32)
        kept = (outs[0], low, gain_acc) if last else outs
        row = epilogue(total, part(0, k), k, aux[:3], kept)
        if last:

            @pl.when(apart)
            def _():
                to_owner(k).start()

        if gather:
            finished[part(0, k), :] = row
            keep_own(k).start()
            for step in range(1, tl):
                own_along(step, k).start()
            across(0, k).start()
        return carry

    def pass_across(k):
        for index in range(1, tl):
            from_along(index, k).wait_recv()
            across(index, k).start()

    if carry_weights:
        steps = {
            "s": spread,
            "r": over_d.relay,
            "f": lambda k: finish(k, 0),
            "a": pass_across,
        }
        here_in().wait()
        here_out().start()
        for step in SUM_ORDER:
            steps[step[0]](int(step[1:]))
    elif last:
        steps = {
            "w": back_home.start,
            "m": back_home.mix,
            "h": back_home.hand,
            "f": lambda k: finish(k, 0),
            "g": send_gains,
        }
        for step in RETURN_ORDER:
            steps[step[0]](int(step[1:]))
    else:
        lax.fori_loop(0, CHUNKS, finish, 0)
        for job in running[-1:]:
            job.run()
        if gather:
            for k in range(CHUNKS):
                pass_across(k)
    if last:
        @pl.when(apart)
        def _():
            for k in range(CHUNKS):
                to_owner(k).wait()
                outs[0][part(0, k), :] = back[part(0, k), :].astype(jnp.float32)

        outs[1][...] = lax.fori_loop(1, count, add_gains, tiles[d * 2 + c])
        lax.fori_loop(1, count, drain_gains, 0)
        for j in range(len(pieces)):
            back_home.finish(j)
    for job in running:
        job.finish()
    if gather:
        for k in range(CHUNKS):
            keep_own(k).wait()
            for index in range(tl):
                across(index, k).wait()
            for step in range(1, tl):
                own_along(step, k).wait_send()
    if carry_weights:
        for j in range(PIECES):
            over_d.finish(j)
            if j < far_pieces:
                for row_part in range(2):
                    from_far(j, row_part).wait_send()
        here_out().wait()
    for k in range(CHUNKS):
        for index in range(tl):
            to_core(index, k).wait_send()
        for step in range(1, tl):
            along(step, k).wait_send()


def exchange(collective_id, partial, aux, outs, epilogue, gather, weight_rows=(), jobs=(), last=()):
    nd, tl = lax.axis_size("d"), lax.axis_size("l")
    total, width = partial.shape
    own = total // (2 * tl)
    dma = pltpu.SemaphoreType.DMA
    vmem = pl.BlockSpec(memory_space=pltpu.VMEM)
    anywhere = pl.BlockSpec(memory_space=pl.ANY)
    out_shape = list(outs)
    out_specs = [vmem] * len(outs)
    scratch = []
    given = tuple(value for job in jobs for value in job.inputs)
    if gather:
        out_shape.append(jax.ShapeDtypeStruct((total, width), jnp.bfloat16))
        out_specs.append(anywhere)
    if weight_rows:
        rows, cols = weight_rows[1].shape
        out_shape.append(jax.ShapeDtypeStruct((nd * rows, 2 * cols), jnp.bfloat16))
        out_specs.append(anywhere)
        scratch += [
            pltpu.VMEM((rows, cols), jnp.bfloat16),
            dma((PIECES, 2)),
            dma((PIECES, 2)),
            dma((PIECES, hop_count(nd))),
            dma((PIECES, hop_count(nd))),
            dma,
            dma,
        ]
    for job in jobs:
        out_shape.append(jax.ShapeDtypeStruct(job.shape, jnp.bfloat16))
        out_specs.append(anywhere)
        scratch += job.scratch()
    if last:
        others = 4 * nd * tl - 1
        scratch += [
            pltpu.VMEM((own, width), jnp.bfloat16),
            pltpu.VMEM((own, width), jnp.bfloat16),
            pltpu.VMEM((1, width), jnp.float32),
            pltpu.VMEM((2 * nd, 8, 128), jnp.float32),
            pltpu.VMEM((others, 8, 128), jnp.float32),
            dma((CHUNKS,)),
            dma((CHUNKS,)),
            dma((others,)),
            dma((others,)),
        ]
        cols = min(array.shape[1] for array in last) // 2
        count = sum(array.shape[1] for array in last) // cols
        scratch += Return.scratch(nd, count, outs[2].shape[0], cols)
    if gather:
        scratch += [
            pltpu.VMEM((own, width), jnp.bfloat16),
            dma(((tl - 1) * CHUNKS,)),
            dma(((tl - 1) * CHUNKS,)),
            dma((tl * CHUNKS,)),
            dma((tl * CHUNKS,)),
            dma((CHUNKS,)),
        ]
    scratch += [
        pltpu.VMEM((tl * own, width), jnp.bfloat16),
        pltpu.VMEM((tl * own, width), jnp.bfloat16),
        pltpu.VMEM(((tl - 1) * own, width), jnp.bfloat16),
        pltpu.VMEM(((tl - 1) * own, width), jnp.bfloat16),
        dma((tl * CHUNKS,)),
        dma((tl * CHUNKS,)),
        dma((tl * CHUNKS,)),
        dma(((tl - 1) * CHUNKS,)),
        dma(((tl - 1) * CHUNKS,)),
    ]
    return pl.pallas_call(
        functools.partial(
            exchange_kernel,
            nd,
            tl,
            epilogue,
            len(aux),
            len(outs),
            gather,
            bool(weight_rows),
            jobs,
            len(last),
        ),
        out_shape=tuple(out_shape),
        in_specs=[anywhere] + [vmem] * len(aux) + [anywhere] * (len(given) + len(weight_rows) + len(last)),
        out_specs=out_specs,
        scratch_shapes=scratch,
        compiler_params=pltpu.CompilerParams(
            has_side_effects=True, collective_id=collective_id, vmem_limit_bytes=60 << 20
        ),
        cost_estimate=pl.CostEstimate(
            flops=0, bytes_accessed=200_000_000 if gather else 110_000_000, transcendentals=0
        ),
    )(partial, *aux, *given, *weight_rows, *last)


def middle_rows(total, rows, k, aux, outs):
    stream, gain = aux
    value = stream[rows, :].astype(jnp.float32) + total
    outs[0][rows, :] = value
    return rms_scale(value, gain[...]).astype(jnp.bfloat16)


def norm_pull(value, gain, grad):
    scale = lax.rsqrt(jnp.mean(value * value, axis=-1, keepdims=True) + EPS)
    scaled = grad * gain
    inner = jnp.mean(value * scaled, axis=-1, keepdims=True)
    return scale * scaled - value * (scale * scale * scale * inner), jnp.sum(
        grad * value * scale, axis=0, keepdims=True
    )


def add_rows(out, value, k):
    @pl.when(k == 0)
    def _():
        out[...] = value

    @pl.when(k > 0)
    def _():
        out[...] += value


def middle_pull_rows(total, rows, k, aux, outs):
    middle, cotangent, gain = aux
    pulled, gain_part = norm_pull(middle[rows, :], gain[...], total)
    value = cotangent[rows, :].astype(jnp.float32) + pulled
    outs[0][rows, :] = value
    add_rows(outs[1], gain_part, k)
    return value.astype(jnp.bfloat16)


def stream_pull_rows(total, rows, k, aux, outs):
    stream, gradient, gain = aux
    pulled, gain_part = norm_pull(stream[rows, :].astype(jnp.float32), gain[...], total)
    value = gradient[rows, :] + pulled
    outs[0][rows, :] = value
    outs[1][rows, :] = value.astype(jnp.bfloat16)
    add_rows(outs[2], gain_part, k)
    return None


def key_tile(rows):
    return next(size for size in (384, 256, 128) if rows % size == 0)


def turn(values):
    return pltpu.roll(values, HEAD_WIDTH // 2, 1)


def head_norm(values):
    return lax.rsqrt(jnp.mean(values * values, axis=-1, keepdims=True) + EPS)


def tile_mask(first, start, tile, row0, rows):
    keys = start + lax.broadcasted_iota(jnp.int32, (rows, tile), 1)
    last = row0 + lax.broadcasted_iota(jnp.int32, (rows, tile), 0)
    return jnp.logical_and(keys >= first, keys <= last)


def dot_last(left, right):
    return lax.dot_general(
        left, right, (((1,), (1,)), ((), ())), preferred_element_type=jnp.float32
    )


def attention_kernel(blocks, repeat, order_ref, *refs):
    q, k, v, cosine, sine, q_gain, k_gain, first = refs[:8]
    qr, kr, vb, out, total = refs[8:13]
    acc, den = refs[13:]
    rows = q.shape[0] // blocks
    tile = key_tile(q.shape[0])
    scale = HEAD_WIDTH**-0.5 * math.log2(math.e)

    def rotated(values, gain, at):
        scaled = values * head_norm(values) * gain
        return (scaled * cosine[at, :] + turn(scaled) * sine[at, :]).astype(jnp.bfloat16)

    def prepare(i, carry):
        at, to = rows_at(i, rows), rows_at(order_ref[i], rows)
        for r in range(repeat):
            head = slice(r * HEAD_WIDTH, (r + 1) * HEAD_WIDTH)
            qr[at, head] = rotated(q[at, head], q_gain[...], at)
        kr[to, :] = rotated(k[at, :], k_gain[...], at)
        vb[to, :] = v[at, :].astype(jnp.bfloat16)
        return carry

    lax.fori_loop(0, blocks, prepare, 0)

    def attend(i, carry):
        at = rows_at(i, rows)
        row0 = order_ref[i] * rows
        acc[...] = jnp.zeros_like(acc)
        den[...] = jnp.zeros_like(den)

        def over_keys(t, inner):
            keys = rows_at(t, tile)
            mask = tile_mask(first[at, :], t * tile, tile, row0, rows)
            for r in range(repeat):
                head = slice(r * HEAD_WIDTH, (r + 1) * HEAD_WIDTH)
                scores = dot_last(qr[at, head], kr[keys, :]) * scale
                weights = jnp.where(mask, jnp.exp2(scores), 0.0)
                den[r] += jnp.sum(weights, axis=-1, keepdims=True)
                acc[r] += jnp.dot(
                    weights.astype(jnp.bfloat16), vb[keys, :], preferred_element_type=jnp.float32
                )
            return inner

        lax.fori_loop(0, (row0 + rows + tile - 1) // tile, over_keys, 0)
        for r in range(repeat):
            head = slice(r * HEAD_WIDTH, (r + 1) * HEAD_WIDTH)
            out[at, head] = (acc[r] / den[r]).astype(jnp.bfloat16)
            total[at, r : r + 1] = den[r]
        return carry

    lax.fori_loop(0, blocks, attend, 0)


def attention_specs(rows, q_heads, kv_heads):
    repeat = q_heads // kv_heads

    def columns(width, start=0):
        return pl.BlockSpec((rows, width * HEAD_WIDTH), lambda g, order: (0, start // width + g))

    def fixed(*shape):
        return pl.BlockSpec(shape, lambda g, order: (0, 0))

    raw = [columns(repeat), columns(1, q_heads), columns(1, q_heads + kv_heads)]
    tables = [
        fixed(rows, HEAD_WIDTH),
        fixed(rows, HEAD_WIDTH),
        fixed(1, HEAD_WIDTH),
        fixed(1, HEAD_WIDTH),
        fixed(rows, 1),
    ]
    return repeat, columns, fixed, raw, tables


def attention(qkv, tables, order, q_heads, kv_heads):
    rows = qkv.shape[0]
    blocks = order.shape[0]
    repeat, columns, _, raw, table_specs = attention_specs(rows, q_heads, kv_heads)
    wide, narrow = q_heads * HEAD_WIDTH, kv_heads * HEAD_WIDTH
    return pl.pallas_call(
        functools.partial(attention_kernel, blocks, repeat),
        name="attention",
        out_shape=(
            jax.ShapeDtypeStruct((rows, wide), jnp.bfloat16),
            jax.ShapeDtypeStruct((rows, narrow), jnp.bfloat16),
            jax.ShapeDtypeStruct((rows, narrow), jnp.bfloat16),
            jax.ShapeDtypeStruct((rows, wide), jnp.bfloat16),
            jax.ShapeDtypeStruct((rows, narrow), jnp.float32),
        ),
        grid_spec=pltpu.PrefetchScalarGridSpec(
            num_scalar_prefetch=1,
            grid=(kv_heads,),
            in_specs=raw + table_specs,
            out_specs=[columns(repeat), columns(1), columns(1), columns(repeat), columns(1)],
            scratch_shapes=[
                pltpu.VMEM((repeat, rows // blocks, HEAD_WIDTH), jnp.float32),
                pltpu.VMEM((repeat, rows // blocks, 1), jnp.float32),
            ],
        ),
        compiler_params=pltpu.CompilerParams(vmem_limit_bytes=50 << 20),
        cost_estimate=pl.CostEstimate(
            flops=4 * rows * rows * wide, bytes_accessed=60_000_000, transcendentals=0
        ),
    )(order, qkv, qkv, qkv, *tables)


def attention_pull_kernel(blocks, repeat, order_ref, *refs):
    q, k, cosine, sine, q_gain, k_gain, first, qr, kr, vb, total, out, grad = refs[:13]
    dq, dk, dv, dq_gain, dk_gain = refs[13:18]
    dq_acc, dk_acc, dv_acc = refs[18:]
    rows = q.shape[0] // blocks
    tile = key_tile(q.shape[0])
    scale = HEAD_WIDTH**-0.5
    dk_acc[...] = jnp.zeros_like(dk_acc)
    dv_acc[...] = jnp.zeros_like(dv_acc)

    @pl.when(pl.program_id(0) == 0)
    def _():
        dq_gain[...] = jnp.zeros_like(dq_gain)
        dk_gain[...] = jnp.zeros_like(dk_gain)

    def pull(raw, gain, turned_grad, at, gain_out):
        scaled_grad = turned_grad * cosine[at, :] + turn(turned_grad * sine[at, :])
        r = head_norm(raw)
        gain_out[0:1, :] += jnp.sum(scaled_grad * raw * r, axis=0, keepdims=True)
        scaled = scaled_grad * gain
        inner = jnp.mean(raw * scaled, axis=-1, keepdims=True)
        return (r * scaled - raw * (r * r * r * inner)).astype(jnp.bfloat16)

    def over_rows(i, carry):
        at = rows_at(i, rows)
        row0 = order_ref[i] * rows
        tiles = (row0 + rows + tile - 1) // tile
        dq_acc[...] = jnp.zeros_like(dq_acc)
        heads = [slice(r * HEAD_WIDTH, (r + 1) * HEAD_WIDTH) for r in range(repeat)]
        inner = [
            jnp.sum(
                grad[at, head].astype(jnp.float32) * out[at, head].astype(jnp.float32),
                axis=-1,
                keepdims=True,
            )
            for head in heads
        ]
        inverse = [1.0 / total[at, r : r + 1] for r in range(repeat)]

        def over_keys(t, carry):
            keys = rows_at(t, tile)
            mask = tile_mask(first[at, :], t * tile, tile, row0, rows)
            for r, head in enumerate(heads):
                scores = dot_last(qr[at, head], kr[keys, :]) * (scale * math.log2(math.e))
                share = jnp.where(mask, jnp.exp2(scores), 0.0) * inverse[r]
                share_grad = dot_last(grad[at, head], vb[keys, :])
                score_grad = (share * (share_grad - inner[r])).astype(jnp.bfloat16)
                dq_acc[r] += jnp.dot(score_grad, kr[keys, :], preferred_element_type=jnp.float32)
                dk_acc[keys, :] += contract_rows(score_grad, qr[at, head])
                dv_acc[keys, :] += contract_rows(share.astype(jnp.bfloat16), grad[at, head])
            return carry

        lax.fori_loop(0, tiles, over_keys, 0)
        for r in range(repeat):
            head = slice(r * HEAD_WIDTH, (r + 1) * HEAD_WIDTH)
            dq[at, head] = pull(q[at, head], q_gain[...], dq_acc[r] * scale, at, dq_gain)
        return carry

    lax.fori_loop(0, blocks, over_rows, 0)

    def finish(i, carry):
        at, to = rows_at(i, rows), rows_at(order_ref[i], rows)
        dk[at, :] = pull(k[at, :], k_gain[...], dk_acc[to, :] * scale, at, dk_gain)
        dv[at, :] = dv_acc[to, :].astype(jnp.bfloat16)
        return carry

    lax.fori_loop(0, blocks, finish, 0)


def attention_pull(qkv, tables, order, kept, grad, q_heads, kv_heads):
    rows = qkv.shape[0]
    blocks = order.shape[0]
    repeat, columns, fixed, raw, table_specs = attention_specs(rows, q_heads, kv_heads)
    wide, narrow = q_heads * HEAD_WIDTH, kv_heads * HEAD_WIDTH
    own = rows // blocks
    return pl.pallas_call(
        functools.partial(attention_pull_kernel, blocks, repeat),
        out_shape=(
            jax.ShapeDtypeStruct((rows, wide), jnp.bfloat16),
            jax.ShapeDtypeStruct((rows, narrow), jnp.bfloat16),
            jax.ShapeDtypeStruct((rows, narrow), jnp.bfloat16),
            jax.ShapeDtypeStruct((8, HEAD_WIDTH), jnp.float32),
            jax.ShapeDtypeStruct((8, HEAD_WIDTH), jnp.float32),
        ),
        grid_spec=pltpu.PrefetchScalarGridSpec(
            num_scalar_prefetch=1,
            grid=(kv_heads,),
            in_specs=raw[:2]
            + table_specs
            + [columns(repeat), columns(1), columns(1), columns(1), columns(repeat), columns(repeat)],
            out_specs=[
                columns(repeat),
                columns(1),
                columns(1),
                fixed(8, HEAD_WIDTH),
                fixed(8, HEAD_WIDTH),
            ],
            scratch_shapes=[
                pltpu.VMEM((repeat, own, HEAD_WIDTH), jnp.float32),
                pltpu.VMEM((rows, HEAD_WIDTH), jnp.float32),
                pltpu.VMEM((rows, HEAD_WIDTH), jnp.float32),
            ],
        ),
        compiler_params=pltpu.CompilerParams(vmem_limit_bytes=56 << 20),
        cost_estimate=pl.CostEstimate(
            flops=10 * rows * rows * wide, bytes_accessed=120_000_000, transcendentals=0
        ),
    )(order, qkv, qkv, *tables, *kept, grad)


def shift_perm(size, step):
    return [((place + step) % size, place) for place in range(size)]


def trade(values):
    return lax.ppermute(values, ("c", "h"), [(0, 0), (1, 2), (2, 1), (3, 3)])


def gather_along(own):
    places = lax.axis_size("l")
    return [own] + [lax.ppermute(own, "l", shift_perm(places, step)) for step in range(1, places)]


def gather_across(parts):
    half = jnp.concatenate(parts, axis=0)
    other = lax.ppermute(half, "c", shift_perm(2, 1))
    return jnp.concatenate([half, other], axis=0)


def scatter_tokens(partial, *first):
    places = lax.axis_size("l")
    half = partial.shape[0] // 2
    rows = half // places
    other = lax.ppermute(partial[half:].astype(jnp.bfloat16), "c", shift_perm(2, 1))
    total = partial[:half] + other.astype(jnp.float32)
    own = total[:rows]
    for step in range(1, places):
        sent = total[step * rows : (step + 1) * rows].astype(jnp.bfloat16)
        moved = lax.ppermute(sent, "l", shift_perm(places, -step))
        moved = after(moved, *first)
        own = own + moved.astype(jnp.float32)
    return own


def after(value, *others):
    return lax.optimization_barrier((value,) + others)[0]


def return_halves(near, far):
    core = lax.axis_index("c")
    far = lax.ppermute(far, "h", shift_perm(2, 1))
    sums = near.astype(jnp.float32) + far.astype(jnp.float32)
    rows = sums.shape[0] // 2
    first, second = sums[:rows], sums[rows:]
    mine = jnp.where(core == 0, first, second)
    sent = jnp.where(core == 0, second, first).astype(jnp.bfloat16)
    other = lax.ppermute(sent, "c", shift_perm(2, 1)).astype(jnp.float32)
    return mine, other


def columns_of(mine, other):
    core = lax.axis_index("c")
    return jnp.concatenate(
        [jnp.where(core == 0, mine, other), jnp.where(core == 0, other, mine)], axis=1
    )


def sum_over_d(partial):
    return lax.psum_scatter(partial.astype(jnp.bfloat16), "d", scatter_dimension=0, tiled=True)


def as_row(values):
    return values.reshape(1, -1)


def split(values):
    half = values.shape[1] // 2
    return values[:, :half], values[:, half:]


def per_device(
    tokens,
    segment_ids,
    attn_gain,
    q_weight,
    key_matrix,
    value_matrix,
    o_weight,
    q_gain,
    k_gain,
    mlp_gain,
    gate_weight,
    up_weight,
    down_weight,
    cotangent,
):
    width = attn_gain.shape[1] * lax.axis_size("d") * 2
    own_rows = tokens.shape[0]
    places = lax.axis_size("l")
    core, place = lax.axis_index("c"), lax.axis_index("l")
    q_cols, kv_cols, ff_cols = q_weight.shape[2], key_matrix.shape[2], gate_weight.shape[2]
    half_cols = ff_cols // 2

    cut = attn_gain.shape[1]
    head_cut = q_gain.shape[1]
    gains = jnp.concatenate([attn_gain[0], mlp_gain[0], q_gain[0], k_gain[0]]).astype(jnp.float32)
    gains = jnp.pad(gains, (0, 1024 - gains.shape[0])).reshape(8, 128)
    labels = trade(segment_ids)[0]
    order = jnp.stack(
        [
            ((core + core_step) % 2) * places + (place + step) % places
            for core_step in range(2)
            for step in range(places)
        ]
    )
    row_index = (order[:, None] * own_rows + jnp.arange(own_rows, dtype=jnp.int32)[None, :]).reshape(-1)
    labels = labels.reshape(2 * places, own_rows)[order].reshape(-1)
    cosine, sine, first_row = rotary_tables(labels, row_index)
    qkv_full, o_full, mid_rows, down_rows, group, cotangent, gains = enter(
        q_weight[0],
        key_matrix[0],
        value_matrix[0],
        o_weight[0],
        gate_weight[0],
        up_weight[0],
        down_weight[0],
        after(tokens, cosine, sine, first_row),
        cotangent,
        gains,
    )
    mid_near = lax.all_gather(mid_rows, "d", axis=0, tiled=True)
    down_near = lax.all_gather(down_rows, "d", axis=0, tiled=True)
    up_far = lax.ppermute(mid_rows[:, half_cols:], "h", shift_perm(2, 1))
    grad_half = gather_along(cotangent)
    gains = gains.reshape(gains.shape[0], -1)
    attn_scale = gains[:, :cut].reshape(-1)
    mlp_scale = gains[:, cut : 2 * cut].reshape(-1)
    q_scale = gains[:, 2 * cut : 2 * cut + head_cut].reshape(-1)
    k_scale = gains[:, 2 * cut + head_cut : 2 * cut + 2 * head_cut].reshape(-1)

    stream = group[:own_rows]
    normed = rms_scale(group.astype(jnp.float32), attn_scale).astype(jnp.bfloat16)
    head_count, kv_heads = q_cols // HEAD_WIDTH, kv_cols // HEAD_WIDTH
    qkv = jnp.dot(normed, qkv_full, preferred_element_type=jnp.float32)
    down_far = lax.ppermute(after(down_rows, qkv), "h", shift_perm(2, 1))
    tables = (cosine, sine, as_row(q_scale), as_row(k_scale), first_row)
    query_reduced, key_reduced, value_reduced, attended, totals = attention(
        qkv, tables, order, head_count, kv_heads
    )


    def whole(values):
        return jax.ShapeDtypeStruct((own_rows, width), values)

    gain_sum = jax.ShapeDtypeStruct((1, width), jnp.float32)
    middle, normed_mid, mid_far = exchange(
        1,
        contract_cols(attended, o_full).astype(jnp.bfloat16),
        (stream, as_row(mlp_scale)),
        (whole(jnp.float32),),
        middle_rows,
        True,
        (mid_rows, after(up_far, attended)),
    )
    grad_rows = gather_across([grad_half[0]] + [after(part, normed_mid) for part in grad_half[1:]])
    down_far = lax.all_gather(after(down_far, normed_mid), "d", axis=0, tiled=True)

    mid = jnp.dot(normed_mid, mid_near, preferred_element_type=jnp.float32)
    gate_near, up_near = split(mid)
    hidden_near = swiglu(gate_near, up_near).astype(jnp.bfloat16)
    mid = jnp.dot(normed_mid, mid_far, preferred_element_type=jnp.float32)
    gate_far, up_far = split(mid)
    hidden_far = swiglu(gate_far, up_far).astype(jnp.bfloat16)
    down_grad_far = contract_rows(grad_rows, hidden_far).astype(jnp.bfloat16)
    down_sum_far = sum_over_d(down_grad_far)
    grad_rows = after(grad_rows, down_grad_far, hidden_near)

    def hidden_pull(gate, up, down):
        hidden_grad = jnp.dot(grad_rows, down, preferred_element_type=jnp.float32)
        _, pull_back = jax.vjp(swiglu, gate, up)
        gate_grad, up_grad = pull_back(hidden_grad)
        return jnp.concatenate(
            [gate_grad.astype(jnp.bfloat16), up_grad.astype(jnp.bfloat16)], axis=1
        )

    mid_back_near = hidden_pull(gate_near, up_near, down_near)
    mid_back_far = hidden_pull(gate_far, up_far, down_far)
    mid_grad_far = contract_rows(normed_mid, mid_back_far).astype(jnp.bfloat16)
    mid_sum_far = sum_over_d(mid_grad_far)
    normed_grad = contract_cols(mid_back_near, mid_near) + contract_cols(mid_back_far, mid_far)
    normed_grad = normed_grad.astype(jnp.bfloat16)
    gradient, mlp_gain_grad, grad_rows, mid_grad_near, down_grad_near, branch = exchange(
        2,
        after(normed_grad, mid_grad_far),
        (middle, cotangent, as_row(mlp_scale)),
        (whole(jnp.float32), gain_sum),
        middle_pull_rows,
        True,
        jobs=(
            Job((normed_mid, mid_back_near), mid_near.shape, 8, weight_grad_tile),
            Job((grad_rows, hidden_near), down_near.shape, 8, weight_grad_tile),
            Job((hidden_near, hidden_far, down_near, down_far), normed_mid.shape, 4, down_tile),
        ),
    )
    down_sum_near = sum_over_d(down_grad_near)
    mid_sum_near = sum_over_d(mid_grad_near)

    out_grad = jnp.dot(grad_rows, o_full, preferred_element_type=jnp.float32).astype(jnp.bfloat16)
    o_wgrad = contract_rows(grad_rows, attended)
    query_back, key_back, value_back, q_gain_grad, k_gain_grad = attention_pull(
        qkv,
        tables,
        order,
        (query_reduced, key_reduced, value_reduced, totals, attended),
        out_grad,
        head_count,
        kv_heads,
    )
    qkv_back = jnp.concatenate([query_back, key_back, value_back], axis=1)
    qkv_grad = contract_rows(normed, qkv_back).astype(jnp.bfloat16)
    o_wgrad = o_wgrad.astype(jnp.bfloat16)
    branch = scatter_tokens(branch, qkv_grad)
    activations = trade((middle + branch).astype(jnp.bfloat16))
    gradient, sums, attn_grad = exchange(
        None,
        contract_cols(after(qkv_back, qkv_grad), qkv_full).astype(jnp.bfloat16),
        (stream, gradient, as_row(attn_scale), mlp_gain_grad, q_gain_grad, k_gain_grad),
        (
            whole(jnp.float32),
            jax.ShapeDtypeStruct((8, 128), jnp.float32),
            jax.ShapeDtypeStruct((q_weight.shape[1], 2 * q_cols + 2 * kv_cols), jnp.float32),
        ),
        stream_pull_rows,
        False,
        last=(qkv_grad, o_wgrad),
    )
    lines = cut // 128
    head_at = (lax.axis_index("d") * 2 + core) * head_cut

    def head_gain(line):
        return lax.dynamic_slice(sums[line], (head_at,), (head_cut,))[None]

    mid_sum_near = after(mid_sum_near, sums)
    down_sum_near = after(down_sum_near, sums)
    down_grad = columns_of(*return_halves(down_sum_near, down_sum_far))
    mine, other = return_halves(mid_sum_near, mid_sum_far)
    gate_grad = columns_of(mine[:, :half_cols], other[:, :half_cols])
    up_grad = columns_of(mine[:, half_cols:], other[:, half_cols:])

    return (
        activations,
        gradient,
        sums[:lines].reshape(1, cut),
        attn_grad[None, :, :q_cols],
        attn_grad[None, :, q_cols : q_cols + kv_cols],
        attn_grad[None, :, q_cols + kv_cols : q_cols + 2 * kv_cols],
        attn_grad[None, :, q_cols + 2 * kv_cols :],
        head_gain(2 * lines),
        head_gain(2 * lines + 1),
        sums[lines : 2 * lines].reshape(1, cut),
        gate_grad[None],
        up_grad[None],
        down_grad[None],
    )


def solution(mesh):
    dp, tensor = mesh.shape["dp"], mesh.shape["tensor"]
    cut = Mesh(mesh.devices.reshape(dp // 2, 2, 2, tensor // 2), ("d", "c", "h", "l"))
    rows, cols = ("d", "c"), ("h", "l")
    tokens, labels = P(rows + cols, None), P(rows, None)
    gain, weight = P(None, rows), P(None, rows, cols)
    return jax.shard_map(
        per_device,
        mesh=cut,
        in_specs=(
            tokens,
            labels,
            gain,
            weight,
            weight,
            weight,
            weight,
            gain,
            gain,
            gain,
            weight,
            weight,
            weight,
            tokens,
        ),
        out_specs=(
            tokens,
            tokens,
            gain,
            weight,
            weight,
            weight,
            weight,
            gain,
            gain,
            gain,
            weight,
            weight,
            weight,
        ),
        check_vma=False,
    )
```

```python
import functools
import math

import jax
import jax.numpy as jnp
from jax import lax
from jax.experimental import pallas as pl
from jax.experimental.pallas import tpu as pltpu
from jax.sharding import Mesh
from jax.sharding import PartitionSpec as P


HEAD_WIDTH = 128
NSEQ = 3


EPS = 1e-06
THETA = 1000000.0


def rms_scale(values, gain):
    return values * lax.rsqrt(jnp.mean(values * values, axis=-1, keepdims=True) + EPS) * gain


def swiglu(gate_raw, up_raw):
    return jax.nn.silu(gate_raw) * up_raw


def rotary_tables(sequence_labels, row_index):
    labels = jnp.arange(NSEQ, dtype=jnp.int32)
    starts = jnp.sum((sequence_labels[None, :] < labels[:, None]).astype(jnp.int32), axis=1)
    first_row = jnp.sum(
        jnp.where(sequence_labels[:, None] == labels[None, :], starts[None, :], 0), axis=1
    )
    position = (row_index - first_row).astype(jnp.float32)
    frequency = THETA ** (-(jnp.arange(HEAD_WIDTH // 2, dtype=jnp.float32) * (2.0 / HEAD_WIDTH)))
    angles = position[:, None] * frequency[None, :]
    sine = jnp.sin(angles)
    cosine = jnp.cos(angles)
    return (
        jnp.concatenate([cosine, cosine], axis=1),
        jnp.concatenate([-sine, sine], axis=1),
        first_row[:, None],
    )


def contract_rows(left, right):
    return lax.dot_general(
        left, right, (((0,), (0,)), ((), ())), preferred_element_type=jnp.float32
    )


def contract_cols(left, right):
    return lax.dot_general(
        left, right, (((1,), (1,)), ((), ())), preferred_element_type=jnp.float32
    )


MESH = pl.DeviceIdType.MESH
CHUNKS = 3


def remote(source, target, send_sem, recv_sem, **place):
    return pltpu.make_async_remote_copy(
        src_ref=source,
        dst_ref=target,
        send_sem=send_sem,
        recv_sem=recv_sem,
        device_id=place,
        device_id_type=MESH,
    )


def rows_at(index, size):
    return pl.ds(pl.multiple_of(index * size, size), size)


WEIGHTS = 5
ENTRY_START = (
    "w0", "t0", "w1", "w2", "t1", "w3", "w4", "t2",
)
ENTRY_ORDER = (
    "s0", "t0", "s1", "r0", "s2", "r1", "t1", "s3", "r2", "s4", "r3", "t2", "r4", "a0", "a1",
    "a2",
)


def hop_plan(nd, d):
    if nd == 4:
        side_x = d + 1 - 2 * lax.rem(d, 2)
        side_y = d + 2 - 4 * (d // 2)
        corner = side_x + side_y - d
        hops = (
            (0, d, side_x),
            (1, d, side_x),
            (0, d, side_y),
            (1, d, side_y),
            (0, side_x, side_y),
            (1, side_y, side_x),
        )
        sources = ((0, side_x), (1, side_x), (0, side_y), (1, side_y), (0, corner), (1, corner))
        return hops, sources, 4, ((0, 4), (3, 5))
    steps = [(part, step) for step in range(1, nd) for part in range(2)]
    hops = tuple((part, d, lax.rem(d + step, nd)) for part, step in steps)
    sources = tuple((part, lax.rem(d + nd - step, nd)) for part, step in steps)
    return hops, sources, len(hops), ()


def hop_count(nd):
    return 6 if nd == 4 else 2 * (nd - 1)


class Spread:
    def __init__(self, nd, d, block, send_sem, recv_sem, own=None):
        self.hops, self.sources, self.first, self.relayed = hop_plan(nd, d)
        self.block, self.send_sem, self.recv_sem = block, send_sem, recv_sem
        self.own = own or (lambda j, part: block(j, d * 2 + part))

    def copy(self, j, kind, source, part, of):
        return remote(
            source,
            self.block(j, of * 2 + part),
            self.send_sem.at[j, kind],
            self.recv_sem.at[j, kind],
            d=self.hops[kind][2],
        )

    def hop(self, j, kind):
        part, of, _ = self.hops[kind]
        source = self.own(j, part) if kind < self.first else self.block(j, of * 2 + part)
        return self.copy(j, kind, source, part, of)

    def arrived(self, j, kind):
        part, of = self.sources[kind]
        return self.copy(j, kind, self.block(j, of * 2 + part), part, of)

    def send(self, j, part):
        for kind in range(self.first):
            if self.hops[kind][0] == part:
                self.hop(j, kind).start()

    def relay(self, j):
        for after_kind, kind in self.relayed:
            self.arrived(j, after_kind).wait_recv()
            self.hop(j, kind).start()

    def finish(self, j):
        handled = {after_kind for after_kind, _ in self.relayed}
        for kind in range(len(self.hops)):
            if kind not in handled:
                self.arrived(j, kind).wait_recv()
            self.hop(j, kind).wait_send()


def entry_kernel(nd, tl, *refs):
    (q_ref, k_ref, v_ref, o_ref, gate_ref, up_ref, down_ref, tok_ref, cot_ref, gain_ref) = refs[:10]
    (qkv_full, o_full, mid_rows, down_rows, tok_full, cot_own, gain_full) = refs[10:17]
    (stage, half_stage, tok_stage, cot_stage) = refs[17:21]
    (zs, zr, cs, li, lo, xs, xr, ts, tr, tli, tlo, ls, lr, fs, fr) = refs[21:36]
    (gs, gr, gl, os, orv, oi, hs, hr, hi, ho) = refs[36:]
    d, c, h, l = (lax.axis_index(name) for name in ("d", "c", "h", "l"))
    same = c == h
    apart = c != h
    rows = q_ref.shape[0]
    own = tok_ref.shape[0]
    chunk = own // CHUNKS
    q_cols, kv_cols = q_ref.shape[1], k_ref.shape[1]
    o_half = o_ref.shape[1] // 2
    qkv_cols = q_cols + 2 * kv_cols
    weights = (
        (q_ref, qkv_full, 0, q_cols, 0),
        (k_ref, qkv_full, q_cols, kv_cols, q_cols),
        (v_ref, qkv_full, q_cols + kv_cols, kv_cols, q_cols + kv_cols),
        (o_ref.at[:, pl.ds(0, o_half)], o_full, 0, o_half, qkv_cols),
        (o_ref.at[:, pl.ds(o_half, o_half)], o_full, o_half, o_half, qkv_cols + o_half),
    )

    def block(j, row):
        _, full, start, cols, _ = weights[j]
        return full.at[rows_at(row, rows), pl.ds(start, cols)]

    def held(j):
        _, _, _, cols, start = weights[j]
        return stage.at[:, pl.ds(start, cols)]

    def from_far(j, part):
        return remote(block(j, d * 2 + part), block(j, d * 2 + part), zs.at[j], zr.at[j, part], h=1 - h)

    def to_far(j):
        return remote(weights[j][0], block(j, d * 2 + c), zs.at[j], zr.at[j, c], c=h, h=1 - h)

    def to_core(j):
        return remote(weights[j][0], block(j, d * 2 + c), cs.at[j], zr.at[j, c], c=h)

    def local_in(j):
        return pltpu.make_async_copy(weights[j][0], held(j), li.at[j])

    def local_out(j):
        return pltpu.make_async_copy(held(j), block(j, d * 2 + c), lo.at[j])

    def tokens_at(index, k):
        return tok_full.at[pl.ds(index * own + k * chunk, chunk)]

    def trade_tokens(k):
        return remote(tok_ref.at[pl.ds(k * chunk, chunk)], tokens_at(0, k), ts.at[k], tr.at[k], c=h, h=c)

    def along(step, k):
        return remote(
            tokens_at(0, k),
            tokens_at(tl - step, k),
            ls.at[(step - 1) * CHUNKS + k],
            lr.at[(tl - step - 1) * CHUNKS + k],
            l=lax.rem(l + step, tl),
        )

    def from_along(index, k):
        return remote(
            tokens_at(index, k),
            tokens_at(index, k),
            ls.at[(index - 1) * CHUNKS + k],
            lr.at[(index - 1) * CHUNKS + k],
            l=l,
        )

    def across(index, k):
        at = index * CHUNKS + k
        return remote(tokens_at(index, k), tokens_at(tl + index, k), fs.at[at], fr.at[at], c=1 - c)

    def gain_peer(step):
        place = lax.rem(d * 2 + c + step, 2 * nd)
        return place // 2, lax.rem(place, 2)

    def gains_to(step):
        to_d, to_c = gain_peer(step)
        return remote(
            gain_ref, gain_full.at[d * 2 + c], gs.at[step - 1], gr.at[2 * nd - step - 1], d=to_d, c=to_c
        )

    def gains_from(step):
        from_d, from_c = gain_peer(step)
        return remote(
            gain_ref, gain_full.at[from_d * 2 + from_c], gs.at[step - 1], gr.at[step - 1], d=from_d, c=from_c
        )

    def local_gains():
        return pltpu.make_async_copy(gain_ref, gain_full.at[d * 2 + c], gl)

    half = gate_ref.shape[1] // 2
    halves = ((gate_ref, mid_rows, 0), (up_ref, mid_rows, half), (down_ref, down_rows, 0))

    def columns_of_core(j, of):
        return halves[j][0].at[:, pl.ds(pl.multiple_of(of * half, half), half)]

    def half_at(j, of):
        return halves[j][1].at[rows_at(of, rows), pl.ds(halves[j][2], half)]

    def half_to_core(j):
        return remote(columns_of_core(j, 1 - c), half_at(j, c), hs.at[j], hr.at[j], c=1 - c)

    def half_from_core(j):
        return remote(half_at(j, 1 - c), half_at(j, 1 - c), hs.at[j], hr.at[j], c=1 - c)

    def half_in(j):
        return pltpu.make_async_copy(columns_of_core(j, c), half_stage.at[j], hi.at[j])

    def half_out(j):
        return pltpu.make_async_copy(half_stage.at[j], half_at(j, c), ho.at[j])

    local_gains().start()

    def start_weights(j):
        to_far(j).start()

        @pl.when(apart)
        def _():
            to_core(j).start()

    def start_tokens(k):
        @pl.when(apart)
        def _():
            trade_tokens(k).start()

    def trade_cotangent():
        return remote(cot_ref, cot_own, os, orv, c=h, h=c)

    def cotangent_in():
        return pltpu.make_async_copy(cot_ref, cot_stage, oi)

    def cotangent_out():
        return pltpu.make_async_copy(cot_stage, cot_own, oi)

    for step in ENTRY_START:
        {"w": start_weights, "t": start_tokens}[step[0]](int(step[1:]))

    @pl.when(apart)
    def _():
        trade_cotangent().start()

    @pl.when(same)
    def _():
        pltpu.make_async_copy(tok_ref, tok_stage, tli).start()
        for j in range(WEIGHTS):
            local_in(j).start()
        pltpu.make_async_copy(tok_ref, tok_stage, tli).wait()
        for k in range(CHUNKS):
            part = pl.ds(k * chunk, chunk)
            pltpu.make_async_copy(tok_stage.at[part], tokens_at(0, k), tlo.at[k]).start()
        for j in range(WEIGHTS):
            local_in(j).wait()
            local_out(j).start()
        cotangent_in().start()
        cotangent_in().wait()
        cotangent_out().start()

    for step in range(1, 2 * nd):
        gains_to(step).start()
    for j in range(3):
        half_in(j).start()
        half_to_core(j).start()
    for j in range(3):
        half_in(j).wait()
        half_out(j).start()

    over_d = Spread(nd, d, block, xs, xr)

    def spread(j):
        for part in range(2):
            here = jnp.logical_and(same, c == part)

            @pl.when(here)
            def _():
                local_out(j).wait()

            @pl.when(jnp.logical_not(here))
            def _():
                from_far(j, part).wait_recv()

            over_d.send(j, part)

    relay = over_d.relay

    def own_tokens(k):
        @pl.when(same)
        def _():
            part = pl.ds(k * chunk, chunk)
            pltpu.make_async_copy(tok_stage.at[part], tokens_at(0, k), tlo.at[k]).wait()

        @pl.when(apart)
        def _():
            remote(tokens_at(0, k), tokens_at(0, k), ts.at[k], tr.at[k], c=1 - c, h=1 - h).wait_recv()

        for step in range(1, tl):
            along(step, k).start()
        across(0, k).start()

    def pass_across(k):
        for index in range(1, tl):
            from_along(index, k).wait_recv()
            across(index, k).start()

    steps = {"t": own_tokens, "s": spread, "r": relay, "a": pass_across}
    for step in ENTRY_ORDER:
        steps[step[0]](int(step[1:]))

    for j in range(WEIGHTS):
        over_d.finish(j)
        to_far(j).wait_send()
    for k in range(CHUNKS):
        for index in range(tl):
            across(index, k).wait()
        for step in range(1, tl):
            along(step, k).wait_send()
    for step in range(1, 2 * nd):
        gains_from(step).wait_recv()
        gains_to(step).wait_send()
    local_gains().wait()
    for j in range(3):
        half_from_core(j).wait_recv()
        half_to_core(j).wait_send()
        half_out(j).wait()

    @pl.when(same)
    def _():
        cotangent_out().wait()

    @pl.when(apart)
    def _():
        trade_cotangent().wait()
        for j in range(WEIGHTS):
            to_core(j).wait_send()
        for k in range(CHUNKS):
            trade_tokens(k).wait_send()


def enter(q_weight, k_weight, v_weight, o_weight, gate, up, down, tokens, cotangent, gains):
    nd, tl = lax.axis_size("d"), lax.axis_size("l")
    rows, q_cols = q_weight.shape
    qkv_cols = q_cols + 2 * k_weight.shape[1]
    own, width = tokens.shape
    half = gate.shape[1] // 2
    dma = pltpu.SemaphoreType.DMA
    counts = (
        (WEIGHTS,),
        (WEIGHTS, 2),
        (WEIGHTS,),
        (WEIGHTS,),
        (WEIGHTS,),
        (WEIGHTS, hop_count(nd)),
        (WEIGHTS, hop_count(nd)),
        (CHUNKS,),
        (CHUNKS,),
        (),
        (CHUNKS,),
        ((tl - 1) * CHUNKS,),
        ((tl - 1) * CHUNKS,),
        (tl * CHUNKS,),
        (tl * CHUNKS,),
        (2 * nd - 1,),
        (2 * nd - 1,),
        (),
        (),
        (),
        (),
        (3,),
        (3,),
        (3,),
        (3,),
    )
    anywhere = pl.BlockSpec(memory_space=pl.ANY)

    def low(*shape):
        return jax.ShapeDtypeStruct(shape, jnp.bfloat16)

    return pl.pallas_call(
        functools.partial(entry_kernel, nd, tl),
        name="entry",
        out_shape=(
            low(width, qkv_cols),
            low(width, o_weight.shape[1]),
            low(2 * rows, 2 * half),
            low(2 * rows, half),
            low(2 * tl * own, width),
            low(own, width),
            jax.ShapeDtypeStruct((2 * nd,) + gains.shape, jnp.float32),
        ),
        in_specs=[anywhere] * 10,
        out_specs=[anywhere] * 7,
        scratch_shapes=[
            pltpu.VMEM((rows, qkv_cols + o_weight.shape[1]), jnp.bfloat16),
            pltpu.VMEM((3, rows, half), jnp.bfloat16),
            pltpu.VMEM((own, width), jnp.bfloat16),
            pltpu.VMEM((own, width), jnp.bfloat16),
        ]
        + [dma(count) if count else dma for count in counts],
        compiler_params=pltpu.CompilerParams(has_side_effects=True),
        cost_estimate=pl.CostEstimate(flops=0, bytes_accessed=250_000_000, transcendentals=0),
    )(q_weight, k_weight, v_weight, o_weight, gate, up, down, tokens, cotangent, gains)


PIECES = 6
RETURN_AHEAD = 2
ROW_CHUNK = 48
RETURN_ORDER = (
    "m0", "w2", "f0", "f1", "m1", "w3", "f2", "f3", "h0", "m2", "w4", "f4", "f5", "g0", "h1", "m3",
    "w5", "h2", "m4", "h3", "m5", "h4", "h5",
)
SUM_ORDER = (
    "s3", "s4", "s5", "f0", "f1", "r3", "s0", "f2", "f3", "r4", "r0", "s1", "f4", "f5", "r5", "r1",
    "s2", "r2", "a0", "a1", "a2", "a3", "a4", "a5",
)


class Return:
    def __init__(self, nd, pieces, outs, scratch):
        self.nd, self.pieces = nd, pieces
        self.held, self.first, self.mixed, self.second, self.sums, self.parts = scratch[:6]
        (self.load, self.fs, self.fr, self.ss, self.sr, self.ps, self.pr) = scratch[6:]
        self.d, self.c, self.h = (lax.axis_index(name) for name in ("d", "c", "h"))
        self.rows = outs[0].shape[0]
        d = self.d
        cols = self.first.shape[3]
        self.places = [(out, start) for out in outs for start in range(0, out.shape[1], cols)]
        if nd == 4:
            side_x = d + 1 - 2 * lax.rem(d, 2)
            side_y = d + 2 - 4 * (d // 2)
            corner = side_x + side_y - d
            self.blocks = ((d, 0), (side_y, 0), (d, 1), (side_x, 1))
            self.sends = (
                (side_x, 0, side_x),
                (corner, 0, side_x),
                (side_y, 1, side_y),
                (corner, 1, side_y),
            )
            self.mixes = ((1, side_y), (3, side_x))
        else:
            self.blocks = ((d, 0), (d, 1))
            self.sends = tuple(
                (lax.rem(d + step, nd), part, lax.rem(d + step, nd))
                for step in range(1, nd)
                for part in range(2)
            )
            self.mixes = ()

    @staticmethod
    def scratch(nd, count, rows, cols):
        dma = pltpu.SemaphoreType.DMA
        blocks, sends, mixes = (4, 4, 2) if nd == 4 else (2, 2 * (nd - 1), 1)

        def buffer(number):
            return pltpu.VMEM((count, number, rows, cols), jnp.bfloat16)

        return [
            buffer(blocks),
            buffer(sends),
            buffer(mixes),
            buffer(mixes),
            buffer(2),
            buffer(2),
            dma((count, blocks)),
            dma((count, sends)),
            dma((count, sends)),
            dma((count, mixes)),
            dma((count, mixes)),
            dma((count, 2)),
            dma((count, 2)),
        ]

    def source(self, j, of, part):
        ref, start = self.pieces[j]
        cols = self.held.shape[3]
        return ref.at[rows_at(of * 2 + part, self.rows), pl.ds(start, cols)]

    def loading(self, j, at):
        return pltpu.make_async_copy(
            self.source(j, *self.blocks[at]), self.held.at[j, at], self.load.at[j, at]
        )

    def sending(self, j, at):
        of, part, to = self.sends[at]
        return remote(
            self.source(j, of, part), self.first.at[j, at], self.fs.at[j, at], self.fr.at[j, at], d=to
        )

    def mixing(self, j, at):
        return remote(
            self.mixed.at[j, at],
            self.second.at[j, at],
            self.ss.at[j, at],
            self.sr.at[j, at],
            d=self.mixes[at][1],
        )

    def handing(self, j, part):
        return remote(
            self.sums.at[j, part],
            self.parts.at[j, self.h],
            self.ps.at[j, part],
            self.pr.at[j, self.h],
            c=part,
            h=self.c,
        )

    def stays(self, part):
        return jnp.logical_and(self.c == part, self.h == self.c)

    def start(self, j):
        for at in range(len(self.sends)):
            self.sending(j, at).start()
        for at in range(len(self.blocks)):
            self.loading(j, at).start()

    def value(self, ref, j, at):
        return ref[j, at].astype(jnp.float32)

    def mix(self, j):
        for at, (block, _) in enumerate(self.mixes):
            self.loading(j, block).wait()
            self.sending(j, block).wait_recv()
            total = self.value(self.held, j, block) + self.value(self.first, j, block)
            self.mixed[j, at] = total.astype(jnp.bfloat16)
            self.mixing(j, at).start()

    def hand(self, j):
        for part in range(2):
            own = 2 * part if self.mixes else part
            self.loading(j, own).wait()
            total = self.value(self.held, j, own)
            for at in [own] if self.mixes else range(part, len(self.sends), 2):
                self.sending(j, at).wait_recv()
                total = total + self.value(self.first, j, at)
            if self.mixes:
                self.mixing(j, part).wait_recv()
                total = total + self.value(self.second, j, part)
            self.sums[j, part] = total.astype(jnp.bfloat16)

            @pl.when(self.stays(part))
            def _():
                self.parts[j, self.h] = self.sums[j, part]

            @pl.when(jnp.logical_not(self.stays(part)))
            def _():
                self.handing(j, part).start()

    def arriving(self, j, of_h):
        return remote(
            self.parts.at[j, of_h], self.parts.at[j, of_h], self.ps.at[j, 0], self.pr.at[j, of_h], h=1 - self.h
        )

    def finish(self, j):
        for of_h in range(2):

            @pl.when(jnp.logical_not(jnp.logical_and(self.c == self.h, self.h == of_h)))
            def _():
                self.arriving(j, of_h).wait_recv()

        out, start = self.places[j]
        out[:, start : start + self.first.shape[3]] = self.value(self.parts, j, 0) + self.value(
            self.parts, j, 1
        )
        for at in range(len(self.sends)):
            self.sending(j, at).wait_send()
        for at in range(len(self.mixes)):
            self.mixing(j, at).wait_send()
        for part in range(2):

            @pl.when(jnp.logical_not(self.stays(part)))
            def _():
                self.handing(j, part).wait_send()


class Job:
    def __init__(self, inputs, shape, tiles, made):
        self.inputs, self.shape, self.tiles, self.made = inputs, shape, tiles, made

    def scratch(self):
        dma = pltpu.SemaphoreType.DMA
        return [pltpu.VMEM(value.shape, value.dtype) for value in self.inputs] + [
            pltpu.VMEM(self.shape, jnp.bfloat16),
            dma((len(self.inputs),)),
            dma((self.tiles,)),
        ]


class RunningJob:
    def __init__(self, job, given, result, scratch):
        self.job, self.given, self.result = job, given, result
        *self.held, self.product, self.in_sem, self.out_sem = scratch
        self.rows = job.shape[0] // job.tiles

    def copy_in(self, at):
        return pltpu.make_async_copy(self.given[at], self.held[at], self.in_sem.at[at])

    def copy_out(self, i):
        rows = rows_at(i, self.rows)
        return pltpu.make_async_copy(
            self.product.at[rows], self.result.at[rows], self.out_sem.at[i]
        )

    def fetch(self):
        for at in range(len(self.given)):
            self.copy_in(at).start()

    def run(self):
        for at in range(len(self.given)):
            self.copy_in(at).wait()

        def one(i, carry):
            self.product[rows_at(i, self.rows), :] = self.job.made(self.held, i, self.rows)
            self.copy_out(i).start()
            return carry

        lax.fori_loop(0, self.job.tiles, one, 0)

    def finish(self):
        for i in range(self.job.tiles):
            self.copy_out(i).wait()


def weight_grad_tile(held, i, rows):
    left, right = held
    return contract_rows(left[:, rows_at(i, rows)], right[...]).astype(jnp.bfloat16)


def down_tile(held, i, rows):
    near, far, down_near, down_far = held
    at = rows_at(i, rows)
    return (
        contract_cols(near[at, :], down_near[...]) + contract_cols(far[at, :], down_far[...])
    ).astype(jnp.bfloat16)


def exchange_kernel(
    nd, tl, epilogue, aux_count, out_count, gather, carry_weights, jobs, last, *refs
):
    partial = refs[0]
    aux = refs[1 : 1 + aux_count]
    refs = refs[1 + aux_count :]
    job_given = []
    for job in jobs:
        count = len(job.inputs)
        job_given.append(refs[:count])
        refs = refs[count:]
    if carry_weights:
        weight_rows, here_rows, refs = refs[0], refs[1], refs[2:]
    gradients, refs = refs[:last], refs[last:]
    outs = refs[:out_count]
    rest = refs[out_count:]
    if gather:
        full, rest = rest[0], rest[1:]
    if carry_weights:
        weights, stage, ws, wr, xs, xr, hi, ho, rest = rest[0], *rest[1:8], rest[8:]
    job_results, rest = rest[: len(jobs)], rest[len(jobs) :]
    running = []
    for job, given, result in zip(jobs, job_given, job_results):
        count = len(job.inputs) + 3
        running.append(RunningJob(job, given, result, rest[:count]))
        rest = rest[count:]
    if last:
        low, back, gain_acc, tiles, got, ts, tr, gs, gr = rest[:9]
        returned, rest = rest[9:22], rest[22:]
        cols = returned[0].shape[3]
        pieces = [
            (array, start) for array in gradients for start in range(0, array.shape[1], cols)
        ]
        back_home = Return(nd, pieces, outs[2:], returned)
    if gather:
        finished, ls, lr, fs, fr, keep, rest = rest[0], *rest[1:6], rest[6:]
    mine, other, sums, arrivals, cs, cr, loc, ss, sr = rest
    c, l = lax.axis_index("c"), lax.axis_index("l")
    d, h = lax.axis_index("d"), lax.axis_index("h")
    own = arrivals.shape[0] // (tl - 1)
    chunk = ROW_CHUNK
    chunks = own // chunk

    def greet():
        barrier = pltpu.get_barrier_semaphore()
        peers = [{"c": 1 - c}] + [{"l": lax.rem(l + step, tl)} for step in range(1, tl)]
        if carry_weights:
            peers += [{"h": 1 - h}] + [{"d": lax.rem(d + step, nd)} for step in range(1, nd)]
        for peer in peers:
            pl.semaphore_signal(barrier, inc=1, device_id=peer, device_id_type=MESH)
        pl.semaphore_wait(barrier, len(peers))

    if not last:
        greet()

    def part(base, k):
        return rows_at(base * chunks + k, chunk)

    def to_core(index, k):
        at = index * chunks + k
        return remote(
            partial.at[part(tl + index, k)], other.at[part(index, k)], cs.at[at], cr.at[at], c=1 - c
        )

    def local(index, k):
        return pltpu.make_async_copy(
            partial.at[part(index, k)], mine.at[part(index, k)], loc.at[index * chunks + k]
        )

    def along(step, k):
        at = (step - 1) * chunks + k
        return remote(
            sums.at[part(step - 1, k)],
            arrivals.at[part(step - 1, k)],
            ss.at[at],
            sr.at[at],
            l=lax.rem(l + step, tl),
        )

    if carry_weights:
        half = weight_rows.shape[0] // 2
        far_pieces = PIECES // 2
        piece = here_rows.shape[1] // far_pieces

        def block(j, row):
            return weights.at[rows_at(row, half), pl.ds(j * piece, piece)]

        def given(j, row_part):
            source = weight_rows if j < far_pieces else here_rows
            return source.at[pl.ds(row_part * half, half), pl.ds(j % far_pieces * piece, piece)]

        def held_here(j, row_part):
            return block(j, d * 2 + row_part) if j < far_pieces else given(j, row_part)

        def from_far(j, row_part):
            return remote(
                given(j, row_part),
                block(j, d * 2 + row_part),
                ws.at[j, row_part],
                wr.at[j, row_part],
                h=1 - h,
            )

        def here_in():
            return pltpu.make_async_copy(here_rows, stage, hi)

        def here_out():
            here = weights.at[rows_at(d, 2 * half), pl.ds(far_pieces * piece, far_pieces * piece)]
            return pltpu.make_async_copy(stage, here, ho)

        over_d = Spread(nd, d, block, xs, xr, held_here)

        def spread(j):
            for row_part in range(2):
                if j < far_pieces:
                    from_far(j, row_part).wait_recv()
                over_d.send(j, row_part)

        for j in range(far_pieces):
            for row_part in range(2):
                from_far(j, row_part).start()
        here_in().start()

    order = list(range(1, tl)) + [0]
    for index in order:
        for k in range(chunks):
            to_core(index, k).start()
            local(index, k).start()

    if last:
        for j in range(RETURN_AHEAD):
            back_home.start(j)

    def both(index, k):
        local(index, k).wait()
        to_core(index, k).wait_recv()
        at = part(index, k)
        return mine[at, :].astype(jnp.float32) + other[at, :].astype(jnp.float32)

    for step in range(1, tl):

        def pass_on(k, carry):
            sums[part(step - 1, k), :] = both(step, k).astype(jnp.bfloat16)
            along(step, k).start()
            return carry

        lax.fori_loop(0, chunks, pass_on, 0)

    for job in running:
        job.fetch()
    for job in running[:-1]:
        job.run()

    if last:
        apart = c != h
        count = 4 * nd * tl
        me = ((d * 2 + c) * 2 + h) * tl + l

        def to_owner(k):
            return remote(low.at[part(0, k)], back.at[part(0, k)], ts.at[k], tr.at[k], c=h, h=c)

        def gains_to(step):
            place = lax.rem(me + step, count)
            row = place // (2 * tl)
            return remote(
                tiles.at[row],
                got.at[step - 1],
                gs.at[step - 1],
                gr.at[step - 1],
                d=row // 2,
                c=lax.rem(row, 2),
                h=lax.rem(place // tl, 2),
                l=lax.rem(place, tl),
            )

        def start_gains(step, carry):
            gains_to(step).start()
            return carry

        def add_gains(step, total):
            gains_to(step).wait_recv()
            return total + got[step - 1]

        def drain_gains(step, carry):
            gains_to(step).wait_send()
            return carry

        def send_gains(_):
            cut = gain_acc.shape[1] // (2 * nd)
            lines = cut // 128
            tiles[...] = jnp.zeros_like(tiles)
            for row in range(2 * nd):
                for line in range(lines):
                    at = slice(row * cut + line * 128, row * cut + (line + 1) * 128)
                    tiles[row, line : line + 1, :] = gain_acc[:, at]
                    tiles[row, lines + line : lines + line + 1, :] = aux[3][:, at]
                tiles[row, 2 * lines : 2 * lines + 1, :] = aux[4][0:1, :]
                tiles[row, 2 * lines + 1 : 2 * lines + 2, :] = aux[5][0:1, :]
            lax.fori_loop(1, count, start_gains, 0)

    def gathered(index, k):
        return full.at[part(index, k)]

    def keep_own(k):
        return pltpu.make_async_copy(finished.at[part(0, k)], gathered(0, k), keep.at[k])

    def own_along(step, k):
        return remote(
            finished.at[part(0, k)],
            gathered(tl - step, k),
            ls.at[(step - 1) * chunks + k],
            lr.at[(tl - step - 1) * chunks + k],
            l=lax.rem(l + step, tl),
        )

    def from_along(index, k):
        at = (index - 1) * chunks + k
        return remote(gathered(index, k), gathered(index, k), ls.at[at], lr.at[at], l=l)

    def across(index, k):
        source = finished.at[part(0, k)] if index == 0 else gathered(index, k)
        at = index * chunks + k
        return remote(source, gathered(tl + index, k), fs.at[at], fr.at[at], c=1 - c)

    def finish(k, carry):
        total = both(0, k)
        for step in range(1, tl):
            along(step, k).wait_recv()
            total = total + arrivals[part(step - 1, k), :].astype(jnp.float32)
        kept = (outs[0], low, gain_acc) if last else outs
        row = epilogue(total, part(0, k), k, aux[:3], kept)
        if last:

            @pl.when(apart)
            def _():
                to_owner(k).start()

        if gather:
            finished[part(0, k), :] = row
            keep_own(k).start()
            for step in range(1, tl):
                own_along(step, k).start()
            across(0, k).start()
        return carry

    def pass_across(k):
        for index in range(1, tl):
            from_along(index, k).wait_recv()
            across(index, k).start()

    if carry_weights:
        steps = {
            "s": spread,
            "r": over_d.relay,
            "f": lambda k: finish(k, 0),
            "a": pass_across,
        }
        here_in().wait()
        here_out().start()
        for step in SUM_ORDER:
            if step[0] in "fa" and int(step[1:]) >= chunks:
                continue
            steps[step[0]](int(step[1:]))
    elif last:
        steps = {
            "w": back_home.start,
            "m": back_home.mix,
            "h": back_home.hand,
            "f": lambda k: finish(k, 0),
            "g": send_gains,
        }
        for step in RETURN_ORDER:
            if step[0] == "f" and int(step[1:]) >= chunks:
                continue
            steps[step[0]](int(step[1:]))
    else:
        lax.fori_loop(0, chunks, finish, 0)
        for job in running[-1:]:
            job.run()
        if gather:
            for k in range(chunks):
                pass_across(k)
    if last:
        @pl.when(apart)
        def _():
            for k in range(chunks):
                to_owner(k).wait()
                outs[0][part(0, k), :] = back[part(0, k), :].astype(jnp.float32)

        outs[1][...] = lax.fori_loop(1, count, add_gains, tiles[d * 2 + c])
        lax.fori_loop(1, count, drain_gains, 0)
        for j in range(len(pieces)):
            back_home.finish(j)
    for job in running:
        job.finish()
    if gather:
        for k in range(chunks):
            keep_own(k).wait()
            for index in range(tl):
                across(index, k).wait()
            for step in range(1, tl):
                own_along(step, k).wait_send()
    if carry_weights:
        for j in range(PIECES):
            over_d.finish(j)
            if j < far_pieces:
                for row_part in range(2):
                    from_far(j, row_part).wait_send()
        here_out().wait()
    for k in range(chunks):
        for index in range(tl):
            to_core(index, k).wait_send()
        for step in range(1, tl):
            along(step, k).wait_send()


def exchange(collective_id, partial, aux, outs, epilogue, gather, weight_rows=(), jobs=(), last=()):
    nd, tl = lax.axis_size("d"), lax.axis_size("l")
    total, width = partial.shape
    own = total // (2 * tl)
    chunks = own // ROW_CHUNK
    dma = pltpu.SemaphoreType.DMA
    vmem = pl.BlockSpec(memory_space=pltpu.VMEM)
    anywhere = pl.BlockSpec(memory_space=pl.ANY)
    out_shape = list(outs)
    out_specs = [vmem] * len(outs)
    scratch = []
    given = tuple(value for job in jobs for value in job.inputs)
    if gather:
        out_shape.append(jax.ShapeDtypeStruct((total, width), jnp.bfloat16))
        out_specs.append(anywhere)
    if weight_rows:
        rows, cols = weight_rows[1].shape
        out_shape.append(jax.ShapeDtypeStruct((nd * rows, 2 * cols), jnp.bfloat16))
        out_specs.append(anywhere)
        scratch += [
            pltpu.VMEM((rows, cols), jnp.bfloat16),
            dma((PIECES, 2)),
            dma((PIECES, 2)),
            dma((PIECES, hop_count(nd))),
            dma((PIECES, hop_count(nd))),
            dma,
            dma,
        ]
    for job in jobs:
        out_shape.append(jax.ShapeDtypeStruct(job.shape, jnp.bfloat16))
        out_specs.append(anywhere)
        scratch += job.scratch()
    if last:
        others = 4 * nd * tl - 1
        scratch += [
            pltpu.VMEM((own, width), jnp.bfloat16),
            pltpu.VMEM((own, width), jnp.bfloat16),
            pltpu.VMEM((1, width), jnp.float32),
            pltpu.VMEM((2 * nd, 8, 128), jnp.float32),
            pltpu.VMEM((others, 8, 128), jnp.float32),
            dma((chunks,)),
            dma((chunks,)),
            dma((others,)),
            dma((others,)),
        ]
        cols = min(array.shape[1] for array in last) // 2
        count = sum(array.shape[1] for array in last) // cols
        scratch += Return.scratch(nd, count, outs[2].shape[0], cols)
    if gather:
        scratch += [
            pltpu.VMEM((own, width), jnp.bfloat16),
            dma(((tl - 1) * chunks,)),
            dma(((tl - 1) * chunks,)),
            dma((tl * chunks,)),
            dma((tl * chunks,)),
            dma((chunks,)),
        ]
    scratch += [
        pltpu.VMEM((tl * own, width), jnp.bfloat16),
        pltpu.VMEM((tl * own, width), jnp.bfloat16),
        pltpu.VMEM(((tl - 1) * own, width), jnp.bfloat16),
        pltpu.VMEM(((tl - 1) * own, width), jnp.bfloat16),
        dma((tl * chunks,)),
        dma((tl * chunks,)),
        dma((tl * chunks,)),
        dma(((tl - 1) * chunks,)),
        dma(((tl - 1) * chunks,)),
    ]
    return pl.pallas_call(
        functools.partial(
            exchange_kernel,
            nd,
            tl,
            epilogue,
            len(aux),
            len(outs),
            gather,
            bool(weight_rows),
            jobs,
            len(last),
        ),
        out_shape=tuple(out_shape),
        in_specs=[anywhere] + [vmem] * len(aux) + [anywhere] * (len(given) + len(weight_rows) + len(last)),
        out_specs=out_specs,
        scratch_shapes=scratch,
        compiler_params=pltpu.CompilerParams(
            has_side_effects=True, collective_id=collective_id, vmem_limit_bytes=60 << 20
        ),
        cost_estimate=pl.CostEstimate(
            flops=0, bytes_accessed=200_000_000 if gather else 110_000_000, transcendentals=0
        ),
    )(partial, *aux, *given, *weight_rows, *last)


def middle_rows(total, rows, k, aux, outs):
    stream, gain = aux
    value = stream[rows, :].astype(jnp.float32) + total
    outs[0][rows, :] = value
    return rms_scale(value, gain[...]).astype(jnp.bfloat16)


def norm_pull(value, gain, grad):
    scale = lax.rsqrt(jnp.mean(value * value, axis=-1, keepdims=True) + EPS)
    scaled = grad * gain
    inner = jnp.mean(value * scaled, axis=-1, keepdims=True)
    return scale * scaled - value * (scale * scale * scale * inner), jnp.sum(
        grad * value * scale, axis=0, keepdims=True
    )


def add_rows(out, value, k):
    @pl.when(k == 0)
    def _():
        out[...] = value

    @pl.when(k > 0)
    def _():
        out[...] += value


def middle_pull_rows(total, rows, k, aux, outs):
    middle, cotangent, gain = aux
    pulled, gain_part = norm_pull(middle[rows, :], gain[...], total)
    value = cotangent[rows, :].astype(jnp.float32) + pulled
    outs[0][rows, :] = value
    add_rows(outs[1], gain_part, k)
    return value.astype(jnp.bfloat16)


def stream_pull_rows(total, rows, k, aux, outs):
    stream, gradient, gain = aux
    pulled, gain_part = norm_pull(stream[rows, :].astype(jnp.float32), gain[...], total)
    value = gradient[rows, :] + pulled
    outs[0][rows, :] = value
    outs[1][rows, :] = value.astype(jnp.bfloat16)
    add_rows(outs[2], gain_part, k)
    return None


def key_tile(rows):
    return next(size for size in (384, 256, 128) if rows % size == 0)


def turn(values):
    return pltpu.roll(values, HEAD_WIDTH // 2, 1)


def head_norm(values):
    return lax.rsqrt(jnp.mean(values * values, axis=-1, keepdims=True) + EPS)


def tile_mask(first, start, tile, row0, rows):
    keys = start + lax.broadcasted_iota(jnp.int32, (rows, tile), 1)
    last = row0 + lax.broadcasted_iota(jnp.int32, (rows, tile), 0)
    return jnp.logical_and(keys >= first, keys <= last)


def dot_last(left, right):
    return lax.dot_general(
        left, right, (((1,), (1,)), ((), ())), preferred_element_type=jnp.float32
    )


def attention_kernel(blocks, repeat, order_ref, *refs):
    q, k, v, cosine, sine, q_gain, k_gain, first = refs[:8]
    qr, kr, vb, out, total = refs[8:13]
    acc, den = refs[13:]
    rows = q.shape[0] // blocks
    tile = key_tile(q.shape[0])
    scale = HEAD_WIDTH**-0.5 * math.log2(math.e)

    def rotated(values, gain, at):
        scaled = values * head_norm(values) * gain
        return (scaled * cosine[at, :] + turn(scaled) * sine[at, :]).astype(jnp.bfloat16)

    def prepare(i, carry):
        at, to = rows_at(i, rows), rows_at(order_ref[i], rows)
        for r in range(repeat):
            head = slice(r * HEAD_WIDTH, (r + 1) * HEAD_WIDTH)
            qr[at, head] = rotated(q[at, head], q_gain[...], at)
        kr[to, :] = rotated(k[at, :], k_gain[...], at)
        vb[to, :] = v[at, :].astype(jnp.bfloat16)
        return carry

    lax.fori_loop(0, blocks, prepare, 0)

    def attend(i, carry):
        at = rows_at(i, rows)
        row0 = order_ref[i] * rows
        acc[...] = jnp.zeros_like(acc)
        den[...] = jnp.zeros_like(den)

        def over_keys(t, inner):
            keys = rows_at(t, tile)
            mask = tile_mask(first[at, :], t * tile, tile, row0, rows)
            for r in range(repeat):
                head = slice(r * HEAD_WIDTH, (r + 1) * HEAD_WIDTH)
                scores = dot_last(qr[at, head], kr[keys, :]) * scale
                weights = jnp.where(mask, jnp.exp2(scores), 0.0)
                den[r] += jnp.sum(weights, axis=-1, keepdims=True)
                acc[r] += jnp.dot(
                    weights.astype(jnp.bfloat16), vb[keys, :], preferred_element_type=jnp.float32
                )
            return inner

        lax.fori_loop(0, (row0 + rows + tile - 1) // tile, over_keys, 0)
        for r in range(repeat):
            head = slice(r * HEAD_WIDTH, (r + 1) * HEAD_WIDTH)
            out[at, head] = (acc[r] / den[r]).astype(jnp.bfloat16)
            total[at, r : r + 1] = den[r]
        return carry

    lax.fori_loop(0, blocks, attend, 0)


def attention_specs(rows, q_heads, kv_heads):
    repeat = q_heads // kv_heads

    def columns(width, start=0):
        return pl.BlockSpec((rows, width * HEAD_WIDTH), lambda g, order: (0, start // width + g))

    def fixed(*shape):
        return pl.BlockSpec(shape, lambda g, order: (0, 0))

    raw = [columns(repeat), columns(1, q_heads), columns(1, q_heads + kv_heads)]
    tables = [
        fixed(rows, HEAD_WIDTH),
        fixed(rows, HEAD_WIDTH),
        fixed(1, HEAD_WIDTH),
        fixed(1, HEAD_WIDTH),
        fixed(rows, 1),
    ]
    return repeat, columns, fixed, raw, tables


def attention(qkv, tables, order, q_heads, kv_heads):
    rows = qkv.shape[0]
    blocks = order.shape[0]
    repeat, columns, _, raw, table_specs = attention_specs(rows, q_heads, kv_heads)
    wide, narrow = q_heads * HEAD_WIDTH, kv_heads * HEAD_WIDTH
    return pl.pallas_call(
        functools.partial(attention_kernel, blocks, repeat),
        name="attention",
        out_shape=(
            jax.ShapeDtypeStruct((rows, wide), jnp.bfloat16),
            jax.ShapeDtypeStruct((rows, narrow), jnp.bfloat16),
            jax.ShapeDtypeStruct((rows, narrow), jnp.bfloat16),
            jax.ShapeDtypeStruct((rows, wide), jnp.bfloat16),
            jax.ShapeDtypeStruct((rows, narrow), jnp.float32),
        ),
        grid_spec=pltpu.PrefetchScalarGridSpec(
            num_scalar_prefetch=1,
            grid=(kv_heads,),
            in_specs=raw + table_specs,
            out_specs=[columns(repeat), columns(1), columns(1), columns(repeat), columns(1)],
            scratch_shapes=[
                pltpu.VMEM((repeat, rows // blocks, HEAD_WIDTH), jnp.float32),
                pltpu.VMEM((repeat, rows // blocks, 1), jnp.float32),
            ],
        ),
        compiler_params=pltpu.CompilerParams(vmem_limit_bytes=50 << 20),
        cost_estimate=pl.CostEstimate(
            flops=4 * rows * rows * wide, bytes_accessed=60_000_000, transcendentals=0
        ),
    )(order, qkv, qkv, qkv, *tables)


def attention_pull_kernel(blocks, repeat, order_ref, *refs):
    q, k, cosine, sine, q_gain, k_gain, first, qr, kr, vb, total, out, grad = refs[:13]
    dq, dk, dv, dq_gain, dk_gain = refs[13:18]
    dq_acc, dk_acc, dv_acc = refs[18:]
    rows = q.shape[0] // blocks
    tile = key_tile(q.shape[0])
    scale = HEAD_WIDTH**-0.5
    dk_acc[...] = jnp.zeros_like(dk_acc)
    dv_acc[...] = jnp.zeros_like(dv_acc)

    @pl.when(pl.program_id(0) == 0)
    def _():
        dq_gain[...] = jnp.zeros_like(dq_gain)
        dk_gain[...] = jnp.zeros_like(dk_gain)

    def pull(raw, gain, turned_grad, at, gain_out):
        scaled_grad = turned_grad * cosine[at, :] + turn(turned_grad * sine[at, :])
        r = head_norm(raw)
        gain_out[0:1, :] += jnp.sum(scaled_grad * raw * r, axis=0, keepdims=True)
        scaled = scaled_grad * gain
        inner = jnp.mean(raw * scaled, axis=-1, keepdims=True)
        return (r * scaled - raw * (r * r * r * inner)).astype(jnp.bfloat16)

    def over_rows(i, carry):
        at = rows_at(i, rows)
        row0 = order_ref[i] * rows
        tiles = (row0 + rows + tile - 1) // tile
        dq_acc[...] = jnp.zeros_like(dq_acc)
        heads = [slice(r * HEAD_WIDTH, (r + 1) * HEAD_WIDTH) for r in range(repeat)]
        inner = [
            jnp.sum(
                grad[at, head].astype(jnp.float32) * out[at, head].astype(jnp.float32),
                axis=-1,
                keepdims=True,
            )
            for head in heads
        ]
        inverse = [1.0 / total[at, r : r + 1] for r in range(repeat)]

        def over_keys(t, carry):
            keys = rows_at(t, tile)
            mask = tile_mask(first[at, :], t * tile, tile, row0, rows)
            for r, head in enumerate(heads):
                scores = dot_last(qr[at, head], kr[keys, :]) * (scale * math.log2(math.e))
                share = jnp.where(mask, jnp.exp2(scores), 0.0) * inverse[r]
                share_grad = dot_last(grad[at, head], vb[keys, :])
                score_grad = (share * (share_grad - inner[r])).astype(jnp.bfloat16)
                dq_acc[r] += jnp.dot(score_grad, kr[keys, :], preferred_element_type=jnp.float32)
                dk_acc[keys, :] += contract_rows(score_grad, qr[at, head])
                dv_acc[keys, :] += contract_rows(share.astype(jnp.bfloat16), grad[at, head])
            return carry

        lax.fori_loop(0, tiles, over_keys, 0)
        for r in range(repeat):
            head = slice(r * HEAD_WIDTH, (r + 1) * HEAD_WIDTH)
            dq[at, head] = pull(q[at, head], q_gain[...], dq_acc[r] * scale, at, dq_gain)
        return carry

    lax.fori_loop(0, blocks, over_rows, 0)

    def finish(i, carry):
        at, to = rows_at(i, rows), rows_at(order_ref[i], rows)
        dk[at, :] = pull(k[at, :], k_gain[...], dk_acc[to, :] * scale, at, dk_gain)
        dv[at, :] = dv_acc[to, :].astype(jnp.bfloat16)
        return carry

    lax.fori_loop(0, blocks, finish, 0)


def attention_pull(qkv, tables, order, kept, grad, q_heads, kv_heads):
    rows = qkv.shape[0]
    blocks = order.shape[0]
    repeat, columns, fixed, raw, table_specs = attention_specs(rows, q_heads, kv_heads)
    wide, narrow = q_heads * HEAD_WIDTH, kv_heads * HEAD_WIDTH
    own = rows // blocks
    return pl.pallas_call(
        functools.partial(attention_pull_kernel, blocks, repeat),
        out_shape=(
            jax.ShapeDtypeStruct((rows, wide), jnp.bfloat16),
            jax.ShapeDtypeStruct((rows, narrow), jnp.bfloat16),
            jax.ShapeDtypeStruct((rows, narrow), jnp.bfloat16),
            jax.ShapeDtypeStruct((8, HEAD_WIDTH), jnp.float32),
            jax.ShapeDtypeStruct((8, HEAD_WIDTH), jnp.float32),
        ),
        grid_spec=pltpu.PrefetchScalarGridSpec(
            num_scalar_prefetch=1,
            grid=(kv_heads,),
            in_specs=raw[:2]
            + table_specs
            + [columns(repeat), columns(1), columns(1), columns(1), columns(repeat), columns(repeat)],
            out_specs=[
                columns(repeat),
                columns(1),
                columns(1),
                fixed(8, HEAD_WIDTH),
                fixed(8, HEAD_WIDTH),
            ],
            scratch_shapes=[
                pltpu.VMEM((repeat, own, HEAD_WIDTH), jnp.float32),
                pltpu.VMEM((rows, HEAD_WIDTH), jnp.float32),
                pltpu.VMEM((rows, HEAD_WIDTH), jnp.float32),
            ],
        ),
        compiler_params=pltpu.CompilerParams(vmem_limit_bytes=56 << 20),
        cost_estimate=pl.CostEstimate(
            flops=10 * rows * rows * wide, bytes_accessed=120_000_000, transcendentals=0
        ),
    )(order, qkv, qkv, *tables, *kept, grad)


def shift_perm(size, step):
    return [((place + step) % size, place) for place in range(size)]


def trade(values):
    return lax.ppermute(values, ("c", "h"), [(0, 0), (1, 2), (2, 1), (3, 3)])


def gather_along(own):
    places = lax.axis_size("l")
    return [own] + [lax.ppermute(own, "l", shift_perm(places, step)) for step in range(1, places)]


def gather_across(parts):
    half = jnp.concatenate(parts, axis=0)
    other = lax.ppermute(half, "c", shift_perm(2, 1))
    return jnp.concatenate([half, other], axis=0)


def scatter_tokens(partial, *first):
    places = lax.axis_size("l")
    half = partial.shape[0] // 2
    rows = half // places
    other = lax.ppermute(partial[half:].astype(jnp.bfloat16), "c", shift_perm(2, 1))
    total = partial[:half] + other.astype(jnp.float32)
    own = total[:rows]
    for step in range(1, places):
        sent = total[step * rows : (step + 1) * rows].astype(jnp.bfloat16)
        moved = lax.ppermute(sent, "l", shift_perm(places, -step))
        moved = after(moved, *first)
        own = own + moved.astype(jnp.float32)
    return own


def after(value, *others):
    return lax.optimization_barrier((value,) + others)[0]


def return_halves(near, far):
    core = lax.axis_index("c")
    far = lax.ppermute(far, "h", shift_perm(2, 1))
    sums = near.astype(jnp.float32) + far.astype(jnp.float32)
    rows = sums.shape[0] // 2
    first, second = sums[:rows], sums[rows:]
    mine = jnp.where(core == 0, first, second)
    sent = jnp.where(core == 0, second, first).astype(jnp.bfloat16)
    other = lax.ppermute(sent, "c", shift_perm(2, 1)).astype(jnp.float32)
    return mine, other


def columns_of(mine, other):
    core = lax.axis_index("c")
    return jnp.concatenate(
        [jnp.where(core == 0, mine, other), jnp.where(core == 0, other, mine)], axis=1
    )


def sum_over_d(partial):
    return lax.psum_scatter(partial.astype(jnp.bfloat16), "d", scatter_dimension=0, tiled=True)


def as_row(values):
    return values.reshape(1, -1)


def split(values):
    half = values.shape[1] // 2
    return values[:, :half], values[:, half:]


def per_device(
    tokens,
    segment_ids,
    attn_gain,
    q_weight,
    key_matrix,
    value_matrix,
    o_weight,
    q_gain,
    k_gain,
    mlp_gain,
    gate_weight,
    up_weight,
    down_weight,
    cotangent,
):
    width = attn_gain.shape[1] * lax.axis_size("d") * 2
    own_rows = tokens.shape[0]
    places = lax.axis_size("l")
    core, place = lax.axis_index("c"), lax.axis_index("l")
    q_cols, kv_cols, ff_cols = q_weight.shape[2], key_matrix.shape[2], gate_weight.shape[2]
    half_cols = ff_cols // 2

    cut = attn_gain.shape[1]
    head_cut = q_gain.shape[1]
    gains = jnp.concatenate([attn_gain[0], mlp_gain[0], q_gain[0], k_gain[0]]).astype(jnp.float32)
    gains = jnp.pad(gains, (0, 1024 - gains.shape[0])).reshape(8, 128)
    labels = trade(segment_ids)[0]
    order = jnp.stack(
        [
            ((core + core_step) % 2) * places + (place + step) % places
            for core_step in range(2)
            for step in range(places)
        ]
    )
    row_index = (order[:, None] * own_rows + jnp.arange(own_rows, dtype=jnp.int32)[None, :]).reshape(-1)
    labels = labels.reshape(2 * places, own_rows)[order].reshape(-1)
    cosine, sine, first_row = rotary_tables(labels, row_index)
    qkv_full, o_full, mid_rows, down_rows, group, cotangent, gains = enter(
        q_weight[0],
        key_matrix[0],
        value_matrix[0],
        o_weight[0],
        gate_weight[0],
        up_weight[0],
        down_weight[0],
        after(tokens, cosine, sine, first_row),
        cotangent,
        gains,
    )
    mid_near = lax.all_gather(mid_rows, "d", axis=0, tiled=True)
    down_near = lax.all_gather(down_rows, "d", axis=0, tiled=True)
    up_far = lax.ppermute(mid_rows[:, half_cols:], "h", shift_perm(2, 1))
    grad_half = gather_along(cotangent)
    gains = gains.reshape(gains.shape[0], -1)
    attn_scale = gains[:, :cut].reshape(-1)
    mlp_scale = gains[:, cut : 2 * cut].reshape(-1)
    q_scale = gains[:, 2 * cut : 2 * cut + head_cut].reshape(-1)
    k_scale = gains[:, 2 * cut + head_cut : 2 * cut + 2 * head_cut].reshape(-1)

    stream = group[:own_rows]
    normed = rms_scale(group.astype(jnp.float32), attn_scale).astype(jnp.bfloat16)
    head_count, kv_heads = q_cols // HEAD_WIDTH, kv_cols // HEAD_WIDTH
    qkv = jnp.dot(normed, qkv_full, preferred_element_type=jnp.float32)
    down_far = lax.ppermute(after(down_rows, qkv), "h", shift_perm(2, 1))
    tables = (cosine, sine, as_row(q_scale), as_row(k_scale), first_row)
    query_reduced, key_reduced, value_reduced, attended, totals = attention(
        qkv, tables, order, head_count, kv_heads
    )


    def whole(values):
        return jax.ShapeDtypeStruct((own_rows, width), values)

    gain_sum = jax.ShapeDtypeStruct((1, width), jnp.float32)
    middle, normed_mid, mid_far = exchange(
        1,
        contract_cols(attended, o_full).astype(jnp.bfloat16),
        (stream, as_row(mlp_scale)),
        (whole(jnp.float32),),
        middle_rows,
        True,
        (mid_rows, after(up_far, attended)),
    )
    grad_rows = gather_across([grad_half[0]] + [after(part, normed_mid) for part in grad_half[1:]])
    down_far = lax.all_gather(after(down_far, normed_mid), "d", axis=0, tiled=True)

    mid = jnp.dot(normed_mid, mid_near, preferred_element_type=jnp.float32)
    gate_near, up_near = split(mid)
    hidden_near = swiglu(gate_near, up_near).astype(jnp.bfloat16)
    mid = jnp.dot(normed_mid, mid_far, preferred_element_type=jnp.float32)
    gate_far, up_far = split(mid)
    hidden_far = swiglu(gate_far, up_far).astype(jnp.bfloat16)
    down_grad_far = contract_rows(grad_rows, hidden_far).astype(jnp.bfloat16)
    down_sum_far = sum_over_d(down_grad_far)
    grad_rows = after(grad_rows, down_grad_far, hidden_near)

    def hidden_pull(gate, up, down):
        hidden_grad = jnp.dot(grad_rows, down, preferred_element_type=jnp.float32)
        _, pull_back = jax.vjp(swiglu, gate, up)
        gate_grad, up_grad = pull_back(hidden_grad)
        return jnp.concatenate(
            [gate_grad.astype(jnp.bfloat16), up_grad.astype(jnp.bfloat16)], axis=1
        )

    mid_back_near = hidden_pull(gate_near, up_near, down_near)
    mid_back_far = hidden_pull(gate_far, up_far, down_far)
    mid_grad_far = contract_rows(normed_mid, mid_back_far).astype(jnp.bfloat16)
    mid_sum_far = sum_over_d(mid_grad_far)
    normed_grad = contract_cols(mid_back_near, mid_near) + contract_cols(mid_back_far, mid_far)
    normed_grad = normed_grad.astype(jnp.bfloat16)
    gradient, mlp_gain_grad, grad_rows, mid_grad_near, down_grad_near, branch = exchange(
        2,
        after(normed_grad, mid_grad_far),
        (middle, cotangent, as_row(mlp_scale)),
        (whole(jnp.float32), gain_sum),
        middle_pull_rows,
        True,
        jobs=(
            Job((normed_mid, mid_back_near), mid_near.shape, 8, weight_grad_tile),
            Job((grad_rows, hidden_near), down_near.shape, 8, weight_grad_tile),
            Job((hidden_near, hidden_far, down_near, down_far), normed_mid.shape, 4, down_tile),
        ),
    )
    down_sum_near = sum_over_d(down_grad_near)
    mid_sum_near = sum_over_d(mid_grad_near)

    out_grad = jnp.dot(grad_rows, o_full, preferred_element_type=jnp.float32).astype(jnp.bfloat16)
    o_wgrad = contract_rows(grad_rows, attended)
    query_back, key_back, value_back, q_gain_grad, k_gain_grad = attention_pull(
        qkv,
        tables,
        order,
        (query_reduced, key_reduced, value_reduced, totals, attended),
        out_grad,
        head_count,
        kv_heads,
    )
    qkv_back = jnp.concatenate([query_back, key_back, value_back], axis=1)
    qkv_grad = contract_rows(normed, qkv_back).astype(jnp.bfloat16)
    o_wgrad = o_wgrad.astype(jnp.bfloat16)
    branch = scatter_tokens(branch, qkv_grad)
    activations = trade((middle + branch).astype(jnp.bfloat16))
    gradient, sums, *attn_grads = exchange(
        None,
        contract_cols(after(qkv_back, qkv_grad), qkv_full).astype(jnp.bfloat16),
        (stream, gradient, as_row(attn_scale), mlp_gain_grad, q_gain_grad, k_gain_grad),
        (
            whole(jnp.float32),
            jax.ShapeDtypeStruct((8, 128), jnp.float32),
        )
        + tuple(
            jax.ShapeDtypeStruct((q_weight.shape[1], cols), jnp.float32)
            for cols in (q_cols, kv_cols, kv_cols, q_cols)
        ),
        stream_pull_rows,
        False,
        last=(qkv_grad, o_wgrad),
    )
    lines = cut // 128
    head_at = (lax.axis_index("d") * 2 + core) * head_cut

    def head_gain(line):
        return lax.dynamic_slice(sums[line], (head_at,), (head_cut,))[None]

    mid_sum_near = after(mid_sum_near, sums)
    down_sum_near = after(down_sum_near, sums)
    down_grad = columns_of(*return_halves(down_sum_near, down_sum_far))
    mine, other = return_halves(mid_sum_near, mid_sum_far)
    gate_grad = columns_of(mine[:, :half_cols], other[:, :half_cols])
    up_grad = columns_of(mine[:, half_cols:], other[:, half_cols:])

    return (
        activations,
        gradient,
        sums[:lines].reshape(1, cut),
        *(array[None] for array in attn_grads),
        head_gain(2 * lines),
        head_gain(2 * lines + 1),
        sums[lines : 2 * lines].reshape(1, cut),
        gate_grad[None],
        up_grad[None],
        down_grad[None],
    )


def solution(mesh):
    dp, tensor = mesh.shape["dp"], mesh.shape["tensor"]
    cut = Mesh(mesh.devices.reshape(dp // 2, 2, 2, tensor // 2), ("d", "c", "h", "l"))
    rows, cols = ("d", "c"), ("h", "l")
    tokens, labels = P(rows + cols, None), P(rows, None)
    gain, weight = P(None, rows), P(None, rows, cols)
    return jax.shard_map(
        per_device,
        mesh=cut,
        in_specs=(
            tokens,
            labels,
            gain,
            weight,
            weight,
            weight,
            weight,
            gain,
            gain,
            gain,
            weight,
            weight,
            weight,
            tokens,
        ),
        out_specs=(
            tokens,
            tokens,
            gain,
            weight,
            weight,
            weight,
            weight,
            gain,
            gain,
            gain,
            weight,
            weight,
            weight,
        ),
        check_vma=False,
    )
```
